32 devices in a mesh: fsdp: 4 (over x, core), ctx: 8 (over z, y).
Axes of the slice: x: 2, y: 2, z: 4, core: 2. Of those that a mesh axis runs over, the one named last changes fastest.
Arguments:
- inputs: bfloat16 [4096, 1536], P(('fsdp', 'ctx')), may hold values from -6 to 6
- positions: int32 [4096], P(('fsdp', 'ctx')), may hold values from 0 to 1023, as said below
- cotangent: bfloat16 [4096, 1536], P(('fsdp', 'ctx')), may hold values from -6 to 6
- attention_gain: bfloat16 [1536], replicated, may hold values from 0.5 to 1.5
- query_weight: bfloat16 [1536, 1536], P('fsdp'), may hold values from -0.15625 to 0.15625
- key_weight: bfloat16 [768, 1536], P('fsdp'), may hold values from -0.15625 to 0.15625
- value_weight: bfloat16 [768, 1536], P('fsdp'), may hold values from -0.15625 to 0.15625
- output_weight: bfloat16 [1536, 1536], P('fsdp'), may hold values from -3 to 3
- feedforward_gain: bfloat16 [1536], replicated, may hold values from 0.5 to 1.5
- gate_weight: bfloat16 [4096, 1536], P('fsdp'), may hold values from -0.15625 to 0.15625
- up_weight: bfloat16 [4096, 1536], P('fsdp'), may hold values from -0.15625 to 0.15625
- down_weight: bfloat16 [4096, 1536], P('fsdp'), may hold values from -0.09375 to 0.09375
Outputs:
- layer_output: bfloat16 [4096, 1536], P(('fsdp', 'ctx'))
- input_grad: float32 [4096, 1536], P(('fsdp', 'ctx'))
- attention_gain_grad: float32 [1536], replicated
- query_weight_grad: float32 [1536, 1536], P('fsdp')
- key_weight_grad: float32 [768, 1536], P('fsdp')
- value_weight_grad: float32 [768, 1536], P('fsdp')
- output_weight_grad: float32 [1536, 1536], P('fsdp')
- feedforward_gain_grad: float32 [1536], replicated
- gate_weight_grad: float32 [4096, 1536], P('fsdp')
- up_weight_grad: float32 [4096, 1536], P('fsdp')
- down_weight_grad: float32 [4096, 1536], P('fsdp')
The draws below stay inside these ranges and needn't reach their ends.
Inputs may be any that keep to these rules, and one draw needn't show every extreme that they name: Within each sequence every position appears once, and each device's 2 * 64 tokens of a sequence are two whole blocks of 64 consecutive rising positions, starting at b * 64 and at (15 - b) * 64 for some b, in either order.
All inputs are finite; a program needn't handle non-finite values.
Results may differ from the reference program's by a relative error of at most 0.022.
Values may be sent and summed in bfloat16 or wider, within the bound.
A program may use at most 384 MiB of HBM per device.

```python
import math
import jax
import jax.numpy as jnp
from jax import lax

D = 1536
HEADS = 16
KV_HEADS = 8
HEAD_DIM = 96
FF = 4096
BLK = 64
SEQS = 4
LENGTH = 1024
TOKENS = 4096


def draw_positions(key, part):
    block_total = LENGTH // BLK
    pair_total = block_total // 2

    def one_sequence(seq_key):
        order_key, flip_key = jax.random.split(seq_key)
        early = jax.random.permutation(order_key, pair_total).astype(jnp.int32)
        flipped = jax.random.randint(flip_key, (pair_total,), 0, 2)
        late = block_total - 1 - early
        lead = jnp.where(flipped == 1, late, early)
        trail = jnp.where(flipped == 1, early, late)
        slots = jnp.stack([lead, trail], axis=1).reshape(block_total)
        offsets = jnp.arange(BLK, dtype=jnp.int32)
        return (slots[:, None] * BLK + offsets[None, :]).reshape(LENGTH).astype(jnp.int32)
    seq_keys = jax.random.split(jax.random.fold_in(key, 11), SEQS)
    return jax.vmap(one_sequence)(seq_keys).reshape(TOKENS)


def block_levels(own_key, shape, shards, low, top_value):
    def one(dim, shards_of):
        heights = jax.random.uniform(jax.random.fold_in(jax.random.fold_in(own_key, 6), dim), (shards_of,), jnp.float32, low / len(shards), top_value / len(shards))
        return jnp.repeat(jnp.exp(heights), shape[dim] // shards_of).reshape((-1,) + (1,) * (len(shape) - dim - 1))

    loudness = one(*shards[0])
    for cut in shards[1:]:
        loudness = loudness * one(*cut)
    return loudness


def gaussian(rng, dims, scale, bound, shards=(), kind=jnp.bfloat16):
    values = jax.random.normal(rng, dims, jnp.float32) * scale
    if len(shards) > 0:
        values = block_levels(rng, dims, shards, -0.22, 0.18) * values
    return jnp.clip(values, min=-bound, max=bound).astype(kind)


def setup_inputs(seed: int = 0) -> dict:
    key_list = jax.random.split(jax.random.key(seed), 13)
    return {
        "inputs": gaussian(key_list[0], (TOKENS, D), 1.0, 6.0, ((0, 32),)),
        "positions": draw_positions(jax.random.fold_in(key_list[12], 71), 0),
        "cotangent": gaussian(key_list[2], (TOKENS, D), 1.0, 6.0, ((0, 32),)),
        "attention_gain": jnp.clip(1.0 + 0.1 * jax.random.normal(key_list[3], (D,), jnp.float32), 0.5, 1.5).astype(jnp.bfloat16),
        "query_weight": gaussian(key_list[4], (HEADS * HEAD_DIM, D), D ** -0.5, 0.15625, ((0, 4),)),
        "key_weight": gaussian(key_list[5], (KV_HEADS * HEAD_DIM, D), D ** -0.5, 0.15625, ((0, 4),)),
        "value_weight": gaussian(key_list[6], (KV_HEADS * HEAD_DIM, D), D ** -0.5, 0.15625, ((0, 4),)),
        "output_weight": gaussian(key_list[7], (HEADS * HEAD_DIM, D), 4 ** -0.5, 3.0, ((0, 4),)),
        "feedforward_gain": jnp.clip(1.0 + 0.1 * jax.random.normal(key_list[8], (D,), jnp.float32), 0.5, 1.5).astype(jnp.bfloat16),
        "gate_weight": gaussian(key_list[9], (FF, D), D ** -0.5, 0.15625, ((0, 4),)),
        "up_weight": gaussian(key_list[10], (FF, D), D ** -0.5, 0.15625, ((0, 4),)),
        "down_weight": gaussian(key_list[11], (FF, D), FF ** -0.5, 0.09375, ((0, 4),)),
    }


@jax.custom_vjp
def low(v):
    return lax.optimization_barrier(v.astype(jnp.bfloat16)).astype(jnp.float32)

@jax.custom_vjp
def low_back(v):
    return v

def low_keep(v):
    return (low(v), None)

def low_pass(kept, grad):
    return (grad,)

def back_keep(v):
    return (v, None)

def back_low(kept, grad):
    return (low(grad),)
low.defvjp(low_keep, low_pass)
low_back.defvjp(back_keep, back_low)
EPSILON = 1e-05
ROPE_BASE = 100000.0

def highest(left, right):
    return jnp.dot(left, right, precision=lax.Precision.HIGHEST, preferred_element_type=jnp.float32)

def rms_scale(values):
    return lax.rsqrt(lax.optimization_barrier(jnp.mean(values * values, axis=-1, keepdims=True)) + EPSILON)

def rotary_tables(places):
    half_width = HEAD_DIM // 2
    frequencies = ROPE_BASE ** (-(jnp.arange(half_width, dtype=jnp.float32) * 2.0 / HEAD_DIM))
    angles = places.astype(jnp.float32)[:, None] * frequencies[None, :]
    return (jnp.cos(angles)[:, None, :], jnp.sin(angles)[:, None, :])

def rotate(values, cosine, sine):
    half_width = values.shape[-1] // 2
    lower_half = values[..., :half_width]
    upper_half = values[..., half_width:]
    return jnp.concatenate([lower_half * cosine - upper_half * sine, upper_half * cosine + lower_half * sine], axis=-1)

def attention(query, key_rows, value_rows, places):
    length = query.shape[0]
    query_block = min(length, 512)
    block_count = length // query_block
    groups = HEADS // KV_HEADS
    grouped = query.reshape(block_count, query_block, KV_HEADS, groups, HEAD_DIM)
    block_places = places.reshape(block_count, query_block)
    score_scale = 1.0 / math.sqrt(HEAD_DIM)

    def one_block(block_items):
        query_part, place_part = block_items
        scores = jnp.einsum('qhgd,khd->hgqk', query_part, key_rows, precision=lax.Precision.HIGHEST) * score_scale
        scores = low_back(scores)
        allowed = places[None, :] <= place_part[:, None]
        scores = jnp.where(allowed[None, None], scores, -1000000000.0)
        row_peak = lax.optimization_barrier(jnp.max(scores, axis=-1, keepdims=True))
        spread = jnp.exp(scores - row_peak)
        soft_weights = low(spread / lax.optimization_barrier(jnp.sum(spread, axis=-1, keepdims=True)))
        return jnp.einsum('hgqk,khd->qhgd', soft_weights, value_rows, precision=lax.Precision.HIGHEST)
    result = lax.map(jax.checkpoint(one_block), (grouped, block_places))
    return result.reshape(length, HEADS * HEAD_DIM)

def layer(rows, attention_gain, query_weight, key_weight, value_weight, output_weight, feedforward_gain, gate_weight, up_weight, down_weight, places):
    length = rows.shape[0]
    cosine, sine = rotary_tables(places)
    normed_one = low(rows * rms_scale(rows) * attention_gain)
    query_pre = low_back(highest(normed_one, query_weight.T)).reshape(length, HEADS, HEAD_DIM)
    query = low(rotate(query_pre, cosine, sine))
    key_pre = low_back(highest(normed_one, key_weight.T)).reshape(length, KV_HEADS, HEAD_DIM)
    key_rows = low(rotate(key_pre, cosine, sine))
    value_rows = low(low_back(highest(normed_one, value_weight.T)).reshape(length, KV_HEADS, HEAD_DIM))
    attended = attention(query, key_rows, value_rows, places)
    attended = low(low_back(attended))
    branch = low_back(highest(attended, output_weight))
    hidden_state = rows + branch
    normed_two = low(hidden_state * rms_scale(hidden_state) * feedforward_gain)
    gate_values = low_back(highest(normed_two, gate_weight.T))
    upward = low_back(highest(normed_two, up_weight.T))
    mixed_hidden = low(jax.nn.silu(gate_values) * upward)
    return hidden_state + low_back(highest(mixed_hidden, down_weight))

def reference(inputs, positions, cotangent, attention_gain, query_weight, key_weight, value_weight, output_weight, feedforward_gain, gate_weight, up_weight, down_weight):
    weights = (attention_gain.astype(jnp.float32), query_weight.astype(jnp.float32), key_weight.astype(jnp.float32), value_weight.astype(jnp.float32), output_weight.astype(jnp.float32), feedforward_gain.astype(jnp.float32), gate_weight.astype(jnp.float32), up_weight.astype(jnp.float32), down_weight.astype(jnp.float32))
    seq_rows = inputs.astype(jnp.float32).reshape(SEQS, LENGTH, D)
    seq_places = positions.reshape(SEQS, LENGTH)
    seq_cotangent = cotangent.astype(jnp.float32).reshape(SEQS, LENGTH, D)

    def one_sequence(totals, seq_items):
        rows, places, seq_grad = seq_items

        def forward(rows_in, gain_one, weight_query, weight_key, weight_value, weight_output, gain_two, weight_gate, weight_up, weight_down):
            return layer(rows_in, gain_one, weight_query, weight_key, weight_value, weight_output, gain_two, weight_gate, weight_up, weight_down, places)
        result, pullback = jax.vjp(forward, rows, weights[0], weights[1], weights[2], weights[3], weights[4], weights[5], weights[6], weights[7], weights[8])
        grads = pullback(seq_grad)
        new_totals = tuple((running + added for running, added in zip(totals, grads[1:])))
        return (new_totals, (result.astype(jnp.bfloat16), grads[0]))
    initial = tuple((jnp.zeros(weight.shape, jnp.float32) for weight in weights))
    totals, (outputs, input_grads) = lax.scan(one_sequence, initial, (seq_rows, seq_places, seq_cotangent))
    return (outputs.reshape(TOKENS, D), input_grads.reshape(TOKENS, D), totals[0], totals[1], totals[2], totals[3], totals[4], totals[5], totals[6], totals[7], totals[8])
```

```python
import math

import jax
import jax.numpy as jnp
from jax import lax
from jax.sharding import PartitionSpec as P

HEADS = 16
KV_HEADS = 8
HEAD_DIM = 96


EPSILON = 1e-05
ROPE_BASE = 100000.0


def product(left, right):
    return jnp.dot(left, right, preferred_element_type=jnp.float32)


def product_back(left, right):
    return lax.dot_general(
        left, right, (((1,), (1,)), ((), ())), preferred_element_type=jnp.float32
    )


def product_rows(left, right):
    return lax.dot_general(
        left, right, (((0,), (0,)), ((), ())), preferred_element_type=jnp.float32
    )


def rms_scale(values):
    return lax.rsqrt(jnp.mean(values * values, axis=-1, keepdims=True) + EPSILON)


def norm_back(scale_rows, unit_rows, grad_unit):
    return scale_rows * (
        grad_unit - unit_rows * jnp.mean(grad_unit * unit_rows, axis=-1, keepdims=True)
    )


def rotary_tables(places):
    half_width = HEAD_DIM // 2
    frequencies = ROPE_BASE ** (-(jnp.arange(half_width, dtype=jnp.float32) * 2.0 / HEAD_DIM))
    angles = places.astype(jnp.float32)[:, None] * frequencies[None, :]
    return (jnp.cos(angles)[:, None, :], jnp.sin(angles)[:, None, :])


def rotate(values, cosine, sine):
    half_width = values.shape[-1] // 2
    lower_half = values[..., :half_width]
    upper_half = values[..., half_width:]
    return jnp.concatenate(
        [lower_half * cosine - upper_half * sine, upper_half * cosine + lower_half * sine], axis=-1
    )


def rotate_back(grads, cosine, sine):
    half_width = grads.shape[-1] // 2
    lower_half = grads[..., :half_width]
    upper_half = grads[..., half_width:]
    return jnp.concatenate(
        [lower_half * cosine + upper_half * sine, upper_half * cosine - lower_half * sine], axis=-1
    )


def block_total_of(total_keys):
    return max(1, total_keys // 512)


def masked_scores(query_grouped, query_places, key_rows, key_places, start, width):
    key_part = lax.dynamic_slice_in_dim(key_rows, start, width, 2)
    place_part = lax.dynamic_slice_in_dim(key_places, start, width, 1)
    scores = jnp.einsum(
        "sqhgd,shkd->shgqk", query_grouped, key_part, preferred_element_type=jnp.float32
    )
    scores = scores * (1.0 / math.sqrt(HEAD_DIM))
    allowed = place_part[:, None, None, None, :] <= query_places[:, None, None, :, None]
    return jnp.where(allowed, scores, -1000000000.0)


def attend_forward(query_grouped, query_places, key_rows, value_rows, key_places):
    seq_count, row_count, head_groups, group_size = query_grouped.shape[:4]
    total_keys = key_rows.shape[2]
    block_total = block_total_of(total_keys)
    width = total_keys // block_total
    stat_shape = (seq_count, head_groups, group_size, row_count)

    def peak_step(index, carry):
        running_top, running_sum = carry
        scores = masked_scores(
            query_grouped, query_places, key_rows, key_places, index * width, width
        )
        new_top = jnp.maximum(running_top, jnp.max(scores, axis=-1))
        running_sum = running_sum * jnp.exp(running_top - new_top) + jnp.sum(
            jnp.exp(scores - new_top[..., None]), axis=-1
        )
        return (new_top, running_sum)

    running_top, running_sum = lax.fori_loop(
        0,
        block_total,
        peak_step,
        (jnp.full(stat_shape, -1e30, jnp.float32), jnp.zeros(stat_shape, jnp.float32)),
    )
    log_total = running_top + jnp.log(running_sum)

    def value_step(index, gathered):
        scores = masked_scores(
            query_grouped, query_places, key_rows, key_places, index * width, width
        )
        soft_low = jnp.exp(scores - log_total[..., None]).astype(jnp.bfloat16)
        value_part = lax.dynamic_slice_in_dim(value_rows, index * width, width, 2)
        return gathered + jnp.einsum(
            "shgqk,shkd->sqhgd", soft_low, value_part, preferred_element_type=jnp.float32
        )

    attended = lax.fori_loop(
        0, block_total, value_step, jnp.zeros(query_grouped.shape, jnp.float32)
    )
    return (attended, log_total)


def attend_backward(
    query_grouped, query_places, key_rows, value_rows, key_places, log_total, grad_attended
):
    total_keys = key_rows.shape[2]
    block_total = block_total_of(total_keys)
    width = total_keys // block_total
    score_scale = 1.0 / math.sqrt(HEAD_DIM)

    def soft_and_grad(index):
        scores = masked_scores(
            query_grouped, query_places, key_rows, key_places, index * width, width
        )
        soft_values = jnp.exp(scores - log_total[..., None])
        value_part = lax.dynamic_slice_in_dim(value_rows, index * width, width, 2)
        grad_soft = jnp.einsum(
            "sqhgd,shkd->shgqk", grad_attended, value_part, preferred_element_type=jnp.float32
        )
        return (soft_values, grad_soft)

    def delta_step(index, row_delta):
        soft_values, grad_soft = soft_and_grad(index)
        return row_delta + jnp.sum(soft_values * grad_soft, axis=-1)

    row_delta = lax.fori_loop(0, block_total, delta_step, jnp.zeros(log_total.shape, jnp.float32))

    def grad_step(index, carry):
        grad_query, grad_keys, grad_values = carry
        soft_values, grad_soft = soft_and_grad(index)
        grad_scores = (soft_values * (grad_soft - row_delta[..., None])).astype(jnp.bfloat16)
        key_part = lax.dynamic_slice_in_dim(key_rows, index * width, width, 2)
        grad_query = (
            grad_query
            + jnp.einsum(
                "shgqk,shkd->sqhgd", grad_scores, key_part, preferred_element_type=jnp.float32
            )
            * score_scale
        )
        key_term = (
            jnp.einsum(
                "shgqk,sqhgd->shkd", grad_scores, query_grouped, preferred_element_type=jnp.float32
            )
            * score_scale
        )
        value_term = jnp.einsum(
            "shgqk,sqhgd->shkd",
            soft_values.astype(jnp.bfloat16),
            grad_attended,
            preferred_element_type=jnp.float32,
        )
        grad_keys = lax.dynamic_update_slice_in_dim(grad_keys, key_term, index * width, 2)
        grad_values = lax.dynamic_update_slice_in_dim(grad_values, value_term, index * width, 2)
        return (grad_query, grad_keys, grad_values)

    initial = (
        jnp.zeros(query_grouped.shape, jnp.float32),
        jnp.zeros(key_rows.shape, jnp.float32),
        jnp.zeros(value_rows.shape, jnp.float32),
    )
    return lax.fori_loop(0, block_total, grad_step, initial)


def gather_rows(values):
    return lax.all_gather(values, "fsdp", axis=0, tiled=True)


def scatter_rows(values):
    return lax.psum_scatter(
        values.astype(jnp.bfloat16), "fsdp", scatter_dimension=0, tiled=True
    ).astype(jnp.float32)


def per_device(
    inputs,
    positions,
    cotangent,
    attention_gain,
    query_weight,
    key_weight,
    value_weight,
    output_weight,
    feedforward_gain,
    gate_weight,
    up_weight,
    down_weight,
):
    row_count = inputs.shape[0]
    groups = HEADS // KV_HEADS
    gain_one = attention_gain.astype(jnp.float32)
    gain_two = feedforward_gain.astype(jnp.float32)
    seq_count = lax.axis_size("fsdp")
    first_row = lax.axis_index("fsdp") * row_count

    def own(values):
        return lax.dynamic_slice_in_dim(values, first_row, row_count, 0)

    query_places = gather_rows(positions).reshape(seq_count, row_count)
    key_places = lax.all_gather(query_places, "ctx", axis=1, tiled=True)
    all_cotangent = gather_rows(cotangent)
    flat_in = gather_rows(inputs).astype(jnp.float32)
    scale_one = rms_scale(flat_in)
    unit_one = flat_in * scale_one
    normed_one = (unit_one * gain_one).astype(jnp.bfloat16)
    total_rows = normed_one.shape[0]
    cosine, sine = rotary_tables(query_places.reshape(-1))
    query_heads = query_weight.shape[0] // HEAD_DIM
    kv_heads = key_weight.shape[0] // HEAD_DIM
    kv_width = kv_heads * HEAD_DIM
    query_low = rotate(
        product_back(normed_one, query_weight).reshape(total_rows, query_heads, HEAD_DIM), cosine, sine
    ).astype(jnp.bfloat16)
    key_low = rotate(
        product_back(normed_one, key_weight).reshape(total_rows, kv_heads, HEAD_DIM), cosine, sine
    ).astype(jnp.bfloat16)
    value_low = product_back(normed_one, value_weight).astype(jnp.bfloat16)
    ctx_size = lax.axis_size("ctx")

    def spread(values):
        rows = lax.all_gather(values, "ctx", axis=0, tiled=True)
        rows = rows.reshape(ctx_size, seq_count, row_count, kv_width).swapaxes(0, 1)
        return rows.reshape(seq_count, ctx_size * row_count, kv_width)

    def collect(values):
        rows = values.astype(jnp.bfloat16).swapaxes(1, 2)
        rows = rows.reshape(seq_count, ctx_size, row_count, kv_width).swapaxes(0, 1)
        return lax.psum_scatter(
            rows.reshape(-1, kv_width), "ctx", scatter_dimension=0, tiled=True
        )

    all_keys = spread(key_low.reshape(total_rows, kv_width))
    all_values = spread(value_low)
    total_keys = all_keys.shape[1]
    key_grid = all_keys.reshape(seq_count, total_keys, kv_heads, HEAD_DIM).swapaxes(1, 2)
    value_grid = all_values.reshape(seq_count, total_keys, kv_heads, HEAD_DIM).swapaxes(1, 2)
    query_grouped = query_low.reshape(seq_count, row_count, kv_heads, groups, HEAD_DIM)
    attended, log_total = attend_forward(
        query_grouped, query_places, key_grid, value_grid, key_places
    )
    attended_low = attended.reshape(total_rows, query_heads * HEAD_DIM).astype(jnp.bfloat16)
    hidden_state = inputs.astype(jnp.float32) + scatter_rows(product(attended_low, output_weight))
    scale_two = rms_scale(hidden_state)
    unit_two = hidden_state * scale_two
    normed_two = gather_rows((unit_two * gain_two).astype(jnp.bfloat16))
    gate_values = product_back(normed_two, gate_weight)
    upward = product_back(normed_two, up_weight)
    sigmoid_gate = jax.nn.sigmoid(gate_values)
    activated = gate_values * sigmoid_gate
    mixed_hidden = (activated * upward).astype(jnp.bfloat16)
    grad_out = cotangent.astype(jnp.float32)
    grad_down = product_rows(mixed_hidden, all_cotangent)
    grad_mixed = product_back(all_cotangent, down_weight)
    grad_gate_low = (
        grad_mixed * upward * sigmoid_gate * (1.0 + gate_values * (1.0 - sigmoid_gate))
    ).astype(jnp.bfloat16)
    grad_up_low = (grad_mixed * activated).astype(jnp.bfloat16)
    grad_normed_two = scatter_rows(
        product(grad_gate_low, gate_weight) + product(grad_up_low, up_weight)
    )
    gain_two_grad = jnp.sum(grad_normed_two * unit_two, axis=0)
    grad_hidden = grad_out + norm_back(scale_two, unit_two, grad_normed_two * gain_two)
    branch_rows = gather_rows(grad_hidden.astype(jnp.bfloat16))
    layer_output = (hidden_state + scatter_rows(product(mixed_hidden, down_weight))).astype(
        jnp.bfloat16
    )
    grad_gate = product_rows(grad_gate_low, normed_two)
    grad_up = product_rows(grad_up_low, normed_two)
    grad_output = product_rows(attended_low, branch_rows)
    grad_attended = product_back(branch_rows, output_weight).astype(jnp.bfloat16)
    grad_attended = grad_attended.reshape(seq_count, row_count, kv_heads, groups, HEAD_DIM)
    grad_query_rot, grad_key_all, grad_value_all = attend_backward(
        query_grouped, query_places, key_grid, value_grid, key_places, log_total, grad_attended
    )
    grad_key_own = collect(grad_key_all).astype(jnp.float32)
    grad_value_low = collect(grad_value_all)
    grad_query_low = (
        rotate_back(grad_query_rot.reshape(total_rows, query_heads, HEAD_DIM), cosine, sine)
        .reshape(total_rows, query_heads * HEAD_DIM)
        .astype(jnp.bfloat16)
    )
    grad_key_low = (
        rotate_back(
            grad_key_own.reshape(total_rows, kv_heads, HEAD_DIM), cosine, sine
        )
        .reshape(total_rows, kv_width)
        .astype(jnp.bfloat16)
    )
    grad_query = product_rows(grad_query_low, normed_one)
    grad_key = product_rows(grad_key_low, normed_one)
    grad_value = product_rows(grad_value_low, normed_one)
    grad_normed_one = scatter_rows(
        product(grad_query_low, query_weight)
        + product(grad_key_low, key_weight)
        + product(grad_value_low, value_weight)
    )
    own_unit = own(unit_one)
    gain_one_grad = jnp.sum(grad_normed_one * own_unit, axis=0)
    input_grad = grad_hidden + norm_back(own(scale_one), own_unit, grad_normed_one * gain_one)

    def ctx_sum(grad):
        return lax.psum(grad.astype(jnp.bfloat16), "ctx").astype(jnp.float32)

    gain_sums = lax.psum(jnp.stack([gain_one_grad, gain_two_grad]), ("fsdp", "ctx"))
    return (
        layer_output,
        input_grad,
        gain_sums[0],
        ctx_sum(grad_query),
        ctx_sum(grad_key),
        ctx_sum(grad_value),
        ctx_sum(grad_output),
        gain_sums[1],
        ctx_sum(grad_gate),
        ctx_sum(grad_up),
        ctx_sum(grad_down),
    )


def solution(mesh):
    in_specs = (
        P(("fsdp", "ctx"), None),
        P(("fsdp", "ctx")),
        P(("fsdp", "ctx"), None),
        P(),
        P("fsdp", None),
        P("fsdp", None),
        P("fsdp", None),
        P("fsdp", None),
        P(),
        P("fsdp", None),
        P("fsdp", None),
        P("fsdp", None),
    )
    out_specs = (
        P(("fsdp", "ctx"), None),
        P(("fsdp", "ctx"), None),
        P(),
        P("fsdp", None),
        P("fsdp", None),
        P("fsdp", None),
        P("fsdp", None),
        P(),
        P("fsdp", None),
        P("fsdp", None),
        P("fsdp", None),
    )
    return jax.shard_map(
        per_device, mesh=mesh, in_specs=in_specs, out_specs=out_specs, check_vma=False
    )
```

```python
import functools
import math

import jax
import jax.numpy as jnp
from jax import lax
from jax.experimental import pallas as pl
from jax.experimental.pallas import tpu as pltpu
from jax.sharding import PartitionSpec as P

HEADS = 16
KV_HEADS = 8
HEAD_DIM = 96


EPSILON = 1e-05
ROPE_BASE = 100000.0


def product(left, right):
    return jnp.dot(left, right, preferred_element_type=jnp.float32)


def product_back(left, right):
    return lax.dot_general(
        left, right, (((1,), (1,)), ((), ())), preferred_element_type=jnp.float32
    )


def product_rows(left, right):
    return lax.dot_general(
        left, right, (((0,), (0,)), ((), ())), preferred_element_type=jnp.float32
    )


def rms_scale(values):
    return lax.rsqrt(jnp.mean(values * values, axis=-1, keepdims=True) + EPSILON)


def norm_back(scale_rows, unit_rows, grad_unit):
    return scale_rows * (
        grad_unit - unit_rows * jnp.mean(grad_unit * unit_rows, axis=-1, keepdims=True)
    )


def rotary_tables(places):
    half_width = HEAD_DIM // 2
    frequencies = ROPE_BASE ** (-(jnp.arange(half_width, dtype=jnp.float32) * 2.0 / HEAD_DIM))
    angles = places.astype(jnp.float32)[:, None] * frequencies[None, :]
    return (jnp.cos(angles)[:, None, :], jnp.sin(angles)[:, None, :])


def rotate(values, cosine, sine):
    half_width = values.shape[-1] // 2
    lower_half = values[..., :half_width]
    upper_half = values[..., half_width:]
    return jnp.concatenate(
        [lower_half * cosine - upper_half * sine, upper_half * cosine + lower_half * sine], axis=-1
    )


def rotate_back(grads, cosine, sine):
    half_width = grads.shape[-1] // 2
    lower_half = grads[..., :half_width]
    upper_half = grads[..., half_width:]
    return jnp.concatenate(
        [lower_half * cosine + upper_half * sine, upper_half * cosine - lower_half * sine], axis=-1
    )


def block_total_of(total_keys):
    return max(1, total_keys // 512)


def masked_scores(query_grouped, query_places, key_rows, key_places, start, width):
    key_part = lax.dynamic_slice_in_dim(key_rows, start, width, 2)
    place_part = lax.dynamic_slice_in_dim(key_places, start, width, 1)
    scores = jnp.einsum(
        "sqhgd,shkd->shgqk", query_grouped, key_part, preferred_element_type=jnp.float32
    )
    scores = scores * (1.0 / math.sqrt(HEAD_DIM))
    allowed = place_part[:, None, None, None, :] <= query_places[:, None, None, :, None]
    return jnp.where(allowed, scores, -1000000000.0)


def attend_forward(query_grouped, query_places, key_rows, value_rows, key_places):
    seq_count, row_count, head_groups, group_size = query_grouped.shape[:4]
    total_keys = key_rows.shape[2]
    block_total = block_total_of(total_keys)
    width = total_keys // block_total
    stat_shape = (seq_count, head_groups, group_size, row_count)

    def peak_step(index, carry):
        running_top, running_sum = carry
        scores = masked_scores(
            query_grouped, query_places, key_rows, key_places, index * width, width
        )
        new_top = jnp.maximum(running_top, jnp.max(scores, axis=-1))
        running_sum = running_sum * jnp.exp(running_top - new_top) + jnp.sum(
            jnp.exp(scores - new_top[..., None]), axis=-1
        )
        return (new_top, running_sum)

    running_top, running_sum = lax.fori_loop(
        0,
        block_total,
        peak_step,
        (jnp.full(stat_shape, -1e30, jnp.float32), jnp.zeros(stat_shape, jnp.float32)),
    )
    log_total = running_top + jnp.log(running_sum)

    def value_step(index, gathered):
        scores = masked_scores(
            query_grouped, query_places, key_rows, key_places, index * width, width
        )
        soft_low = jnp.exp(scores - log_total[..., None]).astype(jnp.bfloat16)
        value_part = lax.dynamic_slice_in_dim(value_rows, index * width, width, 2)
        return gathered + jnp.einsum(
            "shgqk,shkd->sqhgd", soft_low, value_part, preferred_element_type=jnp.float32
        )

    attended = lax.fori_loop(
        0, block_total, value_step, jnp.zeros(query_grouped.shape, jnp.float32)
    )
    return (attended, log_total)


def attend_backward(
    query_grouped, query_places, key_rows, value_rows, key_places, log_total, grad_attended
):
    total_keys = key_rows.shape[2]
    block_total = block_total_of(total_keys)
    width = total_keys // block_total
    score_scale = 1.0 / math.sqrt(HEAD_DIM)

    def soft_and_grad(index):
        scores = masked_scores(
            query_grouped, query_places, key_rows, key_places, index * width, width
        )
        soft_values = jnp.exp(scores - log_total[..., None])
        value_part = lax.dynamic_slice_in_dim(value_rows, index * width, width, 2)
        grad_soft = jnp.einsum(
            "sqhgd,shkd->shgqk", grad_attended, value_part, preferred_element_type=jnp.float32
        )
        return (soft_values, grad_soft)

    def delta_step(index, row_delta):
        soft_values, grad_soft = soft_and_grad(index)
        return row_delta + jnp.sum(soft_values * grad_soft, axis=-1)

    row_delta = lax.fori_loop(0, block_total, delta_step, jnp.zeros(log_total.shape, jnp.float32))

    def grad_step(index, carry):
        grad_query, grad_keys, grad_values = carry
        soft_values, grad_soft = soft_and_grad(index)
        grad_scores = (soft_values * (grad_soft - row_delta[..., None])).astype(jnp.bfloat16)
        key_part = lax.dynamic_slice_in_dim(key_rows, index * width, width, 2)
        grad_query = (
            grad_query
            + jnp.einsum(
                "shgqk,shkd->sqhgd", grad_scores, key_part, preferred_element_type=jnp.float32
            )
            * score_scale
        )
        key_term = (
            jnp.einsum(
                "shgqk,sqhgd->shkd", grad_scores, query_grouped, preferred_element_type=jnp.float32
            )
            * score_scale
        )
        value_term = jnp.einsum(
            "shgqk,sqhgd->shkd",
            soft_values.astype(jnp.bfloat16),
            grad_attended,
            preferred_element_type=jnp.float32,
        )
        grad_keys = lax.dynamic_update_slice_in_dim(grad_keys, key_term, index * width, 2)
        grad_values = lax.dynamic_update_slice_in_dim(grad_values, value_term, index * width, 2)
        return (grad_query, grad_keys, grad_values)

    initial = (
        jnp.zeros(query_grouped.shape, jnp.float32),
        jnp.zeros(key_rows.shape, jnp.float32),
        jnp.zeros(value_rows.shape, jnp.float32),
    )
    return lax.fori_loop(0, block_total, grad_step, initial)


def softmax_parts(query_rows, key_rows, first_row):
    scores = product_back(query_rows, key_rows) * (1.0 / math.sqrt(HEAD_DIM))
    rows = lax.broadcasted_iota(jnp.int32, scores.shape, 0) + first_row
    columns = lax.broadcasted_iota(jnp.int32, scores.shape, 1)
    scores = jnp.where(columns <= rows, scores, -1e30)
    spread = jnp.exp(scores - jnp.max(scores, axis=-1, keepdims=True))
    return spread * (1.0 / jnp.sum(spread, axis=-1, keepdims=True))


def sort_blocks(place_ref, source_ref, targets, block):
    block_total = source_ref.shape[0] // block
    for slot in range(block_total):
        place = place_ref[slot * block]
        rows = source_ref[pl.ds(slot * block, block), :]
        start = 0
        for target in targets:
            width = target.shape[-1]
            target[pl.ds(pl.multiple_of(place, block), block), :] = rows[:, start : start + width]
            start += width


def attention_forward_kernel(block, place_ref, packed_ref, out_ref, q0, q1, k, v, result):
    sort_blocks(place_ref, packed_ref, (q0, q1, k, v), block)
    length = packed_ref.shape[0]
    tile = min(256, length)
    for first in range(0, length, tile):
        parts = []
        for q in (q0, q1):
            soft = softmax_parts(q[first : first + tile, :], k[: first + tile, :], first)
            parts.append(product(soft.astype(jnp.bfloat16), v[: first + tile, :]))
        result[first : first + tile, :] = jnp.concatenate(parts, axis=-1)
    for slot in range(length // block):
        place = pl.multiple_of(place_ref[slot * block], block)
        out_ref[pl.ds(slot * block, block), :] = result[pl.ds(place, block), :].astype(
            jnp.bfloat16
        )


def attention_backward_kernel(
    block, place_ref, packed_ref, grad_ref, out_ref, q0, q1, k, v, g0, g1, result, dk, dv
):
    sort_blocks(place_ref, packed_ref, (q0, q1, k, v), block)
    sort_blocks(place_ref, grad_ref, (g0, g1), block)
    length = packed_ref.shape[0]
    tile = min(256, length)
    scale = 1.0 / math.sqrt(HEAD_DIM)
    dk[...] = jnp.zeros_like(dk)
    dv[...] = jnp.zeros_like(dv)
    for first in range(0, length, tile):
        top = first + tile
        parts = []
        for q, g in ((q0, g0), (q1, g1)):
            query_rows = q[first:top, :]
            grad_rows = g[first:top, :]
            soft = softmax_parts(query_rows, k[:top, :], first)
            grad_soft = product_back(grad_rows, v[:top, :])
            delta = jnp.sum(soft * grad_soft, axis=-1, keepdims=True)
            grad_scores = (soft * (grad_soft - delta)).astype(jnp.bfloat16)
            parts.append(product(grad_scores, k[:top, :]) * scale)
            dk[:top, :] += product_rows(grad_scores, query_rows) * scale
            dv[:top, :] += product_rows(soft.astype(jnp.bfloat16), grad_rows)
        result[first:top, :] = jnp.concatenate(parts, axis=-1)
    for slot in range(length // block):
        place = pl.multiple_of(place_ref[slot * block], block)
        span = pl.ds(place, block)
        out_ref[pl.ds(slot * block, block), :] = jnp.concatenate(
            [result[span, :], dk[span, :], dv[span, :]], axis=-1
        ).astype(jnp.bfloat16)


def vmem():
    return pl.BlockSpec(memory_space=pltpu.VMEM)


def attention_calls(length, block):
    wide = 4 * HEAD_DIM
    pair = 2 * HEAD_DIM
    half = [pltpu.VMEM((length, HEAD_DIM), jnp.bfloat16)]
    full = [pltpu.VMEM((length, HEAD_DIM), jnp.float32)]
    params = pltpu.CompilerParams(vmem_limit_bytes=48 * 2**20)
    places = pl.BlockSpec(memory_space=pltpu.SMEM)
    forward = pl.pallas_call(
        functools.partial(attention_forward_kernel, block),
        out_shape=jax.ShapeDtypeStruct((length, pair), jnp.bfloat16),
        in_specs=[places, vmem()],
        out_specs=vmem(),
        scratch_shapes=half * 4 + [pltpu.VMEM((length, pair), jnp.float32)],
        compiler_params=params,
        name="attention_forward",
    )
    backward = pl.pallas_call(
        functools.partial(attention_backward_kernel, block),
        out_shape=jax.ShapeDtypeStruct((length, wide), jnp.bfloat16),
        in_specs=[places, vmem(), vmem()],
        out_specs=vmem(),
        scratch_shapes=half * 6 + [pltpu.VMEM((length, pair), jnp.float32)] + full * 2,
        compiler_params=params,
        name="attention_backward",
    )
    return forward, backward


def peer(ctx_index):
    return dict(device_id={"ctx": ctx_index}, device_id_type=pl.DeviceIdType.MESH)


def exchange_kernel(count, in_ref, out_ref, send_sem, recv_sem, own_sem):
    me = lax.axis_index("ctx")
    barrier = pltpu.get_barrier_semaphore()
    for step in range(1, count):
        pl.semaphore_signal(barrier, inc=1, **peer(lax.rem(me + step, count)))
    own = pltpu.make_async_copy(in_ref.at[me], out_ref.at[me], own_sem)
    own.start()
    pl.semaphore_wait(barrier, count - 1)
    copies = []
    for step in range(1, count):
        other = lax.rem(me + step, count)
        copies.append(
            pltpu.make_async_remote_copy(
                src_ref=in_ref.at[other],
                dst_ref=out_ref.at[me],
                send_sem=send_sem.at[step],
                recv_sem=recv_sem.at[step],
                **peer(other),
            )
        )
    for copy in copies:
        copy.start()
    own.wait()
    for copy in copies:
        copy.wait()


def exchange(values, key):
    count = values.shape[0]
    return pl.pallas_call(
        functools.partial(exchange_kernel, count),
        out_shape=jax.ShapeDtypeStruct(values.shape, values.dtype),
        in_specs=[pl.BlockSpec(memory_space=pl.ANY)],
        out_specs=pl.BlockSpec(memory_space=pl.ANY),
        scratch_shapes=[
            pltpu.SemaphoreType.DMA((count,)),
            pltpu.SemaphoreType.DMA((count,)),
            pltpu.SemaphoreType.DMA,
        ],
        compiler_params=pltpu.CompilerParams(collective_id=key, has_side_effects=True),
        name=f"exchange_{key}",
    )(values)


def gather_rows(values):
    return lax.all_gather(values, "fsdp", axis=0, tiled=True)


def scatter_rows(values):
    return lax.psum_scatter(
        values.astype(jnp.bfloat16), "fsdp", scatter_dimension=0, tiled=True
    ).astype(jnp.float32)


def per_device(
    inputs,
    positions,
    cotangent,
    attention_gain,
    query_weight,
    key_weight,
    value_weight,
    output_weight,
    feedforward_gain,
    gate_weight,
    up_weight,
    down_weight,
):
    row_count = inputs.shape[0]
    groups = HEADS // KV_HEADS
    gain_one = attention_gain.astype(jnp.float32)
    gain_two = feedforward_gain.astype(jnp.float32)
    seq_count = lax.axis_size("fsdp")
    first_row = lax.axis_index("fsdp") * row_count

    def own(values):
        return lax.dynamic_slice_in_dim(values, first_row, row_count, 0)

    query_places = gather_rows(positions).reshape(seq_count, row_count)
    key_places = lax.all_gather(query_places, "ctx", axis=1, tiled=True)
    all_cotangent = gather_rows(cotangent)
    flat_in = gather_rows(inputs).astype(jnp.float32)
    scale_one = rms_scale(flat_in)
    unit_one = flat_in * scale_one
    normed_one = (unit_one * gain_one).astype(jnp.bfloat16)
    total_rows = normed_one.shape[0]
    cosine, sine = rotary_tables(query_places.reshape(-1))
    query_heads = query_weight.shape[0] // HEAD_DIM
    kv_heads = key_weight.shape[0] // HEAD_DIM
    kv_width = kv_heads * HEAD_DIM
    query_low = rotate(
        product_back(normed_one, query_weight).reshape(total_rows, query_heads, HEAD_DIM), cosine, sine
    ).astype(jnp.bfloat16)
    key_low = rotate(
        product_back(normed_one, key_weight).reshape(total_rows, kv_heads, HEAD_DIM), cosine, sine
    ).astype(jnp.bfloat16)
    value_low = product_back(normed_one, value_weight).astype(jnp.bfloat16)
    ctx_size = lax.axis_size("ctx")
    by_head = ctx_size == seq_count * kv_heads

    def to_heads(parts):
        grouped = [
            part.reshape(seq_count, row_count, kv_heads, -1).swapaxes(1, 2) for part in parts
        ]
        return jnp.concatenate(grouped, axis=-1).reshape(ctx_size, row_count, -1)

    def from_heads(values, widths):
        grouped = values.reshape(seq_count, kv_heads, row_count, -1).swapaxes(1, 2)
        parts, start = [], 0
        for width in widths:
            parts.append(grouped[..., start : start + width].reshape(total_rows, kv_heads * width))
            start += width
        return parts

    pair = groups * HEAD_DIM
    flat_query = query_low.reshape(total_rows, query_heads * HEAD_DIM)
    if by_head:
        own_sequence = lax.axis_index("ctx") // kv_heads
        head_places = lax.dynamic_index_in_dim(key_places, own_sequence, 0, keepdims=False)
        length = head_places.shape[0]
        block = row_count // 2
        forward_call, backward_call = attention_calls(length, block)
        packed = exchange(
            to_heads([flat_query, key_low.reshape(total_rows, kv_width), value_low]), 1
        ).reshape(length, -1)
        attended_low = from_heads(
            exchange(forward_call(head_places, packed).reshape(ctx_size, row_count, pair), 2),
            (pair,),
        )[0]
    else:
        def spread(values):
            rows = lax.all_gather(values, "ctx", axis=0, tiled=True)
            rows = rows.reshape(ctx_size, seq_count, row_count, kv_width).swapaxes(0, 1)
            return rows.reshape(seq_count, ctx_size * row_count, kv_width)

        def collect(values):
            rows = values.astype(jnp.bfloat16).swapaxes(1, 2)
            rows = rows.reshape(seq_count, ctx_size, row_count, kv_width).swapaxes(0, 1)
            return lax.psum_scatter(
                rows.reshape(-1, kv_width), "ctx", scatter_dimension=0, tiled=True
            )

        all_keys = spread(key_low.reshape(total_rows, kv_width))
        all_values = spread(value_low)
        total_keys = all_keys.shape[1]
        key_grid = all_keys.reshape(seq_count, total_keys, kv_heads, HEAD_DIM).swapaxes(1, 2)
        value_grid = all_values.reshape(seq_count, total_keys, kv_heads, HEAD_DIM).swapaxes(1, 2)
        query_grouped = query_low.reshape(seq_count, row_count, kv_heads, groups, HEAD_DIM)
        attended, log_total = attend_forward(
            query_grouped, query_places, key_grid, value_grid, key_places
        )
        attended_low = attended.reshape(total_rows, query_heads * HEAD_DIM).astype(jnp.bfloat16)
    hidden_state = inputs.astype(jnp.float32) + scatter_rows(product(attended_low, output_weight))
    scale_two = rms_scale(hidden_state)
    unit_two = hidden_state * scale_two
    normed_two = gather_rows((unit_two * gain_two).astype(jnp.bfloat16))
    gate_values = product_back(normed_two, gate_weight)
    upward = product_back(normed_two, up_weight)
    sigmoid_gate = jax.nn.sigmoid(gate_values)
    activated = gate_values * sigmoid_gate
    mixed_hidden = (activated * upward).astype(jnp.bfloat16)
    grad_out = cotangent.astype(jnp.float32)
    grad_down = product_rows(mixed_hidden, all_cotangent)
    grad_mixed = product_back(all_cotangent, down_weight)
    grad_gate_low = (
        grad_mixed * upward * sigmoid_gate * (1.0 + gate_values * (1.0 - sigmoid_gate))
    ).astype(jnp.bfloat16)
    grad_up_low = (grad_mixed * activated).astype(jnp.bfloat16)
    grad_normed_two = scatter_rows(
        product(grad_gate_low, gate_weight) + product(grad_up_low, up_weight)
    )
    gain_two_grad = jnp.sum(grad_normed_two * unit_two, axis=0)
    grad_hidden = grad_out + norm_back(scale_two, unit_two, grad_normed_two * gain_two)
    branch_rows = gather_rows(grad_hidden.astype(jnp.bfloat16))
    layer_output = (hidden_state + scatter_rows(product(mixed_hidden, down_weight))).astype(
        jnp.bfloat16
    )
    grad_gate = product_rows(grad_gate_low, normed_two)
    grad_up = product_rows(grad_up_low, normed_two)
    grad_output = product_rows(attended_low, branch_rows)
    grad_attended = product_back(branch_rows, output_weight).astype(jnp.bfloat16)
    if by_head:
        grad_heads = exchange(to_heads([grad_attended]), 3).reshape(length, pair)
        packed_grads = exchange(
            backward_call(head_places, packed, grad_heads).reshape(ctx_size, row_count, -1), 4
        )
        grad_query_rot, grad_key_own, grad_value_low = from_heads(
            packed_grads, (pair, HEAD_DIM, HEAD_DIM)
        )
        grad_query_rot = grad_query_rot.astype(jnp.float32)
        grad_key_own = grad_key_own.astype(jnp.float32)
    else:
        grad_attended = grad_attended.reshape(seq_count, row_count, kv_heads, groups, HEAD_DIM)
        grad_query_rot, grad_key_all, grad_value_all = attend_backward(
            query_grouped, query_places, key_grid, value_grid, key_places, log_total, grad_attended
        )
        grad_key_own = collect(grad_key_all).astype(jnp.float32)
        grad_value_low = collect(grad_value_all)
    grad_query_low = (
        rotate_back(grad_query_rot.reshape(total_rows, query_heads, HEAD_DIM), cosine, sine)
        .reshape(total_rows, query_heads * HEAD_DIM)
        .astype(jnp.bfloat16)
    )
    grad_key_low = (
        rotate_back(
            grad_key_own.reshape(total_rows, kv_heads, HEAD_DIM), cosine, sine
        )
        .reshape(total_rows, kv_width)
        .astype(jnp.bfloat16)
    )
    grad_query = product_rows(grad_query_low, normed_one)
    grad_key = product_rows(grad_key_low, normed_one)
    grad_value = product_rows(grad_value_low, normed_one)
    grad_normed_one = scatter_rows(
        product(grad_query_low, query_weight)
        + product(grad_key_low, key_weight)
        + product(grad_value_low, value_weight)
    )
    own_unit = own(unit_one)
    gain_one_grad = jnp.sum(grad_normed_one * own_unit, axis=0)
    input_grad = grad_hidden + norm_back(own(scale_one), own_unit, grad_normed_one * gain_one)

    def ctx_sum(grad):
        return lax.psum(grad.astype(jnp.bfloat16), "ctx").astype(jnp.float32)

    gain_sums = lax.psum(jnp.stack([gain_one_grad, gain_two_grad]), ("fsdp", "ctx"))
    return (
        layer_output,
        input_grad,
        gain_sums[0],
        ctx_sum(grad_query),
        ctx_sum(grad_key),
        ctx_sum(grad_value),
        ctx_sum(grad_output),
        gain_sums[1],
        ctx_sum(grad_gate),
        ctx_sum(grad_up),
        ctx_sum(grad_down),
    )


def solution(mesh):
    in_specs = (
        P(("fsdp", "ctx"), None),
        P(("fsdp", "ctx")),
        P(("fsdp", "ctx"), None),
        P(),
        P("fsdp", None),
        P("fsdp", None),
        P("fsdp", None),
        P("fsdp", None),
        P(),
        P("fsdp", None),
        P("fsdp", None),
        P("fsdp", None),
    )
    out_specs = (
        P(("fsdp", "ctx"), None),
        P(("fsdp", "ctx"), None),
        P(),
        P("fsdp", None),
        P("fsdp", None),
        P("fsdp", None),
        P("fsdp", None),
        P(),
        P("fsdp", None),
        P("fsdp", None),
        P("fsdp", None),
    )
    return jax.shard_map(
        per_device, mesh=mesh, in_specs=in_specs, out_specs=out_specs, check_vma=False
    )
```

```python
import functools
import math

import jax
import jax.numpy as jnp
from jax import lax
from jax.experimental import pallas as pl
from jax.experimental.pallas import tpu as pltpu
from jax.sharding import PartitionSpec as P

HEADS = 16
KV_HEADS = 8
HEAD_DIM = 96


EPSILON = 1e-05
ROPE_BASE = 100000.0


def product(left, right):
    return jnp.dot(left, right, preferred_element_type=jnp.float32)


def product_back(left, right):
    return lax.dot_general(
        left, right, (((1,), (1,)), ((), ())), preferred_element_type=jnp.float32
    )


def product_rows(left, right):
    return lax.dot_general(
        left, right, (((0,), (0,)), ((), ())), preferred_element_type=jnp.float32
    )


def rms_scale(values):
    return lax.rsqrt(jnp.mean(values * values, axis=-1, keepdims=True) + EPSILON)


def norm_back(scale_rows, unit_rows, grad_unit):
    return scale_rows * (
        grad_unit - unit_rows * jnp.mean(grad_unit * unit_rows, axis=-1, keepdims=True)
    )


def rotary_tables(places):
    half_width = HEAD_DIM // 2
    frequencies = ROPE_BASE ** (-(jnp.arange(half_width, dtype=jnp.float32) * 2.0 / HEAD_DIM))
    angles = places.astype(jnp.float32)[:, None] * frequencies[None, :]
    return (jnp.cos(angles)[:, None, :], jnp.sin(angles)[:, None, :])


def rotate(values, cosine, sine):
    half_width = values.shape[-1] // 2
    lower_half = values[..., :half_width]
    upper_half = values[..., half_width:]
    return jnp.concatenate(
        [lower_half * cosine - upper_half * sine, upper_half * cosine + lower_half * sine], axis=-1
    )


def rotate_back(grads, cosine, sine):
    half_width = grads.shape[-1] // 2
    lower_half = grads[..., :half_width]
    upper_half = grads[..., half_width:]
    return jnp.concatenate(
        [lower_half * cosine + upper_half * sine, upper_half * cosine - lower_half * sine], axis=-1
    )


def block_total_of(total_keys):
    return max(1, total_keys // 512)


def masked_scores(query_grouped, query_places, key_rows, key_places, start, width):
    key_part = lax.dynamic_slice_in_dim(key_rows, start, width, 2)
    place_part = lax.dynamic_slice_in_dim(key_places, start, width, 1)
    scores = jnp.einsum(
        "sqhgd,shkd->shgqk", query_grouped, key_part, preferred_element_type=jnp.float32
    )
    scores = scores * (1.0 / math.sqrt(HEAD_DIM))
    allowed = place_part[:, None, None, None, :] <= query_places[:, None, None, :, None]
    return jnp.where(allowed, scores, -1000000000.0)


def attend_forward(query_grouped, query_places, key_rows, value_rows, key_places):
    seq_count, row_count, head_groups, group_size = query_grouped.shape[:4]
    total_keys = key_rows.shape[2]
    block_total = block_total_of(total_keys)
    width = total_keys // block_total
    stat_shape = (seq_count, head_groups, group_size, row_count)

    def peak_step(index, carry):
        running_top, running_sum = carry
        scores = masked_scores(
            query_grouped, query_places, key_rows, key_places, index * width, width
        )
        new_top = jnp.maximum(running_top, jnp.max(scores, axis=-1))
        running_sum = running_sum * jnp.exp(running_top - new_top) + jnp.sum(
            jnp.exp(scores - new_top[..., None]), axis=-1
        )
        return (new_top, running_sum)

    running_top, running_sum = lax.fori_loop(
        0,
        block_total,
        peak_step,
        (jnp.full(stat_shape, -1e30, jnp.float32), jnp.zeros(stat_shape, jnp.float32)),
    )
    log_total = running_top + jnp.log(running_sum)

    def value_step(index, gathered):
        scores = masked_scores(
            query_grouped, query_places, key_rows, key_places, index * width, width
        )
        soft_low = jnp.exp(scores - log_total[..., None]).astype(jnp.bfloat16)
        value_part = lax.dynamic_slice_in_dim(value_rows, index * width, width, 2)
        return gathered + jnp.einsum(
            "shgqk,shkd->sqhgd", soft_low, value_part, preferred_element_type=jnp.float32
        )

    attended = lax.fori_loop(
        0, block_total, value_step, jnp.zeros(query_grouped.shape, jnp.float32)
    )
    return (attended, log_total)


def attend_backward(
    query_grouped, query_places, key_rows, value_rows, key_places, log_total, grad_attended
):
    total_keys = key_rows.shape[2]
    block_total = block_total_of(total_keys)
    width = total_keys // block_total
    score_scale = 1.0 / math.sqrt(HEAD_DIM)

    def soft_and_grad(index):
        scores = masked_scores(
            query_grouped, query_places, key_rows, key_places, index * width, width
        )
        soft_values = jnp.exp(scores - log_total[..., None])
        value_part = lax.dynamic_slice_in_dim(value_rows, index * width, width, 2)
        grad_soft = jnp.einsum(
            "sqhgd,shkd->shgqk", grad_attended, value_part, preferred_element_type=jnp.float32
        )
        return (soft_values, grad_soft)

    def delta_step(index, row_delta):
        soft_values, grad_soft = soft_and_grad(index)
        return row_delta + jnp.sum(soft_values * grad_soft, axis=-1)

    row_delta = lax.fori_loop(0, block_total, delta_step, jnp.zeros(log_total.shape, jnp.float32))

    def grad_step(index, carry):
        grad_query, grad_keys, grad_values = carry
        soft_values, grad_soft = soft_and_grad(index)
        grad_scores = (soft_values * (grad_soft - row_delta[..., None])).astype(jnp.bfloat16)
        key_part = lax.dynamic_slice_in_dim(key_rows, index * width, width, 2)
        grad_query = (
            grad_query
            + jnp.einsum(
                "shgqk,shkd->sqhgd", grad_scores, key_part, preferred_element_type=jnp.float32
            )
            * score_scale
        )
        key_term = (
            jnp.einsum(
                "shgqk,sqhgd->shkd", grad_scores, query_grouped, preferred_element_type=jnp.float32
            )
            * score_scale
        )
        value_term = jnp.einsum(
            "shgqk,sqhgd->shkd",
            soft_values.astype(jnp.bfloat16),
            grad_attended,
            preferred_element_type=jnp.float32,
        )
        grad_keys = lax.dynamic_update_slice_in_dim(grad_keys, key_term, index * width, 2)
        grad_values = lax.dynamic_update_slice_in_dim(grad_values, value_term, index * width, 2)
        return (grad_query, grad_keys, grad_values)

    initial = (
        jnp.zeros(query_grouped.shape, jnp.float32),
        jnp.zeros(key_rows.shape, jnp.float32),
        jnp.zeros(value_rows.shape, jnp.float32),
    )
    return lax.fori_loop(0, block_total, grad_step, initial)


def softmax_parts(query_rows, key_rows, first_row):
    scores = product_back(query_rows, key_rows) * (1.0 / math.sqrt(HEAD_DIM))
    rows = lax.broadcasted_iota(jnp.int32, scores.shape, 0) + first_row
    columns = lax.broadcasted_iota(jnp.int32, scores.shape, 1)
    scores = jnp.where(columns <= rows, scores, -1e30)
    spread = jnp.exp(scores - jnp.max(scores, axis=-1, keepdims=True))
    return spread * (1.0 / jnp.sum(spread, axis=-1, keepdims=True))


def sort_blocks(place_ref, source_ref, targets, block):
    block_total = source_ref.shape[0] // block
    for slot in range(block_total):
        place = place_ref[slot * block]
        rows = source_ref[pl.ds(slot * block, block), :]
        start = 0
        for target in targets:
            width = target.shape[-1]
            target[pl.ds(pl.multiple_of(place, block), block), :] = rows[:, start : start + width]
            start += width


def attention_forward_kernel(block, place_ref, packed_ref, out_ref, q0, q1, k, v, result):
    sort_blocks(place_ref, packed_ref, (q0, q1, k, v), block)
    length = packed_ref.shape[0]
    tile = min(256, length)
    for first in range(0, length, tile):
        parts = []
        for q in (q0, q1):
            soft = softmax_parts(q[first : first + tile, :], k[: first + tile, :], first)
            parts.append(product(soft.astype(jnp.bfloat16), v[: first + tile, :]))
        result[first : first + tile, :] = jnp.concatenate(parts, axis=-1)
    for slot in range(length // block):
        place = pl.multiple_of(place_ref[slot * block], block)
        out_ref[pl.ds(slot * block, block), :] = result[pl.ds(place, block), :].astype(
            jnp.bfloat16
        )


def attention_backward_kernel(
    block, place_ref, packed_ref, grad_ref, out_ref, q0, q1, k, v, g0, g1, result, dk, dv
):
    sort_blocks(place_ref, packed_ref, (q0, q1, k, v), block)
    sort_blocks(place_ref, grad_ref, (g0, g1), block)
    length = packed_ref.shape[0]
    tile = min(256, length)
    scale = 1.0 / math.sqrt(HEAD_DIM)
    dk[...] = jnp.zeros_like(dk)
    dv[...] = jnp.zeros_like(dv)
    for first in range(0, length, tile):
        top = first + tile
        parts = []
        for q, g in ((q0, g0), (q1, g1)):
            query_rows = q[first:top, :]
            grad_rows = g[first:top, :]
            soft = softmax_parts(query_rows, k[:top, :], first)
            grad_soft = product_back(grad_rows, v[:top, :])
            delta = jnp.sum(soft * grad_soft, axis=-1, keepdims=True)
            grad_scores = (soft * (grad_soft - delta)).astype(jnp.bfloat16)
            parts.append(product(grad_scores, k[:top, :]) * scale)
            dk[:top, :] += product_rows(grad_scores, query_rows) * scale
            dv[:top, :] += product_rows(soft.astype(jnp.bfloat16), grad_rows)
        result[first:top, :] = jnp.concatenate(parts, axis=-1)
    for slot in range(length // block):
        place = pl.multiple_of(place_ref[slot * block], block)
        span = pl.ds(place, block)
        out_ref[pl.ds(slot * block, block), :] = jnp.concatenate(
            [result[span, :], dk[span, :], dv[span, :]], axis=-1
        ).astype(jnp.bfloat16)


def vmem():
    return pl.BlockSpec(memory_space=pltpu.VMEM)


def attention_calls(length, block):
    wide = 4 * HEAD_DIM
    pair = 2 * HEAD_DIM
    half = [pltpu.VMEM((length, HEAD_DIM), jnp.bfloat16)]
    full = [pltpu.VMEM((length, HEAD_DIM), jnp.float32)]
    params = pltpu.CompilerParams(vmem_limit_bytes=48 * 2**20)
    places = pl.BlockSpec(memory_space=pltpu.SMEM)
    forward = pl.pallas_call(
        functools.partial(attention_forward_kernel, block),
        out_shape=jax.ShapeDtypeStruct((length, pair), jnp.bfloat16),
        in_specs=[places, vmem()],
        out_specs=vmem(),
        scratch_shapes=half * 4 + [pltpu.VMEM((length, pair), jnp.float32)],
        compiler_params=params,
        name="attention_forward",
    )
    backward = pl.pallas_call(
        functools.partial(attention_backward_kernel, block),
        out_shape=jax.ShapeDtypeStruct((length, wide), jnp.bfloat16),
        in_specs=[places, vmem(), vmem()],
        out_specs=vmem(),
        scratch_shapes=half * 6 + [pltpu.VMEM((length, pair), jnp.float32)] + full * 2,
        compiler_params=params,
        name="attention_backward",
    )
    return forward, backward


def peer(ctx_index):
    return dict(device_id={"ctx": ctx_index}, device_id_type=pl.DeviceIdType.MESH)


def exchange_kernel(count, in_ref, out_ref, send_sem, recv_sem, own_sem):
    me = lax.axis_index("ctx")
    barrier = pltpu.get_barrier_semaphore()
    for step in range(1, count):
        pl.semaphore_signal(barrier, inc=1, **peer(lax.rem(me + step, count)))
    own = pltpu.make_async_copy(in_ref.at[me], out_ref.at[me], own_sem)
    own.start()
    pl.semaphore_wait(barrier, count - 1)
    copies = []
    for step in range(1, count):
        other = lax.rem(me + step, count)
        copies.append(
            pltpu.make_async_remote_copy(
                src_ref=in_ref.at[other],
                dst_ref=out_ref.at[me],
                send_sem=send_sem.at[step],
                recv_sem=recv_sem.at[step],
                **peer(other),
            )
        )
    for copy in copies:
        copy.start()
    own.wait()
    for copy in copies:
        copy.wait()


def exchange(values, key):
    count = values.shape[0]
    return pl.pallas_call(
        functools.partial(exchange_kernel, count),
        out_shape=jax.ShapeDtypeStruct(values.shape, values.dtype),
        in_specs=[pl.BlockSpec(memory_space=pl.ANY)],
        out_specs=pl.BlockSpec(memory_space=pl.ANY),
        scratch_shapes=[
            pltpu.SemaphoreType.DMA((count,)),
            pltpu.SemaphoreType.DMA((count,)),
            pltpu.SemaphoreType.DMA,
        ],
        compiler_params=pltpu.CompilerParams(collective_id=key, has_side_effects=True),
        name=f"exchange_{key}",
    )(values)


SPINE_ROWS = 48
LINE_ROWS = 64
ROUND_ROWS = 2 * SPINE_ROWS + LINE_ROWS
LEAD = 2


def reduce_kernel(
    rounds,
    grads_ref,
    gain_ref,
    out_ref,
    gain_out_ref,
    own,
    spine_in,
    line_in,
    gain_near,
    gain_far,
    load_sem,
    spine_up,
    spine_got,
    leaf_up,
    line_up,
    line_got,
    spine_down,
    spine_back,
    leaf_back,
    line_down,
    line_back,
    near_send,
    near_recv,
    far_send,
    far_recv,
):
    me = lax.axis_index("ctx")
    row = lax.axis_index("fsdp")
    depth = lax.div(me, 2)
    side = lax.rem(me, 2)
    other_side = me + 1 - 2 * side
    above, below = depth < 3, depth > 0
    barrier = pltpu.get_barrier_semaphore()

    for step in range(1, 4):
        pl.semaphore_signal(
            barrier,
            inc=1,
            device_id={"fsdp": lax.rem(row + step, 4)},
            device_id_type=pl.DeviceIdType.MESH,
        )
    for step in range(1, 8):
        pl.semaphore_signal(barrier, inc=1, **peer(lax.rem(me + step, 8)))

    def load(index):
        span = pl.ds(pl.multiple_of(index * ROUND_ROWS, 16), ROUND_ROWS)
        return pltpu.make_async_copy(grads_ref.at[span], own.at[span], load_sem.at[index])

    @pl.loop(0, rounds)
    def _(index):
        load(index).start()

    pl.semaphore_wait(barrier, 10)
    gain_near[row] = gain_ref[...]
    near = [
        pltpu.make_async_remote_copy(
            src_ref=gain_ref,
            dst_ref=gain_near.at[row],
            send_sem=near_send.at[step],
            recv_sem=near_recv.at[step],
            device_id={"fsdp": lax.rem(row + step, 4)},
            device_id_type=pl.DeviceIdType.MESH,
        )
        for step in range(1, 4)
    ]
    for copy in near:
        copy.start()
    far = [
        pltpu.make_async_remote_copy(
            src_ref=gain_far.at[me],
            dst_ref=gain_far.at[me],
            send_sem=far_send.at[step],
            recv_sem=far_recv.at[step],
            **peer(lax.rem(me + step, 8)),
        )
        for step in range(1, 8)
    ]

    def rows_at(start, count):
        return pl.ds(pl.multiple_of(start, 16), count)

    class Tree:
        def __init__(self, index, line):
            self.line = line
            if line:
                center = lax.rem(index, 4)
                count = LINE_ROWS
                start = index * ROUND_ROWS + 2 * SPINE_ROWS
                self.box, self.up, self.got = line_in, line_up, line_got
                self.down, self.back = line_down, line_back
                root_side = lax.rem(index, 2)
                on_cross = depth == center
                self.root = jnp.logical_and(on_cross, side == root_side)
                has_side = self.root
                to_side = jnp.logical_and(on_cross, side != root_side)
                reach = jnp.maximum(center, 3 - center)
                away = jnp.abs(depth - center)
                crossed = jnp.where(side == root_side, 0, 1)
                self.rise_age = reach - away + jnp.where(self.root, 1, 0)
                self.fall_age = reach + 1 + away + crossed
            else:
                center = 1 + side
                count = SPINE_ROWS
                start = index * ROUND_ROWS + side * SPINE_ROWS
                self.box, self.up, self.got = spine_in, spine_up, spine_got
                self.down, self.back = spine_down, spine_back
                self.root = depth == center
                has_side = None
                to_side = None
            self.rows = rows_at(start, count)
            self.slot_rows = rows_at(index * count, count)
            self.index = index
            self.children = (
                (jnp.logical_and(below, depth <= center), me - 2, 0),
                (jnp.logical_and(above, depth >= center), me + 2, 1),
                (has_side, other_side, 2),
            )
            parent = jnp.where(depth < center, me + 2, me - 2)
            slot = jnp.where(depth < center, 0, 1)
            if line:
                parent = jnp.where(to_side, other_side, parent)
                slot = jnp.where(to_side, 2, slot)
            self.parent = jnp.where(self.root, other_side, parent)
            self.parent_slot = jnp.where(self.root, 2, slot)

        def up_copy(self):
            return pltpu.make_async_remote_copy(
                src_ref=own.at[self.rows],
                dst_ref=self.box.at[self.parent_slot, self.slot_rows],
                send_sem=self.up.at[self.index],
                recv_sem=self.got.at[self.parent_slot, self.index],
                **peer(self.parent),
            )

        def got_copy(self, child, slot):
            return pltpu.make_async_remote_copy(
                src_ref=own.at[self.rows],
                dst_ref=self.box.at[slot, self.slot_rows],
                send_sem=self.up.at[self.index],
                recv_sem=self.got.at[slot, self.index],
                **peer(child),
            )

        def down_copy(self, child, slot, source):
            return pltpu.make_async_remote_copy(
                src_ref=source.at[self.rows],
                dst_ref=out_ref.at[self.rows],
                send_sem=self.down.at[slot, self.index],
                recv_sem=(self.back if slot < 2 or self.line else leaf_back).at[self.index],
                **peer(child),
            )

        def each_child(self, action):
            for present, child, slot in self.children:
                if present is None:
                    action(child, slot)
                else:
                    pl.when(present)(functools.partial(action, child, slot))

        def rise(self):
            self.each_child(lambda child, slot: self.got_copy(child, slot).wait_recv())
            first, count = self.rows.start, self.rows.size
            base = self.slot_rows.start
            for piece in range(0, count, 16):
                span = rows_at(first + piece, 16)
                total = own[span, :].astype(jnp.float32)
                for present, _, slot in self.children:
                    part = self.box[slot, rows_at(base + piece, 16), :].astype(jnp.float32)
                    total += part if present is None else jnp.where(present, part, 0.0)
                own[span, :] = total.astype(jnp.bfloat16)

            @pl.when(jnp.logical_not(self.root))
            def _():
                self.up_copy().start()

            @pl.when(self.root)
            def _():
                self.keep().start()
                self.each_child(lambda child, slot: self.down_copy(child, slot, own).start())

        def keep(self):
            return pltpu.make_async_copy(
                own.at[self.rows], out_ref.at[self.rows], self.up.at[self.index]
            )

        def fall(self):
            @pl.when(jnp.logical_not(self.root))
            def _():
                self.down_copy(self.parent, 0, out_ref).wait_recv()
                self.each_child(lambda child, slot: self.down_copy(child, slot, out_ref).start())

        def finish(self):
            @pl.when(jnp.logical_not(self.root))
            def _():
                self.up_copy().wait_send()

            @pl.when(self.root)
            def _():
                self.keep().wait()

            self.each_child(lambda child, slot: self.down_copy(child, slot, out_ref).wait_send())

    def leaf_rows(index):
        return rows_at(index * ROUND_ROWS + (1 - side) * SPINE_ROWS, SPINE_ROWS)

    def leaf_copy(index):
        return pltpu.make_async_remote_copy(
            src_ref=grads_ref.at[leaf_rows(index)],
            dst_ref=spine_in.at[2, rows_at(index * SPINE_ROWS, SPINE_ROWS)],
            send_sem=leaf_up.at[index],
            recv_sem=spine_got.at[2, index],
            **peer(other_side),
        )

    def leaf_result(index):
        return pltpu.make_async_remote_copy(
            src_ref=own.at[leaf_rows(index)],
            dst_ref=out_ref.at[leaf_rows(index)],
            send_sem=leaf_up.at[index],
            recv_sem=leaf_back.at[index],
            **peer(other_side),
        )

    for index in range(min(LEAD, rounds)):
        leaf_copy(index).start()

    def valid(index):
        return jnp.logical_and(index >= 0, index < rounds)

    @pl.loop(0, rounds + 9)
    def _(now):
        @pl.when(now < rounds)
        def _():
            load(now).wait()

        @pl.when(now + LEAD < rounds)
        def _():
            leaf_copy(now + LEAD).start()

        @pl.when(now == 1)
        def _():
            for copy in near:
                copy.wait()
            gain_far[me] = gain_near[0] + gain_near[1] + gain_near[2] + gain_near[3]
            for copy in far:
                copy.start()

        far_side = jnp.abs(depth - 2 + side)
        off_center = jnp.abs(depth - 1 - side)
        spine_rise = Tree(now - 3 + off_center, False)
        pl.when(valid(spine_rise.index))(spine_rise.rise)

        @pl.loop(0, 5)
        def _(age):
            tree = Tree(now - age, True)
            pl.when(jnp.logical_and(valid(tree.index), tree.rise_age == age))(tree.rise)

        spine_fall = Tree(now - 3 - off_center, False)
        pl.when(valid(spine_fall.index))(spine_fall.fall)

        @pl.loop(4, 9)
        def _(age):
            tree = Tree(now - age, True)
            pl.when(jnp.logical_and(valid(tree.index), tree.fall_age == age))(tree.fall)

        leaf_fall = now - 4 - far_side
        pl.when(valid(leaf_fall))(lambda: leaf_result(leaf_fall).wait_recv())

    for copy in far:
        copy.wait()
    gain_total = gain_far[0]
    for step in range(1, 8):
        gain_total += gain_far[step]
    gain_out_ref[...] = gain_total

    @pl.loop(0, rounds)
    def _(index):
        Tree(index, False).finish()
        Tree(index, True).finish()
        leaf_copy(index).wait_send()


def reduce_gradients(grads, gains, key):
    rounds = grads.shape[0] // ROUND_ROWS
    width = grads.shape[1]
    dma = pltpu.SemaphoreType.DMA
    return pl.pallas_call(
        functools.partial(reduce_kernel, rounds),
        out_shape=(
            jax.ShapeDtypeStruct(grads.shape, grads.dtype),
            jax.ShapeDtypeStruct(gains.shape, gains.dtype),
        ),
        in_specs=[pl.BlockSpec(memory_space=pl.ANY), vmem()],
        out_specs=(pl.BlockSpec(memory_space=pl.ANY), vmem()),
        scratch_shapes=[
            pltpu.VMEM(grads.shape, grads.dtype),
            pltpu.VMEM((3, rounds * SPINE_ROWS, width), grads.dtype),
            pltpu.VMEM((3, rounds * LINE_ROWS, width), grads.dtype),
            pltpu.VMEM((4,) + gains.shape, gains.dtype),
            pltpu.VMEM((8,) + gains.shape, gains.dtype),
            dma((rounds,)),
            dma((rounds,)),
            dma((3, rounds)),
            dma((rounds,)),
            dma((rounds,)),
            dma((3, rounds)),
            dma((3, rounds)),
            dma((rounds,)),
            dma((rounds,)),
            dma((3, rounds)),
            dma((rounds,)),
            dma((4,)),
            dma((4,)),
            dma((8,)),
            dma((8,)),
        ],
        compiler_params=pltpu.CompilerParams(
            collective_id=key, has_side_effects=True, vmem_limit_bytes=60 * 2**20
        ),
        name="reduce_gradients",
    )(grads, gains)


def gather_rows(values):
    return lax.all_gather(values, "fsdp", axis=0, tiled=True)


def scatter_rows(values):
    return lax.psum_scatter(
        values.astype(jnp.bfloat16), "fsdp", scatter_dimension=0, tiled=True
    ).astype(jnp.float32)


def per_device(
    inputs,
    positions,
    cotangent,
    attention_gain,
    query_weight,
    key_weight,
    value_weight,
    output_weight,
    feedforward_gain,
    gate_weight,
    up_weight,
    down_weight,
):
    row_count = inputs.shape[0]
    groups = HEADS // KV_HEADS
    gain_one = attention_gain.astype(jnp.float32)
    gain_two = feedforward_gain.astype(jnp.float32)
    seq_count = lax.axis_size("fsdp")
    first_row = lax.axis_index("fsdp") * row_count

    def own(values):
        return lax.dynamic_slice_in_dim(values, first_row, row_count, 0)

    query_places = gather_rows(positions).reshape(seq_count, row_count)
    key_places = lax.all_gather(query_places, "ctx", axis=1, tiled=True)
    all_cotangent = gather_rows(cotangent)
    flat_in = gather_rows(inputs).astype(jnp.float32)
    scale_one = rms_scale(flat_in)
    unit_one = flat_in * scale_one
    normed_one = (unit_one * gain_one).astype(jnp.bfloat16)
    total_rows = normed_one.shape[0]
    cosine, sine = rotary_tables(query_places.reshape(-1))
    query_heads = query_weight.shape[0] // HEAD_DIM
    kv_heads = key_weight.shape[0] // HEAD_DIM
    kv_width = kv_heads * HEAD_DIM
    query_low = rotate(
        product_back(normed_one, query_weight).reshape(total_rows, query_heads, HEAD_DIM), cosine, sine
    ).astype(jnp.bfloat16)
    key_low = rotate(
        product_back(normed_one, key_weight).reshape(total_rows, kv_heads, HEAD_DIM), cosine, sine
    ).astype(jnp.bfloat16)
    value_low = product_back(normed_one, value_weight).astype(jnp.bfloat16)
    ctx_size = lax.axis_size("ctx")
    by_head = ctx_size == seq_count * kv_heads

    def to_heads(parts):
        grouped = [
            part.reshape(seq_count, row_count, kv_heads, -1).swapaxes(1, 2) for part in parts
        ]
        return jnp.concatenate(grouped, axis=-1).reshape(ctx_size, row_count, -1)

    def from_heads(values, widths):
        grouped = values.reshape(seq_count, kv_heads, row_count, -1).swapaxes(1, 2)
        parts, start = [], 0
        for width in widths:
            parts.append(grouped[..., start : start + width].reshape(total_rows, kv_heads * width))
            start += width
        return parts

    pair = groups * HEAD_DIM
    flat_query = query_low.reshape(total_rows, query_heads * HEAD_DIM)
    if by_head:
        own_sequence = lax.axis_index("ctx") // kv_heads
        head_places = lax.dynamic_index_in_dim(key_places, own_sequence, 0, keepdims=False)
        length = head_places.shape[0]
        block = row_count // 2
        forward_call, backward_call = attention_calls(length, block)
        packed = exchange(
            to_heads([flat_query, key_low.reshape(total_rows, kv_width), value_low]), 1
        ).reshape(length, -1)
        attended_low = from_heads(
            exchange(forward_call(head_places, packed).reshape(ctx_size, row_count, pair), 2),
            (pair,),
        )[0]
    else:
        def spread(values):
            rows = lax.all_gather(values, "ctx", axis=0, tiled=True)
            rows = rows.reshape(ctx_size, seq_count, row_count, kv_width).swapaxes(0, 1)
            return rows.reshape(seq_count, ctx_size * row_count, kv_width)

        def collect(values):
            rows = values.astype(jnp.bfloat16).swapaxes(1, 2)
            rows = rows.reshape(seq_count, ctx_size, row_count, kv_width).swapaxes(0, 1)
            return lax.psum_scatter(
                rows.reshape(-1, kv_width), "ctx", scatter_dimension=0, tiled=True
            )

        all_keys = spread(key_low.reshape(total_rows, kv_width))
        all_values = spread(value_low)
        total_keys = all_keys.shape[1]
        key_grid = all_keys.reshape(seq_count, total_keys, kv_heads, HEAD_DIM).swapaxes(1, 2)
        value_grid = all_values.reshape(seq_count, total_keys, kv_heads, HEAD_DIM).swapaxes(1, 2)
        query_grouped = query_low.reshape(seq_count, row_count, kv_heads, groups, HEAD_DIM)
        attended, log_total = attend_forward(
            query_grouped, query_places, key_grid, value_grid, key_places
        )
        attended_low = attended.reshape(total_rows, query_heads * HEAD_DIM).astype(jnp.bfloat16)
    hidden_state = inputs.astype(jnp.float32) + scatter_rows(product(attended_low, output_weight))
    scale_two = rms_scale(hidden_state)
    unit_two = hidden_state * scale_two
    normed_two = gather_rows((unit_two * gain_two).astype(jnp.bfloat16))
    gate_values = product_back(normed_two, gate_weight)
    upward = product_back(normed_two, up_weight)
    sigmoid_gate = jax.nn.sigmoid(gate_values)
    activated = gate_values * sigmoid_gate
    mixed_hidden = (activated * upward).astype(jnp.bfloat16)
    grad_out = cotangent.astype(jnp.float32)
    grad_down = product_rows(mixed_hidden, all_cotangent)
    grad_mixed = product_back(all_cotangent, down_weight)
    grad_gate_low = (
        grad_mixed * upward * sigmoid_gate * (1.0 + gate_values * (1.0 - sigmoid_gate))
    ).astype(jnp.bfloat16)
    grad_up_low = (grad_mixed * activated).astype(jnp.bfloat16)
    grad_normed_two = scatter_rows(
        product(grad_gate_low, gate_weight) + product(grad_up_low, up_weight)
    )
    gain_two_grad = jnp.sum(grad_normed_two * unit_two, axis=0)
    grad_hidden = grad_out + norm_back(scale_two, unit_two, grad_normed_two * gain_two)
    branch_rows = gather_rows(grad_hidden.astype(jnp.bfloat16))
    layer_output = (hidden_state + scatter_rows(product(mixed_hidden, down_weight))).astype(
        jnp.bfloat16
    )
    grad_gate = product_rows(grad_gate_low, normed_two)
    grad_up = product_rows(grad_up_low, normed_two)
    grad_output = product_rows(attended_low, branch_rows)
    grad_attended = product_back(branch_rows, output_weight).astype(jnp.bfloat16)
    if by_head:
        grad_heads = exchange(to_heads([grad_attended]), 3).reshape(length, pair)
        packed_grads = exchange(
            backward_call(head_places, packed, grad_heads).reshape(ctx_size, row_count, -1), 4
        )
        grad_query_rot, grad_key_own, grad_value_low = from_heads(
            packed_grads, (pair, HEAD_DIM, HEAD_DIM)
        )
        grad_query_rot = grad_query_rot.astype(jnp.float32)
        grad_key_own = grad_key_own.astype(jnp.float32)
    else:
        grad_attended = grad_attended.reshape(seq_count, row_count, kv_heads, groups, HEAD_DIM)
        grad_query_rot, grad_key_all, grad_value_all = attend_backward(
            query_grouped, query_places, key_grid, value_grid, key_places, log_total, grad_attended
        )
        grad_key_own = collect(grad_key_all).astype(jnp.float32)
        grad_value_low = collect(grad_value_all)
    grad_query_low = (
        rotate_back(grad_query_rot.reshape(total_rows, query_heads, HEAD_DIM), cosine, sine)
        .reshape(total_rows, query_heads * HEAD_DIM)
        .astype(jnp.bfloat16)
    )
    grad_key_low = (
        rotate_back(
            grad_key_own.reshape(total_rows, kv_heads, HEAD_DIM), cosine, sine
        )
        .reshape(total_rows, kv_width)
        .astype(jnp.bfloat16)
    )
    grad_query = product_rows(grad_query_low, normed_one)
    grad_key = product_rows(grad_key_low, normed_one)
    grad_value = product_rows(grad_value_low, normed_one)
    grad_normed_one = scatter_rows(
        product(grad_query_low, query_weight)
        + product(grad_key_low, key_weight)
        + product(grad_value_low, value_weight)
    )
    own_unit = own(unit_one)
    gain_one_grad = jnp.sum(grad_normed_one * own_unit, axis=0)
    input_grad = grad_hidden + norm_back(own(scale_one), own_unit, grad_normed_one * gain_one)

    grads = (grad_query, grad_key, grad_value, grad_output, grad_gate, grad_up, grad_down)
    if by_head:
        rows = sum(grad.shape[0] for grad in grads)
        spare = jnp.zeros((-rows % ROUND_ROWS, grads[0].shape[1]), jnp.bfloat16)
        gain_parts = jnp.stack([gain_one_grad, gain_two_grad]).reshape(24, 128)
        summed, gain_sums = reduce_gradients(
            jnp.concatenate([grad.astype(jnp.bfloat16) for grad in grads] + [spare]),
            gain_parts,
            5,
        )
        gain_sums = gain_sums.reshape(2, -1)
        parts, start = [], 0
        for grad in grads:
            parts.append(summed[start : start + grad.shape[0]].astype(jnp.float32))
            start += grad.shape[0]
    else:
        parts = [
            lax.psum(grad.astype(jnp.bfloat16), "ctx").astype(jnp.float32) for grad in grads
        ]
        gain_sums = lax.psum(jnp.stack([gain_one_grad, gain_two_grad]), ("fsdp", "ctx"))
    return (
        layer_output,
        input_grad,
        gain_sums[0],
        parts[0],
        parts[1],
        parts[2],
        parts[3],
        gain_sums[1],
        parts[4],
        parts[5],
        parts[6],
    )


def solution(mesh):
    in_specs = (
        P(("fsdp", "ctx"), None),
        P(("fsdp", "ctx")),
        P(("fsdp", "ctx"), None),
        P(),
        P("fsdp", None),
        P("fsdp", None),
        P("fsdp", None),
        P("fsdp", None),
        P(),
        P("fsdp", None),
        P("fsdp", None),
        P("fsdp", None),
    )
    out_specs = (
        P(("fsdp", "ctx"), None),
        P(("fsdp", "ctx"), None),
        P(),
        P("fsdp", None),
        P("fsdp", None),
        P("fsdp", None),
        P("fsdp", None),
        P(),
        P("fsdp", None),
        P("fsdp", None),
        P("fsdp", None),
    )
    return jax.shard_map(
        per_device, mesh=mesh, in_specs=in_specs, out_specs=out_specs, check_vma=False
    )
```

```python
import functools
import math

import jax
import jax.numpy as jnp
from jax import lax
from jax.experimental import pallas as pl
from jax.experimental.pallas import tpu as pltpu
from jax.sharding import PartitionSpec as P

HEADS = 16
KV_HEADS = 8
HEAD_DIM = 96


EPSILON = 1e-05
ROPE_BASE = 100000.0


def product(left, right):
    return jnp.dot(left, right, preferred_element_type=jnp.float32)


def product_back(left, right):
    return lax.dot_general(
        left, right, (((1,), (1,)), ((), ())), preferred_element_type=jnp.float32
    )


def product_rows(left, right):
    return lax.dot_general(
        left, right, (((0,), (0,)), ((), ())), preferred_element_type=jnp.float32
    )


def rms_scale(values):
    return lax.rsqrt(jnp.mean(values * values, axis=-1, keepdims=True) + EPSILON)


def norm_back(scale_rows, unit_rows, grad_unit):
    return scale_rows * (
        grad_unit - unit_rows * jnp.mean(grad_unit * unit_rows, axis=-1, keepdims=True)
    )


def rotary_tables(places):
    half_width = HEAD_DIM // 2
    frequencies = ROPE_BASE ** (-(jnp.arange(half_width, dtype=jnp.float32) * 2.0 / HEAD_DIM))
    angles = places.astype(jnp.float32)[:, None] * frequencies[None, :]
    return (jnp.cos(angles)[:, None, :], jnp.sin(angles)[:, None, :])


def rotate(values, cosine, sine):
    half_width = values.shape[-1] // 2
    lower_half = values[..., :half_width]
    upper_half = values[..., half_width:]
    return jnp.concatenate(
        [lower_half * cosine - upper_half * sine, upper_half * cosine + lower_half * sine], axis=-1
    )


def rotate_back(grads, cosine, sine):
    half_width = grads.shape[-1] // 2
    lower_half = grads[..., :half_width]
    upper_half = grads[..., half_width:]
    return jnp.concatenate(
        [lower_half * cosine + upper_half * sine, upper_half * cosine - lower_half * sine], axis=-1
    )


def block_total_of(total_keys):
    return max(1, total_keys // 512)


def masked_scores(query_grouped, query_places, key_rows, key_places, start, width):
    key_part = lax.dynamic_slice_in_dim(key_rows, start, width, 2)
    place_part = lax.dynamic_slice_in_dim(key_places, start, width, 1)
    scores = jnp.einsum(
        "sqhgd,shkd->shgqk", query_grouped, key_part, preferred_element_type=jnp.float32
    )
    scores = scores * (1.0 / math.sqrt(HEAD_DIM))
    allowed = place_part[:, None, None, None, :] <= query_places[:, None, None, :, None]
    return jnp.where(allowed, scores, -1000000000.0)


def attend_forward(query_grouped, query_places, key_rows, value_rows, key_places):
    seq_count, row_count, head_groups, group_size = query_grouped.shape[:4]
    total_keys = key_rows.shape[2]
    block_total = block_total_of(total_keys)
    width = total_keys // block_total
    stat_shape = (seq_count, head_groups, group_size, row_count)

    def peak_step(index, carry):
        running_top, running_sum = carry
        scores = masked_scores(
            query_grouped, query_places, key_rows, key_places, index * width, width
        )
        new_top = jnp.maximum(running_top, jnp.max(scores, axis=-1))
        running_sum = running_sum * jnp.exp(running_top - new_top) + jnp.sum(
            jnp.exp(scores - new_top[..., None]), axis=-1
        )
        return (new_top, running_sum)

    running_top, running_sum = lax.fori_loop(
        0,
        block_total,
        peak_step,
        (jnp.full(stat_shape, -1e30, jnp.float32), jnp.zeros(stat_shape, jnp.float32)),
    )
    log_total = running_top + jnp.log(running_sum)

    def value_step(index, gathered):
        scores = masked_scores(
            query_grouped, query_places, key_rows, key_places, index * width, width
        )
        soft_low = jnp.exp(scores - log_total[..., None]).astype(jnp.bfloat16)
        value_part = lax.dynamic_slice_in_dim(value_rows, index * width, width, 2)
        return gathered + jnp.einsum(
            "shgqk,shkd->sqhgd", soft_low, value_part, preferred_element_type=jnp.float32
        )

    attended = lax.fori_loop(
        0, block_total, value_step, jnp.zeros(query_grouped.shape, jnp.float32)
    )
    return (attended, log_total)


def attend_backward(
    query_grouped, query_places, key_rows, value_rows, key_places, log_total, grad_attended
):
    total_keys = key_rows.shape[2]
    block_total = block_total_of(total_keys)
    width = total_keys // block_total
    score_scale = 1.0 / math.sqrt(HEAD_DIM)

    def soft_and_grad(index):
        scores = masked_scores(
            query_grouped, query_places, key_rows, key_places, index * width, width
        )
        soft_values = jnp.exp(scores - log_total[..., None])
        value_part = lax.dynamic_slice_in_dim(value_rows, index * width, width, 2)
        grad_soft = jnp.einsum(
            "sqhgd,shkd->shgqk", grad_attended, value_part, preferred_element_type=jnp.float32
        )
        return (soft_values, grad_soft)

    def delta_step(index, row_delta):
        soft_values, grad_soft = soft_and_grad(index)
        return row_delta + jnp.sum(soft_values * grad_soft, axis=-1)

    row_delta = lax.fori_loop(0, block_total, delta_step, jnp.zeros(log_total.shape, jnp.float32))

    def grad_step(index, carry):
        grad_query, grad_keys, grad_values = carry
        soft_values, grad_soft = soft_and_grad(index)
        grad_scores = (soft_values * (grad_soft - row_delta[..., None])).astype(jnp.bfloat16)
        key_part = lax.dynamic_slice_in_dim(key_rows, index * width, width, 2)
        grad_query = (
            grad_query
            + jnp.einsum(
                "shgqk,shkd->sqhgd", grad_scores, key_part, preferred_element_type=jnp.float32
            )
            * score_scale
        )
        key_term = (
            jnp.einsum(
                "shgqk,sqhgd->shkd", grad_scores, query_grouped, preferred_element_type=jnp.float32
            )
            * score_scale
        )
        value_term = jnp.einsum(
            "shgqk,sqhgd->shkd",
            soft_values.astype(jnp.bfloat16),
            grad_attended,
            preferred_element_type=jnp.float32,
        )
        grad_keys = lax.dynamic_update_slice_in_dim(grad_keys, key_term, index * width, 2)
        grad_values = lax.dynamic_update_slice_in_dim(grad_values, value_term, index * width, 2)
        return (grad_query, grad_keys, grad_values)

    initial = (
        jnp.zeros(query_grouped.shape, jnp.float32),
        jnp.zeros(key_rows.shape, jnp.float32),
        jnp.zeros(value_rows.shape, jnp.float32),
    )
    return lax.fori_loop(0, block_total, grad_step, initial)


def sort_places(place_ref, source_ref, targets, block):
    block_total = source_ref.shape[0] // block
    for slot in range(block_total):
        place = place_ref[slot * block]
        rows = source_ref[pl.ds(slot * block, block), :]
        start = 0
        for target in targets:
            width = target.shape[-1]
            target[pl.ds(pl.multiple_of(place, block), block), :] = rows[:, start : start + width]
            start += width


def attention_forward_kernel(block, place_ref, packed_ref, out_ref, q0, q1, k, v, result):
    sort_places(place_ref, packed_ref, (q0, q1, k, v), block)
    length = packed_ref.shape[0]
    tile = min(256, length)
    for first in range(0, length, tile):
        parts = []
        for q in (q0, q1):
            soft = softmax_parts(q[first : first + tile, :], k[: first + tile, :], first)
            parts.append(product(soft.astype(jnp.bfloat16), v[: first + tile, :]))
        result[first : first + tile, :] = jnp.concatenate(parts, axis=-1)
    for slot in range(length // block):
        place = pl.multiple_of(place_ref[slot * block], block)
        out_ref[pl.ds(slot * block, block), :] = result[pl.ds(place, block), :].astype(
            jnp.bfloat16
        )


def vmem():
    return pl.BlockSpec(memory_space=pltpu.VMEM)


def attention_call(length, block):
    pair = 2 * HEAD_DIM
    half = [pltpu.VMEM((length, HEAD_DIM), jnp.bfloat16)]
    params = pltpu.CompilerParams(vmem_limit_bytes=48 * 2**20)
    places = pl.BlockSpec(memory_space=pltpu.SMEM)
    forward = pl.pallas_call(
        functools.partial(attention_forward_kernel, block),
        out_shape=jax.ShapeDtypeStruct((length, pair), jnp.bfloat16),
        in_specs=[places, vmem()],
        out_specs=vmem(),
        scratch_shapes=half * 4 + [pltpu.VMEM((length, pair), jnp.float32)],
        compiler_params=params,
        name="attention_forward",
    )
    return forward


def peer(ctx_index):
    return dict(device_id={"ctx": ctx_index}, device_id_type=pl.DeviceIdType.MESH)


def exchange_kernel(count, in_ref, out_ref, send_sem, recv_sem, own_sem):
    me = lax.axis_index("ctx")
    barrier = pltpu.get_barrier_semaphore()
    for step in range(1, count):
        pl.semaphore_signal(barrier, inc=1, **peer(lax.rem(me + step, count)))
    own = pltpu.make_async_copy(in_ref.at[me], out_ref.at[me], own_sem)
    own.start()
    pl.semaphore_wait(barrier, count - 1)
    copies = []
    for step in range(1, count):
        other = lax.rem(me + step, count)
        copies.append(
            pltpu.make_async_remote_copy(
                src_ref=in_ref.at[other],
                dst_ref=out_ref.at[me],
                send_sem=send_sem.at[step],
                recv_sem=recv_sem.at[step],
                **peer(other),
            )
        )
    for copy in copies:
        copy.start()
    own.wait()
    for copy in copies:
        copy.wait()


def exchange(values, key):
    count = values.shape[0]
    return pl.pallas_call(
        functools.partial(exchange_kernel, count),
        out_shape=jax.ShapeDtypeStruct(values.shape, values.dtype),
        in_specs=[pl.BlockSpec(memory_space=pl.ANY)],
        out_specs=pl.BlockSpec(memory_space=pl.ANY),
        scratch_shapes=[
            pltpu.SemaphoreType.DMA((count,)),
            pltpu.SemaphoreType.DMA((count,)),
            pltpu.SemaphoreType.DMA,
        ],
        compiler_params=pltpu.CompilerParams(collective_id=key, has_side_effects=True),
        name=f"exchange_{key}",
    )(values)


SPINE_ROWS = 48
LINE_ROWS = 64
ROUND_ROWS = 2 * SPINE_ROWS + LINE_ROWS
LEAD = 2
RING = 12
TILE = 128
PAIR = (HEADS // KV_HEADS) * HEAD_DIM
WIDE = PAIR + 2 * HEAD_DIM


def near_fsdp(index):
    return dict(device_id={"fsdp": index}, device_id_type=pl.DeviceIdType.MESH)


def rows_at(start, count):
    return pl.ds(pl.multiple_of(start, 16), count)


class Place:
    def __init__(self):
        self.ctx = lax.axis_index("ctx")
        self.row = lax.axis_index("fsdp")
        self.chip, self.core = lax.div(self.row, 2), lax.rem(self.row, 2)
        self.partner = 2 * self.chip + 1 - self.core
        self.across = 2 * (1 - self.chip) + self.core
        self.corner = 2 * (1 - self.chip) + 1 - self.core

    def greet(self):
        barrier = pltpu.get_barrier_semaphore()
        for step in range(1, 4):
            pl.semaphore_signal(barrier, inc=1, **near_fsdp(lax.rem(self.row + step, 4)))
        for step in range(1, 8):
            pl.semaphore_signal(barrier, inc=1, **peer(lax.rem(self.ctx + step, 8)))
        pl.semaphore_wait(barrier, 10)


class Fold:
    def __init__(self, place, part, near, send, far, send_sem, recv_sem):
        self.place, self.part, self.near, self.send, self.far = place, part, near, send, far
        self.send_sem, self.recv_sem = send_sem, recv_sem

    def partner_copy(self, chip):
        block = 2 * chip + 1 - self.place.core
        return pltpu.make_async_remote_copy(
            src_ref=self.part.at[rows_at(block * TILE, TILE)],
            dst_ref=self.near.at[chip],
            send_sem=self.send_sem.at[chip],
            recv_sem=self.recv_sem.at[chip],
            **near_fsdp(self.place.partner),
        )

    def across_copy(self):
        return pltpu.make_async_remote_copy(
            src_ref=self.send,
            dst_ref=self.far,
            send_sem=self.send_sem.at[2],
            recv_sem=self.recv_sem.at[2],
            **near_fsdp(self.place.across),
        )

    def start(self):
        self.partner_copy(1 - self.place.chip).start()
        self.partner_copy(self.place.chip).start()

    def relay(self):
        there = 1 - self.place.chip
        self.partner_copy(there).wait_recv()
        base = self.place.across * TILE

        @pl.loop(0, TILE // 32)
        def _(piece):
            mine = self.part[rows_at(base + piece * 32, 32), :].astype(jnp.float32)
            span = rows_at(piece * 32, 32)
            self.send[span, :] = (
                mine + self.near[there, span, :].astype(jnp.float32)
            ).astype(jnp.bfloat16)

        self.across_copy().start()

    def arrive(self):
        self.partner_copy(self.place.chip).wait_recv()
        copy = self.across_copy()
        copy.wait_recv()
        copy.wait_send()
        self.partner_copy(0).wait_send()
        self.partner_copy(1).wait_send()

    def rows(self, start, count):
        mine = self.part[rows_at(self.place.row * TILE + start, count), :].astype(jnp.float32)
        span = rows_at(start, count)
        near = self.near[self.place.chip, span, :].astype(jnp.float32)
        return mine + near + self.far[span, :].astype(jnp.float32)


class Gather:
    def __init__(self, place, full, send_sem, recv_sem):
        self.place, self.full, self.send_sem, self.recv_sem = place, full, send_sem, recv_sem

    def copy(self, block, target, key):
        span = rows_at(block * TILE, TILE)
        return pltpu.make_async_remote_copy(
            src_ref=self.full.at[span],
            dst_ref=self.full.at[span],
            send_sem=self.send_sem.at[key],
            recv_sem=self.recv_sem.at[key],
            **near_fsdp(target),
        )

    def start(self):
        self.copy(self.place.row, self.place.across, 1).start()
        self.copy(self.place.row, self.place.partner, 0).start()

    def relay(self):
        self.copy(self.place.across, self.place.across, 1).wait_recv()
        self.copy(self.place.across, self.place.partner, 2).start()

    def arrive(self):
        self.copy(self.place.partner, self.place.partner, 0).wait_recv()
        self.copy(self.place.corner, self.place.partner, 2).wait_recv()
        self.copy(self.place.row, self.place.across, 1).wait_send()
        self.copy(self.place.row, self.place.partner, 0).wait_send()
        self.copy(self.place.across, self.place.partner, 2).wait_send()


class Swap:
    def __init__(self, place, source, target, send_sem, recv_sem):
        self.place, self.source, self.target = place, source, target
        self.send_sem, self.recv_sem = send_sem, recv_sem

    def copy(self, step):
        other = lax.rem(self.place.ctx + step, 8)
        return pltpu.make_async_remote_copy(
            src_ref=self.source.at[self.span(other)],
            dst_ref=self.target.at[self.span(self.place.ctx)],
            send_sem=self.send_sem.at[step],
            recv_sem=self.recv_sem.at[step],
            **peer(other),
        )

    def span(self, index):
        blocks = self.source.shape[0] // 8
        return pl.ds(index * blocks, blocks)

    def start(self):
        for step in range(1, 8):
            self.copy(step).start()
        own = self.span(self.place.ctx)
        self.target[own] = self.source[own]

    def arrive(self):
        for step in range(1, 8):
            self.copy(step).wait()


class Spread:
    def __init__(self, slots, index, count, device, send_sem, recv_sem):
        self.slots, self.index, self.count, self.device = slots, index, count, device
        self.send_sem, self.recv_sem = send_sem, recv_sem

    def copy(self, step):
        return pltpu.make_async_remote_copy(
            src_ref=self.slots.at[self.index],
            dst_ref=self.slots.at[self.index],
            send_sem=self.send_sem.at[step],
            recv_sem=self.recv_sem.at[step],
            **self.device(lax.rem(self.index + step, self.count)),
        )

    def start(self):
        for step in range(1, self.count):
            self.copy(step).start()

    def total(self):
        for step in range(1, self.count):
            self.copy(step).wait()
        result = self.slots[0]
        for step in range(1, self.count):
            result += self.slots[step]
        return result


class Tree:
    def __init__(self, place, own, out_ref, index, line, box, sems, leaf_back):
        me = place.ctx
        depth, side = lax.div(me, 2), lax.rem(me, 2)
        other_side = me + 1 - 2 * side
        self.own, self.out, self.box, self.index, self.line = own, out_ref, box, index, line
        self.up, self.got, self.down, self.back = sems
        self.leaf_back = leaf_back
        if line:
            center = lax.rem(index, 4)
            count = LINE_ROWS
            start = index * ROUND_ROWS + 2 * SPINE_ROWS
            root_side = lax.rem(index, 2)
            on_cross = depth == center
            self.root = jnp.logical_and(on_cross, side == root_side)
            has_side = self.root
            to_side = jnp.logical_and(on_cross, side != root_side)
            reach = jnp.maximum(center, 3 - center)
            away = jnp.abs(depth - center)
            crossed = jnp.where(side == root_side, 0, 1)
            self.rise_age = reach - away + jnp.where(self.root, 1, 0)
            self.fall_age = reach + 1 + away + crossed
        else:
            center = 1 + side
            count = SPINE_ROWS
            start = index * ROUND_ROWS + side * SPINE_ROWS
            self.root = depth == center
            has_side = None
        self.count = count
        self.start = start
        self.slot = lax.rem(index, RING)
        self.rows = rows_at(start, count)
        self.children = (
            (jnp.logical_and(depth > 0, depth <= center), me - 2, 0),
            (jnp.logical_and(depth < 3, depth >= center), me + 2, 1),
            (has_side, other_side, 2),
        )
        parent = jnp.where(depth < center, me + 2, me - 2)
        slot = jnp.where(depth < center, 0, 1)
        if line:
            parent = jnp.where(to_side, other_side, parent)
            slot = jnp.where(to_side, 2, slot)
        self.parent = jnp.where(self.root, other_side, parent)
        self.parent_slot = jnp.where(self.root, 2, slot)

    def boxed(self, slot):
        return self.box.at[slot, rows_at(self.slot * self.count, self.count)]

    def up_copy(self, target, slot):
        return pltpu.make_async_remote_copy(
            src_ref=self.own.at[self.rows],
            dst_ref=self.boxed(slot),
            send_sem=self.up.at[self.slot],
            recv_sem=self.got.at[slot, self.slot],
            **peer(target),
        )

    def down_copy(self, child, slot, source):
        back = self.back if slot < 2 or self.line else self.leaf_back
        return pltpu.make_async_remote_copy(
            src_ref=source.at[self.rows],
            dst_ref=self.out.at[self.rows],
            send_sem=self.down.at[slot, self.slot],
            recv_sem=back.at[self.slot],
            **peer(child),
        )

    def each_child(self, action):
        for present, child, slot in self.children:
            if present is None:
                action(child, slot)
            else:
                pl.when(present)(functools.partial(action, child, slot))

    def keep(self):
        return pltpu.make_async_copy(
            self.own.at[self.rows], self.out.at[self.rows], self.up.at[self.slot]
        )

    def rise(self):
        self.each_child(lambda child, slot: self.up_copy(child, slot).wait_recv())
        base = self.slot * self.count
        for piece in range(0, self.count, 16):
            span = rows_at(self.start + piece, 16)
            total = self.own[span, :].astype(jnp.float32)
            for present, _, slot in self.children:
                part = self.box[slot, rows_at(base + piece, 16), :].astype(jnp.float32)
                total += part if present is None else jnp.where(present, part, 0.0)
            self.own[span, :] = total.astype(jnp.bfloat16)

        @pl.when(jnp.logical_not(self.root))
        def _():
            self.up_copy(self.parent, self.parent_slot).start()

        @pl.when(self.root)
        def _():
            self.keep().start()
            self.each_child(lambda child, slot: self.down_copy(child, slot, self.own).start())

    def fall(self):
        @pl.when(jnp.logical_not(self.root))
        def _():
            self.down_copy(self.parent, 0, self.out).wait_recv()
            self.each_child(lambda child, slot: self.down_copy(child, slot, self.out).start())

    def finish(self):
        @pl.when(jnp.logical_not(self.root))
        def _():
            self.up_copy(self.parent, self.parent_slot).wait_send()

        @pl.when(self.root)
        def _():
            self.keep().wait()

        self.each_child(lambda child, slot: self.down_copy(child, slot, self.out).wait_send())


def softmax_parts(query_rows, key_rows, first_row):
    scores = product_back(query_rows, key_rows) * (1.0 / math.sqrt(HEAD_DIM))
    rows = lax.broadcasted_iota(jnp.int32, scores.shape, 0) + first_row
    columns = lax.broadcasted_iota(jnp.int32, scores.shape, 1)
    scores = jnp.where(columns <= rows, scores, -1e30)
    spread = jnp.exp(scores - jnp.max(scores, axis=-1, keepdims=True))
    return spread * (1.0 / jnp.sum(spread, axis=-1, keepdims=True))


def sort_blocks(slot_ref, source, targets):
    block_total, block, _ = source.shape
    for index in range(block_total):
        rows = source[slot_ref[index]]
        start = 0
        for target in targets:
            width = target.shape[-1]
            target[index * block : (index + 1) * block, :] = rows[:, start : start + width]
            start += width


def norm_back_rows(values, grad_unit):
    scale = rms_scale(values)
    unit = values * scale
    return unit, lambda grad: norm_back(scale, unit, grad)


def backward_kernel(
    rounds,
    block,
    order_ref,
    gate_ref,
    up_ref,
    down_ref,
    part_ref,
    hidden_ref,
    cotangent_ref,
    input_ref,
    gain_ref,
    output_weight_ref,
    attended_ref,
    packed_ref,
    normed_ref,
    cosine_ref,
    sine_ref,
    half_swap_ref,
    weight_ref,
    out_ref,
    gain_out_ref,
    input_grad_ref,
    own,
    spine_in,
    line_in,
    part,
    hidden,
    cotangent,
    inputs,
    output_weight,
    attended,
    packed,
    normed,
    cosine,
    sine,
    half_swap,
    weight,
    near,
    send,
    far,
    branch,
    grad_hidden,
    gain_part,
    heads_out,
    heads_in,
    q0,
    q1,
    k,
    v,
    g0,
    g1,
    result,
    dk,
    dv,
    packed_out,
    packed_in,
    turned,
    gain_near,
    gain_far,
    fetch_sem,
    spine_up,
    spine_got,
    spine_down,
    spine_back,
    leaf_up,
    leaf_back,
    line_up,
    line_got,
    line_down,
    line_back,
    fold_send,
    fold_recv,
    gather_send,
    gather_recv,
    swap_send,
    swap_recv,
    near_send,
    near_recv,
    far_send,
    far_recv,
):
    place = Place()
    me = place.ctx
    depth, side = lax.div(me, 2), lax.rem(me, 2)
    other_side = me + 1 - 2 * side
    hidden_units = gate_ref.shape[0]
    base = 3 * hidden_units
    spare = rounds * ROUND_ROWS - base - 3 * WIDE
    length = q0.shape[0]
    halves = TILE // block
    tile = min(256, length)
    tiles = length // tile
    scale = 1.0 / math.sqrt(HEAD_DIM)

    fetches = {}
    for key, (source, target) in enumerate(
        (
            (part_ref, part),
            (gate_ref, own.at[pl.ds(0, hidden_units)]),
            (up_ref, own.at[pl.ds(hidden_units, hidden_units)]),
            (hidden_ref, hidden),
            (cotangent_ref, cotangent),
            (output_weight_ref, output_weight),
            (packed_ref, packed),
            (attended_ref, attended),
            (down_ref, own.at[pl.ds(2 * hidden_units, hidden_units)]),
            (normed_ref, normed),
            (cosine_ref, cosine),
            (sine_ref, sine),
            (half_swap_ref, half_swap),
            (weight_ref, weight),
            (input_ref, inputs),
        )
    ):
        fetches[id(source)] = pltpu.make_async_copy(source, target, fetch_sem.at[key])

    def fetch(*sources):
        for source in sources:
            fetches[id(source)].wait()

    for copy in fetches.values():
        copy.start()
    if spare:
        own[base + 3 * WIDE :, :] = jnp.zeros((spare, own.shape[1]), own.dtype)
    place.greet()
    fetch(part_ref)
    fold_two = Fold(place, part, near.at[0], send.at[0], far.at[0], fold_send.at[0], fold_recv.at[0])
    fold_one = Fold(place, part, near.at[1], send.at[1], far.at[1], fold_send.at[1], fold_recv.at[1])
    gather = Gather(place, branch, gather_send, gather_recv)
    swap_heads = Swap(place, heads_out, heads_in, swap_send.at[0], swap_recv.at[0])
    swap_packed = Swap(place, packed_out, packed_in, swap_send.at[1], swap_recv.at[1])
    spread_near = Spread(gain_near, place.row, 4, near_fsdp, near_send, near_recv)
    spread_far = Spread(gain_far, me, 8, peer, far_send, far_recv)
    fold_two.start()
    fetch(gate_ref, up_ref, down_ref)

    spine_sems = (spine_up, spine_got, spine_down, spine_back)
    line_sems = (line_up, line_got, line_down, line_back)

    def spine(index):
        return Tree(place, own, out_ref, index, False, spine_in, spine_sems, leaf_back)

    def line(index):
        return Tree(place, own, out_ref, index, True, line_in, line_sems, None)

    def leaf_rows(index):
        return rows_at(index * ROUND_ROWS + (1 - side) * SPINE_ROWS, SPINE_ROWS)

    def leaf_copy(index):
        slot = lax.rem(index, RING)
        return pltpu.make_async_remote_copy(
            src_ref=own.at[leaf_rows(index)],
            dst_ref=spine_in.at[2, rows_at(slot * SPINE_ROWS, SPINE_ROWS)],
            send_sem=leaf_up.at[slot],
            recv_sem=spine_got.at[2, slot],
            **peer(other_side),
        )

    def leaf_result(index):
        slot = lax.rem(index, RING)
        return pltpu.make_async_remote_copy(
            src_ref=own.at[leaf_rows(index)],
            dst_ref=out_ref.at[leaf_rows(index)],
            send_sem=leaf_up.at[slot],
            recv_sem=leaf_back.at[slot],
            **peer(other_side),
        )

    def stage_norm_two():
        fetch(hidden_ref, cotangent_ref)
        fold_two.arrive()
        gain_part[...] = jnp.zeros_like(gain_part)

        @pl.loop(0, TILE // 16)
        def _(piece):
            span = rows_at(piece * 16, 16)
            grad = fold_two.rows(piece * 16, 16)
            unit, back = norm_back_rows(hidden[span, :], None)
            gain_part[1] += (grad * unit).reshape(2, 8, -1).sum(axis=0)
            total = cotangent[span, :].astype(jnp.float32) + back(grad * gain_ref[1:2, :])
            grad_hidden[span, :] = total
            branch[rows_at(place.row * TILE + piece * 16, 16), :] = total.astype(jnp.bfloat16)

        gather.start()

    def stage_heads():
        fetch(output_weight_ref)
        gather.arrive()

        @pl.loop(0, 4)
        def _(sequence):
            rows = branch[rows_at(sequence * TILE, TILE), :]
            grads = product_back(rows, output_weight[...]).astype(jnp.bfloat16)
            for head in range(2):
                heads_out[pl.ds((2 * sequence + head) * halves, halves)] = grads[
                    :, head * PAIR : (head + 1) * PAIR
                ].reshape(halves, block, PAIR)

        swap_heads.start()

    def stage_sort():
        fetch(packed_ref)
        sort_blocks(order_ref, packed, (q0, q1, k, v))

    def stage_output_grad():
        fetch(attended_ref)
        for first in range(0, own.shape[1], 512):
            columns = slice(first, first + 512)
            own[base + 2 * WIDE :base + 3 * WIDE, columns] = product_rows(
                attended[...], branch[:, columns]
            ).astype(jnp.bfloat16)

    def stage_sort_grads():
        swap_heads.arrive()
        sort_blocks(order_ref, heads_in, (g0, g1))
        dk[...] = jnp.zeros_like(dk)
        dv[...] = jnp.zeros_like(dv)

    def stage_attention(index):
        first, top = index * tile, (index + 1) * tile
        parts = []
        for q, g in ((q0, g0), (q1, g1)):
            query_rows = q[first:top, :]
            grad_rows = g[first:top, :]
            soft = softmax_parts(query_rows, k[:top, :], first)
            grad_soft = product_back(grad_rows, v[:top, :])
            delta = jnp.sum(soft * grad_soft, axis=-1, keepdims=True)
            grad_scores = (soft * (grad_soft - delta)).astype(jnp.bfloat16)
            parts.append(product(grad_scores, k[:top, :]) * scale)
            key_term = product_rows(grad_scores, query_rows) * scale
            value_term = product_rows(soft.astype(jnp.bfloat16), grad_rows)
            dk[: top // block] += key_term.reshape(-1, block, HEAD_DIM)
            dv[: top // block] += value_term.reshape(-1, block, HEAD_DIM)
        result[first // block : top // block] = jnp.concatenate(parts, axis=-1).reshape(
            -1, block, PAIR
        )

    def stage_unsort():
        for slot in range(length // block):
            spot = order_ref[length // block + slot]
            packed_out[slot] = jnp.concatenate(
                [result[spot], dk[spot], dv[spot]], axis=-1
            ).astype(jnp.bfloat16)
        swap_packed.start()

    def stage_turn():
        fetch(cosine_ref, sine_ref, half_swap_ref, weight_ref)
        swap_packed.arrive()

        @pl.loop(0, 4)
        def _(sequence):
            span = rows_at(sequence * TILE, TILE)
            total = None
            for head in range(2):
                grads = packed_in[pl.ds((2 * sequence + head) * halves, halves)]
                grads = grads.reshape(TILE, WIDE)
                swapped = product(grads, half_swap[...])
                low = (
                    grads.astype(jnp.float32) * cosine[span, :] + swapped * sine[span, :]
                ).astype(jnp.bfloat16)
                turned[head, span, :] = low
                term = product(low, weight[head])
                total = term if total is None else total + term
            part[span, :] = total.astype(jnp.bfloat16)

        fold_one.start()

    def stage_projection_grads(head):
        if head == 0:
            fetch(normed_ref)
        query_base = base + head * PAIR
        key_base = base + WIDE + head * HEAD_DIM
        value_base = key_base + 2 * HEAD_DIM
        for first in range(0, own.shape[1], 512):
            columns = slice(first, first + 512)
            grads = product_rows(turned[head], normed[:, columns]).astype(jnp.bfloat16)
            own[query_base : query_base + PAIR, columns] = grads[:PAIR]
            own[key_base : key_base + HEAD_DIM, columns] = grads[PAIR : PAIR + HEAD_DIM]
            own[value_base : value_base + HEAD_DIM, columns] = grads[PAIR + HEAD_DIM :]

    def stage_norm_one():
        fetch(input_ref)
        fold_one.arrive()

        @pl.loop(0, TILE // 16)
        def _(piece):
            span = rows_at(piece * 16, 16)
            grad = fold_one.rows(piece * 16, 16)
            unit, back = norm_back_rows(inputs[span, :].astype(jnp.float32), None)
            gain_part[0] += (grad * unit).reshape(2, 8, -1).sum(axis=0)
            input_grad_ref[span, :] = grad_hidden[span, :] + back(grad * gain_ref[0:1, :])

        gain_near[place.row] = jnp.sum(gain_part[...], axis=1)
        spread_near.start()

    def stage_gain():
        gain_far[me] = spread_near.total()
        spread_far.start()

    stages = [
        (0, fold_two.relay),
        (0, stage_sort),
        (2, stage_norm_two),
        (3, gather.relay),
        (4, stage_heads),
        (5, stage_output_grad),
        (6, stage_sort_grads),
    ]
    stages += [(6 + index, functools.partial(stage_attention, index)) for index in range(tiles)]
    now = 6 + tiles - 1
    stages += [
        (now, stage_unsort),
        (now + 2, stage_turn),
        (now + 3, fold_one.relay),
        (now + 3, functools.partial(stage_projection_grads, 0)),
        (now + 4, functools.partial(stage_projection_grads, 1)),
        (now + 5, stage_norm_one),
        (now + 6, stage_gain),
    ]
    needed = base // ROUND_ROWS - LEAD
    assert now + 4 < needed

    for index in range(LEAD):
        leaf_copy(index).start()

    def valid(index):
        return jnp.logical_and(index >= 0, index < rounds)

    @pl.loop(0, rounds + RING)
    def _(now):
        far_side = jnp.abs(depth - 2 + side)
        off_center = jnp.abs(depth - 1 - side)
        done = now - RING + 1
        for tree in (spine(done), line(done)):
            pl.when(valid(done))(tree.finish)

        @pl.when(now + LEAD < rounds)
        def _():
            leaf_copy(now + LEAD).start()

        rising = spine(now - 3 + off_center)
        pl.when(valid(rising.index))(rising.rise)

        @pl.loop(0, 5)
        def _(age):
            tree = line(now - age)
            pl.when(jnp.logical_and(valid(tree.index), tree.rise_age == age))(tree.rise)

        falling = spine(now - 3 - off_center)
        pl.when(valid(falling.index))(falling.fall)

        @pl.loop(4, 9)
        def _(age):
            tree = line(now - age)
            pl.when(jnp.logical_and(valid(tree.index), tree.fall_age == age))(tree.fall)

        leaf_fall = now - 4 - far_side

        @pl.when(valid(leaf_fall))
        def _():
            leaf_result(leaf_fall).wait_recv()
            leaf_copy(leaf_fall).wait_send()

        for when, stage in stages:
            pl.when(now == when)(stage)

    gain_out_ref[...] = spread_far.total()


def backward(order, grads, part, hidden, cotangent, inputs, gains, output_weight, attended,
             packed, normed, cosine, sine, half_swap, weight, block, key):
    width = hidden.shape[1]
    rows = 3 * grads[0].shape[0] + 3 * WIDE
    rounds = -(-rows // ROUND_ROWS)
    length = packed.shape[0]
    packed = packed.reshape(-1, block, WIDE)
    dma = pltpu.SemaphoreType.DMA
    low, full = jnp.bfloat16, jnp.float32
    any_spec = pl.BlockSpec(memory_space=pl.ANY)
    operands = (
        order, *grads, part, hidden, cotangent, inputs, gains, output_weight, attended,
        packed, normed, cosine, sine, half_swap, weight,
    )

    def like(array):
        return pltpu.VMEM(array.shape, array.dtype)

    return pl.pallas_call(
        functools.partial(backward_kernel, rounds, block),
        out_shape=(
            jax.ShapeDtypeStruct((rounds * ROUND_ROWS, width), low),
            jax.ShapeDtypeStruct((2, width), full),
            jax.ShapeDtypeStruct((TILE, width), full),
        ),
        in_specs=[pl.BlockSpec(memory_space=pltpu.SMEM)]
        + [any_spec] * 7
        + [vmem()]
        + [any_spec] * 8,
        out_specs=(any_spec, vmem(), vmem()),
        scratch_shapes=[
            pltpu.VMEM((rounds * ROUND_ROWS, width), low),
            pltpu.VMEM((3, RING * SPINE_ROWS, width), low),
            pltpu.VMEM((3, RING * LINE_ROWS, width), low),
            like(part), like(hidden), like(cotangent), like(inputs), like(output_weight),
            like(attended), like(packed), like(normed), like(cosine), like(sine),
            like(half_swap), like(weight),
            pltpu.VMEM((2, 2, TILE, width), low),
            pltpu.VMEM((2, TILE, width), low),
            pltpu.VMEM((2, TILE, width), low),
            pltpu.VMEM((4 * TILE, width), low),
            pltpu.VMEM((TILE, width), full),
            pltpu.VMEM((2, 8, width), full),
            pltpu.VMEM((length // block, block, PAIR), low),
            pltpu.VMEM((length // block, block, PAIR), low),
        ]
        + [pltpu.VMEM((length, HEAD_DIM), low)] * 6
        + [pltpu.VMEM((length // block, block, PAIR), full)]
        + [pltpu.VMEM((length // block, block, HEAD_DIM), full)] * 2
        + [
            pltpu.VMEM((length // block, block, WIDE), low),
            pltpu.VMEM((length // block, block, WIDE), low),
            pltpu.VMEM((2, 4 * TILE, WIDE), low),
            pltpu.VMEM((4, 2, width), full),
            pltpu.VMEM((8, 2, width), full),
            dma((15,)),
            dma((RING,)), dma((3, RING)), dma((3, RING)), dma((RING,)),
            dma((RING,)), dma((RING,)),
            dma((RING,)), dma((3, RING)), dma((3, RING)), dma((RING,)),
            dma((2, 3)), dma((2, 3)),
            dma((3,)), dma((3,)),
            dma((2, 8)), dma((2, 8)),
            dma((4,)), dma((4,)), dma((8,)), dma((8,)),
        ],
        compiler_params=pltpu.CompilerParams(
            collective_id=key, has_side_effects=True, vmem_limit_bytes=63 * 2**20
        ),
        name="backward",
    )(*operands)


def gather_rows(values):
    return lax.all_gather(values, "fsdp", axis=0, tiled=True)


def scatter_rows(values):
    return lax.psum_scatter(
        values.astype(jnp.bfloat16), "fsdp", scatter_dimension=0, tiled=True
    ).astype(jnp.float32)


def per_device(
    inputs,
    positions,
    cotangent,
    attention_gain,
    query_weight,
    key_weight,
    value_weight,
    output_weight,
    feedforward_gain,
    gate_weight,
    up_weight,
    down_weight,
):
    row_count = inputs.shape[0]
    groups = HEADS // KV_HEADS
    gain_one = attention_gain.astype(jnp.float32)
    gain_two = feedforward_gain.astype(jnp.float32)
    seq_count = lax.axis_size("fsdp")
    first_row = lax.axis_index("fsdp") * row_count

    def own(values):
        return lax.dynamic_slice_in_dim(values, first_row, row_count, 0)

    query_places = gather_rows(positions).reshape(seq_count, row_count)
    key_places = lax.all_gather(query_places, "ctx", axis=1, tiled=True)
    all_cotangent = gather_rows(cotangent)
    flat_in = gather_rows(inputs).astype(jnp.float32)
    scale_one = rms_scale(flat_in)
    unit_one = flat_in * scale_one
    normed_one = (unit_one * gain_one).astype(jnp.bfloat16)
    total_rows = normed_one.shape[0]
    cosine, sine = rotary_tables(query_places.reshape(-1))
    query_heads = query_weight.shape[0] // HEAD_DIM
    kv_heads = key_weight.shape[0] // HEAD_DIM
    kv_width = kv_heads * HEAD_DIM
    query_low = rotate(
        product_back(normed_one, query_weight).reshape(total_rows, query_heads, HEAD_DIM), cosine, sine
    ).astype(jnp.bfloat16)
    key_low = rotate(
        product_back(normed_one, key_weight).reshape(total_rows, kv_heads, HEAD_DIM), cosine, sine
    ).astype(jnp.bfloat16)
    value_low = product_back(normed_one, value_weight).astype(jnp.bfloat16)
    ctx_size = lax.axis_size("ctx")
    by_head = ctx_size == seq_count * kv_heads

    def to_heads(parts):
        grouped = [
            part.reshape(seq_count, row_count, kv_heads, -1).swapaxes(1, 2) for part in parts
        ]
        return jnp.concatenate(grouped, axis=-1).reshape(ctx_size, row_count, -1)

    def from_heads(values, widths):
        grouped = values.reshape(seq_count, kv_heads, row_count, -1).swapaxes(1, 2)
        parts, start = [], 0
        for width in widths:
            parts.append(grouped[..., start : start + width].reshape(total_rows, kv_heads * width))
            start += width
        return parts

    pair = groups * HEAD_DIM
    flat_query = query_low.reshape(total_rows, query_heads * HEAD_DIM)
    if by_head:
        own_sequence = lax.axis_index("ctx") // kv_heads
        head_places = lax.dynamic_index_in_dim(key_places, own_sequence, 0, keepdims=False)
        length = head_places.shape[0]
        block = row_count // 2
        forward_call = attention_call(length, block)
        packed = exchange(
            to_heads([flat_query, key_low.reshape(total_rows, kv_width), value_low]), 1
        ).reshape(length, -1)
        attended_low = from_heads(
            exchange(forward_call(head_places, packed).reshape(ctx_size, row_count, pair), 2),
            (pair,),
        )[0]
    else:
        def spread(values):
            rows = lax.all_gather(values, "ctx", axis=0, tiled=True)
            rows = rows.reshape(ctx_size, seq_count, row_count, kv_width).swapaxes(0, 1)
            return rows.reshape(seq_count, ctx_size * row_count, kv_width)

        def collect(values):
            rows = values.astype(jnp.bfloat16).swapaxes(1, 2)
            rows = rows.reshape(seq_count, ctx_size, row_count, kv_width).swapaxes(0, 1)
            return lax.psum_scatter(
                rows.reshape(-1, kv_width), "ctx", scatter_dimension=0, tiled=True
            )

        all_keys = spread(key_low.reshape(total_rows, kv_width))
        all_values = spread(value_low)
        total_keys = all_keys.shape[1]
        key_grid = all_keys.reshape(seq_count, total_keys, kv_heads, HEAD_DIM).swapaxes(1, 2)
        value_grid = all_values.reshape(seq_count, total_keys, kv_heads, HEAD_DIM).swapaxes(1, 2)
        query_grouped = query_low.reshape(seq_count, row_count, kv_heads, groups, HEAD_DIM)
        attended, log_total = attend_forward(
            query_grouped, query_places, key_grid, value_grid, key_places
        )
        attended_low = attended.reshape(total_rows, query_heads * HEAD_DIM).astype(jnp.bfloat16)
    hidden_state = inputs.astype(jnp.float32) + scatter_rows(product(attended_low, output_weight))
    scale_two = rms_scale(hidden_state)
    unit_two = hidden_state * scale_two
    normed_two = gather_rows((unit_two * gain_two).astype(jnp.bfloat16))
    gate_values = product_back(normed_two, gate_weight)
    upward = product_back(normed_two, up_weight)
    sigmoid_gate = jax.nn.sigmoid(gate_values)
    activated = gate_values * sigmoid_gate
    mixed_hidden = (activated * upward).astype(jnp.bfloat16)
    grad_out = cotangent.astype(jnp.float32)
    grad_down = product_rows(mixed_hidden, all_cotangent)
    grad_mixed = product_back(all_cotangent, down_weight)
    grad_gate_low = (
        grad_mixed * upward * sigmoid_gate * (1.0 + gate_values * (1.0 - sigmoid_gate))
    ).astype(jnp.bfloat16)
    grad_up_low = (grad_mixed * activated).astype(jnp.bfloat16)
    grad_unit_part = (
        product(grad_gate_low, gate_weight) + product(grad_up_low, up_weight)
    ).astype(jnp.bfloat16)
    if by_head:
        starts = head_places.reshape(-1, block)[:, 0] // block
        slots = jnp.arange(length // block, dtype=jnp.int32)
        found = jnp.where(starts[None, :] == slots[:, None], slots[None, :], 0)
        order = jnp.concatenate([jnp.sum(found, axis=1), starts]).astype(jnp.int32)
        half = HEAD_DIM // 2
        flat_cosine, flat_sine = cosine[:, 0, :], sine[:, 0, :]
        ones = jnp.ones((total_rows, HEAD_DIM), jnp.float32)
        wide_cosine = jnp.concatenate([flat_cosine] * (2 * groups + 2) + [ones], axis=1)
        wide_sine = jnp.concatenate(
            [flat_sine, -flat_sine] * (groups + 1) + [jnp.zeros_like(ones)], axis=1
        )
        lanes = jnp.arange(WIDE, dtype=jnp.int32)
        partner_lane = lanes + jnp.where(lanes % HEAD_DIM < half, half, -half)
        half_swap = jnp.logical_and(
            lanes[:, None] == partner_lane[None, :], lanes[None, :] < PAIR + HEAD_DIM
        ).astype(jnp.bfloat16)
        width = inputs.shape[1]
        weight = jnp.concatenate(
            [
                query_weight.reshape(kv_heads, pair, width),
                key_weight.reshape(kv_heads, HEAD_DIM, width),
                value_weight.reshape(kv_heads, HEAD_DIM, width),
            ],
            axis=1,
        )
        layer_output = (hidden_state + scatter_rows(product(mixed_hidden, down_weight))).astype(
            jnp.bfloat16
        )
        ff_grads = (
            product_rows(grad_gate_low, normed_two).astype(jnp.bfloat16),
            product_rows(grad_up_low, normed_two).astype(jnp.bfloat16),
            grad_down.astype(jnp.bfloat16),
        )
        summed, gain_sums, input_grad = backward(
            order, ff_grads, grad_unit_part, hidden_state, cotangent, inputs,
            jnp.stack([gain_one, gain_two]), output_weight, attended_low, packed, normed_one,
            wide_cosine, wide_sine, half_swap, weight, block, 5,
        )
        parts, start = [], 0
        for grad in (gate_weight, up_weight, down_weight, query_weight, key_weight, value_weight,
                     output_weight):
            parts.append(summed[start : start + grad.shape[0]].astype(jnp.float32))
            start += grad.shape[0]
        return (
            layer_output, input_grad, gain_sums[0], *parts[3:], gain_sums[1], *parts[:3],
        )
    grad_normed_two = scatter_rows(grad_unit_part)
    gain_two_grad = jnp.sum(grad_normed_two * unit_two, axis=0)
    grad_hidden = grad_out + norm_back(scale_two, unit_two, grad_normed_two * gain_two)
    branch_rows = gather_rows(grad_hidden.astype(jnp.bfloat16))
    layer_output = (hidden_state + scatter_rows(product(mixed_hidden, down_weight))).astype(
        jnp.bfloat16
    )
    grad_gate = product_rows(grad_gate_low, normed_two)
    grad_up = product_rows(grad_up_low, normed_two)
    grad_output = product_rows(attended_low, branch_rows)
    grad_attended = product_back(branch_rows, output_weight).astype(jnp.bfloat16)
    grad_attended = grad_attended.reshape(seq_count, row_count, kv_heads, groups, HEAD_DIM)
    grad_query_rot, grad_key_all, grad_value_all = attend_backward(
        query_grouped, query_places, key_grid, value_grid, key_places, log_total, grad_attended
    )
    grad_key_own = collect(grad_key_all).astype(jnp.float32)
    grad_value_low = collect(grad_value_all)
    grad_query_low = (
        rotate_back(grad_query_rot.reshape(total_rows, query_heads, HEAD_DIM), cosine, sine)
        .reshape(total_rows, query_heads * HEAD_DIM)
        .astype(jnp.bfloat16)
    )
    grad_key_low = (
        rotate_back(
            grad_key_own.reshape(total_rows, kv_heads, HEAD_DIM), cosine, sine
        )
        .reshape(total_rows, kv_width)
        .astype(jnp.bfloat16)
    )
    grad_query = product_rows(grad_query_low, normed_one)
    grad_key = product_rows(grad_key_low, normed_one)
    grad_value = product_rows(grad_value_low, normed_one)
    grad_normed_one = scatter_rows(
        product(grad_query_low, query_weight)
        + product(grad_key_low, key_weight)
        + product(grad_value_low, value_weight)
    )
    own_unit = own(unit_one)
    gain_one_grad = jnp.sum(grad_normed_one * own_unit, axis=0)
    input_grad = grad_hidden + norm_back(own(scale_one), own_unit, grad_normed_one * gain_one)

    grads = (grad_query, grad_key, grad_value, grad_output, grad_gate, grad_up, grad_down)
    parts = [lax.psum(grad.astype(jnp.bfloat16), "ctx").astype(jnp.float32) for grad in grads]
    gain_sums = lax.psum(jnp.stack([gain_one_grad, gain_two_grad]), ("fsdp", "ctx"))
    return (
        layer_output,
        input_grad,
        gain_sums[0],
        parts[0],
        parts[1],
        parts[2],
        parts[3],
        gain_sums[1],
        parts[4],
        parts[5],
        parts[6],
    )


def solution(mesh):
    in_specs = (
        P(("fsdp", "ctx"), None),
        P(("fsdp", "ctx")),
        P(("fsdp", "ctx"), None),
        P(),
        P("fsdp", None),
        P("fsdp", None),
        P("fsdp", None),
        P("fsdp", None),
        P(),
        P("fsdp", None),
        P("fsdp", None),
        P("fsdp", None),
    )
    out_specs = (
        P(("fsdp", "ctx"), None),
        P(("fsdp", "ctx"), None),
        P(),
        P("fsdp", None),
        P("fsdp", None),
        P("fsdp", None),
        P("fsdp", None),
        P(),
        P("fsdp", None),
        P("fsdp", None),
        P("fsdp", None),
    )
    return jax.shard_map(
        per_device, mesh=mesh, in_specs=in_specs, out_specs=out_specs, check_vma=False
    )
```

```python
import functools
import math

import jax
import jax.numpy as jnp
from jax import lax
from jax.experimental import pallas as pl
from jax.experimental.pallas import tpu as pltpu
from jax.sharding import PartitionSpec as P

HEADS = 16
KV_HEADS = 8
HEAD_DIM = 96


EPSILON = 1e-05
ROPE_BASE = 100000.0


def product(left, right):
    return jnp.dot(left, right, preferred_element_type=jnp.float32)


def product_back(left, right):
    return lax.dot_general(
        left, right, (((1,), (1,)), ((), ())), preferred_element_type=jnp.float32
    )


def product_rows(left, right):
    return lax.dot_general(
        left, right, (((0,), (0,)), ((), ())), preferred_element_type=jnp.float32
    )


def rms_scale(values):
    return lax.rsqrt(jnp.mean(values * values, axis=-1, keepdims=True) + EPSILON)


def norm_back(scale_rows, unit_rows, grad_unit):
    return scale_rows * (
        grad_unit - unit_rows * jnp.mean(grad_unit * unit_rows, axis=-1, keepdims=True)
    )


def rotary_tables(places):
    half_width = HEAD_DIM // 2
    frequencies = ROPE_BASE ** (-(jnp.arange(half_width, dtype=jnp.float32) * 2.0 / HEAD_DIM))
    angles = places.astype(jnp.float32)[:, None] * frequencies[None, :]
    return (jnp.cos(angles)[:, None, :], jnp.sin(angles)[:, None, :])


def rotate(values, cosine, sine):
    half_width = values.shape[-1] // 2
    lower_half = values[..., :half_width]
    upper_half = values[..., half_width:]
    return jnp.concatenate(
        [lower_half * cosine - upper_half * sine, upper_half * cosine + lower_half * sine], axis=-1
    )


def rotate_back(grads, cosine, sine):
    half_width = grads.shape[-1] // 2
    lower_half = grads[..., :half_width]
    upper_half = grads[..., half_width:]
    return jnp.concatenate(
        [lower_half * cosine + upper_half * sine, upper_half * cosine - lower_half * sine], axis=-1
    )


def block_total_of(total_keys):
    return max(1, total_keys // 512)


def masked_scores(query_grouped, query_places, key_rows, key_places, start, width):
    key_part = lax.dynamic_slice_in_dim(key_rows, start, width, 2)
    place_part = lax.dynamic_slice_in_dim(key_places, start, width, 1)
    scores = jnp.einsum(
        "sqhgd,shkd->shgqk", query_grouped, key_part, preferred_element_type=jnp.float32
    )
    scores = scores * (1.0 / math.sqrt(HEAD_DIM))
    allowed = place_part[:, None, None, None, :] <= query_places[:, None, None, :, None]
    return jnp.where(allowed, scores, -1000000000.0)


def attend_forward(query_grouped, query_places, key_rows, value_rows, key_places):
    seq_count, row_count, head_groups, group_size = query_grouped.shape[:4]
    total_keys = key_rows.shape[2]
    block_total = block_total_of(total_keys)
    width = total_keys // block_total
    stat_shape = (seq_count, head_groups, group_size, row_count)

    def peak_step(index, carry):
        running_top, running_sum = carry
        scores = masked_scores(
            query_grouped, query_places, key_rows, key_places, index * width, width
        )
        new_top = jnp.maximum(running_top, jnp.max(scores, axis=-1))
        running_sum = running_sum * jnp.exp(running_top - new_top) + jnp.sum(
            jnp.exp(scores - new_top[..., None]), axis=-1
        )
        return (new_top, running_sum)

    running_top, running_sum = lax.fori_loop(
        0,
        block_total,
        peak_step,
        (jnp.full(stat_shape, -1e30, jnp.float32), jnp.zeros(stat_shape, jnp.float32)),
    )
    log_total = running_top + jnp.log(running_sum)

    def value_step(index, gathered):
        scores = masked_scores(
            query_grouped, query_places, key_rows, key_places, index * width, width
        )
        soft_low = jnp.exp(scores - log_total[..., None]).astype(jnp.bfloat16)
        value_part = lax.dynamic_slice_in_dim(value_rows, index * width, width, 2)
        return gathered + jnp.einsum(
            "shgqk,shkd->sqhgd", soft_low, value_part, preferred_element_type=jnp.float32
        )

    attended = lax.fori_loop(
        0, block_total, value_step, jnp.zeros(query_grouped.shape, jnp.float32)
    )
    return (attended, log_total)


def attend_backward(
    query_grouped, query_places, key_rows, value_rows, key_places, log_total, grad_attended
):
    total_keys = key_rows.shape[2]
    block_total = block_total_of(total_keys)
    width = total_keys // block_total
    score_scale = 1.0 / math.sqrt(HEAD_DIM)

    def soft_and_grad(index):
        scores = masked_scores(
            query_grouped, query_places, key_rows, key_places, index * width, width
        )
        soft_values = jnp.exp(scores - log_total[..., None])
        value_part = lax.dynamic_slice_in_dim(value_rows, index * width, width, 2)
        grad_soft = jnp.einsum(
            "sqhgd,shkd->shgqk", grad_attended, value_part, preferred_element_type=jnp.float32
        )
        return (soft_values, grad_soft)

    def delta_step(index, row_delta):
        soft_values, grad_soft = soft_and_grad(index)
        return row_delta + jnp.sum(soft_values * grad_soft, axis=-1)

    row_delta = lax.fori_loop(0, block_total, delta_step, jnp.zeros(log_total.shape, jnp.float32))

    def grad_step(index, carry):
        grad_query, grad_keys, grad_values = carry
        soft_values, grad_soft = soft_and_grad(index)
        grad_scores = (soft_values * (grad_soft - row_delta[..., None])).astype(jnp.bfloat16)
        key_part = lax.dynamic_slice_in_dim(key_rows, index * width, width, 2)
        grad_query = (
            grad_query
            + jnp.einsum(
                "shgqk,shkd->sqhgd", grad_scores, key_part, preferred_element_type=jnp.float32
            )
            * score_scale
        )
        key_term = (
            jnp.einsum(
                "shgqk,sqhgd->shkd", grad_scores, query_grouped, preferred_element_type=jnp.float32
            )
            * score_scale
        )
        value_term = jnp.einsum(
            "shgqk,sqhgd->shkd",
            soft_values.astype(jnp.bfloat16),
            grad_attended,
            preferred_element_type=jnp.float32,
        )
        grad_keys = lax.dynamic_update_slice_in_dim(grad_keys, key_term, index * width, 2)
        grad_values = lax.dynamic_update_slice_in_dim(grad_values, value_term, index * width, 2)
        return (grad_query, grad_keys, grad_values)

    initial = (
        jnp.zeros(query_grouped.shape, jnp.float32),
        jnp.zeros(key_rows.shape, jnp.float32),
        jnp.zeros(value_rows.shape, jnp.float32),
    )
    return lax.fori_loop(0, block_total, grad_step, initial)


def vmem():
    return pl.BlockSpec(memory_space=pltpu.VMEM)


def peer(ctx_index):
    return dict(device_id={"ctx": ctx_index}, device_id_type=pl.DeviceIdType.MESH)


SPINE_ROWS = 48
LINE_ROWS = 64
ROUND_ROWS = 2 * SPINE_ROWS + LINE_ROWS
LEAD = 2
RING = 12
TILE = 128
PAIR = (HEADS // KV_HEADS) * HEAD_DIM
WIDE = PAIR + 2 * HEAD_DIM


def near_fsdp(index):
    return dict(device_id={"fsdp": index}, device_id_type=pl.DeviceIdType.MESH)


def rows_at(start, count):
    return pl.ds(pl.multiple_of(start, 16), count)


class Place:
    def __init__(self):
        self.ctx = lax.axis_index("ctx")
        self.row = lax.axis_index("fsdp")
        self.chip, self.core = lax.div(self.row, 2), lax.rem(self.row, 2)
        self.partner = 2 * self.chip + 1 - self.core
        self.across = 2 * (1 - self.chip) + self.core
        self.corner = 2 * (1 - self.chip) + 1 - self.core

    def greet(self):
        barrier = pltpu.get_barrier_semaphore()
        for step in range(1, 4):
            pl.semaphore_signal(barrier, inc=1, **near_fsdp(lax.rem(self.row + step, 4)))
        for step in range(1, 8):
            pl.semaphore_signal(barrier, inc=1, **peer(lax.rem(self.ctx + step, 8)))
        pl.semaphore_wait(barrier, 10)


class Fold:
    def __init__(self, place, part, near, send, far, send_sem, recv_sem):
        self.place, self.part, self.near, self.send, self.far = place, part, near, send, far
        self.send_sem, self.recv_sem = send_sem, recv_sem

    def partner_copy(self, chip):
        block = 2 * chip + 1 - self.place.core
        return pltpu.make_async_remote_copy(
            src_ref=self.part.at[rows_at(block * TILE, TILE)],
            dst_ref=self.near.at[chip],
            send_sem=self.send_sem.at[chip],
            recv_sem=self.recv_sem.at[chip],
            **near_fsdp(self.place.partner),
        )

    def across_copy(self):
        return pltpu.make_async_remote_copy(
            src_ref=self.send,
            dst_ref=self.far,
            send_sem=self.send_sem.at[2],
            recv_sem=self.recv_sem.at[2],
            **near_fsdp(self.place.across),
        )

    def start(self):
        self.partner_copy(1 - self.place.chip).start()
        self.partner_copy(self.place.chip).start()

    def relay(self):
        there = 1 - self.place.chip
        self.partner_copy(there).wait_recv()
        base = self.place.across * TILE

        @pl.loop(0, TILE // 32)
        def _(piece):
            mine = self.part[rows_at(base + piece * 32, 32), :].astype(jnp.float32)
            span = rows_at(piece * 32, 32)
            self.send[span, :] = (
                mine + self.near[there, span, :].astype(jnp.float32)
            ).astype(jnp.bfloat16)

        self.across_copy().start()

    def arrive(self):
        self.partner_copy(self.place.chip).wait_recv()
        copy = self.across_copy()
        copy.wait_recv()
        copy.wait_send()
        self.partner_copy(0).wait_send()
        self.partner_copy(1).wait_send()

    def rows(self, start, count):
        mine = self.part[rows_at(self.place.row * TILE + start, count), :].astype(jnp.float32)
        span = rows_at(start, count)
        near = self.near[self.place.chip, span, :].astype(jnp.float32)
        return mine + near + self.far[span, :].astype(jnp.float32)


class Gather:
    def __init__(self, place, full, send_sem, recv_sem, count=TILE):
        self.place, self.full, self.send_sem, self.recv_sem = place, full, send_sem, recv_sem
        self.count = count

    def copy(self, block, target, key):
        span = pl.ds(pl.multiple_of(block * self.count, self.count), self.count)
        return pltpu.make_async_remote_copy(
            src_ref=self.full.at[span],
            dst_ref=self.full.at[span],
            send_sem=self.send_sem.at[key],
            recv_sem=self.recv_sem.at[key],
            **near_fsdp(target),
        )

    def start(self):
        self.copy(self.place.row, self.place.across, 1).start()
        self.copy(self.place.row, self.place.partner, 0).start()

    def relay(self):
        self.copy(self.place.across, self.place.across, 1).wait_recv()
        self.copy(self.place.across, self.place.partner, 2).start()

    def first(self):
        self.copy(self.place.partner, self.place.partner, 0).wait_recv()

    def arrive(self):
        self.copy(self.place.corner, self.place.partner, 2).wait_recv()
        self.copy(self.place.row, self.place.across, 1).wait_send()
        self.copy(self.place.row, self.place.partner, 0).wait_send()
        self.copy(self.place.across, self.place.partner, 2).wait_send()


class Swap:
    def __init__(self, place, source, target, send_sem, recv_sem, count, share=1):
        self.place, self.source, self.target = place, source, target
        self.send_sem, self.recv_sem, self.count, self.share = send_sem, recv_sem, count, share

    def span(self, index):
        return pl.ds(pl.multiple_of(index * self.count, self.count), self.count)

    def copy(self, other, sender):
        return pltpu.make_async_remote_copy(
            src_ref=self.source.at[self.span(lax.div(other, self.share))],
            dst_ref=self.target.at[self.span(sender)],
            send_sem=self.send_sem.at[other],
            recv_sem=self.recv_sem.at[sender],
            **peer(other),
        )

    def start(self, other):
        me = self.place.ctx

        @pl.when(other != me)
        def _():
            self.copy(other, me).start()

        @pl.when(other == me)
        def _():
            self.target[self.span(me)] = self.source[self.span(lax.div(me, self.share))]

    def start_all(self):
        for step in range(1, 9):
            self.start(lax.rem(self.place.ctx + step, 8))

    def arrive(self):
        for step in range(1, 8):
            other = lax.rem(self.place.ctx + step, 8)
            self.copy(other, other).wait()


class Spread:
    def __init__(self, slots, index, count, device, send_sem, recv_sem):
        self.slots, self.index, self.count, self.device = slots, index, count, device
        self.send_sem, self.recv_sem = send_sem, recv_sem

    def copy(self, step):
        return pltpu.make_async_remote_copy(
            src_ref=self.slots.at[self.index],
            dst_ref=self.slots.at[self.index],
            send_sem=self.send_sem.at[step],
            recv_sem=self.recv_sem.at[step],
            **self.device(lax.rem(self.index + step, self.count)),
        )

    def start(self):
        for step in range(1, self.count):
            self.copy(step).start()

    def total(self):
        for step in range(1, self.count):
            self.copy(step).wait()
        result = self.slots[0]
        for step in range(1, self.count):
            result += self.slots[step]
        return result


class Tree:
    def __init__(self, place, own, out_ref, index, line, box, sems, leaf_back):
        me = place.ctx
        depth, side = lax.div(me, 2), lax.rem(me, 2)
        other_side = me + 1 - 2 * side
        self.own, self.out, self.box, self.index, self.line = own, out_ref, box, index, line
        self.up, self.got, self.down, self.back = sems
        self.leaf_back = leaf_back
        if line:
            center = lax.rem(index, 4)
            count = LINE_ROWS
            start = index * ROUND_ROWS + 2 * SPINE_ROWS
            root_side = lax.rem(index, 2)
            on_cross = depth == center
            self.root = jnp.logical_and(on_cross, side == root_side)
            has_side = self.root
            to_side = jnp.logical_and(on_cross, side != root_side)
            reach = jnp.maximum(center, 3 - center)
            away = jnp.abs(depth - center)
            crossed = jnp.where(side == root_side, 0, 1)
            self.rise_age = reach - away + jnp.where(self.root, 1, 0)
            self.fall_age = reach + 1 + away + crossed
        else:
            center = 1 + side
            count = SPINE_ROWS
            start = index * ROUND_ROWS + side * SPINE_ROWS
            self.root = depth == center
            has_side = None
        self.count = count
        self.start = start
        self.slot = lax.rem(index, RING)
        self.rows = rows_at(start, count)
        self.children = (
            (jnp.logical_and(depth > 0, depth <= center), me - 2, 0),
            (jnp.logical_and(depth < 3, depth >= center), me + 2, 1),
            (has_side, other_side, 2),
        )
        parent = jnp.where(depth < center, me + 2, me - 2)
        slot = jnp.where(depth < center, 0, 1)
        if line:
            parent = jnp.where(to_side, other_side, parent)
            slot = jnp.where(to_side, 2, slot)
        self.parent = jnp.where(self.root, other_side, parent)
        self.parent_slot = jnp.where(self.root, 2, slot)

    def boxed(self, slot):
        return self.box.at[slot, rows_at(self.slot * self.count, self.count)]

    def up_copy(self, target, slot):
        return pltpu.make_async_remote_copy(
            src_ref=self.own.at[self.rows],
            dst_ref=self.boxed(slot),
            send_sem=self.up.at[self.slot],
            recv_sem=self.got.at[slot, self.slot],
            **peer(target),
        )

    def down_copy(self, child, slot, source):
        back = self.back if slot < 2 or self.line else self.leaf_back
        return pltpu.make_async_remote_copy(
            src_ref=source.at[self.rows],
            dst_ref=self.out.at[self.rows],
            send_sem=self.down.at[slot, self.slot],
            recv_sem=back.at[self.slot],
            **peer(child),
        )

    def each_child(self, action):
        for present, child, slot in self.children:
            if present is None:
                action(child, slot)
            else:
                pl.when(present)(functools.partial(action, child, slot))

    def keep(self):
        return pltpu.make_async_copy(
            self.own.at[self.rows], self.out.at[self.rows], self.up.at[self.slot]
        )

    def rise(self):
        self.each_child(lambda child, slot: self.up_copy(child, slot).wait_recv())
        base = self.slot * self.count
        for piece in range(0, self.count, 16):
            span = rows_at(self.start + piece, 16)
            total = self.own[span, :].astype(jnp.float32)
            for present, _, slot in self.children:
                part = self.box[slot, rows_at(base + piece, 16), :].astype(jnp.float32)
                total += part if present is None else jnp.where(present, part, 0.0)
            self.own[span, :] = total.astype(jnp.bfloat16)

        @pl.when(jnp.logical_not(self.root))
        def _():
            self.up_copy(self.parent, self.parent_slot).start()

        @pl.when(self.root)
        def _():
            self.keep().start()
            self.each_child(lambda child, slot: self.down_copy(child, slot, self.own).start())

    def fall(self):
        @pl.when(jnp.logical_not(self.root))
        def _():
            self.down_copy(self.parent, 0, self.out).wait_recv()
            self.each_child(lambda child, slot: self.down_copy(child, slot, self.out).start())

    def finish(self):
        @pl.when(jnp.logical_not(self.root))
        def _():
            self.up_copy(self.parent, self.parent_slot).wait_send()

        @pl.when(self.root)
        def _():
            self.keep().wait()

        self.each_child(lambda child, slot: self.down_copy(child, slot, self.out).wait_send())


def softmax_parts(query_rows, key_rows, first_row):
    scores = product_back(query_rows, key_rows) * (1.0 / math.sqrt(HEAD_DIM))
    rows = lax.broadcasted_iota(jnp.int32, scores.shape, 0) + first_row
    columns = lax.broadcasted_iota(jnp.int32, scores.shape, 1)
    scores = jnp.where(columns <= rows, scores, -1e30)
    spread = jnp.exp(scores - jnp.max(scores, axis=-1, keepdims=True))
    return spread * (1.0 / jnp.sum(spread, axis=-1, keepdims=True))


def sort_blocks(slot_ref, source, targets):
    block_total, block, _ = source.shape
    for index in range(block_total):
        rows = source[slot_ref[index]]
        start = 0
        for target in targets:
            width = target.shape[-1]
            target[index * block : (index + 1) * block, :] = rows[:, start : start + width]
            start += width


def norm_back_rows(values, grad_unit):
    scale = rms_scale(values)
    unit = values * scale
    return unit, lambda grad: norm_back(scale, unit, grad)


def backward_kernel(
    rounds,
    block,
    order_ref,
    gate_ref,
    up_ref,
    down_ref,
    part_ref,
    hidden_ref,
    cotangent_ref,
    input_ref,
    gain_ref,
    output_weight_ref,
    attended_ref,
    packed_ref,
    normed_ref,
    cosine_ref,
    sine_ref,
    half_swap_ref,
    weight_ref,
    out_ref,
    gain_out_ref,
    input_grad_ref,
    own,
    spine_in,
    line_in,
    part,
    hidden,
    cotangent,
    inputs,
    output_weight,
    attended,
    packed,
    normed,
    cosine,
    sine,
    half_swap,
    weight,
    near,
    send,
    far,
    branch,
    grad_hidden,
    gain_part,
    heads_out,
    heads_in,
    q0,
    q1,
    k,
    v,
    g0,
    g1,
    result,
    dk,
    dv,
    packed_out,
    packed_in,
    turned,
    gain_near,
    gain_far,
    fetch_sem,
    spine_up,
    spine_got,
    spine_down,
    spine_back,
    leaf_up,
    leaf_back,
    line_up,
    line_got,
    line_down,
    line_back,
    fold_send,
    fold_recv,
    gather_send,
    gather_recv,
    swap_send,
    swap_recv,
    near_send,
    near_recv,
    far_send,
    far_recv,
):
    place = Place()
    me = place.ctx
    depth, side = lax.div(me, 2), lax.rem(me, 2)
    other_side = me + 1 - 2 * side
    hidden_units = gate_ref.shape[0]
    base = 3 * hidden_units
    spare = rounds * ROUND_ROWS - base - 3 * WIDE
    length = q0.shape[0]
    halves = TILE // block
    tile = min(256, length)
    tiles = length // tile
    scale = 1.0 / math.sqrt(HEAD_DIM)

    fetches = {}
    for key, (source, target) in enumerate(
        (
            (part_ref, part),
            (gate_ref, own.at[pl.ds(0, hidden_units)]),
            (up_ref, own.at[pl.ds(hidden_units, hidden_units)]),
            (hidden_ref, hidden),
            (cotangent_ref, cotangent),
            (output_weight_ref, output_weight),
            (packed_ref, packed),
            (attended_ref, attended),
            (down_ref, own.at[pl.ds(2 * hidden_units, hidden_units)]),
            (normed_ref, normed),
            (cosine_ref, cosine),
            (sine_ref, sine),
            (half_swap_ref, half_swap),
            (weight_ref, weight),
            (input_ref, inputs),
        )
    ):
        fetches[id(source)] = pltpu.make_async_copy(source, target, fetch_sem.at[key])

    def fetch(*sources):
        for source in sources:
            fetches[id(source)].wait()

    for copy in fetches.values():
        copy.start()
    if spare:
        own[base + 3 * WIDE :, :] = jnp.zeros((spare, own.shape[1]), own.dtype)
    place.greet()
    fetch(part_ref)
    fold_two = Fold(place, part, near.at[0], send.at[0], far.at[0], fold_send.at[0], fold_recv.at[0])
    fold_one = Fold(place, part, near.at[1], send.at[1], far.at[1], fold_send.at[1], fold_recv.at[1])
    gather = Gather(place, branch, gather_send, gather_recv)
    swap_heads = Swap(place, heads_out, heads_in, swap_send.at[0], swap_recv.at[0], halves)
    swap_packed = Swap(place, packed_out, packed_in, swap_send.at[1], swap_recv.at[1], halves)
    spread_near = Spread(gain_near, place.row, 4, near_fsdp, near_send, near_recv)
    spread_far = Spread(gain_far, me, 8, peer, far_send, far_recv)
    fold_two.start()
    fetch(gate_ref, up_ref, down_ref)

    spine_sems = (spine_up, spine_got, spine_down, spine_back)
    line_sems = (line_up, line_got, line_down, line_back)

    def spine(index):
        return Tree(place, own, out_ref, index, False, spine_in, spine_sems, leaf_back)

    def line(index):
        return Tree(place, own, out_ref, index, True, line_in, line_sems, None)

    def leaf_rows(index):
        return rows_at(index * ROUND_ROWS + (1 - side) * SPINE_ROWS, SPINE_ROWS)

    def leaf_copy(index):
        slot = lax.rem(index, RING)
        return pltpu.make_async_remote_copy(
            src_ref=own.at[leaf_rows(index)],
            dst_ref=spine_in.at[2, rows_at(slot * SPINE_ROWS, SPINE_ROWS)],
            send_sem=leaf_up.at[slot],
            recv_sem=spine_got.at[2, slot],
            **peer(other_side),
        )

    def leaf_result(index):
        slot = lax.rem(index, RING)
        return pltpu.make_async_remote_copy(
            src_ref=own.at[leaf_rows(index)],
            dst_ref=out_ref.at[leaf_rows(index)],
            send_sem=leaf_up.at[slot],
            recv_sem=leaf_back.at[slot],
            **peer(other_side),
        )

    def stage_norm_two():
        fetch(hidden_ref, cotangent_ref)
        fold_two.arrive()
        gain_part[...] = jnp.zeros_like(gain_part)

        @pl.loop(0, TILE // 16)
        def _(piece):
            span = rows_at(piece * 16, 16)
            grad = fold_two.rows(piece * 16, 16)
            unit, back = norm_back_rows(hidden[span, :], None)
            gain_part[1] += (grad * unit).reshape(2, 8, -1).sum(axis=0)
            total = cotangent[span, :].astype(jnp.float32) + back(grad * gain_ref[1:2, :])
            grad_hidden[span, :] = total
            branch[rows_at(place.row * TILE + piece * 16, 16), :] = total.astype(jnp.bfloat16)

        gather.start()

    def stage_heads():
        fetch(output_weight_ref)
        gather.first()
        gather.arrive()

        @pl.loop(0, 4)
        def _(sequence):
            rows = branch[rows_at(sequence * TILE, TILE), :]
            grads = product_back(rows, output_weight[...]).astype(jnp.bfloat16)
            for head in range(2):
                heads_out[pl.ds((2 * sequence + head) * halves, halves)] = grads[
                    :, head * PAIR : (head + 1) * PAIR
                ].reshape(halves, block, PAIR)

        swap_heads.start_all()

    def stage_sort():
        fetch(packed_ref)
        sort_blocks(order_ref, packed, (q0, q1, k, v))

    def stage_output_grad():
        fetch(attended_ref)
        for head in range(2):
            rows = [
                attended[(2 * index + head) * halves : (2 * index + head + 1) * halves]
                for index in range(4)
            ]
            rows = jnp.concatenate(rows, axis=0).reshape(4 * TILE, PAIR)
            first_row = base + 2 * WIDE + head * PAIR
            for first in range(0, own.shape[1], 512):
                columns = slice(first, first + 512)
                own[first_row : first_row + PAIR, columns] = product_rows(
                    rows, branch[:, columns]
                ).astype(jnp.bfloat16)

    def stage_sort_grads():
        swap_heads.arrive()
        sort_blocks(order_ref, heads_in, (g0, g1))
        dk[...] = jnp.zeros_like(dk)
        dv[...] = jnp.zeros_like(dv)

    def stage_attention(index):
        first, top = index * tile, (index + 1) * tile
        parts = []
        for q, g in ((q0, g0), (q1, g1)):
            query_rows = q[first:top, :]
            grad_rows = g[first:top, :]
            soft = softmax_parts(query_rows, k[:top, :], first)
            grad_soft = product_back(grad_rows, v[:top, :])
            delta = jnp.sum(soft * grad_soft, axis=-1, keepdims=True)
            grad_scores = (soft * (grad_soft - delta)).astype(jnp.bfloat16)
            parts.append(product(grad_scores, k[:top, :]) * scale)
            key_term = product_rows(grad_scores, query_rows) * scale
            value_term = product_rows(soft.astype(jnp.bfloat16), grad_rows)
            dk[: top // block] += key_term.reshape(-1, block, HEAD_DIM)
            dv[: top // block] += value_term.reshape(-1, block, HEAD_DIM)
        result[first // block : top // block] = jnp.concatenate(parts, axis=-1).reshape(
            -1, block, PAIR
        )

    def stage_unsort():
        for slot in range(length // block):
            spot = order_ref[length // block + slot]
            packed_out[slot] = jnp.concatenate(
                [result[spot], dk[spot], dv[spot]], axis=-1
            ).astype(jnp.bfloat16)
        swap_packed.start_all()

    def stage_turn():
        fetch(cosine_ref, sine_ref, half_swap_ref, weight_ref)
        swap_packed.arrive()

        @pl.loop(0, 4)
        def _(sequence):
            span = rows_at(sequence * TILE, TILE)
            total = None
            for head in range(2):
                grads = packed_in[pl.ds((2 * sequence + head) * halves, halves)]
                grads = grads.reshape(TILE, WIDE)
                swapped = product(grads, half_swap[...])
                low = (
                    grads.astype(jnp.float32) * cosine[span, :] - swapped * sine[span, :]
                ).astype(jnp.bfloat16)
                turned[head, span, :] = low
                term = product(low, weight[head])
                total = term if total is None else total + term
            part[span, :] = total.astype(jnp.bfloat16)

        fold_one.start()

    def stage_projection_grads(head):
        if head == 0:
            fetch(normed_ref)
        query_base = base + head * PAIR
        key_base = base + WIDE + head * HEAD_DIM
        value_base = key_base + 2 * HEAD_DIM
        for first in range(0, own.shape[1], 512):
            columns = slice(first, first + 512)
            grads = product_rows(turned[head], normed[:, columns]).astype(jnp.bfloat16)
            own[query_base : query_base + PAIR, columns] = grads[:PAIR]
            own[key_base : key_base + HEAD_DIM, columns] = grads[PAIR : PAIR + HEAD_DIM]
            own[value_base : value_base + HEAD_DIM, columns] = grads[PAIR + HEAD_DIM :]

    def stage_norm_one():
        fetch(input_ref)
        fold_one.arrive()

        @pl.loop(0, TILE // 16)
        def _(piece):
            span = rows_at(piece * 16, 16)
            grad = fold_one.rows(piece * 16, 16)
            unit, back = norm_back_rows(inputs[span, :].astype(jnp.float32), None)
            gain_part[0] += (grad * unit).reshape(2, 8, -1).sum(axis=0)
            input_grad_ref[span, :] = grad_hidden[span, :] + back(grad * gain_ref[0:1, :])

        gain_near[place.row] = jnp.sum(gain_part[...], axis=1)
        spread_near.start()

    def stage_gain():
        gain_far[me] = spread_near.total()
        spread_far.start()

    stages = [
        (0, fold_two.relay),
        (0, stage_sort),
        (2, stage_norm_two),
        (3, gather.relay),
        (4, stage_heads),
        (5, stage_output_grad),
        (6, stage_sort_grads),
    ]
    stages += [(6 + index, functools.partial(stage_attention, index)) for index in range(tiles)]
    now = 6 + tiles - 1
    stages += [
        (now, stage_unsort),
        (now + 2, stage_turn),
        (now + 3, fold_one.relay),
        (now + 3, functools.partial(stage_projection_grads, 0)),
        (now + 4, functools.partial(stage_projection_grads, 1)),
        (now + 5, stage_norm_one),
        (now + 6, stage_gain),
    ]
    needed = base // ROUND_ROWS - LEAD
    assert now + 4 < needed

    for index in range(LEAD):
        leaf_copy(index).start()

    def valid(index):
        return jnp.logical_and(index >= 0, index < rounds)

    @pl.loop(0, rounds + RING)
    def _(now):
        far_side = jnp.abs(depth - 2 + side)
        off_center = jnp.abs(depth - 1 - side)
        done = now - RING + 1
        for tree in (spine(done), line(done)):
            pl.when(valid(done))(tree.finish)

        @pl.when(now + LEAD < rounds)
        def _():
            leaf_copy(now + LEAD).start()

        rising = spine(now - 3 + off_center)
        pl.when(valid(rising.index))(rising.rise)

        @pl.loop(0, 5)
        def _(age):
            tree = line(now - age)
            pl.when(jnp.logical_and(valid(tree.index), tree.rise_age == age))(tree.rise)

        falling = spine(now - 3 - off_center)
        pl.when(valid(falling.index))(falling.fall)

        @pl.loop(4, 9)
        def _(age):
            tree = line(now - age)
            pl.when(jnp.logical_and(valid(tree.index), tree.fall_age == age))(tree.fall)

        leaf_fall = now - 4 - far_side

        @pl.when(valid(leaf_fall))
        def _():
            leaf_result(leaf_fall).wait_recv()
            leaf_copy(leaf_fall).wait_send()

        for when, stage in stages:
            pl.when(now == when)(stage)

    gain_out_ref[...] = spread_far.total()


def backward(order, grads, part, hidden, cotangent, inputs, gains, output_weight, attended,
             packed, normed, cosine, sine, half_swap, weight, block, key):
    width = hidden.shape[1]
    rows = 3 * grads[0].shape[0] + 3 * WIDE
    rounds = -(-rows // ROUND_ROWS)
    length = packed.shape[0] * block
    dma = pltpu.SemaphoreType.DMA
    low, full = jnp.bfloat16, jnp.float32
    any_spec = pl.BlockSpec(memory_space=pl.ANY)
    operands = (
        order, *grads, part, hidden, cotangent, inputs, gains, output_weight, attended,
        packed, normed, cosine, sine, half_swap, weight,
    )

    def like(array):
        return pltpu.VMEM(array.shape, array.dtype)

    return pl.pallas_call(
        functools.partial(backward_kernel, rounds, block),
        out_shape=(
            jax.ShapeDtypeStruct((rounds * ROUND_ROWS, width), low),
            jax.ShapeDtypeStruct((2, width), full),
            jax.ShapeDtypeStruct((TILE, width), full),
        ),
        in_specs=[pl.BlockSpec(memory_space=pltpu.SMEM)]
        + [any_spec] * 7
        + [vmem()]
        + [any_spec] * 8,
        out_specs=(any_spec, vmem(), vmem()),
        scratch_shapes=[
            pltpu.VMEM((rounds * ROUND_ROWS, width), low),
            pltpu.VMEM((3, RING * SPINE_ROWS, width), low),
            pltpu.VMEM((3, RING * LINE_ROWS, width), low),
            like(part), like(hidden), like(cotangent), like(inputs), like(output_weight),
            like(attended), like(packed), like(normed), like(cosine), like(sine),
            like(half_swap), like(weight),
            pltpu.VMEM((2, 2, TILE, width), low),
            pltpu.VMEM((2, TILE, width), low),
            pltpu.VMEM((2, TILE, width), low),
            pltpu.VMEM((4 * TILE, width), low),
            pltpu.VMEM((TILE, width), full),
            pltpu.VMEM((2, 8, width), full),
            pltpu.VMEM((length // block, block, PAIR), low),
            pltpu.VMEM((length // block, block, PAIR), low),
        ]
        + [pltpu.VMEM((length, HEAD_DIM), low)] * 6
        + [pltpu.VMEM((length // block, block, PAIR), full)]
        + [pltpu.VMEM((length // block, block, HEAD_DIM), full)] * 2
        + [
            pltpu.VMEM((length // block, block, WIDE), low),
            pltpu.VMEM((length // block, block, WIDE), low),
            pltpu.VMEM((2, 4 * TILE, WIDE), low),
            pltpu.VMEM((4, 2, width), full),
            pltpu.VMEM((8, 2, width), full),
            dma((15,)),
            dma((RING,)), dma((3, RING)), dma((3, RING)), dma((RING,)),
            dma((RING,)), dma((RING,)),
            dma((RING,)), dma((3, RING)), dma((3, RING)), dma((RING,)),
            dma((2, 3)), dma((2, 3)),
            dma((3,)), dma((3,)),
            dma((2, 8)), dma((2, 8)),
            dma((4,)), dma((4,)), dma((8,)), dma((8,)),
        ],
        compiler_params=pltpu.CompilerParams(
            collective_id=key, has_side_effects=True, vmem_limit_bytes=63 * 2**20
        ),
        name="backward",
    )(*operands)


def forward_kernel(
    block,
    place_ref,
    table_ref,
    gain_ref,
    input_ref,
    cotangent_ref,
    query_weight_ref,
    key_weight_ref,
    value_weight_ref,
    output_weight_ref,
    gate_weight_ref,
    up_weight_ref,
    down_weight_ref,
    place_out,
    part_out,
    hidden_out,
    attended_out,
    packed_out,
    normed_one_out,
    cosine_out,
    sine_out,
    cotangent_out,
    normed_two_out,
    mixed_out,
    grad_gate_out,
    grad_up_out,
    places,
    tables,
    inputs,
    cotangents,
    normed_one,
    normed_two,
    cosine,
    sine,
    weight,
    output_weight,
    gate_weight,
    up_weight,
    down_weight,
    packed_from,
    packed,
    q0,
    q1,
    k,
    v,
    result,
    heads_from,
    heads,
    part,
    near,
    send,
    far,
    hidden,
    mixed,
    grad_gate,
    grad_up,
    fetch_sem,
    store_sem,
    gather_send,
    gather_recv,
    swap_send,
    swap_recv,
    fold_send,
    fold_recv,
):
    place = Place()
    length, width = q0.shape[0], inputs.shape[1]
    halves = TILE // block
    half = HEAD_DIM // 2
    pair_rows = 2 * TILE
    fetches, stores = {}, []

    def fetch_all(key, *copies):
        base = sum(len(group) for group in fetches.values())
        fetches[key] = [
            pltpu.make_async_copy(part_of, target, fetch_sem.at[base + index])
            for index, (part_of, target) in enumerate(copies)
        ]
        for copy in fetches[key]:
            copy.start()

    def fetch(*keys):
        for key in keys:
            for copy in fetches[key]:
                copy.wait()

    def store(source, target):
        copy = pltpu.make_async_copy(source, target, store_sem.at[len(stores)])
        copy.start()
        stores.append(copy)

    own_rows = rows_at(place.row * TILE, TILE)
    fetch_all("inputs", (input_ref, inputs.at[own_rows]))
    fetch_all("cotangent", (cotangent_ref, cotangents.at[own_rows]))
    copies = []
    for head in range(2):
        query_base, key_base = head * PAIR, head * HEAD_DIM
        target = weight.at[head]
        heads_of = [(query_weight_ref, query_base), (query_weight_ref, query_base + HEAD_DIM)]
        heads_of += [(key_weight_ref, key_base), (value_weight_ref, key_base)]
        for index, (source, first) in enumerate(heads_of):
            copies.append(
                (source.at[pl.ds(first, HEAD_DIM)], target.at[pl.ds(index * HEAD_DIM, HEAD_DIM)])
            )
            for side in range(2):
                copies.append(
                    (
                        source.at[pl.ds(first + (1 - side) * half, half)],
                        target.at[pl.ds(WIDE + index * HEAD_DIM + side * half, half)],
                    )
                )
    fetch_all("weight", *copies)
    fetch_all("output", (output_weight_ref, output_weight))
    fetch_all("gate", (gate_weight_ref, gate_weight))
    fetch_all("up", (up_weight_ref, up_weight))
    fetch_all("down", (down_weight_ref, down_weight))
    places[pl.ds(pl.multiple_of(place.row * 8, 8), 8), :] = place_ref[...]
    tables[own_rows, :] = table_ref[...]
    gather_places = Gather(place, places, gather_send.at[0], gather_recv.at[0], 8)
    gather_tables = Gather(place, tables, gather_send.at[1], gather_recv.at[1])
    gather_inputs = Gather(place, inputs, gather_send.at[2], gather_recv.at[2])
    gather_cotangents = Gather(place, cotangents, gather_send.at[3], gather_recv.at[3])
    gather_two = Gather(place, normed_two, gather_send.at[4], gather_recv.at[4])
    swap_places = Swap(place, places, place_out, swap_send.at[0], swap_recv.at[0], 8, 2)
    swap_packed = Swap(place, packed_from, packed, swap_send.at[1], swap_recv.at[1], halves)
    swap_heads = Swap(place, heads_from, heads, swap_send.at[2], swap_recv.at[2], halves)
    fold = Fold(place, part, near, send, far, fold_send, fold_recv)
    place.greet()
    fetch("inputs")
    gather_tables.start()
    gather_inputs.start()
    gather_places.start()
    fetch("cotangent")
    gather_cotangents.start()

    def project(chip):
        base = chip * pair_rows

        @pl.loop(0, pair_rows // 16)
        def _(piece):
            span = rows_at(base + piece * 16, 16)
            rows = inputs[span, :].astype(jnp.float32)
            normed_one[span, :] = (rows * rms_scale(rows) * gain_ref[0:1, :]).astype(jnp.bfloat16)

        span = rows_at(base, pair_rows)
        low_cosine, low_sine = tables[span, :half], tables[span, half:HEAD_DIM]
        ones = jnp.ones((pair_rows, HEAD_DIM), jnp.float32)
        cosine[span, :] = jnp.concatenate([low_cosine] * 6 + [ones], axis=-1)
        sine[span, :] = jnp.concatenate([-low_sine, low_sine] * 3 + [ones * 0.0], axis=-1)

        for head in range(2):
            products = product_back(normed_one[span, :], weight[head])
            low = (
                products[:, :WIDE] * cosine[span, :] + products[:, WIDE:] * sine[span, :]
            ).astype(jnp.bfloat16)
            for index in range(2):
                packed_from[pl.ds(((2 * chip + index) * 2 + head) * halves, halves)] = low[
                    index * TILE : (index + 1) * TILE
                ].reshape(halves, block, WIDE)
        for index in range(4):
            swap_packed.start(4 * chip + index)

    gather_tables.first()
    gather_inputs.first()
    gather_places.first()
    fetch("weight")
    project(place.chip)
    gather_tables.relay()
    gather_inputs.relay()
    gather_places.relay()
    gather_tables.arrive()
    gather_inputs.arrive()
    gather_places.arrive()
    project(1 - place.chip)
    swap_places.start_all()
    store(normed_one, normed_one_out)
    store(cosine, cosine_out)
    store(sine, sine_out)
    swap_places.arrive()
    swap_packed.arrive()
    store(packed, packed_out)

    def place_row(first, count):
        blocks = [place_out[8 * index : 8 * index + 1, :] for index in range(first, first + count)]
        return jnp.concatenate(blocks, axis=-1)

    tile = min(256, length)
    order = place_row(0, length // TILE)
    flat = packed[...].reshape(length, WIDE)
    for first in range(0, length, tile):
        rows = lax.broadcasted_iota(jnp.int32, (tile, length), 0) + first
        chosen = jnp.where(rows == order, 1.0, 0.0).astype(jnp.bfloat16)
        moved = product(chosen, flat).astype(jnp.bfloat16)
        for index, target in enumerate((q0, q1, k, v)):
            target[first : first + tile, :] = moved[:, index * HEAD_DIM : (index + 1) * HEAD_DIM]
    for first in range(0, length, tile):
        parts = []
        for q in (q0, q1):
            soft = softmax_parts(q[first : first + tile, :], k[: first + tile, :], first)
            parts.append(product(soft.astype(jnp.bfloat16), v[: first + tile, :]))
        result[first : first + tile, :] = jnp.concatenate(parts, axis=-1).astype(jnp.bfloat16)
    for first in range(0, length, tile):
        rows = lax.broadcasted_iota(jnp.int32, (length, tile), 0)
        chosen = jnp.where(rows == place_row(first // TILE, tile // TILE), 1.0, 0.0)
        moved = product_rows(chosen.astype(jnp.bfloat16), result[...]).astype(jnp.bfloat16)
        heads_from[first // block : (first + tile) // block] = moved.reshape(-1, block, PAIR)
    swap_heads.start_all()
    gather_cotangents.first()
    gather_cotangents.relay()
    fetch("output")
    swap_heads.arrive()
    store(heads, attended_out)

    @pl.loop(0, 4)
    def _(sequence):
        total = None
        for head in range(2):
            rows = heads[pl.ds((2 * sequence + head) * halves, halves)].reshape(TILE, PAIR)
            term = product(rows, output_weight[head * PAIR : (head + 1) * PAIR, :])
            total = term if total is None else total + term
        part[rows_at(sequence * TILE, TILE), :] = total.astype(jnp.bfloat16)

    fold.start()
    gather_cotangents.arrive()
    store(cotangents, cotangent_out)
    fold.relay()
    fold.arrive()

    @pl.loop(0, TILE // 16)
    def _(piece):
        span = rows_at(piece * 16, 16)
        own = rows_at(place.row * TILE + piece * 16, 16)
        rows = inputs[own, :].astype(jnp.float32) + fold.rows(piece * 16, 16)
        hidden[span, :] = rows
        normed_two[own, :] = (rows * rms_scale(rows) * gain_ref[1:2, :]).astype(jnp.bfloat16)

    gather_two.start()
    store(hidden, hidden_out)
    fetch("gate", "up", "down")

    def feed(chip):
        span = rows_at(chip * pair_rows, pair_rows)

        @pl.loop(0, mixed.shape[1] // 256)
        def _(index):
            units = rows_at(index * 256, 256)
            columns = pl.ds(pl.multiple_of(index * 256, 256), 256)
            gate = product_back(normed_two[span, :], gate_weight[units, :])
            upward = product_back(normed_two[span, :], up_weight[units, :])
            grad_mixed = product_back(cotangents[span, :], down_weight[units, :])
            sigmoid = jax.nn.sigmoid(gate)
            activated = gate * sigmoid
            mixed[span, columns] = (activated * upward).astype(jnp.bfloat16)
            grad_gate[span, columns] = (
                grad_mixed * upward * sigmoid * (1.0 + gate * (1.0 - sigmoid))
            ).astype(jnp.bfloat16)
            grad_up[span, columns] = (grad_mixed * activated).astype(jnp.bfloat16)

        @pl.loop(0, width // 512)
        def _(index):
            columns = pl.ds(pl.multiple_of(index * 512, 512), 512)
            part[span, columns] = (
                product(grad_gate[span, :], gate_weight[:, columns])
                + product(grad_up[span, :], up_weight[:, columns])
            ).astype(jnp.bfloat16)

    gather_two.first()
    feed(place.chip)
    gather_two.relay()
    gather_two.arrive()
    store(normed_two, normed_two_out)
    feed(1 - place.chip)
    store(part, part_out)
    store(mixed, mixed_out)
    store(grad_gate, grad_gate_out)
    store(grad_up, grad_up_out)
    for copy in stores:
        copy.wait()


def forward(places, table, gains, inputs, cotangent, query_weight, key_weight, value_weight,
            output_weight, gate_weight, up_weight, down_weight, length, block, key):
    width = inputs.shape[1]
    hidden_units = gate_weight.shape[0]
    rows = 4 * TILE
    blocks = length // block
    low, full = jnp.bfloat16, jnp.float32
    dma = pltpu.SemaphoreType.DMA
    any_spec = pl.BlockSpec(memory_space=pl.ANY)

    def out(shape, dtype):
        return jax.ShapeDtypeStruct(shape, dtype)

    wide = (rows, width)
    return pl.pallas_call(
        functools.partial(forward_kernel, block),
        out_shape=(
            out((64, 128), jnp.int32),
            out(wide, low), out((TILE, width), full),
            out((blocks, block, PAIR), low), out((blocks, block, WIDE), low),
            out(wide, low), out((rows, WIDE), full), out((rows, WIDE), full),
            out(wide, low), out(wide, low),
            out((rows, hidden_units), low), out((rows, hidden_units), low),
            out((rows, hidden_units), low),
        ),
        in_specs=[vmem()] * 3 + [any_spec] * 9,
        out_specs=(vmem(),) + (any_spec,) * 12,
        scratch_shapes=[
            pltpu.VMEM((32, 128), jnp.int32),
            pltpu.VMEM((rows, 128), full),
            pltpu.VMEM(wide, low), pltpu.VMEM(wide, low),
            pltpu.VMEM(wide, low), pltpu.VMEM(wide, low),
            pltpu.VMEM((rows, WIDE), full), pltpu.VMEM((rows, WIDE), full),
            pltpu.VMEM((2, 2 * WIDE, width), low),
            pltpu.VMEM(output_weight.shape, low),
            pltpu.VMEM((hidden_units, width), low), pltpu.VMEM((hidden_units, width), low),
            pltpu.VMEM((hidden_units, width), low),
            pltpu.VMEM((blocks, block, WIDE), low), pltpu.VMEM((blocks, block, WIDE), low),
        ]
        + [pltpu.VMEM((length, HEAD_DIM), low)] * 4
        + [
            pltpu.VMEM((length, PAIR), low),
            pltpu.VMEM((blocks, block, PAIR), low), pltpu.VMEM((blocks, block, PAIR), low),
            pltpu.VMEM(wide, low),
            pltpu.VMEM((2, TILE, width), low),
            pltpu.VMEM((TILE, width), low), pltpu.VMEM((TILE, width), low),
            pltpu.VMEM((TILE, width), full),
            pltpu.VMEM((rows, hidden_units), low), pltpu.VMEM((rows, hidden_units), low),
            pltpu.VMEM((rows, hidden_units), low),
            dma((30,)), dma((12,)),
            dma((5, 3)), dma((5, 3)),
            dma((3, 8)), dma((3, 8)),
            dma((3,)), dma((3,)),
        ],
        compiler_params=pltpu.CompilerParams(
            collective_id=key, has_side_effects=True, vmem_limit_bytes=63 * 2**20
        ),
        name="forward",
    )(places, table, gains, inputs, cotangent, query_weight, key_weight, value_weight,
      output_weight, gate_weight, up_weight, down_weight)


def gather_rows(values):
    return lax.all_gather(values, "fsdp", axis=0, tiled=True)


def scatter_rows(values):
    return lax.psum_scatter(
        values.astype(jnp.bfloat16), "fsdp", scatter_dimension=0, tiled=True
    ).astype(jnp.float32)


def per_device_gathered(
    inputs,
    positions,
    cotangent,
    attention_gain,
    query_weight,
    key_weight,
    value_weight,
    output_weight,
    feedforward_gain,
    gate_weight,
    up_weight,
    down_weight,
):
    row_count = inputs.shape[0]
    groups = HEADS // KV_HEADS
    gain_one = attention_gain.astype(jnp.float32)
    gain_two = feedforward_gain.astype(jnp.float32)
    seq_count = lax.axis_size("fsdp")
    first_row = lax.axis_index("fsdp") * row_count

    def own(values):
        return lax.dynamic_slice_in_dim(values, first_row, row_count, 0)

    query_places = gather_rows(positions).reshape(seq_count, row_count)
    key_places = lax.all_gather(query_places, "ctx", axis=1, tiled=True)
    all_cotangent = gather_rows(cotangent)
    flat_in = gather_rows(inputs).astype(jnp.float32)
    scale_one = rms_scale(flat_in)
    unit_one = flat_in * scale_one
    normed_one = (unit_one * gain_one).astype(jnp.bfloat16)
    total_rows = normed_one.shape[0]
    cosine, sine = rotary_tables(query_places.reshape(-1))
    query_heads = query_weight.shape[0] // HEAD_DIM
    kv_heads = key_weight.shape[0] // HEAD_DIM
    kv_width = kv_heads * HEAD_DIM
    query_low = rotate(
        product_back(normed_one, query_weight).reshape(total_rows, query_heads, HEAD_DIM), cosine, sine
    ).astype(jnp.bfloat16)
    key_low = rotate(
        product_back(normed_one, key_weight).reshape(total_rows, kv_heads, HEAD_DIM), cosine, sine
    ).astype(jnp.bfloat16)
    value_low = product_back(normed_one, value_weight).astype(jnp.bfloat16)
    ctx_size = lax.axis_size("ctx")

    def spread(values):
        rows = lax.all_gather(values, "ctx", axis=0, tiled=True)
        rows = rows.reshape(ctx_size, seq_count, row_count, kv_width).swapaxes(0, 1)
        return rows.reshape(seq_count, ctx_size * row_count, kv_width)

    def collect(values):
        rows = values.astype(jnp.bfloat16).swapaxes(1, 2)
        rows = rows.reshape(seq_count, ctx_size, row_count, kv_width).swapaxes(0, 1)
        return lax.psum_scatter(
            rows.reshape(-1, kv_width), "ctx", scatter_dimension=0, tiled=True
        )

    all_keys = spread(key_low.reshape(total_rows, kv_width))
    all_values = spread(value_low)
    total_keys = all_keys.shape[1]
    key_grid = all_keys.reshape(seq_count, total_keys, kv_heads, HEAD_DIM).swapaxes(1, 2)
    value_grid = all_values.reshape(seq_count, total_keys, kv_heads, HEAD_DIM).swapaxes(1, 2)
    query_grouped = query_low.reshape(seq_count, row_count, kv_heads, groups, HEAD_DIM)
    attended, log_total = attend_forward(
        query_grouped, query_places, key_grid, value_grid, key_places
    )
    attended_low = attended.reshape(total_rows, query_heads * HEAD_DIM).astype(jnp.bfloat16)
    hidden_state = inputs.astype(jnp.float32) + scatter_rows(product(attended_low, output_weight))
    scale_two = rms_scale(hidden_state)
    unit_two = hidden_state * scale_two
    normed_two = gather_rows((unit_two * gain_two).astype(jnp.bfloat16))
    gate_values = product_back(normed_two, gate_weight)
    upward = product_back(normed_two, up_weight)
    sigmoid_gate = jax.nn.sigmoid(gate_values)
    activated = gate_values * sigmoid_gate
    mixed_hidden = (activated * upward).astype(jnp.bfloat16)
    grad_out = cotangent.astype(jnp.float32)
    grad_down = product_rows(mixed_hidden, all_cotangent)
    grad_mixed = product_back(all_cotangent, down_weight)
    grad_gate_low = (
        grad_mixed * upward * sigmoid_gate * (1.0 + gate_values * (1.0 - sigmoid_gate))
    ).astype(jnp.bfloat16)
    grad_up_low = (grad_mixed * activated).astype(jnp.bfloat16)
    grad_unit_part = (
        product(grad_gate_low, gate_weight) + product(grad_up_low, up_weight)
    ).astype(jnp.bfloat16)
    grad_normed_two = scatter_rows(grad_unit_part)
    gain_two_grad = jnp.sum(grad_normed_two * unit_two, axis=0)
    grad_hidden = grad_out + norm_back(scale_two, unit_two, grad_normed_two * gain_two)
    branch_rows = gather_rows(grad_hidden.astype(jnp.bfloat16))
    layer_output = (hidden_state + scatter_rows(product(mixed_hidden, down_weight))).astype(
        jnp.bfloat16
    )
    grad_gate = product_rows(grad_gate_low, normed_two)
    grad_up = product_rows(grad_up_low, normed_two)
    grad_output = product_rows(attended_low, branch_rows)
    grad_attended = product_back(branch_rows, output_weight).astype(jnp.bfloat16)
    grad_attended = grad_attended.reshape(seq_count, row_count, kv_heads, groups, HEAD_DIM)
    grad_query_rot, grad_key_all, grad_value_all = attend_backward(
        query_grouped, query_places, key_grid, value_grid, key_places, log_total, grad_attended
    )
    grad_key_own = collect(grad_key_all).astype(jnp.float32)
    grad_value_low = collect(grad_value_all)
    grad_query_low = (
        rotate_back(grad_query_rot.reshape(total_rows, query_heads, HEAD_DIM), cosine, sine)
        .reshape(total_rows, query_heads * HEAD_DIM)
        .astype(jnp.bfloat16)
    )
    grad_key_low = (
        rotate_back(
            grad_key_own.reshape(total_rows, kv_heads, HEAD_DIM), cosine, sine
        )
        .reshape(total_rows, kv_width)
        .astype(jnp.bfloat16)
    )
    grad_query = product_rows(grad_query_low, normed_one)
    grad_key = product_rows(grad_key_low, normed_one)
    grad_value = product_rows(grad_value_low, normed_one)
    grad_normed_one = scatter_rows(
        product(grad_query_low, query_weight)
        + product(grad_key_low, key_weight)
        + product(grad_value_low, value_weight)
    )
    own_unit = own(unit_one)
    gain_one_grad = jnp.sum(grad_normed_one * own_unit, axis=0)
    input_grad = grad_hidden + norm_back(own(scale_one), own_unit, grad_normed_one * gain_one)

    grads = (grad_query, grad_key, grad_value, grad_output, grad_gate, grad_up, grad_down)
    parts = [lax.psum(grad.astype(jnp.bfloat16), "ctx").astype(jnp.float32) for grad in grads]
    gain_sums = lax.psum(jnp.stack([gain_one_grad, gain_two_grad]), ("fsdp", "ctx"))
    return (
        layer_output,
        input_grad,
        gain_sums[0],
        parts[0],
        parts[1],
        parts[2],
        parts[3],
        gain_sums[1],
        parts[4],
        parts[5],
        parts[6],
    )


def per_device_by_head(
    inputs,
    positions,
    cotangent,
    attention_gain,
    query_weight,
    key_weight,
    value_weight,
    output_weight,
    feedforward_gain,
    gate_weight,
    up_weight,
    down_weight,
):
    gains = jnp.stack([attention_gain, feedforward_gain]).astype(jnp.float32)
    block = TILE // 2
    length = TILE * 8
    cosine, sine = rotary_tables(positions)
    table = jnp.concatenate([cosine[:, 0, :], sine[:, 0, :]], axis=1)
    table = jnp.pad(table, ((0, 0), (0, 128 - table.shape[1])))
    (
        places, part, hidden, attended, packed, normed_one, wide_cosine, wide_sine,
        cotangents, normed_two, mixed, grad_gate, grad_up,
    ) = forward(
        jnp.broadcast_to(positions[None, :], (8, TILE)), table, gains, inputs, cotangent,
        query_weight, key_weight, value_weight, output_weight, gate_weight, up_weight,
        down_weight, length, block, 1,
    )
    starts = places.reshape(8, 8, TILE)[:, 0, ::block].reshape(-1) // block
    slots = jnp.arange(length // block, dtype=jnp.int32)
    found = jnp.where(starts[None, :] == slots[:, None], slots[None, :], 0)
    order = jnp.concatenate([jnp.sum(found, axis=1), starts]).astype(jnp.int32)
    half = HEAD_DIM // 2
    lanes = jnp.arange(WIDE, dtype=jnp.int32)
    partner_lane = lanes + jnp.where(lanes % HEAD_DIM < half, half, -half)
    half_swap = jnp.logical_and(
        lanes[:, None] == partner_lane[None, :], lanes[None, :] < PAIR + HEAD_DIM
    ).astype(jnp.bfloat16)
    width = inputs.shape[1]
    weight = jnp.concatenate(
        [
            query_weight.reshape(2, PAIR, width),
            key_weight.reshape(2, HEAD_DIM, width),
            value_weight.reshape(2, HEAD_DIM, width),
        ],
        axis=1,
    )
    layer_output = (hidden + scatter_rows(product(mixed, down_weight))).astype(jnp.bfloat16)
    ff_grads = (
        product_rows(grad_gate, normed_two).astype(jnp.bfloat16),
        product_rows(grad_up, normed_two).astype(jnp.bfloat16),
        product_rows(mixed, cotangents).astype(jnp.bfloat16),
    )
    summed, gain_sums, input_grad = backward(
        order, ff_grads, part, hidden, cotangent, inputs, gains, output_weight, attended,
        packed, normed_one, wide_cosine, wide_sine, half_swap, weight, block, 5,
    )
    parts, start = [], 0
    for grad in (gate_weight, up_weight, down_weight, query_weight, key_weight, value_weight,
                 output_weight):
        parts.append(summed[start : start + grad.shape[0]].astype(jnp.float32))
        start += grad.shape[0]
    return (layer_output, input_grad, gain_sums[0], *parts[3:], gain_sums[1], *parts[:3])


def per_device(*arrays):
    fits = lax.axis_size("fsdp") == 4 and lax.axis_size("ctx") == 8
    return (per_device_by_head if fits else per_device_gathered)(*arrays)


def solution(mesh):
    in_specs = (
        P(("fsdp", "ctx"), None),
        P(("fsdp", "ctx")),
        P(("fsdp", "ctx"), None),
        P(),
        P("fsdp", None),
        P("fsdp", None),
        P("fsdp", None),
        P("fsdp", None),
        P(),
        P("fsdp", None),
        P("fsdp", None),
        P("fsdp", None),
    )
    out_specs = (
        P(("fsdp", "ctx"), None),
        P(("fsdp", "ctx"), None),
        P(),
        P("fsdp", None),
        P("fsdp", None),
        P("fsdp", None),
        P("fsdp", None),
        P(),
        P("fsdp", None),
        P("fsdp", None),
        P("fsdp", None),
    )
    return jax.shard_map(
        per_device, mesh=mesh, in_specs=in_specs, out_specs=out_specs, check_vma=False
    )
```

```python
import functools
import math

import jax
import jax.numpy as jnp
from jax import lax
from jax.experimental import pallas as pl
from jax.experimental.pallas import tpu as pltpu
from jax.sharding import PartitionSpec as P

HEADS = 16
KV_HEADS = 8
HEAD_DIM = 96


EPSILON = 1e-05
ROPE_BASE = 100000.0


def product(left, right):
    return jnp.dot(left, right, preferred_element_type=jnp.float32)


def product_back(left, right):
    return lax.dot_general(
        left, right, (((1,), (1,)), ((), ())), preferred_element_type=jnp.float32
    )


def product_rows(left, right):
    return lax.dot_general(
        left, right, (((0,), (0,)), ((), ())), preferred_element_type=jnp.float32
    )


def rms_scale(values):
    return lax.rsqrt(jnp.mean(values * values, axis=-1, keepdims=True) + EPSILON)


def norm_back(scale_rows, unit_rows, grad_unit):
    return scale_rows * (
        grad_unit - unit_rows * jnp.mean(grad_unit * unit_rows, axis=-1, keepdims=True)
    )


def rotary_tables(places):
    half_width = HEAD_DIM // 2
    frequencies = ROPE_BASE ** (-(jnp.arange(half_width, dtype=jnp.float32) * 2.0 / HEAD_DIM))
    angles = places.astype(jnp.float32)[:, None] * frequencies[None, :]
    return (jnp.cos(angles)[:, None, :], jnp.sin(angles)[:, None, :])


def rotate(values, cosine, sine):
    half_width = values.shape[-1] // 2
    lower_half = values[..., :half_width]
    upper_half = values[..., half_width:]
    return jnp.concatenate(
        [lower_half * cosine - upper_half * sine, upper_half * cosine + lower_half * sine], axis=-1
    )


def rotate_back(grads, cosine, sine):
    half_width = grads.shape[-1] // 2
    lower_half = grads[..., :half_width]
    upper_half = grads[..., half_width:]
    return jnp.concatenate(
        [lower_half * cosine + upper_half * sine, upper_half * cosine - lower_half * sine], axis=-1
    )


def block_total_of(total_keys):
    return max(1, total_keys // 512)


def masked_scores(query_grouped, query_places, key_rows, key_places, start, width):
    key_part = lax.dynamic_slice_in_dim(key_rows, start, width, 2)
    place_part = lax.dynamic_slice_in_dim(key_places, start, width, 1)
    scores = jnp.einsum(
        "sqhgd,shkd->shgqk", query_grouped, key_part, preferred_element_type=jnp.float32
    )
    scores = scores * (1.0 / math.sqrt(HEAD_DIM))
    allowed = place_part[:, None, None, None, :] <= query_places[:, None, None, :, None]
    return jnp.where(allowed, scores, -1000000000.0)


def attend_forward(query_grouped, query_places, key_rows, value_rows, key_places):
    seq_count, row_count, head_groups, group_size = query_grouped.shape[:4]
    total_keys = key_rows.shape[2]
    block_total = block_total_of(total_keys)
    width = total_keys // block_total
    stat_shape = (seq_count, head_groups, group_size, row_count)

    def peak_step(index, carry):
        running_top, running_sum = carry
        scores = masked_scores(
            query_grouped, query_places, key_rows, key_places, index * width, width
        )
        new_top = jnp.maximum(running_top, jnp.max(scores, axis=-1))
        running_sum = running_sum * jnp.exp(running_top - new_top) + jnp.sum(
            jnp.exp(scores - new_top[..., None]), axis=-1
        )
        return (new_top, running_sum)

    running_top, running_sum = lax.fori_loop(
        0,
        block_total,
        peak_step,
        (jnp.full(stat_shape, -1e30, jnp.float32), jnp.zeros(stat_shape, jnp.float32)),
    )
    log_total = running_top + jnp.log(running_sum)

    def value_step(index, gathered):
        scores = masked_scores(
            query_grouped, query_places, key_rows, key_places, index * width, width
        )
        soft_low = jnp.exp(scores - log_total[..., None]).astype(jnp.bfloat16)
        value_part = lax.dynamic_slice_in_dim(value_rows, index * width, width, 2)
        return gathered + jnp.einsum(
            "shgqk,shkd->sqhgd", soft_low, value_part, preferred_element_type=jnp.float32
        )

    attended = lax.fori_loop(
        0, block_total, value_step, jnp.zeros(query_grouped.shape, jnp.float32)
    )
    return (attended, log_total)


def attend_backward(
    query_grouped, query_places, key_rows, value_rows, key_places, log_total, grad_attended
):
    total_keys = key_rows.shape[2]
    block_total = block_total_of(total_keys)
    width = total_keys // block_total
    score_scale = 1.0 / math.sqrt(HEAD_DIM)

    def soft_and_grad(index):
        scores = masked_scores(
            query_grouped, query_places, key_rows, key_places, index * width, width
        )
        soft_values = jnp.exp(scores - log_total[..., None])
        value_part = lax.dynamic_slice_in_dim(value_rows, index * width, width, 2)
        grad_soft = jnp.einsum(
            "sqhgd,shkd->shgqk", grad_attended, value_part, preferred_element_type=jnp.float32
        )
        return (soft_values, grad_soft)

    def delta_step(index, row_delta):
        soft_values, grad_soft = soft_and_grad(index)
        return row_delta + jnp.sum(soft_values * grad_soft, axis=-1)

    row_delta = lax.fori_loop(0, block_total, delta_step, jnp.zeros(log_total.shape, jnp.float32))

    def grad_step(index, carry):
        grad_query, grad_keys, grad_values = carry
        soft_values, grad_soft = soft_and_grad(index)
        grad_scores = (soft_values * (grad_soft - row_delta[..., None])).astype(jnp.bfloat16)
        key_part = lax.dynamic_slice_in_dim(key_rows, index * width, width, 2)
        grad_query = (
            grad_query
            + jnp.einsum(
                "shgqk,shkd->sqhgd", grad_scores, key_part, preferred_element_type=jnp.float32
            )
            * score_scale
        )
        key_term = (
            jnp.einsum(
                "shgqk,sqhgd->shkd", grad_scores, query_grouped, preferred_element_type=jnp.float32
            )
            * score_scale
        )
        value_term = jnp.einsum(
            "shgqk,sqhgd->shkd",
            soft_values.astype(jnp.bfloat16),
            grad_attended,
            preferred_element_type=jnp.float32,
        )
        grad_keys = lax.dynamic_update_slice_in_dim(grad_keys, key_term, index * width, 2)
        grad_values = lax.dynamic_update_slice_in_dim(grad_values, value_term, index * width, 2)
        return (grad_query, grad_keys, grad_values)

    initial = (
        jnp.zeros(query_grouped.shape, jnp.float32),
        jnp.zeros(key_rows.shape, jnp.float32),
        jnp.zeros(value_rows.shape, jnp.float32),
    )
    return lax.fori_loop(0, block_total, grad_step, initial)


def vmem():
    return pl.BlockSpec(memory_space=pltpu.VMEM)


def peer(ctx_index):
    return dict(device_id={"ctx": ctx_index}, device_id_type=pl.DeviceIdType.MESH)


SPINE_ROWS = 48
LINE_ROWS = 64
ROUND_ROWS = 2 * SPINE_ROWS + LINE_ROWS
LEAD = 2
RING = 12
TILE = 128
PAIR = (HEADS // KV_HEADS) * HEAD_DIM
WIDE = PAIR + 2 * HEAD_DIM


def near_fsdp(index):
    return dict(device_id={"fsdp": index}, device_id_type=pl.DeviceIdType.MESH)


def rows_at(start, count):
    return pl.ds(pl.multiple_of(start, 16), count)


class Place:
    def __init__(self):
        self.ctx = lax.axis_index("ctx")
        self.row = lax.axis_index("fsdp")
        self.chip, self.core = lax.div(self.row, 2), lax.rem(self.row, 2)
        self.partner = 2 * self.chip + 1 - self.core
        self.across = 2 * (1 - self.chip) + self.core
        self.corner = 2 * (1 - self.chip) + 1 - self.core

    def greet(self):
        barrier = pltpu.get_barrier_semaphore()
        for step in range(1, 4):
            pl.semaphore_signal(barrier, inc=1, **near_fsdp(lax.rem(self.row + step, 4)))
        for step in range(1, 8):
            pl.semaphore_signal(barrier, inc=1, **peer(lax.rem(self.ctx + step, 8)))
        pl.semaphore_wait(barrier, 10)


class Fold:
    def __init__(self, place, part, near, send, far, send_sem, recv_sem):
        self.place, self.part, self.near, self.send, self.far = place, part, near, send, far
        self.send_sem, self.recv_sem = send_sem, recv_sem

    def partner_copy(self, chip):
        block = 2 * chip + 1 - self.place.core
        return pltpu.make_async_remote_copy(
            src_ref=self.part.at[rows_at(block * TILE, TILE)],
            dst_ref=self.near.at[chip],
            send_sem=self.send_sem.at[chip],
            recv_sem=self.recv_sem.at[chip],
            **near_fsdp(self.place.partner),
        )

    def across_copy(self):
        return pltpu.make_async_remote_copy(
            src_ref=self.send,
            dst_ref=self.far,
            send_sem=self.send_sem.at[2],
            recv_sem=self.recv_sem.at[2],
            **near_fsdp(self.place.across),
        )

    def start(self):
        self.partner_copy(1 - self.place.chip).start()
        self.partner_copy(self.place.chip).start()

    def relay(self):
        there = 1 - self.place.chip
        self.partner_copy(there).wait_recv()
        base = self.place.across * TILE

        @pl.loop(0, TILE // 32)
        def _(piece):
            mine = self.part[rows_at(base + piece * 32, 32), :].astype(jnp.float32)
            span = rows_at(piece * 32, 32)
            self.send[span, :] = (
                mine + self.near[there, span, :].astype(jnp.float32)
            ).astype(jnp.bfloat16)

        self.across_copy().start()

    def arrive(self):
        self.partner_copy(self.place.chip).wait_recv()
        copy = self.across_copy()
        copy.wait_recv()
        copy.wait_send()
        self.partner_copy(0).wait_send()
        self.partner_copy(1).wait_send()

    def rows(self, start, count):
        mine = self.part[rows_at(self.place.row * TILE + start, count), :].astype(jnp.float32)
        span = rows_at(start, count)
        near = self.near[self.place.chip, span, :].astype(jnp.float32)
        return mine + near + self.far[span, :].astype(jnp.float32)


class Gather:
    def __init__(self, place, full, send_sem, recv_sem, count=TILE):
        self.place, self.full, self.send_sem, self.recv_sem = place, full, send_sem, recv_sem
        self.count = count

    def copy(self, block, target, key):
        span = pl.ds(pl.multiple_of(block * self.count, self.count), self.count)
        return pltpu.make_async_remote_copy(
            src_ref=self.full.at[span],
            dst_ref=self.full.at[span],
            send_sem=self.send_sem.at[key],
            recv_sem=self.recv_sem.at[key],
            **near_fsdp(target),
        )

    def start(self):
        self.copy(self.place.row, self.place.across, 1).start()
        self.copy(self.place.row, self.place.partner, 0).start()

    def relay(self):
        self.copy(self.place.across, self.place.across, 1).wait_recv()
        self.copy(self.place.across, self.place.partner, 2).start()

    def first(self):
        self.copy(self.place.partner, self.place.partner, 0).wait_recv()

    def arrive(self):
        self.copy(self.place.corner, self.place.partner, 2).wait_recv()
        self.copy(self.place.row, self.place.across, 1).wait_send()
        self.copy(self.place.row, self.place.partner, 0).wait_send()
        self.copy(self.place.across, self.place.partner, 2).wait_send()


class Swap:
    def __init__(self, place, source, target, send_sem, recv_sem, count, share=1):
        self.place, self.source, self.target = place, source, target
        self.send_sem, self.recv_sem, self.count, self.share = send_sem, recv_sem, count, share

    def span(self, index):
        return pl.ds(pl.multiple_of(index * self.count, self.count), self.count)

    def copy(self, other, sender):
        return pltpu.make_async_remote_copy(
            src_ref=self.source.at[self.span(lax.div(other, self.share))],
            dst_ref=self.target.at[self.span(sender)],
            send_sem=self.send_sem.at[other],
            recv_sem=self.recv_sem.at[sender],
            **peer(other),
        )

    def start(self, other):
        me = self.place.ctx

        @pl.when(other != me)
        def _():
            self.copy(other, me).start()

        @pl.when(other == me)
        def _():
            self.target[self.span(me)] = self.source[self.span(lax.div(me, self.share))]

    def start_all(self):
        for step in range(1, 9):
            self.start(lax.rem(self.place.ctx + step, 8))

    def arrive(self):
        for step in range(1, 8):
            other = lax.rem(self.place.ctx + step, 8)
            self.copy(other, other).wait()


class Spread:
    def __init__(self, slots, index, count, device, send_sem, recv_sem):
        self.slots, self.index, self.count, self.device = slots, index, count, device
        self.send_sem, self.recv_sem = send_sem, recv_sem

    def copy(self, step):
        return pltpu.make_async_remote_copy(
            src_ref=self.slots.at[self.index],
            dst_ref=self.slots.at[self.index],
            send_sem=self.send_sem.at[step],
            recv_sem=self.recv_sem.at[step],
            **self.device(lax.rem(self.index + step, self.count)),
        )

    def start(self):
        for step in range(1, self.count):
            self.copy(step).start()

    def total(self):
        for step in range(1, self.count):
            self.copy(step).wait()
        result = self.slots[0]
        for step in range(1, self.count):
            result += self.slots[step]
        return result


class Tree:
    def __init__(self, place, own, out_ref, index, line, box, sems, leaf_back):
        me = place.ctx
        depth, side = lax.div(me, 2), lax.rem(me, 2)
        other_side = me + 1 - 2 * side
        self.own, self.out, self.box, self.index, self.line = own, out_ref, box, index, line
        self.up, self.got, self.down, self.back = sems
        self.leaf_back = leaf_back
        if line:
            center = lax.rem(index, 4)
            count = LINE_ROWS
            start = index * ROUND_ROWS + 2 * SPINE_ROWS
            root_side = lax.rem(index, 2)
            on_cross = depth == center
            self.root = jnp.logical_and(on_cross, side == root_side)
            has_side = self.root
            to_side = jnp.logical_and(on_cross, side != root_side)
            reach = jnp.maximum(center, 3 - center)
            away = jnp.abs(depth - center)
            crossed = jnp.where(side == root_side, 0, 1)
            self.rise_age = reach - away + jnp.where(self.root, 1, 0)
            self.fall_age = reach + 1 + away + crossed
        else:
            center = 1 + side
            count = SPINE_ROWS
            start = index * ROUND_ROWS + side * SPINE_ROWS
            self.root = depth == center
            has_side = None
        self.count = count
        self.start = start
        self.slot = lax.rem(index, RING)
        self.rows = rows_at(start, count)
        self.children = (
            (jnp.logical_and(depth > 0, depth <= center), me - 2, 0),
            (jnp.logical_and(depth < 3, depth >= center), me + 2, 1),
            (has_side, other_side, 2),
        )
        parent = jnp.where(depth < center, me + 2, me - 2)
        slot = jnp.where(depth < center, 0, 1)
        if line:
            parent = jnp.where(to_side, other_side, parent)
            slot = jnp.where(to_side, 2, slot)
        self.parent = jnp.where(self.root, other_side, parent)
        self.parent_slot = jnp.where(self.root, 2, slot)

    def boxed(self, slot):
        return self.box.at[slot, rows_at(self.slot * self.count, self.count)]

    def up_copy(self, target, slot):
        return pltpu.make_async_remote_copy(
            src_ref=self.own.at[self.rows],
            dst_ref=self.boxed(slot),
            send_sem=self.up.at[self.slot],
            recv_sem=self.got.at[slot, self.slot],
            **peer(target),
        )

    def down_copy(self, child, slot, source):
        back = self.back if slot < 2 or self.line else self.leaf_back
        return pltpu.make_async_remote_copy(
            src_ref=source.at[self.rows],
            dst_ref=self.out.at[self.rows],
            send_sem=self.down.at[slot, self.slot],
            recv_sem=back.at[self.slot],
            **peer(child),
        )

    def each_child(self, action):
        for present, child, slot in self.children:
            if present is None:
                action(child, slot)
            else:
                pl.when(present)(functools.partial(action, child, slot))

    def keep(self):
        return pltpu.make_async_copy(
            self.own.at[self.rows], self.out.at[self.rows], self.up.at[self.slot]
        )

    def rise(self):
        self.each_child(lambda child, slot: self.up_copy(child, slot).wait_recv())
        base = self.slot * self.count
        for piece in range(0, self.count, 16):
            span = rows_at(self.start + piece, 16)
            total = self.own[span, :].astype(jnp.float32)
            for present, _, slot in self.children:
                part = self.box[slot, rows_at(base + piece, 16), :].astype(jnp.float32)
                total += part if present is None else jnp.where(present, part, 0.0)
            self.own[span, :] = total.astype(jnp.bfloat16)

        @pl.when(jnp.logical_not(self.root))
        def _():
            self.up_copy(self.parent, self.parent_slot).start()

        @pl.when(self.root)
        def _():
            self.keep().start()
            self.each_child(lambda child, slot: self.down_copy(child, slot, self.own).start())

    def fall(self):
        @pl.when(jnp.logical_not(self.root))
        def _():
            self.down_copy(self.parent, 0, self.out).wait_recv()
            self.each_child(lambda child, slot: self.down_copy(child, slot, self.out).start())

    def finish(self):
        @pl.when(jnp.logical_not(self.root))
        def _():
            self.up_copy(self.parent, self.parent_slot).wait_send()

        @pl.when(self.root)
        def _():
            self.keep().wait()

        self.each_child(lambda child, slot: self.down_copy(child, slot, self.out).wait_send())


def softmax_parts(query_rows, key_rows, first_row):
    scores = product_back(query_rows, key_rows) * (1.0 / math.sqrt(HEAD_DIM))
    rows = lax.broadcasted_iota(jnp.int32, scores.shape, 0) + first_row
    columns = lax.broadcasted_iota(jnp.int32, scores.shape, 1)
    scores = jnp.where(columns <= rows, scores, -1e30)
    spread = jnp.exp(scores - jnp.max(scores, axis=-1, keepdims=True))
    return spread * (1.0 / jnp.sum(spread, axis=-1, keepdims=True))


def sort_blocks(slot_ref, source, targets):
    block_total, block, _ = source.shape
    for index in range(block_total):
        rows = source[slot_ref[index]]
        start = 0
        for target in targets:
            width = target.shape[-1]
            target[index * block : (index + 1) * block, :] = rows[:, start : start + width]
            start += width


def norm_back_rows(values, grad_unit):
    scale = rms_scale(values)
    unit = values * scale
    return unit, lambda grad: norm_back(scale, unit, grad)


def backward_kernel(
    rounds,
    block,
    order_ref,
    gain_one_ref,
    gain_two_ref,
    grad_gate_ref,
    grad_up_ref,
    mixed_ref,
    normed_two_ref,
    cotangent_ref,
    part_ref,
    hidden_ref,
    input_ref,
    query_weight_ref,
    key_weight_ref,
    value_weight_ref,
    output_weight_ref,
    down_weight_ref,
    attended_ref,
    packed_ref,
    normed_ref,
    cosine_ref,
    sine_ref,
    out_ref,
    gain_out_ref,
    input_grad_ref,
    layer_output_ref,
    own,
    spine_in,
    line_in,
    grad_gate,
    grad_up,
    mixed,
    normed_two,
    cotangents,
    part,
    hidden,
    inputs,
    output_weight,
    attended,
    packed,
    normed,
    cosine,
    sine,
    half_swap,
    weight,
    near,
    send,
    far,
    branch,
    grad_hidden,
    gain_part,
    heads_out,
    heads_in,
    q0,
    q1,
    k,
    v,
    g0,
    g1,
    result,
    dk,
    dv,
    packed_out,
    packed_in,
    turned,
    gain_near,
    gain_far,
    fetch_sem,
    spine_up,
    spine_got,
    spine_down,
    spine_back,
    leaf_up,
    leaf_back,
    line_up,
    line_got,
    line_down,
    line_back,
    fold_send,
    fold_recv,
    gather_send,
    gather_recv,
    swap_send,
    swap_recv,
    near_send,
    near_recv,
    far_send,
    far_recv,
):
    place = Place()
    me = place.ctx
    depth, side = lax.div(me, 2), lax.rem(me, 2)
    other_side = me + 1 - 2 * side
    hidden_units = mixed.shape[1]
    width = own.shape[1]
    base = 3 * hidden_units
    spare = rounds * ROUND_ROWS - base - 3 * WIDE
    length = q0.shape[0]
    halves = TILE // block
    tile = min(256, length)
    tiles = length // tile
    scale = 1.0 / math.sqrt(HEAD_DIM)

    fetches = {}

    def fetch_all(source, *copies):
        first = sum(len(group) for group in fetches.values())
        fetches[id(source)] = [
            pltpu.make_async_copy(*copy, fetch_sem.at[first + index])
            for index, copy in enumerate(copies or ())
        ]
        for copy in fetches[id(source)]:
            copy.start()

    def fetch(*sources):
        for source in sources:
            for copy in fetches[id(source)]:
                copy.wait()

    for source, target in (
        (part_ref, part),
        (grad_gate_ref, grad_gate),
        (normed_two_ref, normed_two),
        (grad_up_ref, grad_up),
        (mixed_ref, mixed),
        (cotangent_ref, cotangents),
        (hidden_ref, hidden),
        (packed_ref, packed),
        (down_weight_ref, own.at[pl.ds(base, hidden_units)]),
        (output_weight_ref, output_weight),
        (attended_ref, attended),
        (normed_ref, normed),
        (cosine_ref, cosine),
        (sine_ref, sine),
        (input_ref, inputs),
    ):
        fetch_all(source, (source, target))
    for source, first, count in (
        (query_weight_ref, 0, PAIR),
        (key_weight_ref, PAIR, HEAD_DIM),
        (value_weight_ref, PAIR + HEAD_DIM, HEAD_DIM),
    ):
        fetch_all(
            source,
            *(
                (source.at[pl.ds(head * count, count)], weight.at[head, pl.ds(first, count)])
                for head in range(2)
            ),
        )
    gain_one = gain_one_ref[...].astype(jnp.float32).reshape(1, -1)
    gain_two = gain_two_ref[...].astype(jnp.float32).reshape(1, -1)
    lanes = (WIDE, WIDE)
    row_lane = lax.broadcasted_iota(jnp.int32, lanes, 0)
    column_lane = lax.broadcasted_iota(jnp.int32, lanes, 1)
    half = HEAD_DIM // 2
    inner = lax.rem(column_lane, HEAD_DIM)
    partner_lane = column_lane + jnp.where(inner < half, half, -half)
    half_swap[...] = jnp.where(row_lane == partner_lane, 1.0, 0.0).astype(jnp.bfloat16)
    place.greet()
    fetch(part_ref)
    fold_two = Fold(place, part, near.at[0], send.at[0], far.at[0], fold_send.at[0], fold_recv.at[0])
    fold_output = Fold(
        place, part, near.at[0], send.at[0], far.at[0], fold_send.at[0], fold_recv.at[0]
    )
    fold_one = Fold(place, part, near.at[1], send.at[1], far.at[1], fold_send.at[1], fold_recv.at[1])
    gather = Gather(place, branch, gather_send, gather_recv)
    swap_heads = Swap(place, heads_out, heads_in, swap_send.at[0], swap_recv.at[0], halves)
    swap_packed = Swap(place, packed_out, packed_in, swap_send.at[1], swap_recv.at[1], halves)
    spread_near = Spread(gain_near, place.row, 4, near_fsdp, near_send, near_recv)
    spread_far = Spread(gain_far, me, 8, peer, far_send, far_recv)
    fold_two.start()

    def stage_feed(first):
        sides = ((grad_gate, normed_two), (grad_up, normed_two), (mixed, cotangents))
        left, right = sides[first // hidden_units]
        if first == 0:
            fetch(grad_gate_ref, normed_two_ref)
        elif first == hidden_units:
            fetch(grad_up_ref)

        @pl.loop(0, 2)
        def _(index):
            start = first % hidden_units + index * 256
            columns = pl.ds(pl.multiple_of(start, 256), 256)
            rows = pl.ds(pl.multiple_of(first + index * 256, 256), 256)
            own[rows, :] = product_rows(left[:, columns], right[...]).astype(jnp.bfloat16)

    stage_feed(0)

    spine_sems = (spine_up, spine_got, spine_down, spine_back)
    line_sems = (line_up, line_got, line_down, line_back)

    def spine(index):
        return Tree(place, own, out_ref, index, False, spine_in, spine_sems, leaf_back)

    def line(index):
        return Tree(place, own, out_ref, index, True, line_in, line_sems, None)

    def leaf_rows(index):
        return rows_at(index * ROUND_ROWS + (1 - side) * SPINE_ROWS, SPINE_ROWS)

    def leaf_copy(index):
        slot = lax.rem(index, RING)
        return pltpu.make_async_remote_copy(
            src_ref=own.at[leaf_rows(index)],
            dst_ref=spine_in.at[2, rows_at(slot * SPINE_ROWS, SPINE_ROWS)],
            send_sem=leaf_up.at[slot],
            recv_sem=spine_got.at[2, slot],
            **peer(other_side),
        )

    def leaf_result(index):
        slot = lax.rem(index, RING)
        return pltpu.make_async_remote_copy(
            src_ref=own.at[leaf_rows(index)],
            dst_ref=out_ref.at[leaf_rows(index)],
            send_sem=leaf_up.at[slot],
            recv_sem=leaf_back.at[slot],
            **peer(other_side),
        )

    def stage_norm_two():
        fetch(hidden_ref, cotangent_ref)
        fold_two.arrive()
        gain_part[...] = jnp.zeros_like(gain_part)

        @pl.loop(0, TILE // 16)
        def _(piece):
            span = rows_at(piece * 16, 16)
            grad = fold_two.rows(piece * 16, 16)
            unit, back = norm_back_rows(hidden[span, :], None)
            gain_part[1] += (grad * unit).reshape(2, 8, -1).sum(axis=0)
            here = rows_at(place.row * TILE + piece * 16, 16)
            total = cotangents[here, :].astype(jnp.float32) + back(grad * gain_two)
            grad_hidden[span, :] = total
            branch[here, :] = total.astype(jnp.bfloat16)

        gather.start()

    def stage_heads():
        fetch(output_weight_ref)
        gather.first()
        gather.arrive()

        @pl.loop(0, 4)
        def _(sequence):
            rows = branch[rows_at(sequence * TILE, TILE), :]
            grads = product_back(rows, output_weight[...]).astype(jnp.bfloat16)
            for head in range(2):
                heads_out[pl.ds((2 * sequence + head) * halves, halves)] = grads[
                    :, head * PAIR : (head + 1) * PAIR
                ].reshape(halves, block, PAIR)

        swap_heads.start_all()

    def stage_sort():
        fetch(packed_ref)
        sort_blocks(order_ref, packed, (q0, q1, k, v))

    def stage_output_grad():
        fetch(attended_ref)
        for head in range(2):
            rows = [
                attended[(2 * index + head) * halves : (2 * index + head + 1) * halves]
                for index in range(4)
            ]
            rows = jnp.concatenate(rows, axis=0).reshape(4 * TILE, PAIR)
            first_row = base + 2 * WIDE + head * PAIR
            for first in range(0, own.shape[1], 512):
                columns = slice(first, first + 512)
                own[first_row : first_row + PAIR, columns] = product_rows(
                    rows, branch[:, columns]
                ).astype(jnp.bfloat16)

    def stage_sort_grads():
        swap_heads.arrive()
        sort_blocks(order_ref, heads_in, (g0, g1))
        dk[...] = jnp.zeros_like(dk)
        dv[...] = jnp.zeros_like(dv)

    def stage_attention(index):
        first, top = index * tile, (index + 1) * tile
        parts = []
        for q, g in ((q0, g0), (q1, g1)):
            query_rows = q[first:top, :]
            grad_rows = g[first:top, :]
            soft = softmax_parts(query_rows, k[:top, :], first)
            grad_soft = product_back(grad_rows, v[:top, :])
            delta = jnp.sum(soft * grad_soft, axis=-1, keepdims=True)
            grad_scores = (soft * (grad_soft - delta)).astype(jnp.bfloat16)
            parts.append(product(grad_scores, k[:top, :]) * scale)
            key_term = product_rows(grad_scores, query_rows) * scale
            value_term = product_rows(soft.astype(jnp.bfloat16), grad_rows)
            dk[: top // block] += key_term.reshape(-1, block, HEAD_DIM)
            dv[: top // block] += value_term.reshape(-1, block, HEAD_DIM)
        result[first // block : top // block] = jnp.concatenate(parts, axis=-1).reshape(
            -1, block, PAIR
        )

    def stage_unsort():
        for slot in range(length // block):
            spot = order_ref[length // block + slot]
            packed_out[slot] = jnp.concatenate(
                [result[spot], dk[spot], dv[spot]], axis=-1
            ).astype(jnp.bfloat16)
        swap_packed.start_all()

    def stage_turn():
        fetch(cosine_ref, sine_ref, query_weight_ref, key_weight_ref, value_weight_ref)
        swap_packed.arrive()

        @pl.loop(0, 4)
        def _(sequence):
            span = rows_at(sequence * TILE, TILE)
            total = None
            for head in range(2):
                grads = packed_in[pl.ds((2 * sequence + head) * halves, halves)]
                grads = grads.reshape(TILE, WIDE)
                swapped = product(grads, half_swap[...])
                low = (
                    grads.astype(jnp.float32) * cosine[span, :] - swapped * sine[span, :]
                ).astype(jnp.bfloat16)
                turned[head, span, :] = low
                term = product(low, weight[head])
                total = term if total is None else total + term
            part[span, :] = total.astype(jnp.bfloat16)

        fold_one.start()

    def stage_projection_grads(head):
        if head == 0:
            fetch(normed_ref)
        query_base = base + head * PAIR
        key_base = base + WIDE + head * HEAD_DIM
        value_base = key_base + 2 * HEAD_DIM
        for first in range(0, own.shape[1], 512):
            columns = slice(first, first + 512)
            grads = product_rows(turned[head], normed[:, columns]).astype(jnp.bfloat16)
            own[query_base : query_base + PAIR, columns] = grads[:PAIR]
            own[key_base : key_base + HEAD_DIM, columns] = grads[PAIR : PAIR + HEAD_DIM]
            own[value_base : value_base + HEAD_DIM, columns] = grads[PAIR + HEAD_DIM :]

    def stage_norm_one():
        fetch(input_ref)
        fold_one.arrive()

        @pl.loop(0, TILE // 16)
        def _(piece):
            span = rows_at(piece * 16, 16)
            grad = fold_one.rows(piece * 16, 16)
            unit, back = norm_back_rows(inputs[span, :].astype(jnp.float32), None)
            gain_part[0] += (grad * unit).reshape(2, 8, -1).sum(axis=0)
            input_grad_ref[span, :] = grad_hidden[span, :] + back(grad * gain_one)

        gain_near[place.row] = jnp.sum(gain_part[...], axis=1)
        spread_near.start()

    def stage_gain():
        gain_far[me] = spread_near.total()
        spread_far.start()

    def stage_output():
        fetch(down_weight_ref)

        @pl.loop(0, 4)
        def _(sequence):
            span = rows_at(sequence * TILE, TILE)
            part[span, :] = product(
                mixed[span, :], own[base : base + hidden_units, :]
            ).astype(jnp.bfloat16)

    def stage_output_sum():
        fold_output.arrive()

        @pl.loop(0, TILE // 16)
        def _(piece):
            span = rows_at(piece * 16, 16)
            total = hidden[span, :] + fold_output.rows(piece * 16, 16)
            layer_output_ref[span, :] = total.astype(jnp.bfloat16)

    def stage_clear():
        if spare:
            own[base + 3 * WIDE :, :] = jnp.zeros((spare, width), own.dtype)

    units = 2 * 256
    stages = [
        (0, fold_two.relay),
        (0, functools.partial(stage_feed, units)),
        (0, stage_sort),
        (1, functools.partial(stage_feed, 2 * units)),
        (1, functools.partial(stage_feed, 3 * units)),
        (2, lambda: fetch(mixed_ref)),
        (2, stage_norm_two),
        (3, gather.relay),
        (3, functools.partial(stage_feed, 4 * units)),
        (3, stage_output),
        (4, stage_heads),
        (4, fold_output.start),
        (5, fold_output.relay),
        (5, functools.partial(stage_feed, 5 * units)),
        (5, stage_output_grad),
        (5, stage_clear),
        (6, stage_sort_grads),
        (8, stage_output_sum),
    ]
    stages += [(6 + index, functools.partial(stage_attention, index)) for index in range(tiles)]
    now = 6 + tiles - 1
    stages += [
        (now, stage_unsort),
        (now + 2, stage_turn),
        (now + 3, fold_one.relay),
        (now + 3, functools.partial(stage_projection_grads, 0)),
        (now + 4, functools.partial(stage_projection_grads, 1)),
        (now + 5, stage_norm_one),
        (now + 6, stage_gain),
    ]
    needed = base // ROUND_ROWS - LEAD
    assert now + 4 < needed

    for index in range(LEAD):
        leaf_copy(index).start()

    def valid(index):
        return jnp.logical_and(index >= 0, index < rounds)

    @pl.loop(0, rounds + RING)
    def _(now):
        far_side = jnp.abs(depth - 2 + side)
        off_center = jnp.abs(depth - 1 - side)
        done = now - RING + 1
        for tree in (spine(done), line(done)):
            pl.when(valid(done))(tree.finish)

        @pl.when(now + LEAD < rounds)
        def _():
            leaf_copy(now + LEAD).start()

        rising = spine(now - 3 + off_center)
        pl.when(valid(rising.index))(rising.rise)

        @pl.loop(0, 5)
        def _(age):
            tree = line(now - age)
            pl.when(jnp.logical_and(valid(tree.index), tree.rise_age == age))(tree.rise)

        falling = spine(now - 3 - off_center)
        pl.when(valid(falling.index))(falling.fall)

        @pl.loop(4, 9)
        def _(age):
            tree = line(now - age)
            pl.when(jnp.logical_and(valid(tree.index), tree.fall_age == age))(tree.fall)

        leaf_fall = now - 4 - far_side

        @pl.when(valid(leaf_fall))
        def _():
            leaf_result(leaf_fall).wait_recv()
            leaf_copy(leaf_fall).wait_send()

        for when, stage in stages:
            pl.when(now == when)(stage)

    gain_out_ref[...] = spread_far.total()


def backward(order, gain_one, gain_two, grad_gate, grad_up, mixed, normed_two, cotangents, part,
             hidden, inputs, query_weight, key_weight, value_weight, output_weight, down_weight,
             attended, packed, normed, cosine, sine, key):
    width = hidden.shape[1]
    rows = 3 * mixed.shape[1] + 3 * WIDE
    rounds = -(-rows // ROUND_ROWS)
    block = packed.shape[1]
    length = packed.shape[0] * block
    dma = pltpu.SemaphoreType.DMA
    low, full = jnp.bfloat16, jnp.float32
    any_spec = pl.BlockSpec(memory_space=pl.ANY)
    operands = (
        order, gain_one, gain_two, grad_gate, grad_up, mixed, normed_two, cotangents, part,
        hidden, inputs, query_weight, key_weight, value_weight, output_weight, down_weight,
        attended, packed, normed, cosine, sine,
    )

    def like(array):
        return pltpu.VMEM(array.shape, array.dtype)

    return pl.pallas_call(
        functools.partial(backward_kernel, rounds, block),
        out_shape=(
            jax.ShapeDtypeStruct((rounds * ROUND_ROWS, width), low),
            jax.ShapeDtypeStruct((2, width), full),
            jax.ShapeDtypeStruct((TILE, width), full),
            jax.ShapeDtypeStruct((TILE, width), low),
        ),
        in_specs=[pl.BlockSpec(memory_space=pltpu.SMEM)] + [vmem()] * 2 + [any_spec] * 18,
        out_specs=(any_spec, vmem(), vmem(), vmem()),
        scratch_shapes=[
            pltpu.VMEM((rounds * ROUND_ROWS, width), low),
            pltpu.VMEM((3, RING * SPINE_ROWS, width), low),
            pltpu.VMEM((3, RING * LINE_ROWS, width), low),
            like(grad_gate), like(grad_up), like(mixed), like(normed_two), like(cotangents),
            like(part), like(hidden), like(inputs), like(output_weight),
            like(attended), like(packed), like(normed), like(cosine), like(sine),
            pltpu.VMEM((WIDE, WIDE), low),
            pltpu.VMEM((2, WIDE, width), low),
            pltpu.VMEM((2, 2, TILE, width), low),
            pltpu.VMEM((2, TILE, width), low),
            pltpu.VMEM((2, TILE, width), low),
            pltpu.VMEM((4 * TILE, width), low),
            pltpu.VMEM((TILE, width), full),
            pltpu.VMEM((2, 8, width), full),
            pltpu.VMEM((length // block, block, PAIR), low),
            pltpu.VMEM((length // block, block, PAIR), low),
        ]
        + [pltpu.VMEM((length, HEAD_DIM), low)] * 6
        + [pltpu.VMEM((length // block, block, PAIR), full)]
        + [pltpu.VMEM((length // block, block, HEAD_DIM), full)] * 2
        + [
            pltpu.VMEM((length // block, block, WIDE), low),
            pltpu.VMEM((length // block, block, WIDE), low),
            pltpu.VMEM((2, 4 * TILE, WIDE), low),
            pltpu.VMEM((4, 2, width), full),
            pltpu.VMEM((8, 2, width), full),
            dma((21,)),
            dma((RING,)), dma((3, RING)), dma((3, RING)), dma((RING,)),
            dma((RING,)), dma((RING,)),
            dma((RING,)), dma((3, RING)), dma((3, RING)), dma((RING,)),
            dma((2, 3)), dma((2, 3)),
            dma((3,)), dma((3,)),
            dma((2, 8)), dma((2, 8)),
            dma((4,)), dma((4,)), dma((8,)), dma((8,)),
        ],
        compiler_params=pltpu.CompilerParams(
            collective_id=key, has_side_effects=True, vmem_limit_bytes=63 * 2**20
        ),
        name="backward",
    )(*operands)


def forward_kernel(
    block,
    place_ref,
    table_ref,
    gain_one_ref,
    gain_two_ref,
    input_ref,
    cotangent_ref,
    query_weight_ref,
    key_weight_ref,
    value_weight_ref,
    output_weight_ref,
    gate_weight_ref,
    up_weight_ref,
    down_weight_ref,
    place_out,
    part_out,
    hidden_out,
    attended_out,
    packed_out,
    normed_one_out,
    cosine_out,
    sine_out,
    cotangent_out,
    normed_two_out,
    mixed_out,
    grad_gate_out,
    grad_up_out,
    places,
    tables,
    inputs,
    cotangents,
    normed_one,
    normed_two,
    cosine,
    sine,
    weight,
    output_weight,
    gate_weight,
    up_weight,
    down_weight,
    packed_from,
    packed,
    q0,
    q1,
    k,
    v,
    result,
    heads_from,
    heads,
    part,
    near,
    send,
    far,
    hidden,
    mixed,
    grad_gate,
    grad_up,
    fetch_sem,
    store_sem,
    gather_send,
    gather_recv,
    swap_send,
    swap_recv,
    fold_send,
    fold_recv,
):
    place = Place()
    length, width = q0.shape[0], inputs.shape[1]
    halves = TILE // block
    half = HEAD_DIM // 2
    pair_rows = 2 * TILE
    fetches, stores = {}, []

    def fetch_all(key, *copies):
        base = sum(len(group) for group in fetches.values())
        fetches[key] = [
            pltpu.make_async_copy(part_of, target, fetch_sem.at[base + index])
            for index, (part_of, target) in enumerate(copies)
        ]
        for copy in fetches[key]:
            copy.start()

    def fetch(*keys):
        for key in keys:
            for copy in fetches[key]:
                copy.wait()

    def store(source, target):
        copy = pltpu.make_async_copy(source, target, store_sem.at[len(stores)])
        copy.start()
        stores.append(copy)

    own_rows = rows_at(place.row * TILE, TILE)
    fetch_all("inputs", (input_ref, inputs.at[own_rows]))
    fetch_all("cotangent", (cotangent_ref, cotangents.at[own_rows]))
    copies = []
    for head in range(2):
        query_base, key_base = head * PAIR, head * HEAD_DIM
        target = weight.at[head]
        heads_of = [(query_weight_ref, query_base), (query_weight_ref, query_base + HEAD_DIM)]
        heads_of += [(key_weight_ref, key_base), (value_weight_ref, key_base)]
        for index, (source, first) in enumerate(heads_of):
            copies.append(
                (source.at[pl.ds(first, HEAD_DIM)], target.at[pl.ds(index * HEAD_DIM, HEAD_DIM)])
            )
            for side in range(2):
                copies.append(
                    (
                        source.at[pl.ds(first + (1 - side) * half, half)],
                        target.at[pl.ds(WIDE + index * HEAD_DIM + side * half, half)],
                    )
                )
    fetch_all("weight", *copies)
    fetch_all("output", (output_weight_ref, output_weight))
    fetch_all("gate", (gate_weight_ref, gate_weight))
    fetch_all("up", (up_weight_ref, up_weight))
    fetch_all("down", (down_weight_ref, down_weight))
    places[pl.ds(pl.multiple_of(place.row * 8, 8), 8), :] = jnp.broadcast_to(
        place_ref[...], (8, place_ref.shape[1])
    )
    gain_one = gain_one_ref[...].astype(jnp.float32).reshape(1, -1)
    gain_two = gain_two_ref[...].astype(jnp.float32).reshape(1, -1)
    tables[own_rows, :] = table_ref[...]
    gather_places = Gather(place, places, gather_send.at[0], gather_recv.at[0], 8)
    gather_tables = Gather(place, tables, gather_send.at[1], gather_recv.at[1])
    gather_inputs = Gather(place, inputs, gather_send.at[2], gather_recv.at[2])
    gather_cotangents = Gather(place, cotangents, gather_send.at[3], gather_recv.at[3])
    gather_two = Gather(place, normed_two, gather_send.at[4], gather_recv.at[4])
    swap_places = Swap(place, places, place_out, swap_send.at[0], swap_recv.at[0], 8, 2)
    swap_packed = Swap(place, packed_from, packed, swap_send.at[1], swap_recv.at[1], halves)
    swap_heads = Swap(place, heads_from, heads, swap_send.at[2], swap_recv.at[2], halves)
    fold = Fold(place, part, near, send, far, fold_send, fold_recv)
    place.greet()
    fetch("inputs")
    gather_tables.start()
    gather_inputs.start()
    gather_places.start()
    fetch("cotangent")
    gather_cotangents.start()

    def project(chip):
        base = chip * pair_rows

        @pl.loop(0, pair_rows // 16)
        def _(piece):
            span = rows_at(base + piece * 16, 16)
            rows = inputs[span, :].astype(jnp.float32)
            normed_one[span, :] = (rows * rms_scale(rows) * gain_one).astype(jnp.bfloat16)

        span = rows_at(base, pair_rows)
        low_cosine, low_sine = tables[span, :half], tables[span, half:HEAD_DIM]
        ones = jnp.ones((pair_rows, HEAD_DIM), jnp.float32)
        cosine[span, :] = jnp.concatenate([low_cosine] * 6 + [ones], axis=-1)
        sine[span, :] = jnp.concatenate([-low_sine, low_sine] * 3 + [ones * 0.0], axis=-1)

        for head in range(2):
            products = product_back(normed_one[span, :], weight[head])
            low = (
                products[:, :WIDE] * cosine[span, :] + products[:, WIDE:] * sine[span, :]
            ).astype(jnp.bfloat16)
            for index in range(2):
                packed_from[pl.ds(((2 * chip + index) * 2 + head) * halves, halves)] = low[
                    index * TILE : (index + 1) * TILE
                ].reshape(halves, block, WIDE)
        for index in range(4):
            swap_packed.start(4 * chip + index)

    gather_tables.first()
    gather_inputs.first()
    gather_places.first()
    fetch("weight")
    project(place.chip)
    gather_tables.relay()
    gather_inputs.relay()
    gather_places.relay()
    gather_tables.arrive()
    gather_inputs.arrive()
    gather_places.arrive()
    project(1 - place.chip)
    swap_places.start_all()
    store(normed_one, normed_one_out)
    store(cosine, cosine_out)
    store(sine, sine_out)
    swap_places.arrive()
    swap_packed.arrive()
    store(packed, packed_out)

    def place_row(first, count):
        blocks = [place_out[8 * index : 8 * index + 1, :] for index in range(first, first + count)]
        return jnp.concatenate(blocks, axis=-1)

    tile = min(256, length)
    order = place_row(0, length // TILE)
    flat = packed[...].reshape(length, WIDE)
    for first in range(0, length, tile):
        rows = lax.broadcasted_iota(jnp.int32, (tile, length), 0) + first
        chosen = jnp.where(rows == order, 1.0, 0.0).astype(jnp.bfloat16)
        moved = product(chosen, flat).astype(jnp.bfloat16)
        for index, target in enumerate((q0, q1, k, v)):
            target[first : first + tile, :] = moved[:, index * HEAD_DIM : (index + 1) * HEAD_DIM]
    for first in range(0, length, tile):
        parts = []
        for q in (q0, q1):
            soft = softmax_parts(q[first : first + tile, :], k[: first + tile, :], first)
            parts.append(product(soft.astype(jnp.bfloat16), v[: first + tile, :]))
        result[first : first + tile, :] = jnp.concatenate(parts, axis=-1).astype(jnp.bfloat16)
    for first in range(0, length, tile):
        rows = lax.broadcasted_iota(jnp.int32, (length, tile), 0)
        chosen = jnp.where(rows == place_row(first // TILE, tile // TILE), 1.0, 0.0)
        moved = product_rows(chosen.astype(jnp.bfloat16), result[...]).astype(jnp.bfloat16)
        heads_from[first // block : (first + tile) // block] = moved.reshape(-1, block, PAIR)
    swap_heads.start_all()
    gather_cotangents.first()
    gather_cotangents.relay()
    fetch("output")
    swap_heads.arrive()
    store(heads, attended_out)

    @pl.loop(0, 4)
    def _(sequence):
        total = None
        for head in range(2):
            rows = heads[pl.ds((2 * sequence + head) * halves, halves)].reshape(TILE, PAIR)
            term = product(rows, output_weight[head * PAIR : (head + 1) * PAIR, :])
            total = term if total is None else total + term
        part[rows_at(sequence * TILE, TILE), :] = total.astype(jnp.bfloat16)

    fold.start()
    gather_cotangents.arrive()
    store(cotangents, cotangent_out)
    fold.relay()
    fold.arrive()

    @pl.loop(0, TILE // 16)
    def _(piece):
        span = rows_at(piece * 16, 16)
        own = rows_at(place.row * TILE + piece * 16, 16)
        rows = inputs[own, :].astype(jnp.float32) + fold.rows(piece * 16, 16)
        hidden[span, :] = rows
        normed_two[own, :] = (rows * rms_scale(rows) * gain_two).astype(jnp.bfloat16)

    gather_two.start()
    store(hidden, hidden_out)
    fetch("gate", "up", "down")

    def feed(chip):
        span = rows_at(chip * pair_rows, pair_rows)

        @pl.loop(0, mixed.shape[1] // 256)
        def _(index):
            units = rows_at(index * 256, 256)
            columns = pl.ds(pl.multiple_of(index * 256, 256), 256)
            gate = product_back(normed_two[span, :], gate_weight[units, :])
            upward = product_back(normed_two[span, :], up_weight[units, :])
            grad_mixed = product_back(cotangents[span, :], down_weight[units, :])
            sigmoid = jax.nn.sigmoid(gate)
            activated = gate * sigmoid
            mixed[span, columns] = (activated * upward).astype(jnp.bfloat16)
            grad_gate[span, columns] = (
                grad_mixed * upward * sigmoid * (1.0 + gate * (1.0 - sigmoid))
            ).astype(jnp.bfloat16)
            grad_up[span, columns] = (grad_mixed * activated).astype(jnp.bfloat16)

        @pl.loop(0, width // 512)
        def _(index):
            columns = pl.ds(pl.multiple_of(index * 512, 512), 512)
            part[span, columns] = (
                product(grad_gate[span, :], gate_weight[:, columns])
                + product(grad_up[span, :], up_weight[:, columns])
            ).astype(jnp.bfloat16)

    gather_two.first()
    feed(place.chip)
    gather_two.relay()
    gather_two.arrive()
    store(normed_two, normed_two_out)
    feed(1 - place.chip)
    store(part, part_out)
    store(mixed, mixed_out)
    store(grad_gate, grad_gate_out)
    store(grad_up, grad_up_out)
    for copy in stores:
        copy.wait()


def forward(places, table, gain_one, gain_two, inputs, cotangent, query_weight, key_weight, value_weight,
            output_weight, gate_weight, up_weight, down_weight, length, block, key):
    width = inputs.shape[1]
    hidden_units = gate_weight.shape[0]
    rows = 4 * TILE
    blocks = length // block
    low, full = jnp.bfloat16, jnp.float32
    dma = pltpu.SemaphoreType.DMA
    any_spec = pl.BlockSpec(memory_space=pl.ANY)

    def out(shape, dtype):
        return jax.ShapeDtypeStruct(shape, dtype)

    wide = (rows, width)
    return pl.pallas_call(
        functools.partial(forward_kernel, block),
        out_shape=(
            out((64, 128), jnp.int32),
            out(wide, low), out((TILE, width), full),
            out((blocks, block, PAIR), low), out((blocks, block, WIDE), low),
            out(wide, low), out((rows, WIDE), full), out((rows, WIDE), full),
            out(wide, low), out(wide, low),
            out((rows, hidden_units), low), out((rows, hidden_units), low),
            out((rows, hidden_units), low),
        ),
        in_specs=[vmem()] * 4 + [any_spec] * 9,
        out_specs=(vmem(),) + (any_spec,) * 12,
        scratch_shapes=[
            pltpu.VMEM((32, 128), jnp.int32),
            pltpu.VMEM((rows, 128), full),
            pltpu.VMEM(wide, low), pltpu.VMEM(wide, low),
            pltpu.VMEM(wide, low), pltpu.VMEM(wide, low),
            pltpu.VMEM((rows, WIDE), full), pltpu.VMEM((rows, WIDE), full),
            pltpu.VMEM((2, 2 * WIDE, width), low),
            pltpu.VMEM(output_weight.shape, low),
            pltpu.VMEM((hidden_units, width), low), pltpu.VMEM((hidden_units, width), low),
            pltpu.VMEM((hidden_units, width), low),
            pltpu.VMEM((blocks, block, WIDE), low), pltpu.VMEM((blocks, block, WIDE), low),
        ]
        + [pltpu.VMEM((length, HEAD_DIM), low)] * 4
        + [
            pltpu.VMEM((length, PAIR), low),
            pltpu.VMEM((blocks, block, PAIR), low), pltpu.VMEM((blocks, block, PAIR), low),
            pltpu.VMEM(wide, low),
            pltpu.VMEM((2, TILE, width), low),
            pltpu.VMEM((TILE, width), low), pltpu.VMEM((TILE, width), low),
            pltpu.VMEM((TILE, width), full),
            pltpu.VMEM((rows, hidden_units), low), pltpu.VMEM((rows, hidden_units), low),
            pltpu.VMEM((rows, hidden_units), low),
            dma((30,)), dma((12,)),
            dma((5, 3)), dma((5, 3)),
            dma((3, 8)), dma((3, 8)),
            dma((3,)), dma((3,)),
        ],
        compiler_params=pltpu.CompilerParams(
            collective_id=key, has_side_effects=True, vmem_limit_bytes=63 * 2**20
        ),
        name="forward",
    )(places, table, gain_one, gain_two, inputs, cotangent, query_weight, key_weight, value_weight,
      output_weight, gate_weight, up_weight, down_weight)


def widen_kernel(plan, source, *refs):
    targets, (low, full, load_sem, store_sem) = refs[:-4], refs[-4:]
    slots = low.shape[0]
    loads, stores = [], []
    for index, (first, which, target_row, chunk) in enumerate(plan):
        slot = index % slots
        span = pl.ds(0, chunk)
        loads.append(
            pltpu.make_async_copy(
                source.at[pl.ds(first, chunk)], low.at[slot, span], load_sem.at[slot]
            )
        )
        stores.append(
            pltpu.make_async_copy(
                full.at[slot, span],
                targets[which].at[pl.ds(target_row, chunk)],
                store_sem.at[slot],
            )
        )
    for load in loads[:slots]:
        load.start()
    for index, (load, store) in enumerate(zip(loads, stores)):
        slot = index % slots
        load.wait()
        if index >= slots:
            stores[index - slots].wait()

        @pl.loop(0, plan[index][3] // 16)
        def _(piece):
            span = rows_at(piece * 16, 16)
            full[slot, span, :] = low[slot, span, :].astype(jnp.float32)

        store.start()
        if index + slots < len(plan):
            loads[index + slots].start()
    for store in stores[-slots:]:
        store.wait()


def widen(values, counts):
    slots, width, first, plan = 6, values.shape[1], 0, []
    for which, count in enumerate(counts):
        chunk = math.gcd(count, 256) if count % 192 else 192
        plan += [(first + row, which, row, chunk) for row in range(0, count, chunk)]
        first += count
    any_spec = pl.BlockSpec(memory_space=pl.ANY)
    return pl.pallas_call(
        functools.partial(widen_kernel, plan),
        out_shape=tuple(jax.ShapeDtypeStruct((count, width), jnp.float32) for count in counts),
        in_specs=[any_spec],
        out_specs=(any_spec,) * len(counts),
        scratch_shapes=[
            pltpu.VMEM((slots, 256, width), values.dtype),
            pltpu.VMEM((slots, 256, width), jnp.float32),
            pltpu.SemaphoreType.DMA((slots,)),
            pltpu.SemaphoreType.DMA((slots,)),
        ],
        compiler_params=pltpu.CompilerParams(vmem_limit_bytes=63 * 2**20),
        name="widen",
    )(values)


def gather_rows(values):
    return lax.all_gather(values, "fsdp", axis=0, tiled=True)


def scatter_rows(values):
    return lax.psum_scatter(
        values.astype(jnp.bfloat16), "fsdp", scatter_dimension=0, tiled=True
    ).astype(jnp.float32)


def per_device_gathered(
    inputs,
    positions,
    cotangent,
    attention_gain,
    query_weight,
    key_weight,
    value_weight,
    output_weight,
    feedforward_gain,
    gate_weight,
    up_weight,
    down_weight,
):
    row_count = inputs.shape[0]
    groups = HEADS // KV_HEADS
    gain_one = attention_gain.astype(jnp.float32)
    gain_two = feedforward_gain.astype(jnp.float32)
    seq_count = lax.axis_size("fsdp")
    first_row = lax.axis_index("fsdp") * row_count

    def own(values):
        return lax.dynamic_slice_in_dim(values, first_row, row_count, 0)

    query_places = gather_rows(positions).reshape(seq_count, row_count)
    key_places = lax.all_gather(query_places, "ctx", axis=1, tiled=True)
    all_cotangent = gather_rows(cotangent)
    flat_in = gather_rows(inputs).astype(jnp.float32)
    scale_one = rms_scale(flat_in)
    unit_one = flat_in * scale_one
    normed_one = (unit_one * gain_one).astype(jnp.bfloat16)
    total_rows = normed_one.shape[0]
    cosine, sine = rotary_tables(query_places.reshape(-1))
    query_heads = query_weight.shape[0] // HEAD_DIM
    kv_heads = key_weight.shape[0] // HEAD_DIM
    kv_width = kv_heads * HEAD_DIM
    query_low = rotate(
        product_back(normed_one, query_weight).reshape(total_rows, query_heads, HEAD_DIM), cosine, sine
    ).astype(jnp.bfloat16)
    key_low = rotate(
        product_back(normed_one, key_weight).reshape(total_rows, kv_heads, HEAD_DIM), cosine, sine
    ).astype(jnp.bfloat16)
    value_low = product_back(normed_one, value_weight).astype(jnp.bfloat16)
    ctx_size = lax.axis_size("ctx")

    def spread(values):
        rows = lax.all_gather(values, "ctx", axis=0, tiled=True)
        rows = rows.reshape(ctx_size, seq_count, row_count, kv_width).swapaxes(0, 1)
        return rows.reshape(seq_count, ctx_size * row_count, kv_width)

    def collect(values):
        rows = values.astype(jnp.bfloat16).swapaxes(1, 2)
        rows = rows.reshape(seq_count, ctx_size, row_count, kv_width).swapaxes(0, 1)
        return lax.psum_scatter(
            rows.reshape(-1, kv_width), "ctx", scatter_dimension=0, tiled=True
        )

    all_keys = spread(key_low.reshape(total_rows, kv_width))
    all_values = spread(value_low)
    total_keys = all_keys.shape[1]
    key_grid = all_keys.reshape(seq_count, total_keys, kv_heads, HEAD_DIM).swapaxes(1, 2)
    value_grid = all_values.reshape(seq_count, total_keys, kv_heads, HEAD_DIM).swapaxes(1, 2)
    query_grouped = query_low.reshape(seq_count, row_count, kv_heads, groups, HEAD_DIM)
    attended, log_total = attend_forward(
        query_grouped, query_places, key_grid, value_grid, key_places
    )
    attended_low = attended.reshape(total_rows, query_heads * HEAD_DIM).astype(jnp.bfloat16)
    hidden_state = inputs.astype(jnp.float32) + scatter_rows(product(attended_low, output_weight))
    scale_two = rms_scale(hidden_state)
    unit_two = hidden_state * scale_two
    normed_two = gather_rows((unit_two * gain_two).astype(jnp.bfloat16))
    gate_values = product_back(normed_two, gate_weight)
    upward = product_back(normed_two, up_weight)
    sigmoid_gate = jax.nn.sigmoid(gate_values)
    activated = gate_values * sigmoid_gate
    mixed_hidden = (activated * upward).astype(jnp.bfloat16)
    grad_out = cotangent.astype(jnp.float32)
    grad_down = product_rows(mixed_hidden, all_cotangent)
    grad_mixed = product_back(all_cotangent, down_weight)
    grad_gate_low = (
        grad_mixed * upward * sigmoid_gate * (1.0 + gate_values * (1.0 - sigmoid_gate))
    ).astype(jnp.bfloat16)
    grad_up_low = (grad_mixed * activated).astype(jnp.bfloat16)
    grad_unit_part = (
        product(grad_gate_low, gate_weight) + product(grad_up_low, up_weight)
    ).astype(jnp.bfloat16)
    grad_normed_two = scatter_rows(grad_unit_part)
    gain_two_grad = jnp.sum(grad_normed_two * unit_two, axis=0)
    grad_hidden = grad_out + norm_back(scale_two, unit_two, grad_normed_two * gain_two)
    branch_rows = gather_rows(grad_hidden.astype(jnp.bfloat16))
    layer_output = (hidden_state + scatter_rows(product(mixed_hidden, down_weight))).astype(
        jnp.bfloat16
    )
    grad_gate = product_rows(grad_gate_low, normed_two)
    grad_up = product_rows(grad_up_low, normed_two)
    grad_output = product_rows(attended_low, branch_rows)
    grad_attended = product_back(branch_rows, output_weight).astype(jnp.bfloat16)
    grad_attended = grad_attended.reshape(seq_count, row_count, kv_heads, groups, HEAD_DIM)
    grad_query_rot, grad_key_all, grad_value_all = attend_backward(
        query_grouped, query_places, key_grid, value_grid, key_places, log_total, grad_attended
    )
    grad_key_own = collect(grad_key_all).astype(jnp.float32)
    grad_value_low = collect(grad_value_all)
    grad_query_low = (
        rotate_back(grad_query_rot.reshape(total_rows, query_heads, HEAD_DIM), cosine, sine)
        .reshape(total_rows, query_heads * HEAD_DIM)
        .astype(jnp.bfloat16)
    )
    grad_key_low = (
        rotate_back(
            grad_key_own.reshape(total_rows, kv_heads, HEAD_DIM), cosine, sine
        )
        .reshape(total_rows, kv_width)
        .astype(jnp.bfloat16)
    )
    grad_query = product_rows(grad_query_low, normed_one)
    grad_key = product_rows(grad_key_low, normed_one)
    grad_value = product_rows(grad_value_low, normed_one)
    grad_normed_one = scatter_rows(
        product(grad_query_low, query_weight)
        + product(grad_key_low, key_weight)
        + product(grad_value_low, value_weight)
    )
    own_unit = own(unit_one)
    gain_one_grad = jnp.sum(grad_normed_one * own_unit, axis=0)
    input_grad = grad_hidden + norm_back(own(scale_one), own_unit, grad_normed_one * gain_one)

    grads = (grad_query, grad_key, grad_value, grad_output, grad_gate, grad_up, grad_down)
    parts = [lax.psum(grad.astype(jnp.bfloat16), "ctx").astype(jnp.float32) for grad in grads]
    gain_sums = lax.psum(jnp.stack([gain_one_grad, gain_two_grad]), ("fsdp", "ctx"))
    return (
        layer_output,
        input_grad,
        gain_sums[0],
        parts[0],
        parts[1],
        parts[2],
        parts[3],
        gain_sums[1],
        parts[4],
        parts[5],
        parts[6],
    )


def per_device_by_head(
    inputs,
    positions,
    cotangent,
    attention_gain,
    query_weight,
    key_weight,
    value_weight,
    output_weight,
    feedforward_gain,
    gate_weight,
    up_weight,
    down_weight,
):
    gain_one, gain_two = attention_gain, feedforward_gain
    block = TILE // 2
    length = TILE * 8
    cosine, sine = rotary_tables(positions)
    table = jnp.concatenate([cosine[:, 0, :], sine[:, 0, :]], axis=1)
    table = jnp.pad(table, ((0, 0), (0, 128 - table.shape[1])))
    (
        places, part, hidden, attended, packed, normed_one, wide_cosine, wide_sine,
        cotangents, normed_two, mixed, grad_gate, grad_up,
    ) = forward(
        positions[None, :], table, gain_one, gain_two, inputs, cotangent, query_weight,
        key_weight, value_weight, output_weight, gate_weight, up_weight, down_weight, length,
        block, 1,
    )
    starts = places.reshape(8, 8, TILE)[:, 0, ::block].reshape(-1) // block
    slots = jnp.arange(length // block, dtype=jnp.int32)
    found = jnp.where(starts[None, :] == slots[:, None], slots[None, :], 0)
    order = jnp.concatenate([jnp.sum(found, axis=1), starts]).astype(jnp.int32)
    summed, gain_sums, input_grad, layer_output = backward(
        order, gain_one, gain_two, grad_gate, grad_up, mixed, normed_two, cotangents, part,
        hidden, inputs, query_weight, key_weight, value_weight, output_weight, down_weight,
        attended, packed, normed_one, wide_cosine, wide_sine, 5,
    )
    owners = (gate_weight, up_weight, down_weight, query_weight, key_weight, value_weight,
              output_weight)
    parts = widen(summed, [owner.shape[0] for owner in owners])
    return (layer_output, input_grad, gain_sums[0], *parts[3:], gain_sums[1], *parts[:3])


def per_device(*arrays):
    fits = lax.axis_size("fsdp") == 4 and lax.axis_size("ctx") == 8
    return (per_device_by_head if fits else per_device_gathered)(*arrays)


def solution(mesh):
    in_specs = (
        P(("fsdp", "ctx"), None),
        P(("fsdp", "ctx")),
        P(("fsdp", "ctx"), None),
        P(),
        P("fsdp", None),
        P("fsdp", None),
        P("fsdp", None),
        P("fsdp", None),
        P(),
        P("fsdp", None),
        P("fsdp", None),
        P("fsdp", None),
    )
    out_specs = (
        P(("fsdp", "ctx"), None),
        P(("fsdp", "ctx"), None),
        P(),
        P("fsdp", None),
        P("fsdp", None),
        P("fsdp", None),
        P("fsdp", None),
        P(),
        P("fsdp", None),
        P("fsdp", None),
        P("fsdp", None),
    )
    return jax.shard_map(
        per_device, mesh=mesh, in_specs=in_specs, out_specs=out_specs, check_vma=False
    )
```

```python
import functools
import math

import jax
import jax.numpy as jnp
from jax import lax
from jax.experimental import pallas as pl
from jax.experimental.pallas import tpu as pltpu
from jax.sharding import PartitionSpec as P

HEADS = 16
KV_HEADS = 8
HEAD_DIM = 96


EPSILON = 1e-05
ROPE_BASE = 100000.0


def product(left, right):
    return jnp.dot(left, right, preferred_element_type=jnp.float32)


def product_back(left, right):
    return lax.dot_general(
        left, right, (((1,), (1,)), ((), ())), preferred_element_type=jnp.float32
    )


def product_rows(left, right):
    return lax.dot_general(
        left, right, (((0,), (0,)), ((), ())), preferred_element_type=jnp.float32
    )


def rms_scale(values):
    return lax.rsqrt(jnp.mean(values * values, axis=-1, keepdims=True) + EPSILON)


def norm_back(scale_rows, unit_rows, grad_unit):
    return scale_rows * (
        grad_unit - unit_rows * jnp.mean(grad_unit * unit_rows, axis=-1, keepdims=True)
    )


def rotary_tables(places):
    half_width = HEAD_DIM // 2
    frequencies = ROPE_BASE ** (-(jnp.arange(half_width, dtype=jnp.float32) * 2.0 / HEAD_DIM))
    angles = places.astype(jnp.float32)[:, None] * frequencies[None, :]
    return (jnp.cos(angles)[:, None, :], jnp.sin(angles)[:, None, :])


def rotate(values, cosine, sine):
    half_width = values.shape[-1] // 2
    lower_half = values[..., :half_width]
    upper_half = values[..., half_width:]
    return jnp.concatenate(
        [lower_half * cosine - upper_half * sine, upper_half * cosine + lower_half * sine], axis=-1
    )


def rotate_back(grads, cosine, sine):
    half_width = grads.shape[-1] // 2
    lower_half = grads[..., :half_width]
    upper_half = grads[..., half_width:]
    return jnp.concatenate(
        [lower_half * cosine + upper_half * sine, upper_half * cosine - lower_half * sine], axis=-1
    )


def block_total_of(total_keys):
    return max(1, total_keys // 512)


def masked_scores(query_grouped, query_places, key_rows, key_places, start, width):
    key_part = lax.dynamic_slice_in_dim(key_rows, start, width, 2)
    place_part = lax.dynamic_slice_in_dim(key_places, start, width, 1)
    scores = jnp.einsum(
        "sqhgd,shkd->shgqk", query_grouped, key_part, preferred_element_type=jnp.float32
    )
    scores = scores * (1.0 / math.sqrt(HEAD_DIM))
    allowed = place_part[:, None, None, None, :] <= query_places[:, None, None, :, None]
    return jnp.where(allowed, scores, -1000000000.0)


def attend_forward(query_grouped, query_places, key_rows, value_rows, key_places):
    seq_count, row_count, head_groups, group_size = query_grouped.shape[:4]
    total_keys = key_rows.shape[2]
    block_total = block_total_of(total_keys)
    width = total_keys // block_total
    stat_shape = (seq_count, head_groups, group_size, row_count)

    def peak_step(index, carry):
        running_top, running_sum = carry
        scores = masked_scores(
            query_grouped, query_places, key_rows, key_places, index * width, width
        )
        new_top = jnp.maximum(running_top, jnp.max(scores, axis=-1))
        running_sum = running_sum * jnp.exp(running_top - new_top) + jnp.sum(
            jnp.exp(scores - new_top[..., None]), axis=-1
        )
        return (new_top, running_sum)

    running_top, running_sum = lax.fori_loop(
        0,
        block_total,
        peak_step,
        (jnp.full(stat_shape, -1e30, jnp.float32), jnp.zeros(stat_shape, jnp.float32)),
    )
    log_total = running_top + jnp.log(running_sum)

    def value_step(index, gathered):
        scores = masked_scores(
            query_grouped, query_places, key_rows, key_places, index * width, width
        )
        soft_low = jnp.exp(scores - log_total[..., None]).astype(jnp.bfloat16)
        value_part = lax.dynamic_slice_in_dim(value_rows, index * width, width, 2)
        return gathered + jnp.einsum(
            "shgqk,shkd->sqhgd", soft_low, value_part, preferred_element_type=jnp.float32
        )

    attended = lax.fori_loop(
        0, block_total, value_step, jnp.zeros(query_grouped.shape, jnp.float32)
    )
    return (attended, log_total)


def attend_backward(
    query_grouped, query_places, key_rows, value_rows, key_places, log_total, grad_attended
):
    total_keys = key_rows.shape[2]
    block_total = block_total_of(total_keys)
    width = total_keys // block_total
    score_scale = 1.0 / math.sqrt(HEAD_DIM)

    def soft_and_grad(index):
        scores = masked_scores(
            query_grouped, query_places, key_rows, key_places, index * width, width
        )
        soft_values = jnp.exp(scores - log_total[..., None])
        value_part = lax.dynamic_slice_in_dim(value_rows, index * width, width, 2)
        grad_soft = jnp.einsum(
            "sqhgd,shkd->shgqk", grad_attended, value_part, preferred_element_type=jnp.float32
        )
        return (soft_values, grad_soft)

    def delta_step(index, row_delta):
        soft_values, grad_soft = soft_and_grad(index)
        return row_delta + jnp.sum(soft_values * grad_soft, axis=-1)

    row_delta = lax.fori_loop(0, block_total, delta_step, jnp.zeros(log_total.shape, jnp.float32))

    def grad_step(index, carry):
        grad_query, grad_keys, grad_values = carry
        soft_values, grad_soft = soft_and_grad(index)
        grad_scores = (soft_values * (grad_soft - row_delta[..., None])).astype(jnp.bfloat16)
        key_part = lax.dynamic_slice_in_dim(key_rows, index * width, width, 2)
        grad_query = (
            grad_query
            + jnp.einsum(
                "shgqk,shkd->sqhgd", grad_scores, key_part, preferred_element_type=jnp.float32
            )
            * score_scale
        )
        key_term = (
            jnp.einsum(
                "shgqk,sqhgd->shkd", grad_scores, query_grouped, preferred_element_type=jnp.float32
            )
            * score_scale
        )
        value_term = jnp.einsum(
            "shgqk,sqhgd->shkd",
            soft_values.astype(jnp.bfloat16),
            grad_attended,
            preferred_element_type=jnp.float32,
        )
        grad_keys = lax.dynamic_update_slice_in_dim(grad_keys, key_term, index * width, 2)
        grad_values = lax.dynamic_update_slice_in_dim(grad_values, value_term, index * width, 2)
        return (grad_query, grad_keys, grad_values)

    initial = (
        jnp.zeros(query_grouped.shape, jnp.float32),
        jnp.zeros(key_rows.shape, jnp.float32),
        jnp.zeros(value_rows.shape, jnp.float32),
    )
    return lax.fori_loop(0, block_total, grad_step, initial)


def vmem():
    return pl.BlockSpec(memory_space=pltpu.VMEM)


def peer(ctx_index):
    return dict(device_id={"ctx": ctx_index}, device_id_type=pl.DeviceIdType.MESH)


SPINE_ROWS = 32
LINE_ROWS = 32
ROUND_ROWS = 2 * SPINE_ROWS + LINE_ROWS
LEAD = 4
HOP = 2
FEED = (1, 3, 5, 8)
CHAIN = (0, 4, 6, 8, 10, 12, 19, 22, 26, 28)
RING = 20
TILE = 128
PAIR = (HEADS // KV_HEADS) * HEAD_DIM
WIDE = PAIR + 2 * HEAD_DIM


def near_fsdp(index):
    return dict(device_id={"fsdp": index}, device_id_type=pl.DeviceIdType.MESH)


def rows_at(start, count):
    return pl.ds(pl.multiple_of(start, 16), count)


class Place:
    def __init__(self):
        self.ctx = lax.axis_index("ctx")
        self.row = lax.axis_index("fsdp")
        self.chip, self.core = lax.div(self.row, 2), lax.rem(self.row, 2)
        self.partner = 2 * self.chip + 1 - self.core
        self.across = 2 * (1 - self.chip) + self.core
        self.corner = 2 * (1 - self.chip) + 1 - self.core

    def greet(self):
        barrier = pltpu.get_barrier_semaphore()
        for step in range(1, 4):
            pl.semaphore_signal(barrier, inc=1, **near_fsdp(lax.rem(self.row + step, 4)))
        for step in range(1, 8):
            pl.semaphore_signal(barrier, inc=1, **peer(lax.rem(self.ctx + step, 8)))
        pl.semaphore_wait(barrier, 10)


class Fold:
    def __init__(self, place, part, near, send, far, send_sem, recv_sem):
        self.place, self.part, self.near, self.send, self.far = place, part, near, send, far
        self.send_sem, self.recv_sem = send_sem, recv_sem

    def partner_copy(self, chip):
        block = 2 * chip + 1 - self.place.core
        return pltpu.make_async_remote_copy(
            src_ref=self.part.at[rows_at(block * TILE, TILE)],
            dst_ref=self.near.at[chip],
            send_sem=self.send_sem.at[chip],
            recv_sem=self.recv_sem.at[chip],
            **near_fsdp(self.place.partner),
        )

    def across_copy(self):
        return pltpu.make_async_remote_copy(
            src_ref=self.send,
            dst_ref=self.far,
            send_sem=self.send_sem.at[2],
            recv_sem=self.recv_sem.at[2],
            **near_fsdp(self.place.across),
        )

    def start(self):
        self.partner_copy(1 - self.place.chip).start()
        self.partner_copy(self.place.chip).start()

    def relay(self):
        there = 1 - self.place.chip
        self.partner_copy(there).wait_recv()
        base = self.place.across * TILE

        @pl.loop(0, TILE // 32)
        def _(piece):
            mine = self.part[rows_at(base + piece * 32, 32), :].astype(jnp.float32)
            span = rows_at(piece * 32, 32)
            self.send[span, :] = (
                mine + self.near[there, span, :].astype(jnp.float32)
            ).astype(jnp.bfloat16)

        self.across_copy().start()

    def arrive(self):
        self.partner_copy(self.place.chip).wait_recv()
        copy = self.across_copy()
        copy.wait_recv()
        copy.wait_send()
        self.partner_copy(0).wait_send()
        self.partner_copy(1).wait_send()

    def rows(self, start, count):
        mine = self.part[rows_at(self.place.row * TILE + start, count), :].astype(jnp.float32)
        span = rows_at(start, count)
        near = self.near[self.place.chip, span, :].astype(jnp.float32)
        return mine + near + self.far[span, :].astype(jnp.float32)


class Gather:
    def __init__(self, place, full, send_sem, recv_sem, count=TILE):
        self.place, self.full, self.send_sem, self.recv_sem = place, full, send_sem, recv_sem
        self.count = count

    def copy(self, block, target, key):
        span = pl.ds(pl.multiple_of(block * self.count, self.count), self.count)
        return pltpu.make_async_remote_copy(
            src_ref=self.full.at[span],
            dst_ref=self.full.at[span],
            send_sem=self.send_sem.at[key],
            recv_sem=self.recv_sem.at[key],
            **near_fsdp(target),
        )

    def start(self):
        self.copy(self.place.row, self.place.across, 1).start()
        self.copy(self.place.row, self.place.partner, 0).start()

    def relay(self):
        self.copy(self.place.across, self.place.across, 1).wait_recv()
        self.copy(self.place.across, self.place.partner, 2).start()

    def first(self):
        self.copy(self.place.partner, self.place.partner, 0).wait_recv()

    def arrive(self):
        self.copy(self.place.corner, self.place.partner, 2).wait_recv()
        self.copy(self.place.row, self.place.across, 1).wait_send()
        self.copy(self.place.row, self.place.partner, 0).wait_send()
        self.copy(self.place.across, self.place.partner, 2).wait_send()


class Swap:
    def __init__(self, place, source, target, send_sem, recv_sem, count, share=1):
        self.place, self.source, self.target = place, source, target
        self.send_sem, self.recv_sem, self.count, self.share = send_sem, recv_sem, count, share

    def span(self, index):
        return pl.ds(pl.multiple_of(index * self.count, self.count), self.count)

    def copy(self, other, sender):
        return pltpu.make_async_remote_copy(
            src_ref=self.source.at[self.span(lax.div(other, self.share))],
            dst_ref=self.target.at[self.span(sender)],
            send_sem=self.send_sem.at[other],
            recv_sem=self.recv_sem.at[sender],
            **peer(other),
        )

    def start(self, other):
        me = self.place.ctx

        @pl.when(other != me)
        def _():
            self.copy(other, me).start()

        @pl.when(other == me)
        def _():
            self.target[self.span(me)] = self.source[self.span(lax.div(me, self.share))]

    def start_all(self):
        for step in range(1, 9):
            self.start(lax.rem(self.place.ctx + step, 8))

    def arrive(self):
        for step in range(1, 8):
            other = lax.rem(self.place.ctx + step, 8)
            self.copy(other, other).wait()


class Spread:
    def __init__(self, slots, index, count, device, send_sem, recv_sem):
        self.slots, self.index, self.count, self.device = slots, index, count, device
        self.send_sem, self.recv_sem = send_sem, recv_sem

    def copy(self, step):
        return pltpu.make_async_remote_copy(
            src_ref=self.slots.at[self.index],
            dst_ref=self.slots.at[self.index],
            send_sem=self.send_sem.at[step],
            recv_sem=self.recv_sem.at[step],
            **self.device(lax.rem(self.index + step, self.count)),
        )

    def start(self):
        for step in range(1, self.count):
            self.copy(step).start()

    def total(self):
        for step in range(1, self.count):
            self.copy(step).wait()
        result = self.slots[0]
        for step in range(1, self.count):
            result += self.slots[step]
        return result


class Tree:
    def __init__(self, place, own, out_ref, index, line, box, sems, leaf_back):
        me = place.ctx
        depth, side = lax.div(me, 2), lax.rem(me, 2)
        other_side = me + 1 - 2 * side
        self.own, self.out, self.box, self.index, self.line = own, out_ref, box, index, line
        self.up, self.got, self.down, self.back = sems
        self.leaf_back = leaf_back
        if line:
            center = lax.rem(index, 4)
            count = LINE_ROWS
            start = index * ROUND_ROWS + 2 * SPINE_ROWS
            root_side = lax.rem(index, 2)
            on_cross = depth == center
            self.root = jnp.logical_and(on_cross, side == root_side)
            has_side = self.root
            to_side = jnp.logical_and(on_cross, side != root_side)
            reach = jnp.maximum(center, 3 - center)
            away = jnp.abs(depth - center)
            crossed = jnp.where(side == root_side, 0, 1)
            self.rise_age = reach - away + jnp.where(self.root, 1, 0)
            self.fall_age = reach + 1 + away + crossed
        else:
            center = 1 + side
            count = SPINE_ROWS
            start = index * ROUND_ROWS + side * SPINE_ROWS
            self.root = depth == center
            has_side = None
        self.count = count
        self.start = start
        self.slot = lax.rem(index, RING)
        self.rows = rows_at(start, count)
        self.children = (
            (jnp.logical_and(depth > 0, depth <= center), me - 2, 0),
            (jnp.logical_and(depth < 3, depth >= center), me + 2, 1),
            (has_side, other_side, 2),
        )
        parent = jnp.where(depth < center, me + 2, me - 2)
        slot = jnp.where(depth < center, 0, 1)
        if line:
            parent = jnp.where(to_side, other_side, parent)
            slot = jnp.where(to_side, 2, slot)
        self.parent = jnp.where(self.root, other_side, parent)
        self.parent_slot = jnp.where(self.root, 2, slot)

    def boxed(self, slot):
        return self.box.at[slot, rows_at(self.slot * self.count, self.count)]

    def up_copy(self, target, slot):
        return pltpu.make_async_remote_copy(
            src_ref=self.own.at[self.rows],
            dst_ref=self.boxed(slot),
            send_sem=self.up.at[self.slot],
            recv_sem=self.got.at[slot, self.slot],
            **peer(target),
        )

    def down_copy(self, child, slot, source):
        back = self.back if slot < 2 or self.line else self.leaf_back
        return pltpu.make_async_remote_copy(
            src_ref=source.at[self.rows],
            dst_ref=self.out.at[self.rows],
            send_sem=self.down.at[slot, self.slot],
            recv_sem=back.at[self.slot],
            **peer(child),
        )

    def each_child(self, action):
        for present, child, slot in self.children:
            if present is None:
                action(child, slot)
            else:
                pl.when(present)(functools.partial(action, child, slot))

    def keep(self):
        return pltpu.make_async_copy(
            self.own.at[self.rows], self.out.at[self.rows], self.up.at[self.slot]
        )

    def rise(self):
        self.each_child(lambda child, slot: self.up_copy(child, slot).wait_recv())
        base = self.slot * self.count
        for piece in range(0, self.count, 16):
            span = rows_at(self.start + piece, 16)
            total = self.own[span, :].astype(jnp.float32)
            for present, _, slot in self.children:
                part = self.box[slot, rows_at(base + piece, 16), :].astype(jnp.float32)
                total += part if present is None else jnp.where(present, part, 0.0)
            self.own[span, :] = total.astype(jnp.bfloat16)

        @pl.when(jnp.logical_not(self.root))
        def _():
            self.up_copy(self.parent, self.parent_slot).start()

        @pl.when(self.root)
        def _():
            self.keep().start()
            self.each_child(lambda child, slot: self.down_copy(child, slot, self.own).start())

    def fall(self):
        @pl.when(jnp.logical_not(self.root))
        def _():
            self.down_copy(self.parent, 0, self.out).wait_recv()
            self.each_child(lambda child, slot: self.down_copy(child, slot, self.out).start())

    def finish(self):
        @pl.when(jnp.logical_not(self.root))
        def _():
            self.up_copy(self.parent, self.parent_slot).wait_send()

        @pl.when(self.root)
        def _():
            self.keep().wait()

        self.each_child(lambda child, slot: self.down_copy(child, slot, self.out).wait_send())


def softmax_parts(query_rows, key_rows, first_row):
    scores = product_back(query_rows, key_rows) * (1.0 / math.sqrt(HEAD_DIM))
    rows = lax.broadcasted_iota(jnp.int32, scores.shape, 0) + first_row
    columns = lax.broadcasted_iota(jnp.int32, scores.shape, 1)
    scores = jnp.where(columns <= rows, scores, -1e30)
    spread = jnp.exp(scores - jnp.max(scores, axis=-1, keepdims=True))
    return spread * (1.0 / jnp.sum(spread, axis=-1, keepdims=True))


def pack_pairs(blocks):
    half = blocks.shape[1] // 2
    return jnp.concatenate([blocks[:, :half], blocks[:, half:]], axis=-1)


def unpack_pairs(blocks):
    return jnp.concatenate([blocks[..., :PAIR], blocks[..., PAIR:]], axis=-2)


def sort_blocks(slot_ref, source, targets, opened=lambda rows: rows):
    block_total = source.shape[0]
    block = targets[0].shape[0] // block_total
    for index in range(block_total):
        rows = opened(source[slot_ref[index]])
        start = 0
        for target in targets:
            width = target.shape[-1]
            target[index * block : (index + 1) * block, :] = rows[:, start : start + width]
            start += width


def norm_back_rows(values, grad_unit):
    scale = rms_scale(values)
    unit = values * scale
    return unit, lambda grad: norm_back(scale, unit, grad)


def backward_kernel(
    rounds,
    block,
    order_ref,
    gain_one_ref,
    gain_two_ref,
    grad_gate_ref,
    grad_up_ref,
    mixed_ref,
    normed_two_ref,
    cotangent_ref,
    part_ref,
    hidden_ref,
    input_ref,
    query_weight_ref,
    key_weight_ref,
    value_weight_ref,
    output_weight_ref,
    down_weight_ref,
    attended_ref,
    packed_ref,
    normed_ref,
    cosine_ref,
    sine_ref,
    out_ref,
    gain_out_ref,
    input_grad_ref,
    layer_output_ref,
    own,
    spine_in,
    line_in,
    grad_gate,
    grad_up,
    mixed,
    normed_two,
    cotangents,
    part,
    hidden,
    inputs,
    output_weight,
    attended,
    packed,
    normed,
    cosine,
    sine,
    half_swap,
    weight,
    near,
    send,
    far,
    branch,
    grad_hidden,
    gain_part,
    heads_out,
    heads_in,
    q0,
    q1,
    k,
    v,
    g0,
    g1,
    result,
    dk,
    dv,
    packed_out,
    packed_in,
    turned,
    gain_near,
    gain_far,
    fetch_sem,
    spine_up,
    spine_got,
    spine_down,
    spine_back,
    leaf_up,
    leaf_back,
    line_up,
    line_got,
    line_down,
    line_back,
    fold_send,
    fold_recv,
    gather_send,
    gather_recv,
    swap_send,
    swap_recv,
    near_send,
    near_recv,
    far_send,
    far_recv,
):
    place = Place()
    me = place.ctx
    depth, side = lax.div(me, 2), lax.rem(me, 2)
    other_side = me + 1 - 2 * side
    hidden_units = mixed.shape[1]
    width = own.shape[1]
    base = 3 * hidden_units
    spare = rounds * ROUND_ROWS - base - 3 * WIDE
    length = q0.shape[0]
    halves = TILE // block
    tile = min(256, length)
    tiles = length // tile
    scale = 1.0 / math.sqrt(HEAD_DIM)

    fetches = {}

    def fetch_all(source, *copies):
        first = sum(len(group) for group in fetches.values())
        fetches[id(source)] = [
            pltpu.make_async_copy(*copy, fetch_sem.at[first + index])
            for index, copy in enumerate(copies or ())
        ]
        for copy in fetches[id(source)]:
            copy.start()

    def fetch(*sources):
        for source in sources:
            for copy in fetches[id(source)]:
                copy.wait()

    for source, target in (
        (part_ref, part),
        (grad_gate_ref, grad_gate),
        (normed_two_ref, normed_two),
        (grad_up_ref, grad_up),
        (mixed_ref, mixed),
        (cotangent_ref, cotangents),
        (hidden_ref, hidden),
        (packed_ref, packed),
        (down_weight_ref, own.at[pl.ds(base, hidden_units)]),
        (output_weight_ref, output_weight),
        (attended_ref, attended),
        (normed_ref, normed),
        (cosine_ref, cosine),
        (sine_ref, sine),
        (input_ref, inputs),
    ):
        fetch_all(source, (source, target))
    for source, first, count in (
        (query_weight_ref, 0, PAIR),
        (key_weight_ref, PAIR, HEAD_DIM),
        (value_weight_ref, PAIR + HEAD_DIM, HEAD_DIM),
    ):
        fetch_all(
            source,
            *(
                (source.at[pl.ds(head * count, count)], weight.at[head, pl.ds(first, count)])
                for head in range(2)
            ),
        )
    gain_one = gain_one_ref[...].astype(jnp.float32).reshape(1, -1)
    gain_two = gain_two_ref[...].astype(jnp.float32).reshape(1, -1)
    lanes = (WIDE, WIDE)
    row_lane = lax.broadcasted_iota(jnp.int32, lanes, 0)
    column_lane = lax.broadcasted_iota(jnp.int32, lanes, 1)
    half = HEAD_DIM // 2
    inner = lax.rem(column_lane, HEAD_DIM)
    partner_lane = column_lane + jnp.where(inner < half, half, -half)
    half_swap[...] = jnp.where(row_lane == partner_lane, 1.0, 0.0).astype(jnp.bfloat16)
    place.greet()
    fetch(part_ref)
    fold_two = Fold(place, part, near.at[0], send.at[0], far.at[0], fold_send.at[0], fold_recv.at[0])
    fold_output = Fold(
        place, part, near.at[0], send.at[0], far.at[0], fold_send.at[0], fold_recv.at[0]
    )
    fold_one = Fold(place, part, near.at[1], send.at[1], far.at[1], fold_send.at[1], fold_recv.at[1])
    gather = Gather(place, branch, gather_send, gather_recv)
    swap_heads = Swap(place, heads_out, heads_in, swap_send.at[0], swap_recv.at[0], halves)
    swap_packed = Swap(place, packed_out, packed_in, swap_send.at[1], swap_recv.at[1], halves)
    spread_near = Spread(gain_near, place.row, 4, near_fsdp, near_send, near_recv)
    spread_far = Spread(gain_far, me, 8, peer, far_send, far_recv)
    fold_two.start()

    def stage_feed(first):
        sides = ((grad_gate, normed_two), (grad_up, normed_two), (mixed, cotangents))
        left, right = sides[first // hidden_units]
        if first == 0:
            fetch(grad_gate_ref, normed_two_ref)
        elif first == hidden_units:
            fetch(grad_up_ref)
        elif first == 2 * hidden_units:
            fetch(mixed_ref)

        @pl.loop(0, 2)
        def _(index):
            start = first % hidden_units + index * 256
            columns = pl.ds(pl.multiple_of(start, 256), 256)
            rows = pl.ds(pl.multiple_of(first + index * 256, 256), 256)
            own[rows, :] = product_rows(left[:, columns], right[...]).astype(jnp.bfloat16)

    stage_feed(0)
    stage_feed(2 * 256)

    spine_sems = (spine_up, spine_got, spine_down, spine_back)
    line_sems = (line_up, line_got, line_down, line_back)

    def spine(index):
        return Tree(place, own, out_ref, index, False, spine_in, spine_sems, leaf_back)

    def line(index):
        return Tree(place, own, out_ref, index, True, line_in, line_sems, None)

    def leaf_rows(index):
        return rows_at(index * ROUND_ROWS + (1 - side) * SPINE_ROWS, SPINE_ROWS)

    def leaf_copy(index):
        slot = lax.rem(index, RING)
        return pltpu.make_async_remote_copy(
            src_ref=own.at[leaf_rows(index)],
            dst_ref=spine_in.at[2, rows_at(slot * SPINE_ROWS, SPINE_ROWS)],
            send_sem=leaf_up.at[slot],
            recv_sem=spine_got.at[2, slot],
            **peer(other_side),
        )

    def leaf_result(index):
        slot = lax.rem(index, RING)
        return pltpu.make_async_remote_copy(
            src_ref=own.at[leaf_rows(index)],
            dst_ref=out_ref.at[leaf_rows(index)],
            send_sem=leaf_up.at[slot],
            recv_sem=leaf_back.at[slot],
            **peer(other_side),
        )

    def stage_norm_two():
        fetch(hidden_ref, cotangent_ref)
        fold_two.arrive()
        gain_part[...] = jnp.zeros_like(gain_part)

        @pl.loop(0, TILE // 16)
        def _(piece):
            span = rows_at(piece * 16, 16)
            grad = fold_two.rows(piece * 16, 16)
            unit, back = norm_back_rows(hidden[span, :], None)
            gain_part[1] += (grad * unit).reshape(2, 8, -1).sum(axis=0)
            here = rows_at(place.row * TILE + piece * 16, 16)
            total = cotangents[here, :].astype(jnp.float32) + back(grad * gain_two)
            grad_hidden[span, :] = total
            branch[here, :] = total.astype(jnp.bfloat16)

        gather.start()

    def stage_heads():
        fetch(output_weight_ref)
        gather.first()
        gather.arrive()

        @pl.loop(0, 4)
        def _(sequence):
            rows = branch[rows_at(sequence * TILE, TILE), :]
            grads = product_back(rows, output_weight[...]).astype(jnp.bfloat16)
            for head in range(2):
                heads_out[pl.ds((2 * sequence + head) * halves, halves)] = pack_pairs(
                    grads[:, head * PAIR : (head + 1) * PAIR].reshape(halves, block, PAIR)
                )

        swap_heads.start_all()

    def stage_sort():
        fetch(packed_ref)
        sort_blocks(order_ref, packed, (q0, q1, k, v))

    def stage_output_grad():
        fetch(attended_ref)
        for head in range(2):
            rows = [
                attended[(2 * index + head) * halves : (2 * index + head + 1) * halves]
                for index in range(4)
            ]
            rows = unpack_pairs(jnp.concatenate(rows, axis=0)).reshape(4 * TILE, PAIR)
            first_row = base + 2 * WIDE + head * PAIR
            for first in range(0, own.shape[1], 512):
                columns = slice(first, first + 512)
                own[first_row : first_row + PAIR, columns] = product_rows(
                    rows, branch[:, columns]
                ).astype(jnp.bfloat16)

    def stage_sort_grads():
        swap_heads.arrive()
        sort_blocks(order_ref, heads_in, (g0, g1), unpack_pairs)
        dk[...] = jnp.zeros_like(dk)
        dv[...] = jnp.zeros_like(dv)

    def stage_attention(index):
        first, top = index * tile, (index + 1) * tile
        parts = []
        for q, g in ((q0, g0), (q1, g1)):
            query_rows = q[first:top, :]
            grad_rows = g[first:top, :]
            soft = softmax_parts(query_rows, k[:top, :], first)
            grad_soft = product_back(grad_rows, v[:top, :])
            delta = jnp.sum(soft * grad_soft, axis=-1, keepdims=True)
            grad_scores = (soft * (grad_soft - delta)).astype(jnp.bfloat16)
            parts.append(product(grad_scores, k[:top, :]) * scale)
            key_term = product_rows(grad_scores, query_rows) * scale
            value_term = product_rows(soft.astype(jnp.bfloat16), grad_rows)
            dk[: top // block] += key_term.reshape(-1, block, HEAD_DIM)
            dv[: top // block] += value_term.reshape(-1, block, HEAD_DIM)
        result[first // block : top // block] = jnp.concatenate(parts, axis=-1).reshape(
            -1, block, PAIR
        )

    def stage_unsort():
        for slot in range(length // block):
            spot = order_ref[length // block + slot]
            packed_out[slot] = jnp.concatenate(
                [result[spot], dk[spot], dv[spot]], axis=-1
            ).astype(jnp.bfloat16)
        swap_packed.start_all()

    def stage_turn():
        fetch(cosine_ref, sine_ref, query_weight_ref, key_weight_ref, value_weight_ref)
        swap_packed.arrive()

        @pl.loop(0, 4)
        def _(sequence):
            span = rows_at(sequence * TILE, TILE)
            total = None
            for head in range(2):
                grads = packed_in[pl.ds((2 * sequence + head) * halves, halves)]
                grads = grads.reshape(TILE, WIDE)
                swapped = product(grads, half_swap[...])
                low = (
                    grads.astype(jnp.float32) * cosine[span, :] - swapped * sine[span, :]
                ).astype(jnp.bfloat16)
                turned[head, span, :] = low
                term = product(low, weight[head])
                total = term if total is None else total + term
            part[span, :] = total.astype(jnp.bfloat16)

        fold_one.start()

    def stage_projection_grads(head):
        if head == 0:
            fetch(normed_ref)
        query_base = base + head * PAIR
        key_base = base + WIDE + head * HEAD_DIM
        value_base = key_base + 2 * HEAD_DIM
        for first in range(0, own.shape[1], 512):
            columns = slice(first, first + 512)
            grads = product_rows(turned[head], normed[:, columns]).astype(jnp.bfloat16)
            own[query_base : query_base + PAIR, columns] = grads[:PAIR]
            own[key_base : key_base + HEAD_DIM, columns] = grads[PAIR : PAIR + HEAD_DIM]
            own[value_base : value_base + HEAD_DIM, columns] = grads[PAIR + HEAD_DIM :]

    def stage_norm_one():
        fetch(input_ref)
        fold_one.arrive()

        @pl.loop(0, TILE // 16)
        def _(piece):
            span = rows_at(piece * 16, 16)
            grad = fold_one.rows(piece * 16, 16)
            unit, back = norm_back_rows(inputs[span, :].astype(jnp.float32), None)
            gain_part[0] += (grad * unit).reshape(2, 8, -1).sum(axis=0)
            input_grad_ref[span, :] = grad_hidden[span, :] + back(grad * gain_one)

        gain_near[place.row] = jnp.sum(gain_part[...], axis=1)
        spread_near.start()

    def stage_gain():
        gain_far[me] = spread_near.total()
        spread_far.start()

    def stage_output():
        fetch(down_weight_ref)

        @pl.loop(0, 4)
        def _(sequence):
            span = rows_at(sequence * TILE, TILE)
            part[span, :] = product(
                mixed[span, :], own[base : base + hidden_units, :]
            ).astype(jnp.bfloat16)

    def stage_output_sum():
        fold_output.arrive()

        @pl.loop(0, TILE // 16)
        def _(piece):
            span = rows_at(piece * 16, 16)
            total = hidden[span, :] + fold_output.rows(piece * 16, 16)
            layer_output_ref[span, :] = total.astype(jnp.bfloat16)

    def stage_clear():
        if spare:
            own[base + 3 * WIDE :, :] = jnp.zeros((spare, width), own.dtype)

    units = 2 * 256
    stages = [
        (FEED[index], functools.partial(stage_feed, (index + 2) * units)) for index in range(4)
    ]
    stages += [
        (CHAIN[0], fold_two.relay),
        (CHAIN[0], stage_sort),
        (CHAIN[1], stage_norm_two),
        (CHAIN[2], gather.relay),
        (CHAIN[2], stage_output),
        (CHAIN[3], stage_heads),
        (CHAIN[3], fold_output.start),
        (CHAIN[4], fold_output.relay),
        (CHAIN[4], stage_output_grad),
        (CHAIN[4], stage_clear),
        (CHAIN[5], stage_sort_grads),
    ]
    stages += [
        (CHAIN[5] + index, functools.partial(stage_attention, index)) for index in range(tiles)
    ]
    stages += [
        (CHAIN[5] + tiles - 1, stage_unsort),
        (CHAIN[5] + tiles, stage_output_sum),
        (CHAIN[6], stage_turn),
        (CHAIN[7], fold_one.relay),
        (CHAIN[7], functools.partial(stage_projection_grads, 0)),
        (CHAIN[7] + 1, functools.partial(stage_projection_grads, 1)),
        (CHAIN[8], stage_norm_one),
        (CHAIN[9], stage_gain),
    ]
    assert CHAIN[7] + 1 < base // ROUND_ROWS - LEAD
    for index in range(4):
        assert FEED[index] < (index + 2) * units // ROUND_ROWS - LEAD

    for index in range(LEAD):
        leaf_copy(index).start()

    def valid(index):
        return jnp.logical_and(index >= 0, index < rounds)

    @pl.loop(0, rounds + RING)
    def _(now):
        far_side = jnp.abs(depth - 2 + side)
        off_center = jnp.abs(depth - 1 - side)
        done = now - RING + 1
        for tree in (spine(done), line(done)):
            pl.when(valid(done))(tree.finish)

        @pl.when(now + LEAD < rounds)
        def _():
            leaf_copy(now + LEAD).start()

        rising = spine(now - HOP * (3 - off_center))
        pl.when(valid(rising.index))(rising.rise)

        @pl.loop(0, 5)
        def _(age):
            tree = line(now - HOP * age)
            pl.when(jnp.logical_and(valid(tree.index), tree.rise_age == age))(tree.rise)

        falling = spine(now - HOP * (3 + off_center))
        pl.when(valid(falling.index))(falling.fall)

        @pl.loop(4, 9)
        def _(age):
            tree = line(now - HOP * age)
            pl.when(jnp.logical_and(valid(tree.index), tree.fall_age == age))(tree.fall)

        leaf_fall = now - HOP * (4 + far_side)

        @pl.when(valid(leaf_fall))
        def _():
            leaf_result(leaf_fall).wait_recv()
            leaf_copy(leaf_fall).wait_send()

        for when, stage in stages:
            pl.when(now == when)(stage)

    gain_out_ref[...] = spread_far.total()


def backward(order, gain_one, gain_two, grad_gate, grad_up, mixed, normed_two, cotangents, part,
             hidden, inputs, query_weight, key_weight, value_weight, output_weight, down_weight,
             attended, packed, normed, cosine, sine, key):
    width = hidden.shape[1]
    rows = 3 * mixed.shape[1] + 3 * WIDE
    rounds = -(-rows // ROUND_ROWS)
    block = packed.shape[1]
    length = packed.shape[0] * block
    dma = pltpu.SemaphoreType.DMA
    low, full = jnp.bfloat16, jnp.float32
    any_spec = pl.BlockSpec(memory_space=pl.ANY)
    operands = (
        order, gain_one, gain_two, grad_gate, grad_up, mixed, normed_two, cotangents, part,
        hidden, inputs, query_weight, key_weight, value_weight, output_weight, down_weight,
        attended, packed, normed, cosine, sine,
    )

    def like(array):
        return pltpu.VMEM(array.shape, array.dtype)

    return pl.pallas_call(
        functools.partial(backward_kernel, rounds, block),
        out_shape=(
            jax.ShapeDtypeStruct((rounds * ROUND_ROWS, width), low),
            jax.ShapeDtypeStruct((2, width), full),
            jax.ShapeDtypeStruct((TILE, width), full),
            jax.ShapeDtypeStruct((TILE, width), low),
        ),
        in_specs=[pl.BlockSpec(memory_space=pltpu.SMEM)] + [vmem()] * 2 + [any_spec] * 18,
        out_specs=(any_spec, vmem(), vmem(), vmem()),
        scratch_shapes=[
            pltpu.VMEM((rounds * ROUND_ROWS, width), low),
            pltpu.VMEM((3, RING * SPINE_ROWS, width), low),
            pltpu.VMEM((3, RING * LINE_ROWS, width), low),
            like(grad_gate), like(grad_up), like(mixed), like(normed_two), like(cotangents),
            like(part), like(hidden), like(inputs), like(output_weight),
            like(attended), like(packed), like(normed), like(cosine), like(sine),
            pltpu.VMEM((WIDE, WIDE), low),
            pltpu.VMEM((2, WIDE, width), low),
            pltpu.VMEM((2, 2, TILE, width), low),
            pltpu.VMEM((2, TILE, width), low),
            pltpu.VMEM((2, TILE, width), low),
            pltpu.VMEM((4 * TILE, width), low),
            pltpu.VMEM((TILE, width), full),
            pltpu.VMEM((2, 8, width), full),
            pltpu.VMEM((length // block, block // 2, 2 * PAIR), low),
            pltpu.VMEM((length // block, block // 2, 2 * PAIR), low),
        ]
        + [pltpu.VMEM((length, HEAD_DIM), low)] * 6
        + [pltpu.VMEM((length // block, block, PAIR), full)]
        + [pltpu.VMEM((length // block, block, HEAD_DIM), full)] * 2
        + [
            pltpu.VMEM((length // block, block, WIDE), low),
            pltpu.VMEM((length // block, block, WIDE), low),
            pltpu.VMEM((2, 4 * TILE, WIDE), low),
            pltpu.VMEM((4, 2, width), full),
            pltpu.VMEM((8, 2, width), full),
            dma((21,)),
            dma((RING,)), dma((3, RING)), dma((3, RING)), dma((RING,)),
            dma((RING,)), dma((RING,)),
            dma((RING,)), dma((3, RING)), dma((3, RING)), dma((RING,)),
            dma((2, 3)), dma((2, 3)),
            dma((3,)), dma((3,)),
            dma((2, 8)), dma((2, 8)),
            dma((4,)), dma((4,)), dma((8,)), dma((8,)),
        ],
        compiler_params=pltpu.CompilerParams(
            collective_id=key, has_side_effects=True, vmem_limit_bytes=63 * 2**20
        ),
        name="backward",
    )(*operands)


def forward_kernel(
    block,
    place_ref,
    table_ref,
    gain_one_ref,
    gain_two_ref,
    input_ref,
    cotangent_ref,
    query_weight_ref,
    key_weight_ref,
    value_weight_ref,
    output_weight_ref,
    gate_weight_ref,
    up_weight_ref,
    down_weight_ref,
    place_out,
    part_out,
    hidden_out,
    attended_out,
    packed_out,
    normed_one_out,
    cosine_out,
    sine_out,
    cotangent_out,
    normed_two_out,
    mixed_out,
    grad_gate_out,
    grad_up_out,
    places,
    tables,
    inputs,
    cotangents,
    normed_one,
    normed_two,
    cosine,
    sine,
    weight,
    output_weight,
    gate_weight,
    up_weight,
    down_weight,
    packed_from,
    packed,
    q0,
    q1,
    k,
    v,
    result,
    heads_from,
    heads,
    part,
    near,
    send,
    far,
    hidden,
    mixed,
    grad_gate,
    grad_up,
    fetch_sem,
    store_sem,
    gather_send,
    gather_recv,
    swap_send,
    swap_recv,
    fold_send,
    fold_recv,
):
    place = Place()
    length, width = q0.shape[0], inputs.shape[1]
    halves = TILE // block
    half = HEAD_DIM // 2
    pair_rows = 2 * TILE
    fetches, stores = {}, []

    def fetch_all(key, *copies):
        base = sum(len(group) for group in fetches.values())
        fetches[key] = [
            pltpu.make_async_copy(part_of, target, fetch_sem.at[base + index])
            for index, (part_of, target) in enumerate(copies)
        ]
        for copy in fetches[key]:
            copy.start()

    def fetch(*keys):
        for key in keys:
            for copy in fetches[key]:
                copy.wait()

    def store(source, target):
        copy = pltpu.make_async_copy(source, target, store_sem.at[len(stores)])
        copy.start()
        stores.append(copy)

    own_rows = rows_at(place.row * TILE, TILE)
    fetch_all("inputs", (input_ref, inputs.at[own_rows]))
    fetch_all("cotangent", (cotangent_ref, cotangents.at[own_rows]))
    copies = []
    for head in range(2):
        query_base, key_base = head * PAIR, head * HEAD_DIM
        target = weight.at[head]
        heads_of = [(query_weight_ref, query_base), (query_weight_ref, query_base + HEAD_DIM)]
        heads_of += [(key_weight_ref, key_base), (value_weight_ref, key_base)]
        for index, (source, first) in enumerate(heads_of):
            copies.append(
                (source.at[pl.ds(first, HEAD_DIM)], target.at[pl.ds(index * HEAD_DIM, HEAD_DIM)])
            )
            for side in range(2):
                copies.append(
                    (
                        source.at[pl.ds(first + (1 - side) * half, half)],
                        target.at[pl.ds(WIDE + index * HEAD_DIM + side * half, half)],
                    )
                )
    fetch_all("weight", *copies)
    fetch_all("output", (output_weight_ref, output_weight))
    fetch_all("gate", (gate_weight_ref, gate_weight))
    fetch_all("up", (up_weight_ref, up_weight))
    fetch_all("down", (down_weight_ref, down_weight))
    places[pl.ds(pl.multiple_of(place.row * 8, 8), 8), :] = jnp.broadcast_to(
        place_ref[...], (8, place_ref.shape[1])
    )
    gain_one = gain_one_ref[...].astype(jnp.float32).reshape(1, -1)
    gain_two = gain_two_ref[...].astype(jnp.float32).reshape(1, -1)
    tables[own_rows, :] = table_ref[...]
    gather_places = Gather(place, places, gather_send.at[0], gather_recv.at[0], 8)
    gather_tables = Gather(place, tables, gather_send.at[1], gather_recv.at[1])
    gather_inputs = Gather(place, inputs, gather_send.at[2], gather_recv.at[2])
    gather_cotangents = Gather(place, cotangents, gather_send.at[3], gather_recv.at[3])
    gather_two = Gather(place, normed_two, gather_send.at[4], gather_recv.at[4])
    swap_places = Swap(place, places, place_out, swap_send.at[0], swap_recv.at[0], 8, 2)
    swap_packed = Swap(place, packed_from, packed, swap_send.at[1], swap_recv.at[1], halves)
    swap_heads = Swap(place, heads_from, heads, swap_send.at[2], swap_recv.at[2], halves)
    fold = Fold(place, part, near, send, far, fold_send, fold_recv)
    place.greet()
    fetch("inputs")
    gather_tables.start()
    gather_inputs.start()
    gather_places.start()
    fetch("cotangent")
    gather_cotangents.start()

    def project(chip):
        base = chip * pair_rows

        @pl.loop(0, pair_rows // 16)
        def _(piece):
            span = rows_at(base + piece * 16, 16)
            rows = inputs[span, :].astype(jnp.float32)
            normed_one[span, :] = (rows * rms_scale(rows) * gain_one).astype(jnp.bfloat16)

        span = rows_at(base, pair_rows)
        low_cosine, low_sine = tables[span, :half], tables[span, half:HEAD_DIM]
        ones = jnp.ones((pair_rows, HEAD_DIM), jnp.float32)
        cosine[span, :] = jnp.concatenate([low_cosine] * 6 + [ones], axis=-1)
        sine[span, :] = jnp.concatenate([-low_sine, low_sine] * 3 + [ones * 0.0], axis=-1)

        for head in range(2):
            products = product_back(normed_one[span, :], weight[head])
            low = (
                products[:, :WIDE] * cosine[span, :] + products[:, WIDE:] * sine[span, :]
            ).astype(jnp.bfloat16)
            for index in range(2):
                packed_from[pl.ds(((2 * chip + index) * 2 + head) * halves, halves)] = low[
                    index * TILE : (index + 1) * TILE
                ].reshape(halves, block, WIDE)
        for index in range(4):
            swap_packed.start(4 * chip + index)

    gather_tables.first()
    gather_inputs.first()
    gather_places.first()
    fetch("weight")
    project(place.chip)
    gather_tables.relay()
    gather_inputs.relay()
    gather_places.relay()
    gather_tables.arrive()
    gather_inputs.arrive()
    gather_places.arrive()
    project(1 - place.chip)
    swap_places.start_all()
    store(normed_one, normed_one_out)
    store(cosine, cosine_out)
    store(sine, sine_out)
    swap_places.arrive()
    swap_packed.arrive()
    store(packed, packed_out)

    def place_row(first, count):
        blocks = [place_out[8 * index : 8 * index + 1, :] for index in range(first, first + count)]
        return jnp.concatenate(blocks, axis=-1)

    tile = min(256, length)
    order = place_row(0, length // TILE)
    flat = packed[...].reshape(length, WIDE)
    for first in range(0, length, tile):
        rows = lax.broadcasted_iota(jnp.int32, (tile, length), 0) + first
        chosen = jnp.where(rows == order, 1.0, 0.0).astype(jnp.bfloat16)
        moved = product(chosen, flat).astype(jnp.bfloat16)
        for index, target in enumerate((q0, q1, k, v)):
            target[first : first + tile, :] = moved[:, index * HEAD_DIM : (index + 1) * HEAD_DIM]
    for first in range(0, length, tile):
        parts = []
        for q in (q0, q1):
            soft = softmax_parts(q[first : first + tile, :], k[: first + tile, :], first)
            parts.append(product(soft.astype(jnp.bfloat16), v[: first + tile, :]))
        result[first : first + tile, :] = jnp.concatenate(parts, axis=-1).astype(jnp.bfloat16)
    for first in range(0, length, tile):
        rows = lax.broadcasted_iota(jnp.int32, (length, tile), 0)
        chosen = jnp.where(rows == place_row(first // TILE, tile // TILE), 1.0, 0.0)
        moved = product_rows(chosen.astype(jnp.bfloat16), result[...]).astype(jnp.bfloat16)
        heads_from[first // block : (first + tile) // block] = pack_pairs(
            moved.reshape(-1, block, PAIR)
        )
    swap_heads.start_all()
    gather_cotangents.first()
    gather_cotangents.relay()
    fetch("output")
    swap_heads.arrive()
    store(heads, attended_out)

    @pl.loop(0, 4)
    def _(sequence):
        total = None
        for head in range(2):
            rows = heads[pl.ds((2 * sequence + head) * halves, halves)]
            rows = unpack_pairs(rows).reshape(TILE, PAIR)
            term = product(rows, output_weight[head * PAIR : (head + 1) * PAIR, :])
            total = term if total is None else total + term
        part[rows_at(sequence * TILE, TILE), :] = total.astype(jnp.bfloat16)

    fold.start()
    gather_cotangents.arrive()
    store(cotangents, cotangent_out)
    fold.relay()
    fold.arrive()

    @pl.loop(0, TILE // 16)
    def _(piece):
        span = rows_at(piece * 16, 16)
        own = rows_at(place.row * TILE + piece * 16, 16)
        rows = inputs[own, :].astype(jnp.float32) + fold.rows(piece * 16, 16)
        hidden[span, :] = rows
        normed_two[own, :] = (rows * rms_scale(rows) * gain_two).astype(jnp.bfloat16)

    gather_two.start()
    store(hidden, hidden_out)
    fetch("gate", "up", "down")

    def feed(chip):
        span = rows_at(chip * pair_rows, pair_rows)

        @pl.loop(0, mixed.shape[1] // 256)
        def _(index):
            units = rows_at(index * 256, 256)
            columns = pl.ds(pl.multiple_of(index * 256, 256), 256)
            gate = product_back(normed_two[span, :], gate_weight[units, :])
            upward = product_back(normed_two[span, :], up_weight[units, :])
            grad_mixed = product_back(cotangents[span, :], down_weight[units, :])
            sigmoid = jax.nn.sigmoid(gate)
            activated = gate * sigmoid
            mixed[span, columns] = (activated * upward).astype(jnp.bfloat16)
            grad_gate[span, columns] = (
                grad_mixed * upward * sigmoid * (1.0 + gate * (1.0 - sigmoid))
            ).astype(jnp.bfloat16)
            grad_up[span, columns] = (grad_mixed * activated).astype(jnp.bfloat16)

        @pl.loop(0, width // 512)
        def _(index):
            columns = pl.ds(pl.multiple_of(index * 512, 512), 512)
            part[span, columns] = (
                product(grad_gate[span, :], gate_weight[:, columns])
                + product(grad_up[span, :], up_weight[:, columns])
            ).astype(jnp.bfloat16)

    gather_two.first()
    feed(place.chip)
    gather_two.relay()
    gather_two.arrive()
    store(normed_two, normed_two_out)
    feed(1 - place.chip)
    store(part, part_out)
    store(mixed, mixed_out)
    store(grad_gate, grad_gate_out)
    store(grad_up, grad_up_out)
    for copy in stores:
        copy.wait()


def forward(places, table, gain_one, gain_two, inputs, cotangent, query_weight, key_weight, value_weight,
            output_weight, gate_weight, up_weight, down_weight, length, block, key):
    width = inputs.shape[1]
    hidden_units = gate_weight.shape[0]
    rows = 4 * TILE
    blocks = length // block
    low, full = jnp.bfloat16, jnp.float32
    dma = pltpu.SemaphoreType.DMA
    any_spec = pl.BlockSpec(memory_space=pl.ANY)

    def out(shape, dtype):
        return jax.ShapeDtypeStruct(shape, dtype)

    wide = (rows, width)
    return pl.pallas_call(
        functools.partial(forward_kernel, block),
        out_shape=(
            out((64, 128), jnp.int32),
            out(wide, low), out((TILE, width), full),
            out((blocks, block // 2, 2 * PAIR), low), out((blocks, block, WIDE), low),
            out(wide, low), out((rows, WIDE), full), out((rows, WIDE), full),
            out(wide, low), out(wide, low),
            out((rows, hidden_units), low), out((rows, hidden_units), low),
            out((rows, hidden_units), low),
        ),
        in_specs=[vmem()] * 4 + [any_spec] * 9,
        out_specs=(vmem(),) + (any_spec,) * 12,
        scratch_shapes=[
            pltpu.VMEM((32, 128), jnp.int32),
            pltpu.VMEM((rows, 128), full),
            pltpu.VMEM(wide, low), pltpu.VMEM(wide, low),
            pltpu.VMEM(wide, low), pltpu.VMEM(wide, low),
            pltpu.VMEM((rows, WIDE), full), pltpu.VMEM((rows, WIDE), full),
            pltpu.VMEM((2, 2 * WIDE, width), low),
            pltpu.VMEM(output_weight.shape, low),
            pltpu.VMEM((hidden_units, width), low), pltpu.VMEM((hidden_units, width), low),
            pltpu.VMEM((hidden_units, width), low),
            pltpu.VMEM((blocks, block, WIDE), low), pltpu.VMEM((blocks, block, WIDE), low),
        ]
        + [pltpu.VMEM((length, HEAD_DIM), low)] * 4
        + [
            pltpu.VMEM((length, PAIR), low),
            pltpu.VMEM((blocks, block // 2, 2 * PAIR), low),
            pltpu.VMEM((blocks, block // 2, 2 * PAIR), low),
            pltpu.VMEM(wide, low),
            pltpu.VMEM((2, TILE, width), low),
            pltpu.VMEM((TILE, width), low), pltpu.VMEM((TILE, width), low),
            pltpu.VMEM((TILE, width), full),
            pltpu.VMEM((rows, hidden_units), low), pltpu.VMEM((rows, hidden_units), low),
            pltpu.VMEM((rows, hidden_units), low),
            dma((30,)), dma((12,)),
            dma((5, 3)), dma((5, 3)),
            dma((3, 8)), dma((3, 8)),
            dma((3,)), dma((3,)),
        ],
        compiler_params=pltpu.CompilerParams(
            collective_id=key, has_side_effects=True, vmem_limit_bytes=63 * 2**20
        ),
        name="forward",
    )(places, table, gain_one, gain_two, inputs, cotangent, query_weight, key_weight, value_weight,
      output_weight, gate_weight, up_weight, down_weight)


def widen_kernel(plan, source, *refs):
    targets, (low, full, load_sem, store_sem) = refs[:-4], refs[-4:]
    slots = low.shape[0]
    loads, stores = [], []
    for index, (first, which, target_row, chunk) in enumerate(plan):
        slot = index % slots
        span = pl.ds(0, chunk)
        loads.append(
            pltpu.make_async_copy(
                source.at[pl.ds(first, chunk)], low.at[slot, span], load_sem.at[slot]
            )
        )
        stores.append(
            pltpu.make_async_copy(
                full.at[slot, span],
                targets[which].at[pl.ds(target_row, chunk)],
                store_sem.at[slot],
            )
        )
    for load in loads[:slots]:
        load.start()
    for index, (load, store) in enumerate(zip(loads, stores)):
        slot = index % slots
        load.wait()
        if index >= slots:
            stores[index - slots].wait()

        @pl.loop(0, plan[index][3] // 16)
        def _(piece):
            span = rows_at(piece * 16, 16)
            full[slot, span, :] = low[slot, span, :].astype(jnp.float32)

        store.start()
        if index + slots < len(plan):
            loads[index + slots].start()
    for store in stores[-slots:]:
        store.wait()


def widen(values, counts):
    slots, width, first, plan = 6, values.shape[1], 0, []
    for which, count in enumerate(counts):
        chunk = math.gcd(count, 256) if count % 192 else 192
        plan += [(first + row, which, row, chunk) for row in range(0, count, chunk)]
        first += count
    any_spec = pl.BlockSpec(memory_space=pl.ANY)
    return pl.pallas_call(
        functools.partial(widen_kernel, plan),
        out_shape=tuple(jax.ShapeDtypeStruct((count, width), jnp.float32) for count in counts),
        in_specs=[any_spec],
        out_specs=(any_spec,) * len(counts),
        scratch_shapes=[
            pltpu.VMEM((slots, 256, width), values.dtype),
            pltpu.VMEM((slots, 256, width), jnp.float32),
            pltpu.SemaphoreType.DMA((slots,)),
            pltpu.SemaphoreType.DMA((slots,)),
        ],
        compiler_params=pltpu.CompilerParams(vmem_limit_bytes=63 * 2**20),
        name="widen",
    )(values)


def gather_rows(values):
    return lax.all_gather(values, "fsdp", axis=0, tiled=True)


def scatter_rows(values):
    return lax.psum_scatter(
        values.astype(jnp.bfloat16), "fsdp", scatter_dimension=0, tiled=True
    ).astype(jnp.float32)


def per_device_gathered(
    inputs,
    positions,
    cotangent,
    attention_gain,
    query_weight,
    key_weight,
    value_weight,
    output_weight,
    feedforward_gain,
    gate_weight,
    up_weight,
    down_weight,
):
    row_count = inputs.shape[0]
    groups = HEADS // KV_HEADS
    gain_one = attention_gain.astype(jnp.float32)
    gain_two = feedforward_gain.astype(jnp.float32)
    seq_count = lax.axis_size("fsdp")
    first_row = lax.axis_index("fsdp") * row_count

    def own(values):
        return lax.dynamic_slice_in_dim(values, first_row, row_count, 0)

    query_places = gather_rows(positions).reshape(seq_count, row_count)
    key_places = lax.all_gather(query_places, "ctx", axis=1, tiled=True)
    all_cotangent = gather_rows(cotangent)
    flat_in = gather_rows(inputs).astype(jnp.float32)
    scale_one = rms_scale(flat_in)
    unit_one = flat_in * scale_one
    normed_one = (unit_one * gain_one).astype(jnp.bfloat16)
    total_rows = normed_one.shape[0]
    cosine, sine = rotary_tables(query_places.reshape(-1))
    query_heads = query_weight.shape[0] // HEAD_DIM
    kv_heads = key_weight.shape[0] // HEAD_DIM
    kv_width = kv_heads * HEAD_DIM
    query_low = rotate(
        product_back(normed_one, query_weight).reshape(total_rows, query_heads, HEAD_DIM), cosine, sine
    ).astype(jnp.bfloat16)
    key_low = rotate(
        product_back(normed_one, key_weight).reshape(total_rows, kv_heads, HEAD_DIM), cosine, sine
    ).astype(jnp.bfloat16)
    value_low = product_back(normed_one, value_weight).astype(jnp.bfloat16)
    ctx_size = lax.axis_size("ctx")

    def spread(values):
        rows = lax.all_gather(values, "ctx", axis=0, tiled=True)
        rows = rows.reshape(ctx_size, seq_count, row_count, kv_width).swapaxes(0, 1)
        return rows.reshape(seq_count, ctx_size * row_count, kv_width)

    def collect(values):
        rows = values.astype(jnp.bfloat16).swapaxes(1, 2)
        rows = rows.reshape(seq_count, ctx_size, row_count, kv_width).swapaxes(0, 1)
        return lax.psum_scatter(
            rows.reshape(-1, kv_width), "ctx", scatter_dimension=0, tiled=True
        )

    all_keys = spread(key_low.reshape(total_rows, kv_width))
    all_values = spread(value_low)
    total_keys = all_keys.shape[1]
    key_grid = all_keys.reshape(seq_count, total_keys, kv_heads, HEAD_DIM).swapaxes(1, 2)
    value_grid = all_values.reshape(seq_count, total_keys, kv_heads, HEAD_DIM).swapaxes(1, 2)
    query_grouped = query_low.reshape(seq_count, row_count, kv_heads, groups, HEAD_DIM)
    attended, log_total = attend_forward(
        query_grouped, query_places, key_grid, value_grid, key_places
    )
    attended_low = attended.reshape(total_rows, query_heads * HEAD_DIM).astype(jnp.bfloat16)
    hidden_state = inputs.astype(jnp.float32) + scatter_rows(product(attended_low, output_weight))
    scale_two = rms_scale(hidden_state)
    unit_two = hidden_state * scale_two
    normed_two = gather_rows((unit_two * gain_two).astype(jnp.bfloat16))
    gate_values = product_back(normed_two, gate_weight)
    upward = product_back(normed_two, up_weight)
    sigmoid_gate = jax.nn.sigmoid(gate_values)
    activated = gate_values * sigmoid_gate
    mixed_hidden = (activated * upward).astype(jnp.bfloat16)
    grad_out = cotangent.astype(jnp.float32)
    grad_down = product_rows(mixed_hidden, all_cotangent)
    grad_mixed = product_back(all_cotangent, down_weight)
    grad_gate_low = (
        grad_mixed * upward * sigmoid_gate * (1.0 + gate_values * (1.0 - sigmoid_gate))
    ).astype(jnp.bfloat16)
    grad_up_low = (grad_mixed * activated).astype(jnp.bfloat16)
    grad_unit_part = (
        product(grad_gate_low, gate_weight) + product(grad_up_low, up_weight)
    ).astype(jnp.bfloat16)
    grad_normed_two = scatter_rows(grad_unit_part)
    gain_two_grad = jnp.sum(grad_normed_two * unit_two, axis=0)
    grad_hidden = grad_out + norm_back(scale_two, unit_two, grad_normed_two * gain_two)
    branch_rows = gather_rows(grad_hidden.astype(jnp.bfloat16))
    layer_output = (hidden_state + scatter_rows(product(mixed_hidden, down_weight))).astype(
        jnp.bfloat16
    )
    grad_gate = product_rows(grad_gate_low, normed_two)
    grad_up = product_rows(grad_up_low, normed_two)
    grad_output = product_rows(attended_low, branch_rows)
    grad_attended = product_back(branch_rows, output_weight).astype(jnp.bfloat16)
    grad_attended = grad_attended.reshape(seq_count, row_count, kv_heads, groups, HEAD_DIM)
    grad_query_rot, grad_key_all, grad_value_all = attend_backward(
        query_grouped, query_places, key_grid, value_grid, key_places, log_total, grad_attended
    )
    grad_key_own = collect(grad_key_all).astype(jnp.float32)
    grad_value_low = collect(grad_value_all)
    grad_query_low = (
        rotate_back(grad_query_rot.reshape(total_rows, query_heads, HEAD_DIM), cosine, sine)
        .reshape(total_rows, query_heads * HEAD_DIM)
        .astype(jnp.bfloat16)
    )
    grad_key_low = (
        rotate_back(
            grad_key_own.reshape(total_rows, kv_heads, HEAD_DIM), cosine, sine
        )
        .reshape(total_rows, kv_width)
        .astype(jnp.bfloat16)
    )
    grad_query = product_rows(grad_query_low, normed_one)
    grad_key = product_rows(grad_key_low, normed_one)
    grad_value = product_rows(grad_value_low, normed_one)
    grad_normed_one = scatter_rows(
        product(grad_query_low, query_weight)
        + product(grad_key_low, key_weight)
        + product(grad_value_low, value_weight)
    )
    own_unit = own(unit_one)
    gain_one_grad = jnp.sum(grad_normed_one * own_unit, axis=0)
    input_grad = grad_hidden + norm_back(own(scale_one), own_unit, grad_normed_one * gain_one)

    grads = (grad_query, grad_key, grad_value, grad_output, grad_gate, grad_up, grad_down)
    parts = [lax.psum(grad.astype(jnp.bfloat16), "ctx").astype(jnp.float32) for grad in grads]
    gain_sums = lax.psum(jnp.stack([gain_one_grad, gain_two_grad]), ("fsdp", "ctx"))
    return (
        layer_output,
        input_grad,
        gain_sums[0],
        parts[0],
        parts[1],
        parts[2],
        parts[3],
        gain_sums[1],
        parts[4],
        parts[5],
        parts[6],
    )


def per_device_by_head(
    inputs,
    positions,
    cotangent,
    attention_gain,
    query_weight,
    key_weight,
    value_weight,
    output_weight,
    feedforward_gain,
    gate_weight,
    up_weight,
    down_weight,
):
    gain_one, gain_two = attention_gain, feedforward_gain
    block = TILE // 2
    length = TILE * 8
    cosine, sine = rotary_tables(positions)
    table = jnp.concatenate([cosine[:, 0, :], sine[:, 0, :]], axis=1)
    table = jnp.pad(table, ((0, 0), (0, 128 - table.shape[1])))
    (
        places, part, hidden, attended, packed, normed_one, wide_cosine, wide_sine,
        cotangents, normed_two, mixed, grad_gate, grad_up,
    ) = forward(
        positions[None, :], table, gain_one, gain_two, inputs, cotangent, query_weight,
        key_weight, value_weight, output_weight, gate_weight, up_weight, down_weight, length,
        block, 1,
    )
    starts = places.reshape(8, 8, TILE)[:, 0, ::block].reshape(-1) // block
    slots = jnp.arange(length // block, dtype=jnp.int32)
    found = jnp.where(starts[None, :] == slots[:, None], slots[None, :], 0)
    order = jnp.concatenate([jnp.sum(found, axis=1), starts]).astype(jnp.int32)
    summed, gain_sums, input_grad, layer_output = backward(
        order, gain_one, gain_two, grad_gate, grad_up, mixed, normed_two, cotangents, part,
        hidden, inputs, query_weight, key_weight, value_weight, output_weight, down_weight,
        attended, packed, normed_one, wide_cosine, wide_sine, 5,
    )
    owners = (gate_weight, up_weight, down_weight, query_weight, key_weight, value_weight,
              output_weight)
    parts = widen(summed, [owner.shape[0] for owner in owners])
    return (layer_output, input_grad, gain_sums[0], *parts[3:], gain_sums[1], *parts[:3])


def per_device(*arrays):
    fits = lax.axis_size("fsdp") == 4 and lax.axis_size("ctx") == 8
    return (per_device_by_head if fits else per_device_gathered)(*arrays)


def solution(mesh):
    in_specs = (
        P(("fsdp", "ctx"), None),
        P(("fsdp", "ctx")),
        P(("fsdp", "ctx"), None),
        P(),
        P("fsdp", None),
        P("fsdp", None),
        P("fsdp", None),
        P("fsdp", None),
        P(),
        P("fsdp", None),
        P("fsdp", None),
        P("fsdp", None),
    )
    out_specs = (
        P(("fsdp", "ctx"), None),
        P(("fsdp", "ctx"), None),
        P(),
        P("fsdp", None),
        P("fsdp", None),
        P("fsdp", None),
        P("fsdp", None),
        P(),
        P("fsdp", None),
        P("fsdp", None),
        P("fsdp", None),
    )
    return jax.shard_map(
        per_device, mesh=mesh, in_specs=in_specs, out_specs=out_specs, check_vma=False
    )
```

```python
import functools
import math

import jax
import jax.numpy as jnp
from jax import lax
from jax.experimental import pallas as pl
from jax.experimental.pallas import tpu as pltpu
from jax.sharding import PartitionSpec as P

HEADS = 16
KV_HEADS = 8
HEAD_DIM = 96


EPSILON = 1e-05
ROPE_BASE = 100000.0


def product(left, right):
    return jnp.dot(left, right, preferred_element_type=jnp.float32)


def product_back(left, right):
    return lax.dot_general(
        left, right, (((1,), (1,)), ((), ())), preferred_element_type=jnp.float32
    )


def product_rows(left, right):
    return lax.dot_general(
        left, right, (((0,), (0,)), ((), ())), preferred_element_type=jnp.float32
    )


def rms_scale(values):
    return lax.rsqrt(jnp.mean(values * values, axis=-1, keepdims=True) + EPSILON)


def norm_back(scale_rows, unit_rows, grad_unit):
    return scale_rows * (
        grad_unit - unit_rows * jnp.mean(grad_unit * unit_rows, axis=-1, keepdims=True)
    )


def rotary_tables(places):
    half_width = HEAD_DIM // 2
    frequencies = ROPE_BASE ** (-(jnp.arange(half_width, dtype=jnp.float32) * 2.0 / HEAD_DIM))
    angles = places.astype(jnp.float32)[:, None] * frequencies[None, :]
    return (jnp.cos(angles)[:, None, :], jnp.sin(angles)[:, None, :])


def rotate(values, cosine, sine):
    half_width = values.shape[-1] // 2
    lower_half = values[..., :half_width]
    upper_half = values[..., half_width:]
    return jnp.concatenate(
        [lower_half * cosine - upper_half * sine, upper_half * cosine + lower_half * sine], axis=-1
    )


def rotate_back(grads, cosine, sine):
    half_width = grads.shape[-1] // 2
    lower_half = grads[..., :half_width]
    upper_half = grads[..., half_width:]
    return jnp.concatenate(
        [lower_half * cosine + upper_half * sine, upper_half * cosine - lower_half * sine], axis=-1
    )


def block_total_of(total_keys):
    return max(1, total_keys // 512)


def masked_scores(query_grouped, query_places, key_rows, key_places, start, width):
    key_part = lax.dynamic_slice_in_dim(key_rows, start, width, 2)
    place_part = lax.dynamic_slice_in_dim(key_places, start, width, 1)
    scores = jnp.einsum(
        "sqhgd,shkd->shgqk", query_grouped, key_part, preferred_element_type=jnp.float32
    )
    scores = scores * (1.0 / math.sqrt(HEAD_DIM))
    allowed = place_part[:, None, None, None, :] <= query_places[:, None, None, :, None]
    return jnp.where(allowed, scores, -1000000000.0)


def attend_forward(query_grouped, query_places, key_rows, value_rows, key_places):
    seq_count, row_count, head_groups, group_size = query_grouped.shape[:4]
    total_keys = key_rows.shape[2]
    block_total = block_total_of(total_keys)
    width = total_keys // block_total
    stat_shape = (seq_count, head_groups, group_size, row_count)

    def peak_step(index, carry):
        running_top, running_sum = carry
        scores = masked_scores(
            query_grouped, query_places, key_rows, key_places, index * width, width
        )
        new_top = jnp.maximum(running_top, jnp.max(scores, axis=-1))
        running_sum = running_sum * jnp.exp(running_top - new_top) + jnp.sum(
            jnp.exp(scores - new_top[..., None]), axis=-1
        )
        return (new_top, running_sum)

    running_top, running_sum = lax.fori_loop(
        0,
        block_total,
        peak_step,
        (jnp.full(stat_shape, -1e30, jnp.float32), jnp.zeros(stat_shape, jnp.float32)),
    )
    log_total = running_top + jnp.log(running_sum)

    def value_step(index, gathered):
        scores = masked_scores(
            query_grouped, query_places, key_rows, key_places, index * width, width
        )
        soft_low = jnp.exp(scores - log_total[..., None]).astype(jnp.bfloat16)
        value_part = lax.dynamic_slice_in_dim(value_rows, index * width, width, 2)
        return gathered + jnp.einsum(
            "shgqk,shkd->sqhgd", soft_low, value_part, preferred_element_type=jnp.float32
        )

    attended = lax.fori_loop(
        0, block_total, value_step, jnp.zeros(query_grouped.shape, jnp.float32)
    )
    return (attended, log_total)


def attend_backward(
    query_grouped, query_places, key_rows, value_rows, key_places, log_total, grad_attended
):
    total_keys = key_rows.shape[2]
    block_total = block_total_of(total_keys)
    width = total_keys // block_total
    score_scale = 1.0 / math.sqrt(HEAD_DIM)

    def soft_and_grad(index):
        scores = masked_scores(
            query_grouped, query_places, key_rows, key_places, index * width, width
        )
        soft_values = jnp.exp(scores - log_total[..., None])
        value_part = lax.dynamic_slice_in_dim(value_rows, index * width, width, 2)
        grad_soft = jnp.einsum(
            "sqhgd,shkd->shgqk", grad_attended, value_part, preferred_element_type=jnp.float32
        )
        return (soft_values, grad_soft)

    def delta_step(index, row_delta):
        soft_values, grad_soft = soft_and_grad(index)
        return row_delta + jnp.sum(soft_values * grad_soft, axis=-1)

    row_delta = lax.fori_loop(0, block_total, delta_step, jnp.zeros(log_total.shape, jnp.float32))

    def grad_step(index, carry):
        grad_query, grad_keys, grad_values = carry
        soft_values, grad_soft = soft_and_grad(index)
        grad_scores = (soft_values * (grad_soft - row_delta[..., None])).astype(jnp.bfloat16)
        key_part = lax.dynamic_slice_in_dim(key_rows, index * width, width, 2)
        grad_query = (
            grad_query
            + jnp.einsum(
                "shgqk,shkd->sqhgd", grad_scores, key_part, preferred_element_type=jnp.float32
            )
            * score_scale
        )
        key_term = (
            jnp.einsum(
                "shgqk,sqhgd->shkd", grad_scores, query_grouped, preferred_element_type=jnp.float32
            )
            * score_scale
        )
        value_term = jnp.einsum(
            "shgqk,sqhgd->shkd",
            soft_values.astype(jnp.bfloat16),
            grad_attended,
            preferred_element_type=jnp.float32,
        )
        grad_keys = lax.dynamic_update_slice_in_dim(grad_keys, key_term, index * width, 2)
        grad_values = lax.dynamic_update_slice_in_dim(grad_values, value_term, index * width, 2)
        return (grad_query, grad_keys, grad_values)

    initial = (
        jnp.zeros(query_grouped.shape, jnp.float32),
        jnp.zeros(key_rows.shape, jnp.float32),
        jnp.zeros(value_rows.shape, jnp.float32),
    )
    return lax.fori_loop(0, block_total, grad_step, initial)


def vmem():
    return pl.BlockSpec(memory_space=pltpu.VMEM)


def peer(ctx_index):
    return dict(device_id={"ctx": ctx_index}, device_id_type=pl.DeviceIdType.MESH)


SPINE_ROWS = 32
LINE_ROWS = 32
ROUND_ROWS = 2 * SPINE_ROWS + LINE_ROWS
LEAD = 4
HOP = 2
FEED = (0, 1, 3, 5, 8)
CHAIN = (0, 4, 6, 8, 10, 13, 24, 26, 30, 32)
RING = 20
TILE = 128
PAIR = (HEADS // KV_HEADS) * HEAD_DIM
WIDE = PAIR + 2 * HEAD_DIM


def near_fsdp(index):
    return dict(device_id={"fsdp": index}, device_id_type=pl.DeviceIdType.MESH)


def rows_at(start, count):
    return pl.ds(pl.multiple_of(start, 16), count)


class Place:
    def __init__(self):
        self.ctx = lax.axis_index("ctx")
        self.row = lax.axis_index("fsdp")
        self.chip, self.core = lax.div(self.row, 2), lax.rem(self.row, 2)
        self.partner = 2 * self.chip + 1 - self.core
        self.across = 2 * (1 - self.chip) + self.core
        self.corner = 2 * (1 - self.chip) + 1 - self.core

    def greet(self):
        barrier = pltpu.get_barrier_semaphore()
        for step in range(1, 4):
            pl.semaphore_signal(barrier, inc=1, **near_fsdp(lax.rem(self.row + step, 4)))
        for step in range(1, 8):
            pl.semaphore_signal(barrier, inc=1, **peer(lax.rem(self.ctx + step, 8)))
        pl.semaphore_wait(barrier, 10)


class Fold:
    def __init__(self, place, part, near, send, far, send_sem, recv_sem):
        self.place, self.part, self.near, self.send, self.far = place, part, near, send, far
        self.send_sem, self.recv_sem = send_sem, recv_sem

    def partner_copy(self, chip):
        block = 2 * chip + 1 - self.place.core
        return pltpu.make_async_remote_copy(
            src_ref=self.part.at[rows_at(block * TILE, TILE)],
            dst_ref=self.near.at[chip],
            send_sem=self.send_sem.at[chip],
            recv_sem=self.recv_sem.at[chip],
            **near_fsdp(self.place.partner),
        )

    def across_copy(self):
        return pltpu.make_async_remote_copy(
            src_ref=self.send,
            dst_ref=self.far,
            send_sem=self.send_sem.at[2],
            recv_sem=self.recv_sem.at[2],
            **near_fsdp(self.place.across),
        )

    def start(self):
        self.partner_copy(1 - self.place.chip).start()
        self.partner_copy(self.place.chip).start()

    def relay(self):
        there = 1 - self.place.chip
        self.partner_copy(there).wait_recv()
        base = self.place.across * TILE

        @pl.loop(0, TILE // 32)
        def _(piece):
            mine = self.part[rows_at(base + piece * 32, 32), :].astype(jnp.float32)
            span = rows_at(piece * 32, 32)
            self.send[span, :] = (
                mine + self.near[there, span, :].astype(jnp.float32)
            ).astype(jnp.bfloat16)

        self.across_copy().start()

    def arrive(self):
        self.partner_copy(self.place.chip).wait_recv()
        copy = self.across_copy()
        copy.wait_recv()
        copy.wait_send()
        self.partner_copy(0).wait_send()
        self.partner_copy(1).wait_send()

    def rows(self, start, count):
        mine = self.part[rows_at(self.place.row * TILE + start, count), :].astype(jnp.float32)
        span = rows_at(start, count)
        near = self.near[self.place.chip, span, :].astype(jnp.float32)
        return mine + near + self.far[span, :].astype(jnp.float32)


class Gather:
    def __init__(self, place, full, send_sem, recv_sem, count=TILE):
        self.place, self.full, self.send_sem, self.recv_sem = place, full, send_sem, recv_sem
        self.count = count

    def copy(self, block, target, key):
        span = pl.ds(pl.multiple_of(block * self.count, self.count), self.count)
        return pltpu.make_async_remote_copy(
            src_ref=self.full.at[span],
            dst_ref=self.full.at[span],
            send_sem=self.send_sem.at[key],
            recv_sem=self.recv_sem.at[key],
            **near_fsdp(target),
        )

    def start(self):
        self.copy(self.place.row, self.place.across, 1).start()
        self.copy(self.place.row, self.place.partner, 0).start()

    def relay(self):
        self.copy(self.place.across, self.place.across, 1).wait_recv()
        self.copy(self.place.across, self.place.partner, 2).start()

    def first(self):
        self.copy(self.place.partner, self.place.partner, 0).wait_recv()

    def arrive(self):
        self.copy(self.place.corner, self.place.partner, 2).wait_recv()
        self.copy(self.place.row, self.place.across, 1).wait_send()
        self.copy(self.place.row, self.place.partner, 0).wait_send()
        self.copy(self.place.across, self.place.partner, 2).wait_send()


class Swap:
    def __init__(self, place, source, target, send_sem, recv_sem, count, share=1):
        self.place, self.source, self.target = place, source, target
        self.send_sem, self.recv_sem, self.count, self.share = send_sem, recv_sem, count, share

    def span(self, index):
        return pl.ds(pl.multiple_of(index * self.count, self.count), self.count)

    def copy(self, other, sender):
        return pltpu.make_async_remote_copy(
            src_ref=self.source.at[self.span(lax.div(other, self.share))],
            dst_ref=self.target.at[self.span(sender)],
            send_sem=self.send_sem.at[other],
            recv_sem=self.recv_sem.at[sender],
            **peer(other),
        )

    def start(self, other):
        me = self.place.ctx

        @pl.when(other != me)
        def _():
            self.copy(other, me).start()

        @pl.when(other == me)
        def _():
            self.target[self.span(me)] = self.source[self.span(lax.div(me, self.share))]

    def start_all(self):
        for step in range(1, 9):
            self.start(lax.rem(self.place.ctx + step, 8))

    def arrive(self):
        for step in range(1, 8):
            other = lax.rem(self.place.ctx + step, 8)
            self.copy(other, other).wait()


class Spread:
    def __init__(self, slots, index, count, device, send_sem, recv_sem):
        self.slots, self.index, self.count, self.device = slots, index, count, device
        self.send_sem, self.recv_sem = send_sem, recv_sem

    def copy(self, step):
        return pltpu.make_async_remote_copy(
            src_ref=self.slots.at[self.index],
            dst_ref=self.slots.at[self.index],
            send_sem=self.send_sem.at[step],
            recv_sem=self.recv_sem.at[step],
            **self.device(lax.rem(self.index + step, self.count)),
        )

    def start(self):
        for step in range(1, self.count):
            self.copy(step).start()

    def total(self):
        for step in range(1, self.count):
            self.copy(step).wait()
        result = self.slots[0]
        for step in range(1, self.count):
            result += self.slots[step]
        return result


class Tree:
    def __init__(self, place, own, out_ref, index, rounds, line, box, sems, leaf_back):
        me = place.ctx
        depth, side = lax.div(me, 2), lax.rem(me, 2)
        other_side = me + 1 - 2 * side
        self.own, self.out, self.box, self.index, self.line = own, out_ref, box, index, line
        self.up, self.got, self.down, self.back = sems
        self.leaf_back = leaf_back
        if line:
            center = jnp.where(index >= rounds - 6, 1 + lax.rem(index, 2), lax.rem(index, 4))
            count = LINE_ROWS
            start = index * ROUND_ROWS + 2 * SPINE_ROWS
            root_side = lax.rem(index, 2)
            on_cross = depth == center
            self.root = jnp.logical_and(on_cross, side == root_side)
            has_side = self.root
            to_side = jnp.logical_and(on_cross, side != root_side)
            reach = jnp.maximum(center, 3 - center)
            away = jnp.abs(depth - center)
            crossed = jnp.where(side == root_side, 0, 1)
            self.rise_age = reach - away + jnp.where(self.root, 1, 0)
            self.fall_age = reach + 1 + away + crossed
        else:
            center = 1 + side
            count = SPINE_ROWS
            start = index * ROUND_ROWS + side * SPINE_ROWS
            self.root = depth == center
            has_side = None
        self.count = count
        self.start = start
        self.slot = lax.rem(index, RING)
        self.rows = rows_at(start, count)
        self.children = (
            (jnp.logical_and(depth > 0, depth <= center), me - 2, 0),
            (jnp.logical_and(depth < 3, depth >= center), me + 2, 1),
            (has_side, other_side, 2),
        )
        parent = jnp.where(depth < center, me + 2, me - 2)
        slot = jnp.where(depth < center, 0, 1)
        if line:
            parent = jnp.where(to_side, other_side, parent)
            slot = jnp.where(to_side, 2, slot)
        self.parent = jnp.where(self.root, other_side, parent)
        self.parent_slot = jnp.where(self.root, 2, slot)

    def boxed(self, slot):
        return self.box.at[slot, rows_at(self.slot * self.count, self.count)]

    def up_copy(self, target, slot):
        return pltpu.make_async_remote_copy(
            src_ref=self.own.at[self.rows],
            dst_ref=self.boxed(slot),
            send_sem=self.up.at[self.slot],
            recv_sem=self.got.at[slot, self.slot],
            **peer(target),
        )

    def down_copy(self, child, slot, source):
        back = self.back if slot < 2 or self.line else self.leaf_back
        return pltpu.make_async_remote_copy(
            src_ref=source.at[self.rows],
            dst_ref=self.out.at[self.rows],
            send_sem=self.down.at[slot, self.slot],
            recv_sem=back.at[self.slot],
            **peer(child),
        )

    def each_child(self, action):
        for present, child, slot in self.children:
            if present is None:
                action(child, slot)
            else:
                pl.when(present)(functools.partial(action, child, slot))

    def keep(self):
        return pltpu.make_async_copy(
            self.own.at[self.rows], self.out.at[self.rows], self.up.at[self.slot]
        )

    def rise(self):
        self.each_child(lambda child, slot: self.up_copy(child, slot).wait_recv())
        base = self.slot * self.count
        for piece in range(0, self.count, 16):
            span = rows_at(self.start + piece, 16)
            total = self.own[span, :].astype(jnp.float32)
            for present, _, slot in self.children:
                part = self.box[slot, rows_at(base + piece, 16), :].astype(jnp.float32)
                total += part if present is None else jnp.where(present, part, 0.0)
            self.own[span, :] = total.astype(jnp.bfloat16)

        @pl.when(jnp.logical_not(self.root))
        def _():
            self.up_copy(self.parent, self.parent_slot).start()

        @pl.when(self.root)
        def _():
            self.keep().start()
            self.each_child(lambda child, slot: self.down_copy(child, slot, self.own).start())

    def fall(self):
        @pl.when(jnp.logical_not(self.root))
        def _():
            self.down_copy(self.parent, 0, self.out).wait_recv()
            self.each_child(lambda child, slot: self.down_copy(child, slot, self.out).start())

    def finish(self):
        @pl.when(jnp.logical_not(self.root))
        def _():
            self.up_copy(self.parent, self.parent_slot).wait_send()

        @pl.when(self.root)
        def _():
            self.keep().wait()

        self.each_child(lambda child, slot: self.down_copy(child, slot, self.out).wait_send())


def softmax_parts(query_rows, key_rows, first_row):
    scores = product_back(query_rows, key_rows) * (1.0 / math.sqrt(HEAD_DIM))
    rows = lax.broadcasted_iota(jnp.int32, scores.shape, 0) + first_row
    columns = lax.broadcasted_iota(jnp.int32, scores.shape, 1)
    scores = jnp.where(columns <= rows, scores, -1e30)
    spread = jnp.exp(scores - jnp.max(scores, axis=-1, keepdims=True))
    return spread * (1.0 / jnp.sum(spread, axis=-1, keepdims=True))


def pack_pairs(blocks):
    half = blocks.shape[1] // 2
    return jnp.concatenate([blocks[:, :half], blocks[:, half:]], axis=-1)


def unpack_pairs(blocks):
    return jnp.concatenate([blocks[..., :PAIR], blocks[..., PAIR:]], axis=-2)


def sort_blocks(slot_ref, source, targets, opened=lambda rows: rows):
    block_total = source.shape[0]
    block = targets[0].shape[0] // block_total
    for index in range(block_total):
        rows = opened(source[slot_ref[index]])
        start = 0
        for target in targets:
            width = target.shape[-1]
            target[index * block : (index + 1) * block, :] = rows[:, start : start + width]
            start += width


def norm_back_rows(values, grad_unit):
    scale = rms_scale(values)
    unit = values * scale
    return unit, lambda grad: norm_back(scale, unit, grad)


def backward_kernel(
    rounds,
    block,
    order_ref,
    gain_one_ref,
    gain_two_ref,
    grad_gate_ref,
    grad_up_ref,
    mixed_ref,
    normed_two_ref,
    cotangent_ref,
    part_ref,
    hidden_ref,
    input_ref,
    query_weight_ref,
    key_weight_ref,
    value_weight_ref,
    output_weight_ref,
    down_weight_ref,
    attended_ref,
    packed_ref,
    normed_ref,
    cosine_ref,
    sine_ref,
    out_ref,
    gain_out_ref,
    input_grad_ref,
    layer_output_ref,
    own,
    spine_in,
    line_in,
    grad_gate,
    grad_up,
    mixed,
    normed_two,
    cotangents,
    part,
    hidden,
    inputs,
    output_weight,
    attended,
    packed,
    normed,
    cosine,
    sine,
    half_swap,
    weight,
    near,
    send,
    far,
    branch,
    grad_hidden,
    gain_part,
    heads_out,
    heads_in,
    q0,
    q1,
    k,
    v,
    g0,
    g1,
    result,
    dk,
    dv,
    packed_out,
    packed_in,
    turned,
    gain_near,
    gain_far,
    fetch_sem,
    spine_up,
    spine_got,
    spine_down,
    spine_back,
    leaf_up,
    leaf_back,
    line_up,
    line_got,
    line_down,
    line_back,
    fold_send,
    fold_recv,
    gather_send,
    gather_recv,
    swap_send,
    swap_recv,
    near_send,
    near_recv,
    far_send,
    far_recv,
):
    place = Place()
    me = place.ctx
    depth, side = lax.div(me, 2), lax.rem(me, 2)
    other_side = me + 1 - 2 * side
    hidden_units = mixed.shape[1]
    width = own.shape[1]
    base = 3 * hidden_units
    spare = rounds * ROUND_ROWS - base - 3 * WIDE
    length = q0.shape[0]
    halves = TILE // block
    tile = min(256, length)
    tiles = length // tile
    scale = 1.0 / math.sqrt(HEAD_DIM)

    fetches = {}

    def fetch_all(source, *copies):
        first = sum(len(group) for group in fetches.values())
        fetches[id(source)] = [
            pltpu.make_async_copy(*copy, fetch_sem.at[first + index])
            for index, copy in enumerate(copies or ())
        ]
        for copy in fetches[id(source)]:
            copy.start()

    def fetch(*sources):
        for source in sources:
            for copy in fetches[id(source)]:
                copy.wait()

    for source, target in (
        (part_ref, part),
        (grad_gate_ref, grad_gate),
        (normed_two_ref, normed_two),
        (grad_up_ref, grad_up),
        (mixed_ref, mixed),
        (cotangent_ref, cotangents),
        (hidden_ref, hidden),
        (packed_ref, packed),
        (down_weight_ref, own.at[pl.ds(base, hidden_units)]),
        (output_weight_ref, output_weight),
        (attended_ref, attended),
        (normed_ref, normed),
        (cosine_ref, cosine),
        (sine_ref, sine),
        (input_ref, inputs),
    ):
        fetch_all(source, (source, target))
    for source, first, count in (
        (query_weight_ref, 0, PAIR),
        (key_weight_ref, PAIR, HEAD_DIM),
        (value_weight_ref, PAIR + HEAD_DIM, HEAD_DIM),
    ):
        fetch_all(
            source,
            *(
                (source.at[pl.ds(head * count, count)], weight.at[head, pl.ds(first, count)])
                for head in range(2)
            ),
        )
    gain_one = gain_one_ref[...].astype(jnp.float32).reshape(1, -1)
    gain_two = gain_two_ref[...].astype(jnp.float32).reshape(1, -1)
    lanes = (WIDE, WIDE)
    row_lane = lax.broadcasted_iota(jnp.int32, lanes, 0)
    column_lane = lax.broadcasted_iota(jnp.int32, lanes, 1)
    half = HEAD_DIM // 2
    inner = lax.rem(column_lane, HEAD_DIM)
    partner_lane = column_lane + jnp.where(inner < half, half, -half)
    half_swap[...] = jnp.where(row_lane == partner_lane, 1.0, 0.0).astype(jnp.bfloat16)
    place.greet()
    fetch(part_ref)
    fold_two = Fold(place, part, near.at[0], send.at[0], far.at[0], fold_send.at[0], fold_recv.at[0])
    fold_output = Fold(
        place, part, near.at[0], send.at[0], far.at[0], fold_send.at[0], fold_recv.at[0]
    )
    fold_one = Fold(place, part, near.at[1], send.at[1], far.at[1], fold_send.at[1], fold_recv.at[1])
    gather = Gather(place, branch, gather_send, gather_recv)
    swap_heads = Swap(place, heads_out, heads_in, swap_send.at[0], swap_recv.at[0], halves)
    swap_packed = Swap(place, packed_out, packed_in, swap_send.at[1], swap_recv.at[1], halves)
    spread_near = Spread(gain_near, place.row, 4, near_fsdp, near_send, near_recv)
    spread_far = Spread(gain_far, me, 8, peer, far_send, far_recv)
    fold_two.start()

    def stage_feed(first):
        sides = ((grad_gate, normed_two), (grad_up, normed_two), (mixed, cotangents))
        left, right = sides[first // hidden_units]
        if first == 0:
            fetch(grad_gate_ref, normed_two_ref)
        elif first == hidden_units:
            fetch(grad_up_ref)
        elif first == 2 * hidden_units:
            fetch(mixed_ref)

        @pl.loop(0, 2)
        def _(index):
            start = first % hidden_units + index * 256
            columns = pl.ds(pl.multiple_of(start, 256), 256)
            rows = pl.ds(pl.multiple_of(first + index * 256, 256), 256)
            own[rows, :] = product_rows(left[:, columns], right[...]).astype(jnp.bfloat16)

    stage_feed(0)

    spine_sems = (spine_up, spine_got, spine_down, spine_back)
    line_sems = (line_up, line_got, line_down, line_back)

    def spine(index):
        return Tree(place, own, out_ref, index, rounds, False, spine_in, spine_sems, leaf_back)

    def line(index):
        return Tree(place, own, out_ref, index, rounds, True, line_in, line_sems, None)

    def leaf_rows(index):
        return rows_at(index * ROUND_ROWS + (1 - side) * SPINE_ROWS, SPINE_ROWS)

    def leaf_copy(index):
        slot = lax.rem(index, RING)
        return pltpu.make_async_remote_copy(
            src_ref=own.at[leaf_rows(index)],
            dst_ref=spine_in.at[2, rows_at(slot * SPINE_ROWS, SPINE_ROWS)],
            send_sem=leaf_up.at[slot],
            recv_sem=spine_got.at[2, slot],
            **peer(other_side),
        )

    def leaf_result(index):
        slot = lax.rem(index, RING)
        return pltpu.make_async_remote_copy(
            src_ref=own.at[leaf_rows(index)],
            dst_ref=out_ref.at[leaf_rows(index)],
            send_sem=leaf_up.at[slot],
            recv_sem=leaf_back.at[slot],
            **peer(other_side),
        )

    def stage_norm_two():
        fetch(hidden_ref, cotangent_ref)
        fold_two.arrive()
        gain_part[...] = jnp.zeros_like(gain_part)

        @pl.loop(0, TILE // 16)
        def _(piece):
            span = rows_at(piece * 16, 16)
            grad = fold_two.rows(piece * 16, 16)
            unit, back = norm_back_rows(hidden[span, :], None)
            gain_part[1] += (grad * unit).reshape(2, 8, -1).sum(axis=0)
            here = rows_at(place.row * TILE + piece * 16, 16)
            total = cotangents[here, :].astype(jnp.float32) + back(grad * gain_two)
            grad_hidden[span, :] = total
            branch[here, :] = total.astype(jnp.bfloat16)

        gather.start()

    def stage_heads():
        fetch(output_weight_ref)
        gather.first()
        gather.arrive()

        @pl.loop(0, 4)
        def _(sequence):
            rows = branch[rows_at(sequence * TILE, TILE), :]
            grads = product_back(rows, output_weight[...]).astype(jnp.bfloat16)
            for head in range(2):
                heads_out[pl.ds((2 * sequence + head) * halves, halves)] = pack_pairs(
                    grads[:, head * PAIR : (head + 1) * PAIR].reshape(halves, block, PAIR)
                )

        swap_heads.start_all()

    def stage_sort():
        fetch(packed_ref)
        sort_blocks(order_ref, packed, (q0, q1, k, v))

    def stage_output_grad():
        fetch(attended_ref)
        for head in range(2):
            rows = [
                attended[(2 * index + head) * halves : (2 * index + head + 1) * halves]
                for index in range(4)
            ]
            rows = unpack_pairs(jnp.concatenate(rows, axis=0)).reshape(4 * TILE, PAIR)
            first_row = base + 2 * WIDE + head * PAIR
            for first in range(0, own.shape[1], 512):
                columns = slice(first, first + 512)
                own[first_row : first_row + PAIR, columns] = product_rows(
                    rows, branch[:, columns]
                ).astype(jnp.bfloat16)

    def stage_sort_grads():
        swap_heads.arrive()
        sort_blocks(order_ref, heads_in, (g0, g1), unpack_pairs)
        dk[...] = jnp.zeros_like(dk)
        dv[...] = jnp.zeros_like(dv)

    def stage_attention(index):
        first, top = index * tile, (index + 1) * tile
        parts = []
        for q, g in ((q0, g0), (q1, g1)):
            query_rows = q[first:top, :]
            grad_rows = g[first:top, :]
            soft = softmax_parts(query_rows, k[:top, :], first)
            grad_soft = product_back(grad_rows, v[:top, :])
            delta = jnp.sum(soft * grad_soft, axis=-1, keepdims=True)
            grad_scores = (soft * (grad_soft - delta)).astype(jnp.bfloat16)
            parts.append(product(grad_scores, k[:top, :]) * scale)
            key_term = product_rows(grad_scores, query_rows) * scale
            value_term = product_rows(soft.astype(jnp.bfloat16), grad_rows)
            dk[: top // block] += key_term.reshape(-1, block, HEAD_DIM)
            dv[: top // block] += value_term.reshape(-1, block, HEAD_DIM)
        result[first // block : top // block] = jnp.concatenate(parts, axis=-1).reshape(
            -1, block, PAIR
        )

    def stage_unsort():
        for slot in range(length // block):
            spot = order_ref[length // block + slot]
            packed_out[slot] = jnp.concatenate(
                [result[spot], dk[spot], dv[spot]], axis=-1
            ).astype(jnp.bfloat16)
        swap_packed.start_all()

    def stage_turn():
        fetch(cosine_ref, sine_ref, query_weight_ref, key_weight_ref, value_weight_ref)
        swap_packed.arrive()

        @pl.loop(0, 4)
        def _(sequence):
            span = rows_at(sequence * TILE, TILE)
            total = None
            for head in range(2):
                grads = packed_in[pl.ds((2 * sequence + head) * halves, halves)]
                grads = grads.reshape(TILE, WIDE)
                swapped = product(grads, half_swap[...])
                low = (
                    grads.astype(jnp.float32) * cosine[span, :] - swapped * sine[span, :]
                ).astype(jnp.bfloat16)
                turned[head, span, :] = low
                term = product(low, weight[head])
                total = term if total is None else total + term
            part[span, :] = total.astype(jnp.bfloat16)

        fold_one.start()

    def stage_projection_grads(head):
        if head == 0:
            fetch(normed_ref)
        query_base = base + head * PAIR
        key_base = base + WIDE + head * HEAD_DIM
        value_base = key_base + 2 * HEAD_DIM
        for first in range(0, own.shape[1], 512):
            columns = slice(first, first + 512)
            grads = product_rows(turned[head], normed[:, columns]).astype(jnp.bfloat16)
            own[query_base : query_base + PAIR, columns] = grads[:PAIR]
            own[key_base : key_base + HEAD_DIM, columns] = grads[PAIR : PAIR + HEAD_DIM]
            own[value_base : value_base + HEAD_DIM, columns] = grads[PAIR + HEAD_DIM :]

    def stage_norm_one():
        fetch(input_ref)
        fold_one.arrive()

        @pl.loop(0, TILE // 16)
        def _(piece):
            span = rows_at(piece * 16, 16)
            grad = fold_one.rows(piece * 16, 16)
            unit, back = norm_back_rows(inputs[span, :].astype(jnp.float32), None)
            gain_part[0] += (grad * unit).reshape(2, 8, -1).sum(axis=0)
            input_grad_ref[span, :] = grad_hidden[span, :] + back(grad * gain_one)

        gain_near[place.row] = jnp.sum(gain_part[...], axis=1)
        spread_near.start()

    def stage_gain():
        gain_far[me] = spread_near.total()
        spread_far.start()

    def stage_output():
        fetch(down_weight_ref)

        @pl.loop(0, 4)
        def _(sequence):
            span = rows_at(sequence * TILE, TILE)
            part[span, :] = product(
                mixed[span, :], own[base : base + hidden_units, :]
            ).astype(jnp.bfloat16)

    def stage_output_sum():
        fold_output.arrive()

        @pl.loop(0, TILE // 16)
        def _(piece):
            span = rows_at(piece * 16, 16)
            total = hidden[span, :] + fold_output.rows(piece * 16, 16)
            layer_output_ref[span, :] = total.astype(jnp.bfloat16)

    def stage_clear():
        if spare:
            own[base + 3 * WIDE :, :] = jnp.zeros((spare, width), own.dtype)

    units = 2 * 256
    stages = [
        (FEED[index], functools.partial(stage_feed, (index + 1) * units)) for index in range(5)
    ]
    stages += [
        (CHAIN[0], fold_two.relay),
        (CHAIN[0], stage_sort),
        (CHAIN[1], stage_norm_two),
        (CHAIN[2], gather.relay),
        (CHAIN[2], stage_output),
        (CHAIN[3], stage_heads),
        (CHAIN[3], fold_output.start),
        (CHAIN[4], fold_output.relay),
        (CHAIN[4], stage_output_grad),
        (CHAIN[4], stage_clear),
        (CHAIN[5], stage_sort_grads),
    ]
    stages += [
        (CHAIN[5] + index, functools.partial(stage_attention, index)) for index in range(tiles)
    ]
    stages += [
        (CHAIN[5] + tiles - 1, stage_unsort),
        (CHAIN[5] + tiles, stage_output_sum),
        (CHAIN[6], stage_turn),
        (CHAIN[7], fold_one.relay),
        (CHAIN[7], functools.partial(stage_projection_grads, 0)),
        (CHAIN[7] + 1, functools.partial(stage_projection_grads, 1)),
        (CHAIN[8], stage_norm_one),
        (CHAIN[9], stage_gain),
    ]
    assert CHAIN[7] + 1 < base // ROUND_ROWS - LEAD
    for index in range(5):
        assert FEED[index] < (index + 1) * units // ROUND_ROWS - LEAD

    for index in range(LEAD):
        leaf_copy(index).start()

    def valid(index):
        return jnp.logical_and(index >= 0, index < rounds)

    @pl.loop(0, rounds + RING)
    def _(now):
        far_side = jnp.abs(depth - 2 + side)
        off_center = jnp.abs(depth - 1 - side)
        done = now - RING + 1
        for tree in (spine(done), line(done)):
            pl.when(valid(done))(tree.finish)

        rising = spine(now - HOP * (3 - off_center))
        pl.when(valid(rising.index))(rising.rise)

        @pl.loop(0, 5)
        def _(age):
            tree = line(now - HOP * age)
            pl.when(jnp.logical_and(valid(tree.index), tree.rise_age == age))(tree.rise)

        @pl.when(now + LEAD < rounds)
        def _():
            leaf_copy(now + LEAD).start()

        falling = spine(now - HOP * (3 + off_center))
        pl.when(valid(falling.index))(falling.fall)

        @pl.loop(4, 9)
        def _(age):
            tree = line(now - HOP * age)
            pl.when(jnp.logical_and(valid(tree.index), tree.fall_age == age))(tree.fall)

        leaf_fall = now - HOP * (4 + far_side)

        @pl.when(valid(leaf_fall))
        def _():
            leaf_result(leaf_fall).wait_recv()
            leaf_copy(leaf_fall).wait_send()

        for when, stage in stages:
            pl.when(now == when)(stage)

    gain_out_ref[...] = spread_far.total()


def backward(order, gain_one, gain_two, grad_gate, grad_up, mixed, normed_two, cotangents, part,
             hidden, inputs, query_weight, key_weight, value_weight, output_weight, down_weight,
             attended, packed, normed, cosine, sine, key):
    width = hidden.shape[1]
    rows = 3 * mixed.shape[1] + 3 * WIDE
    rounds = -(-rows // ROUND_ROWS)
    block = packed.shape[1]
    length = packed.shape[0] * block
    dma = pltpu.SemaphoreType.DMA
    low, full = jnp.bfloat16, jnp.float32
    any_spec = pl.BlockSpec(memory_space=pl.ANY)
    operands = (
        order, gain_one, gain_two, grad_gate, grad_up, mixed, normed_two, cotangents, part,
        hidden, inputs, query_weight, key_weight, value_weight, output_weight, down_weight,
        attended, packed, normed, cosine, sine,
    )

    def like(array):
        return pltpu.VMEM(array.shape, array.dtype)

    return pl.pallas_call(
        functools.partial(backward_kernel, rounds, block),
        out_shape=(
            jax.ShapeDtypeStruct((rounds * ROUND_ROWS, width), low),
            jax.ShapeDtypeStruct((2, width), full),
            jax.ShapeDtypeStruct((TILE, width), full),
            jax.ShapeDtypeStruct((TILE, width), low),
        ),
        in_specs=[pl.BlockSpec(memory_space=pltpu.SMEM)] + [vmem()] * 2 + [any_spec] * 18,
        out_specs=(any_spec, vmem(), vmem(), vmem()),
        scratch_shapes=[
            pltpu.VMEM((rounds * ROUND_ROWS, width), low),
            pltpu.VMEM((3, RING * SPINE_ROWS, width), low),
            pltpu.VMEM((3, RING * LINE_ROWS, width), low),
            like(grad_gate), like(grad_up), like(mixed), like(normed_two), like(cotangents),
            like(part), like(hidden), like(inputs), like(output_weight),
            like(attended), like(packed), like(normed), like(cosine), like(sine),
            pltpu.VMEM((WIDE, WIDE), low),
            pltpu.VMEM((2, WIDE, width), low),
            pltpu.VMEM((2, 2, TILE, width), low),
            pltpu.VMEM((2, TILE, width), low),
            pltpu.VMEM((2, TILE, width), low),
            pltpu.VMEM((4 * TILE, width), low),
            pltpu.VMEM((TILE, width), full),
            pltpu.VMEM((2, 8, width), full),
            pltpu.VMEM((length // block, block // 2, 2 * PAIR), low),
            pltpu.VMEM((length // block, block // 2, 2 * PAIR), low),
        ]
        + [pltpu.VMEM((length, HEAD_DIM), low)] * 6
        + [pltpu.VMEM((length // block, block, PAIR), full)]
        + [pltpu.VMEM((length // block, block, HEAD_DIM), full)] * 2
        + [
            pltpu.VMEM((length // block, block, WIDE), low),
            pltpu.VMEM((length // block, block, WIDE), low),
            pltpu.VMEM((2, 4 * TILE, WIDE), low),
            pltpu.VMEM((4, 2, width), full),
            pltpu.VMEM((8, 2, width), full),
            dma((21,)),
            dma((RING,)), dma((3, RING)), dma((3, RING)), dma((RING,)),
            dma((RING,)), dma((RING,)),
            dma((RING,)), dma((3, RING)), dma((3, RING)), dma((RING,)),
            dma((2, 3)), dma((2, 3)),
            dma((3,)), dma((3,)),
            dma((2, 8)), dma((2, 8)),
            dma((4,)), dma((4,)), dma((8,)), dma((8,)),
        ],
        compiler_params=pltpu.CompilerParams(
            collective_id=key, has_side_effects=True, vmem_limit_bytes=63 * 2**20
        ),
        name="backward",
    )(*operands)


def forward_kernel(
    block,
    place_ref,
    table_ref,
    gain_one_ref,
    gain_two_ref,
    input_ref,
    cotangent_ref,
    query_weight_ref,
    key_weight_ref,
    value_weight_ref,
    output_weight_ref,
    gate_weight_ref,
    up_weight_ref,
    down_weight_ref,
    place_out,
    part_out,
    hidden_out,
    attended_out,
    packed_out,
    normed_one_out,
    cosine_out,
    sine_out,
    cotangent_out,
    normed_two_out,
    mixed_out,
    grad_gate_out,
    grad_up_out,
    places,
    tables,
    inputs,
    cotangents,
    normed_one,
    normed_two,
    cosine,
    sine,
    weight,
    output_weight,
    gate_weight,
    up_weight,
    down_weight,
    packed_from,
    packed,
    q0,
    q1,
    k,
    v,
    result,
    heads_from,
    heads,
    part,
    near,
    send,
    far,
    hidden,
    mixed,
    grad_gate,
    grad_up,
    fetch_sem,
    store_sem,
    gather_send,
    gather_recv,
    swap_send,
    swap_recv,
    fold_send,
    fold_recv,
):
    place = Place()
    length, width = q0.shape[0], inputs.shape[1]
    halves = TILE // block
    half = HEAD_DIM // 2
    pair_rows = 2 * TILE
    fetches, stores = {}, []

    def fetch_all(key, *copies):
        base = sum(len(group) for group in fetches.values())
        fetches[key] = [
            pltpu.make_async_copy(part_of, target, fetch_sem.at[base + index])
            for index, (part_of, target) in enumerate(copies)
        ]
        for copy in fetches[key]:
            copy.start()

    def fetch(*keys):
        for key in keys:
            for copy in fetches[key]:
                copy.wait()

    def store(source, target):
        copy = pltpu.make_async_copy(source, target, store_sem.at[len(stores)])
        copy.start()
        stores.append(copy)

    own_rows = rows_at(place.row * TILE, TILE)
    fetch_all("inputs", (input_ref, inputs.at[own_rows]))
    fetch_all("cotangent", (cotangent_ref, cotangents.at[own_rows]))
    copies = []
    for head in range(2):
        query_base, key_base = head * PAIR, head * HEAD_DIM
        target = weight.at[head]
        heads_of = [(query_weight_ref, query_base), (query_weight_ref, query_base + HEAD_DIM)]
        heads_of += [(key_weight_ref, key_base), (value_weight_ref, key_base)]
        for index, (source, first) in enumerate(heads_of):
            copies.append(
                (source.at[pl.ds(first, HEAD_DIM)], target.at[pl.ds(index * HEAD_DIM, HEAD_DIM)])
            )
            for side in range(2):
                copies.append(
                    (
                        source.at[pl.ds(first + (1 - side) * half, half)],
                        target.at[pl.ds(WIDE + index * HEAD_DIM + side * half, half)],
                    )
                )
    fetch_all("weight", *copies)
    fetch_all("output", (output_weight_ref, output_weight))
    fetch_all("gate", (gate_weight_ref, gate_weight))
    fetch_all("up", (up_weight_ref, up_weight))
    fetch_all("down", (down_weight_ref, down_weight))
    places[pl.ds(pl.multiple_of(place.row * 8, 8), 8), :] = jnp.broadcast_to(
        place_ref[...], (8, place_ref.shape[1])
    )
    gain_one = gain_one_ref[...].astype(jnp.float32).reshape(1, -1)
    gain_two = gain_two_ref[...].astype(jnp.float32).reshape(1, -1)
    tables[own_rows, :] = table_ref[...]
    gather_places = Gather(place, places, gather_send.at[0], gather_recv.at[0], 8)
    gather_tables = Gather(place, tables, gather_send.at[1], gather_recv.at[1])
    gather_inputs = Gather(place, inputs, gather_send.at[2], gather_recv.at[2])
    gather_cotangents = Gather(place, cotangents, gather_send.at[3], gather_recv.at[3])
    gather_two = Gather(place, normed_two, gather_send.at[4], gather_recv.at[4])
    swap_places = Swap(place, places, place_out, swap_send.at[0], swap_recv.at[0], 8, 2)
    swap_packed = Swap(place, packed_from, packed, swap_send.at[1], swap_recv.at[1], halves)
    swap_heads = Swap(place, heads_from, heads, swap_send.at[2], swap_recv.at[2], halves)
    fold = Fold(place, part, near, send, far, fold_send, fold_recv)
    place.greet()
    fetch("inputs")
    gather_tables.start()
    gather_inputs.start()
    gather_places.start()
    fetch("cotangent")
    gather_cotangents.start()

    def project(chip):
        base = chip * pair_rows

        @pl.loop(0, pair_rows // 16)
        def _(piece):
            span = rows_at(base + piece * 16, 16)
            rows = inputs[span, :].astype(jnp.float32)
            normed_one[span, :] = (rows * rms_scale(rows) * gain_one).astype(jnp.bfloat16)

        span = rows_at(base, pair_rows)
        low_cosine, low_sine = tables[span, :half], tables[span, half:HEAD_DIM]
        ones = jnp.ones((pair_rows, HEAD_DIM), jnp.float32)
        cosine[span, :] = jnp.concatenate([low_cosine] * 6 + [ones], axis=-1)
        sine[span, :] = jnp.concatenate([-low_sine, low_sine] * 3 + [ones * 0.0], axis=-1)

        for head in range(2):
            products = product_back(normed_one[span, :], weight[head])
            low = (
                products[:, :WIDE] * cosine[span, :] + products[:, WIDE:] * sine[span, :]
            ).astype(jnp.bfloat16)
            for index in range(2):
                packed_from[pl.ds(((2 * chip + index) * 2 + head) * halves, halves)] = low[
                    index * TILE : (index + 1) * TILE
                ].reshape(halves, block, WIDE)
        for index in range(4):
            swap_packed.start(4 * chip + index)

    gather_tables.first()
    gather_inputs.first()
    gather_places.first()
    fetch("weight")
    project(place.chip)
    gather_tables.relay()
    gather_inputs.relay()
    gather_places.relay()
    gather_tables.arrive()
    gather_inputs.arrive()
    gather_places.arrive()
    project(1 - place.chip)
    swap_places.start_all()
    store(normed_one, normed_one_out)
    store(cosine, cosine_out)
    store(sine, sine_out)
    swap_places.arrive()
    swap_packed.arrive()
    store(packed, packed_out)

    def place_row(first, count):
        blocks = [place_out[8 * index : 8 * index + 1, :] for index in range(first, first + count)]
        return jnp.concatenate(blocks, axis=-1)

    tile = min(256, length)
    order = place_row(0, length // TILE)
    flat = packed[...].reshape(length, WIDE)
    for first in range(0, length, tile):
        rows = lax.broadcasted_iota(jnp.int32, (tile, length), 0) + first
        chosen = jnp.where(rows == order, 1.0, 0.0).astype(jnp.bfloat16)
        moved = product(chosen, flat).astype(jnp.bfloat16)
        for index, target in enumerate((q0, q1, k, v)):
            target[first : first + tile, :] = moved[:, index * HEAD_DIM : (index + 1) * HEAD_DIM]
    for first in range(0, length, tile):
        parts = []
        for q in (q0, q1):
            soft = softmax_parts(q[first : first + tile, :], k[: first + tile, :], first)
            parts.append(product(soft.astype(jnp.bfloat16), v[: first + tile, :]))
        result[first : first + tile, :] = jnp.concatenate(parts, axis=-1).astype(jnp.bfloat16)
    for first in range(0, length, tile):
        rows = lax.broadcasted_iota(jnp.int32, (length, tile), 0)
        chosen = jnp.where(rows == place_row(first // TILE, tile // TILE), 1.0, 0.0)
        moved = product_rows(chosen.astype(jnp.bfloat16), result[...]).astype(jnp.bfloat16)
        heads_from[first // block : (first + tile) // block] = pack_pairs(
            moved.reshape(-1, block, PAIR)
        )
    swap_heads.start_all()
    gather_cotangents.first()
    gather_cotangents.relay()
    fetch("output")
    swap_heads.arrive()
    store(heads, attended_out)

    def project_out(sequence):
        total = None
        for head in range(2):
            rows = heads[pl.ds((2 * sequence + head) * halves, halves)]
            rows = unpack_pairs(rows).reshape(TILE, PAIR)
            term = product(rows, output_weight[head * PAIR : (head + 1) * PAIR, :])
            total = term if total is None else total + term
        part[rows_at(sequence * TILE, TILE), :] = total.astype(jnp.bfloat16)

    for chip in (1 - place.chip, place.chip):
        project_out(2 * chip + 1 - place.core)
        fold.partner_copy(chip).start()
        project_out(2 * chip + place.core)
    gather_cotangents.arrive()
    store(cotangents, cotangent_out)
    fold.relay()
    fold.arrive()

    @pl.loop(0, TILE // 16)
    def _(piece):
        span = rows_at(piece * 16, 16)
        own = rows_at(place.row * TILE + piece * 16, 16)
        rows = inputs[own, :].astype(jnp.float32) + fold.rows(piece * 16, 16)
        hidden[span, :] = rows
        normed_two[own, :] = (rows * rms_scale(rows) * gain_two).astype(jnp.bfloat16)

    gather_two.start()
    store(hidden, hidden_out)
    fetch("gate", "up", "down")

    def feed(chip):
        span = rows_at(chip * pair_rows, pair_rows)

        @pl.loop(0, mixed.shape[1] // 256)
        def _(index):
            units = rows_at(index * 256, 256)
            columns = pl.ds(pl.multiple_of(index * 256, 256), 256)
            gate = product_back(normed_two[span, :], gate_weight[units, :])
            upward = product_back(normed_two[span, :], up_weight[units, :])
            grad_mixed = product_back(cotangents[span, :], down_weight[units, :])
            sigmoid = jax.nn.sigmoid(gate)
            activated = gate * sigmoid
            mixed[span, columns] = (activated * upward).astype(jnp.bfloat16)
            grad_gate[span, columns] = (
                grad_mixed * upward * sigmoid * (1.0 + gate * (1.0 - sigmoid))
            ).astype(jnp.bfloat16)
            grad_up[span, columns] = (grad_mixed * activated).astype(jnp.bfloat16)

        @pl.loop(0, width // 512)
        def _(index):
            columns = pl.ds(pl.multiple_of(index * 512, 512), 512)
            part[span, columns] = (
                product(grad_gate[span, :], gate_weight[:, columns])
                + product(grad_up[span, :], up_weight[:, columns])
            ).astype(jnp.bfloat16)

    def store_feed(chip):
        span = rows_at(chip * pair_rows, pair_rows)
        for source, target in (
            (part, part_out), (mixed, mixed_out), (grad_gate, grad_gate_out),
            (grad_up, grad_up_out),
        ):
            store(source.at[span], target.at[span])

    gather_two.first()
    feed(place.chip)
    store_feed(place.chip)
    gather_two.relay()
    gather_two.arrive()
    store(normed_two, normed_two_out)
    feed(1 - place.chip)
    store_feed(1 - place.chip)
    for copy in stores:
        copy.wait()


def forward(places, table, gain_one, gain_two, inputs, cotangent, query_weight, key_weight, value_weight,
            output_weight, gate_weight, up_weight, down_weight, length, block, key):
    width = inputs.shape[1]
    hidden_units = gate_weight.shape[0]
    rows = 4 * TILE
    blocks = length // block
    low, full = jnp.bfloat16, jnp.float32
    dma = pltpu.SemaphoreType.DMA
    any_spec = pl.BlockSpec(memory_space=pl.ANY)

    def out(shape, dtype):
        return jax.ShapeDtypeStruct(shape, dtype)

    wide = (rows, width)
    return pl.pallas_call(
        functools.partial(forward_kernel, block),
        out_shape=(
            out((64, 128), jnp.int32),
            out(wide, low), out((TILE, width), full),
            out((blocks, block // 2, 2 * PAIR), low), out((blocks, block, WIDE), low),
            out(wide, low), out((rows, WIDE), full), out((rows, WIDE), full),
            out(wide, low), out(wide, low),
            out((rows, hidden_units), low), out((rows, hidden_units), low),
            out((rows, hidden_units), low),
        ),
        in_specs=[vmem()] * 4 + [any_spec] * 9,
        out_specs=(vmem(),) + (any_spec,) * 12,
        scratch_shapes=[
            pltpu.VMEM((32, 128), jnp.int32),
            pltpu.VMEM((rows, 128), full),
            pltpu.VMEM(wide, low), pltpu.VMEM(wide, low),
            pltpu.VMEM(wide, low), pltpu.VMEM(wide, low),
            pltpu.VMEM((rows, WIDE), full), pltpu.VMEM((rows, WIDE), full),
            pltpu.VMEM((2, 2 * WIDE, width), low),
            pltpu.VMEM(output_weight.shape, low),
            pltpu.VMEM((hidden_units, width), low), pltpu.VMEM((hidden_units, width), low),
            pltpu.VMEM((hidden_units, width), low),
            pltpu.VMEM((blocks, block, WIDE), low), pltpu.VMEM((blocks, block, WIDE), low),
        ]
        + [pltpu.VMEM((length, HEAD_DIM), low)] * 4
        + [
            pltpu.VMEM((length, PAIR), low),
            pltpu.VMEM((blocks, block // 2, 2 * PAIR), low),
            pltpu.VMEM((blocks, block // 2, 2 * PAIR), low),
            pltpu.VMEM(wide, low),
            pltpu.VMEM((2, TILE, width), low),
            pltpu.VMEM((TILE, width), low), pltpu.VMEM((TILE, width), low),
            pltpu.VMEM((TILE, width), full),
            pltpu.VMEM((rows, hidden_units), low), pltpu.VMEM((rows, hidden_units), low),
            pltpu.VMEM((rows, hidden_units), low),
            dma((30,)), dma((16,)),
            dma((5, 3)), dma((5, 3)),
            dma((3, 8)), dma((3, 8)),
            dma((3,)), dma((3,)),
        ],
        compiler_params=pltpu.CompilerParams(
            collective_id=key, has_side_effects=True, vmem_limit_bytes=63 * 2**20
        ),
        name="forward",
    )(places, table, gain_one, gain_two, inputs, cotangent, query_weight, key_weight, value_weight,
      output_weight, gate_weight, up_weight, down_weight)


def widen_kernel(plan, kept, source, *refs):
    sources, refs = refs[:kept], refs[kept:]
    holds, refs, hold_sem = refs[-1 - kept : -1], refs[: -1 - kept], refs[-1]
    targets, (low, full, load_sem, store_sem) = refs[:-4], refs[-4:]
    targets, copies = targets[: len(targets) - kept], targets[len(targets) - kept :]
    takes = [
        pltpu.make_async_copy(sources[index], holds[index], hold_sem.at[index])
        for index in range(kept)
    ]
    gives = [
        pltpu.make_async_copy(holds[index], copies[index], hold_sem.at[kept + index])
        for index in range(kept)
    ]
    slots = low.shape[0]
    loads, stores = [], []
    for index, (first, which, target_row, chunk) in enumerate(plan):
        slot = index % slots
        span = pl.ds(0, chunk)
        loads.append(
            pltpu.make_async_copy(
                source.at[pl.ds(first, chunk)], low.at[slot, span], load_sem.at[slot]
            )
        )
        stores.append(
            pltpu.make_async_copy(
                full.at[slot, span],
                targets[which].at[pl.ds(target_row, chunk)],
                store_sem.at[slot],
            )
        )
    for load in loads[:slots] + takes:
        load.start()
    for index, (load, store) in enumerate(zip(loads, stores)):
        slot = index % slots
        load.wait()
        if index >= slots:
            stores[index - slots].wait()

        @pl.loop(0, plan[index][3] // 16)
        def _(piece):
            span = rows_at(piece * 16, 16)
            full[slot, span, :] = low[slot, span, :].astype(jnp.float32)

        store.start()
        if index + slots < len(plan):
            loads[index + slots].start()
        if index == slots:
            for take, give in zip(takes, gives):
                take.wait()
                give.start()
    for store in stores[-slots:] + gives:
        store.wait()


def widen(values, counts, keep):
    slots, width, first, plan = 6, values.shape[1], 0, []
    for which, count in enumerate(counts):
        chunk = math.gcd(count, 256) if count % 192 else 192
        plan += [(first + row, which, row, chunk) for row in range(0, count, chunk)]
        first += count
    any_spec = pl.BlockSpec(memory_space=pl.ANY)
    return pl.pallas_call(
        functools.partial(widen_kernel, plan, len(keep)),
        out_shape=tuple(jax.ShapeDtypeStruct((count, width), jnp.float32) for count in counts)
        + tuple(jax.ShapeDtypeStruct(array.shape, array.dtype) for array in keep),
        in_specs=[any_spec] * (1 + len(keep)),
        out_specs=(any_spec,) * (len(counts) + len(keep)),
        scratch_shapes=[
            pltpu.VMEM((slots, 256, width), values.dtype),
            pltpu.VMEM((slots, 256, width), jnp.float32),
            pltpu.SemaphoreType.DMA((slots,)),
            pltpu.SemaphoreType.DMA((slots,)),
        ]
        + [pltpu.VMEM(array.shape, array.dtype) for array in keep]
        + [pltpu.SemaphoreType.DMA((2 * len(keep),))],
        compiler_params=pltpu.CompilerParams(vmem_limit_bytes=63 * 2**20),
        name="widen",
    )(values, *keep)


def gather_rows(values):
    return lax.all_gather(values, "fsdp", axis=0, tiled=True)


def scatter_rows(values):
    return lax.psum_scatter(
        values.astype(jnp.bfloat16), "fsdp", scatter_dimension=0, tiled=True
    ).astype(jnp.float32)


def per_device_gathered(
    inputs,
    positions,
    cotangent,
    attention_gain,
    query_weight,
    key_weight,
    value_weight,
    output_weight,
    feedforward_gain,
    gate_weight,
    up_weight,
    down_weight,
):
    row_count = inputs.shape[0]
    groups = HEADS // KV_HEADS
    gain_one = attention_gain.astype(jnp.float32)
    gain_two = feedforward_gain.astype(jnp.float32)
    seq_count = lax.axis_size("fsdp")
    first_row = lax.axis_index("fsdp") * row_count

    def own(values):
        return lax.dynamic_slice_in_dim(values, first_row, row_count, 0)

    query_places = gather_rows(positions).reshape(seq_count, row_count)
    key_places = lax.all_gather(query_places, "ctx", axis=1, tiled=True)
    all_cotangent = gather_rows(cotangent)
    flat_in = gather_rows(inputs).astype(jnp.float32)
    scale_one = rms_scale(flat_in)
    unit_one = flat_in * scale_one
    normed_one = (unit_one * gain_one).astype(jnp.bfloat16)
    total_rows = normed_one.shape[0]
    cosine, sine = rotary_tables(query_places.reshape(-1))
    query_heads = query_weight.shape[0] // HEAD_DIM
    kv_heads = key_weight.shape[0] // HEAD_DIM
    kv_width = kv_heads * HEAD_DIM
    query_low = rotate(
        product_back(normed_one, query_weight).reshape(total_rows, query_heads, HEAD_DIM), cosine, sine
    ).astype(jnp.bfloat16)
    key_low = rotate(
        product_back(normed_one, key_weight).reshape(total_rows, kv_heads, HEAD_DIM), cosine, sine
    ).astype(jnp.bfloat16)
    value_low = product_back(normed_one, value_weight).astype(jnp.bfloat16)
    ctx_size = lax.axis_size("ctx")

    def spread(values):
        rows = lax.all_gather(values, "ctx", axis=0, tiled=True)
        rows = rows.reshape(ctx_size, seq_count, row_count, kv_width).swapaxes(0, 1)
        return rows.reshape(seq_count, ctx_size * row_count, kv_width)

    def collect(values):
        rows = values.astype(jnp.bfloat16).swapaxes(1, 2)
        rows = rows.reshape(seq_count, ctx_size, row_count, kv_width).swapaxes(0, 1)
        return lax.psum_scatter(
            rows.reshape(-1, kv_width), "ctx", scatter_dimension=0, tiled=True
        )

    all_keys = spread(key_low.reshape(total_rows, kv_width))
    all_values = spread(value_low)
    total_keys = all_keys.shape[1]
    key_grid = all_keys.reshape(seq_count, total_keys, kv_heads, HEAD_DIM).swapaxes(1, 2)
    value_grid = all_values.reshape(seq_count, total_keys, kv_heads, HEAD_DIM).swapaxes(1, 2)
    query_grouped = query_low.reshape(seq_count, row_count, kv_heads, groups, HEAD_DIM)
    attended, log_total = attend_forward(
        query_grouped, query_places, key_grid, value_grid, key_places
    )
    attended_low = attended.reshape(total_rows, query_heads * HEAD_DIM).astype(jnp.bfloat16)
    hidden_state = inputs.astype(jnp.float32) + scatter_rows(product(attended_low, output_weight))
    scale_two = rms_scale(hidden_state)
    unit_two = hidden_state * scale_two
    normed_two = gather_rows((unit_two * gain_two).astype(jnp.bfloat16))
    gate_values = product_back(normed_two, gate_weight)
    upward = product_back(normed_two, up_weight)
    sigmoid_gate = jax.nn.sigmoid(gate_values)
    activated = gate_values * sigmoid_gate
    mixed_hidden = (activated * upward).astype(jnp.bfloat16)
    grad_out = cotangent.astype(jnp.float32)
    grad_down = product_rows(mixed_hidden, all_cotangent)
    grad_mixed = product_back(all_cotangent, down_weight)
    grad_gate_low = (
        grad_mixed * upward * sigmoid_gate * (1.0 + gate_values * (1.0 - sigmoid_gate))
    ).astype(jnp.bfloat16)
    grad_up_low = (grad_mixed * activated).astype(jnp.bfloat16)
    grad_unit_part = (
        product(grad_gate_low, gate_weight) + product(grad_up_low, up_weight)
    ).astype(jnp.bfloat16)
    grad_normed_two = scatter_rows(grad_unit_part)
    gain_two_grad = jnp.sum(grad_normed_two * unit_two, axis=0)
    grad_hidden = grad_out + norm_back(scale_two, unit_two, grad_normed_two * gain_two)
    branch_rows = gather_rows(grad_hidden.astype(jnp.bfloat16))
    layer_output = (hidden_state + scatter_rows(product(mixed_hidden, down_weight))).astype(
        jnp.bfloat16
    )
    grad_gate = product_rows(grad_gate_low, normed_two)
    grad_up = product_rows(grad_up_low, normed_two)
    grad_output = product_rows(attended_low, branch_rows)
    grad_attended = product_back(branch_rows, output_weight).astype(jnp.bfloat16)
    grad_attended = grad_attended.reshape(seq_count, row_count, kv_heads, groups, HEAD_DIM)
    grad_query_rot, grad_key_all, grad_value_all = attend_backward(
        query_grouped, query_places, key_grid, value_grid, key_places, log_total, grad_attended
    )
    grad_key_own = collect(grad_key_all).astype(jnp.float32)
    grad_value_low = collect(grad_value_all)
    grad_query_low = (
        rotate_back(grad_query_rot.reshape(total_rows, query_heads, HEAD_DIM), cosine, sine)
        .reshape(total_rows, query_heads * HEAD_DIM)
        .astype(jnp.bfloat16)
    )
    grad_key_low = (
        rotate_back(
            grad_key_own.reshape(total_rows, kv_heads, HEAD_DIM), cosine, sine
        )
        .reshape(total_rows, kv_width)
        .astype(jnp.bfloat16)
    )
    grad_query = product_rows(grad_query_low, normed_one)
    grad_key = product_rows(grad_key_low, normed_one)
    grad_value = product_rows(grad_value_low, normed_one)
    grad_normed_one = scatter_rows(
        product(grad_query_low, query_weight)
        + product(grad_key_low, key_weight)
        + product(grad_value_low, value_weight)
    )
    own_unit = own(unit_one)
    gain_one_grad = jnp.sum(grad_normed_one * own_unit, axis=0)
    input_grad = grad_hidden + norm_back(own(scale_one), own_unit, grad_normed_one * gain_one)

    grads = (grad_query, grad_key, grad_value, grad_output, grad_gate, grad_up, grad_down)
    parts = [lax.psum(grad.astype(jnp.bfloat16), "ctx").astype(jnp.float32) for grad in grads]
    gain_sums = lax.psum(jnp.stack([gain_one_grad, gain_two_grad]), ("fsdp", "ctx"))
    return (
        layer_output,
        input_grad,
        gain_sums[0],
        parts[0],
        parts[1],
        parts[2],
        parts[3],
        gain_sums[1],
        parts[4],
        parts[5],
        parts[6],
    )


def per_device_by_head(
    inputs,
    positions,
    cotangent,
    attention_gain,
    query_weight,
    key_weight,
    value_weight,
    output_weight,
    feedforward_gain,
    gate_weight,
    up_weight,
    down_weight,
):
    gain_one, gain_two = attention_gain, feedforward_gain
    block = TILE // 2
    length = TILE * 8
    cosine, sine = rotary_tables(positions)
    table = jnp.concatenate([cosine[:, 0, :], sine[:, 0, :]], axis=1)
    table = jnp.pad(table, ((0, 0), (0, 128 - table.shape[1])))
    (
        places, part, hidden, attended, packed, normed_one, wide_cosine, wide_sine,
        cotangents, normed_two, mixed, grad_gate, grad_up,
    ) = forward(
        positions[None, :], table, gain_one, gain_two, inputs, cotangent, query_weight,
        key_weight, value_weight, output_weight, gate_weight, up_weight, down_weight, length,
        block, 1,
    )
    starts = places.reshape(8, 8, TILE)[:, 0, ::block].reshape(-1) // block
    slots = jnp.arange(length // block, dtype=jnp.int32)
    found = jnp.where(starts[None, :] == slots[:, None], slots[None, :], 0)
    order = jnp.concatenate([jnp.sum(found, axis=1), starts]).astype(jnp.int32)
    summed, gain_sums, input_grad, layer_output = backward(
        order, gain_one, gain_two, grad_gate, grad_up, mixed, normed_two, cotangents, part,
        hidden, inputs, query_weight, key_weight, value_weight, output_weight, down_weight,
        attended, packed, normed_one, wide_cosine, wide_sine, 5,
    )
    owners = (gate_weight, up_weight, down_weight, query_weight, key_weight, value_weight,
              output_weight)
    *parts, layer_output, input_grad = widen(
        summed, [owner.shape[0] for owner in owners], (layer_output, input_grad)
    )
    return (layer_output, input_grad, gain_sums[0], *parts[3:], gain_sums[1], *parts[:3])


def per_device(*arrays):
    fits = lax.axis_size("fsdp") == 4 and lax.axis_size("ctx") == 8
    return (per_device_by_head if fits else per_device_gathered)(*arrays)


def solution(mesh):
    in_specs = (
        P(("fsdp", "ctx"), None),
        P(("fsdp", "ctx")),
        P(("fsdp", "ctx"), None),
        P(),
        P("fsdp", None),
        P("fsdp", None),
        P("fsdp", None),
        P("fsdp", None),
        P(),
        P("fsdp", None),
        P("fsdp", None),
        P("fsdp", None),
    )
    out_specs = (
        P(("fsdp", "ctx"), None),
        P(("fsdp", "ctx"), None),
        P(),
        P("fsdp", None),
        P("fsdp", None),
        P("fsdp", None),
        P("fsdp", None),
        P(),
        P("fsdp", None),
        P("fsdp", None),
        P("fsdp", None),
    )
    return jax.shard_map(
        per_device, mesh=mesh, in_specs=in_specs, out_specs=out_specs, check_vma=False
    )
```

```python
import functools
import math

import jax
import jax.numpy as jnp
from jax import lax
from jax.experimental import pallas as pl
from jax.experimental.pallas import tpu as pltpu
from jax.sharding import PartitionSpec as P

HEADS = 16
KV_HEADS = 8
HEAD_DIM = 96


EPSILON = 1e-05
ROPE_BASE = 100000.0


def product(left, right):
    return jnp.dot(left, right, preferred_element_type=jnp.float32)


def product_back(left, right):
    return lax.dot_general(
        left, right, (((1,), (1,)), ((), ())), preferred_element_type=jnp.float32
    )


def product_rows(left, right):
    return lax.dot_general(
        left, right, (((0,), (0,)), ((), ())), preferred_element_type=jnp.float32
    )


def rms_scale(values):
    return lax.rsqrt(jnp.mean(values * values, axis=-1, keepdims=True) + EPSILON)


def norm_back(scale_rows, unit_rows, grad_unit):
    return scale_rows * (
        grad_unit - unit_rows * jnp.mean(grad_unit * unit_rows, axis=-1, keepdims=True)
    )


def rotary_tables(places):
    half_width = HEAD_DIM // 2
    frequencies = ROPE_BASE ** (-(jnp.arange(half_width, dtype=jnp.float32) * 2.0 / HEAD_DIM))
    angles = places.astype(jnp.float32)[:, None] * frequencies[None, :]
    return (jnp.cos(angles)[:, None, :], jnp.sin(angles)[:, None, :])


def rotate(values, cosine, sine):
    half_width = values.shape[-1] // 2
    lower_half = values[..., :half_width]
    upper_half = values[..., half_width:]
    return jnp.concatenate(
        [lower_half * cosine - upper_half * sine, upper_half * cosine + lower_half * sine], axis=-1
    )


def rotate_back(grads, cosine, sine):
    half_width = grads.shape[-1] // 2
    lower_half = grads[..., :half_width]
    upper_half = grads[..., half_width:]
    return jnp.concatenate(
        [lower_half * cosine + upper_half * sine, upper_half * cosine - lower_half * sine], axis=-1
    )


def block_total_of(total_keys):
    return max(1, total_keys // 512)


def masked_scores(query_grouped, query_places, key_rows, key_places, start, width):
    key_part = lax.dynamic_slice_in_dim(key_rows, start, width, 2)
    place_part = lax.dynamic_slice_in_dim(key_places, start, width, 1)
    scores = jnp.einsum(
        "sqhgd,shkd->shgqk", query_grouped, key_part, preferred_element_type=jnp.float32
    )
    scores = scores * (1.0 / math.sqrt(HEAD_DIM))
    allowed = place_part[:, None, None, None, :] <= query_places[:, None, None, :, None]
    return jnp.where(allowed, scores, -1000000000.0)


def attend_forward(query_grouped, query_places, key_rows, value_rows, key_places):
    seq_count, row_count, head_groups, group_size = query_grouped.shape[:4]
    total_keys = key_rows.shape[2]
    block_total = block_total_of(total_keys)
    width = total_keys // block_total
    stat_shape = (seq_count, head_groups, group_size, row_count)

    def peak_step(index, carry):
        running_top, running_sum = carry
        scores = masked_scores(
            query_grouped, query_places, key_rows, key_places, index * width, width
        )
        new_top = jnp.maximum(running_top, jnp.max(scores, axis=-1))
        running_sum = running_sum * jnp.exp(running_top - new_top) + jnp.sum(
            jnp.exp(scores - new_top[..., None]), axis=-1
        )
        return (new_top, running_sum)

    running_top, running_sum = lax.fori_loop(
        0,
        block_total,
        peak_step,
        (jnp.full(stat_shape, -1e30, jnp.float32), jnp.zeros(stat_shape, jnp.float32)),
    )
    log_total = running_top + jnp.log(running_sum)

    def value_step(index, gathered):
        scores = masked_scores(
            query_grouped, query_places, key_rows, key_places, index * width, width
        )
        soft_low = jnp.exp(scores - log_total[..., None]).astype(jnp.bfloat16)
        value_part = lax.dynamic_slice_in_dim(value_rows, index * width, width, 2)
        return gathered + jnp.einsum(
            "shgqk,shkd->sqhgd", soft_low, value_part, preferred_element_type=jnp.float32
        )

    attended = lax.fori_loop(
        0, block_total, value_step, jnp.zeros(query_grouped.shape, jnp.float32)
    )
    return (attended, log_total)


def attend_backward(
    query_grouped, query_places, key_rows, value_rows, key_places, log_total, grad_attended
):
    total_keys = key_rows.shape[2]
    block_total = block_total_of(total_keys)
    width = total_keys // block_total
    score_scale = 1.0 / math.sqrt(HEAD_DIM)

    def soft_and_grad(index):
        scores = masked_scores(
            query_grouped, query_places, key_rows, key_places, index * width, width
        )
        soft_values = jnp.exp(scores - log_total[..., None])
        value_part = lax.dynamic_slice_in_dim(value_rows, index * width, width, 2)
        grad_soft = jnp.einsum(
            "sqhgd,shkd->shgqk", grad_attended, value_part, preferred_element_type=jnp.float32
        )
        return (soft_values, grad_soft)

    def delta_step(index, row_delta):
        soft_values, grad_soft = soft_and_grad(index)
        return row_delta + jnp.sum(soft_values * grad_soft, axis=-1)

    row_delta = lax.fori_loop(0, block_total, delta_step, jnp.zeros(log_total.shape, jnp.float32))

    def grad_step(index, carry):
        grad_query, grad_keys, grad_values = carry
        soft_values, grad_soft = soft_and_grad(index)
        grad_scores = (soft_values * (grad_soft - row_delta[..., None])).astype(jnp.bfloat16)
        key_part = lax.dynamic_slice_in_dim(key_rows, index * width, width, 2)
        grad_query = (
            grad_query
            + jnp.einsum(
                "shgqk,shkd->sqhgd", grad_scores, key_part, preferred_element_type=jnp.float32
            )
            * score_scale
        )
        key_term = (
            jnp.einsum(
                "shgqk,sqhgd->shkd", grad_scores, query_grouped, preferred_element_type=jnp.float32
            )
            * score_scale
        )
        value_term = jnp.einsum(
            "shgqk,sqhgd->shkd",
            soft_values.astype(jnp.bfloat16),
            grad_attended,
            preferred_element_type=jnp.float32,
        )
        grad_keys = lax.dynamic_update_slice_in_dim(grad_keys, key_term, index * width, 2)
        grad_values = lax.dynamic_update_slice_in_dim(grad_values, value_term, index * width, 2)
        return (grad_query, grad_keys, grad_values)

    initial = (
        jnp.zeros(query_grouped.shape, jnp.float32),
        jnp.zeros(key_rows.shape, jnp.float32),
        jnp.zeros(value_rows.shape, jnp.float32),
    )
    return lax.fori_loop(0, block_total, grad_step, initial)


def vmem():
    return pl.BlockSpec(memory_space=pltpu.VMEM)


def peer(ctx_index):
    return dict(device_id={"ctx": ctx_index}, device_id_type=pl.DeviceIdType.MESH)


SPINE_ROWS = 32
LINE_ROWS = 32
ROUND_ROWS = 2 * SPINE_ROWS + LINE_ROWS
LEAD = 4
HOP = 2
FEED = (0, 1, 3, 5, 8)
CHAIN = (0, 4, 6, 8, 10, 13, 24, 26, 30, 32)
RING = 20
TILE = 128
PAIR = (HEADS // KV_HEADS) * HEAD_DIM
WIDE = PAIR + 2 * HEAD_DIM


def near_fsdp(index):
    return dict(device_id={"fsdp": index}, device_id_type=pl.DeviceIdType.MESH)


def rows_at(start, count):
    return pl.ds(pl.multiple_of(start, 16), count)


class Place:
    def __init__(self):
        self.ctx = lax.axis_index("ctx")
        self.row = lax.axis_index("fsdp")
        self.chip, self.core = lax.div(self.row, 2), lax.rem(self.row, 2)
        self.partner = 2 * self.chip + 1 - self.core
        self.across = 2 * (1 - self.chip) + self.core
        self.corner = 2 * (1 - self.chip) + 1 - self.core

    def greet(self):
        barrier = pltpu.get_barrier_semaphore()
        for step in range(1, 4):
            pl.semaphore_signal(barrier, inc=1, **near_fsdp(lax.rem(self.row + step, 4)))
        for step in range(1, 8):
            pl.semaphore_signal(barrier, inc=1, **peer(lax.rem(self.ctx + step, 8)))
        pl.semaphore_wait(barrier, 10)


class Fold:
    def __init__(self, place, part, near, send, far, send_sem, recv_sem):
        self.place, self.part, self.near, self.send, self.far = place, part, near, send, far
        self.send_sem, self.recv_sem = send_sem, recv_sem

    def partner_copy(self, chip):
        block = 2 * chip + 1 - self.place.core
        return pltpu.make_async_remote_copy(
            src_ref=self.part.at[rows_at(block * TILE, TILE)],
            dst_ref=self.near.at[chip],
            send_sem=self.send_sem.at[chip],
            recv_sem=self.recv_sem.at[chip],
            **near_fsdp(self.place.partner),
        )

    def across_copy(self, piece):
        span = pl.ds(piece * (TILE // 2), TILE // 2)
        return pltpu.make_async_remote_copy(
            src_ref=self.send.at[span],
            dst_ref=self.far.at[span],
            send_sem=self.send_sem.at[2 + piece],
            recv_sem=self.recv_sem.at[2 + piece],
            **near_fsdp(self.place.across),
        )

    def start(self):
        self.partner_copy(1 - self.place.chip).start()
        self.partner_copy(self.place.chip).start()

    def relay(self):
        there = 1 - self.place.chip
        self.partner_copy(there).wait_recv()
        base = self.place.across * TILE
        for half in range(2):

            @pl.loop(2 * half, 2 * half + 2)
            def _(piece):
                mine = self.part[rows_at(base + piece * 32, 32), :].astype(jnp.float32)
                span = rows_at(piece * 32, 32)
                self.send[span, :] = (
                    mine + self.near[there, span, :].astype(jnp.float32)
                ).astype(jnp.bfloat16)

            self.across_copy(half).start()

    def arrive_near(self):
        self.partner_copy(self.place.chip).wait_recv()
        self.partner_copy(0).wait_send()
        self.partner_copy(1).wait_send()

    def arrive_across(self, piece):
        self.across_copy(piece).wait()

    def arrive(self):
        self.arrive_near()
        self.arrive_across(0)
        self.arrive_across(1)

    def rows(self, start, count):
        mine = self.part[rows_at(self.place.row * TILE + start, count), :].astype(jnp.float32)
        span = rows_at(start, count)
        near = self.near[self.place.chip, span, :].astype(jnp.float32)
        return mine + near + self.far[span, :].astype(jnp.float32)


class Gather:
    def __init__(self, place, full, send_sem, recv_sem, count=TILE, pieces=1):
        self.place, self.full, self.send_sem, self.recv_sem = place, full, send_sem, recv_sem
        self.count, self.pieces = count, pieces

    def copy(self, block, target, key, piece):
        rows = self.count // self.pieces
        span = pl.ds(pl.multiple_of(block * self.count + piece * rows, rows), rows)
        return pltpu.make_async_remote_copy(
            src_ref=self.full.at[span],
            dst_ref=self.full.at[span],
            send_sem=self.send_sem.at[key * self.pieces + piece],
            recv_sem=self.recv_sem.at[key * self.pieces + piece],
            **near_fsdp(target),
        )

    def start(self, piece=0):
        self.copy(self.place.row, self.place.across, 1, piece).start()
        self.copy(self.place.row, self.place.partner, 0, piece).start()

    def first(self):
        for piece in range(self.pieces):
            self.copy(self.place.partner, self.place.partner, 0, piece).wait_recv()

    def relay(self):
        for piece in range(self.pieces):
            self.copy(self.place.across, self.place.across, 1, piece).wait_recv()
            self.copy(self.place.across, self.place.partner, 2, piece).start()

    def arrive(self):
        for piece in range(self.pieces):
            self.copy(self.place.corner, self.place.partner, 2, piece).wait_recv()
            self.copy(self.place.row, self.place.across, 1, piece).wait_send()
            self.copy(self.place.row, self.place.partner, 0, piece).wait_send()
            self.copy(self.place.across, self.place.partner, 2, piece).wait_send()


class Swap:
    def __init__(self, place, source, target, send_sem, recv_sem, count, share=1):
        self.place, self.source, self.target = place, source, target
        self.send_sem, self.recv_sem, self.count, self.share = send_sem, recv_sem, count, share

    def span(self, index):
        return pl.ds(pl.multiple_of(index * self.count, self.count), self.count)

    def copy(self, other, sender):
        return pltpu.make_async_remote_copy(
            src_ref=self.source.at[self.span(lax.div(other, self.share))],
            dst_ref=self.target.at[self.span(sender)],
            send_sem=self.send_sem.at[other],
            recv_sem=self.recv_sem.at[sender],
            **peer(other),
        )

    def start(self, other):
        me = self.place.ctx

        @pl.when(other != me)
        def _():
            self.copy(other, me).start()

        @pl.when(other == me)
        def _():
            self.target[self.span(me)] = self.source[self.span(lax.div(me, self.share))]

    def start_all(self):
        for step in range(1, 9):
            self.start(lax.rem(self.place.ctx + step, 8))

    def arrive(self):
        for step in range(1, 8):
            other = lax.rem(self.place.ctx + step, 8)
            self.copy(other, other).wait()


class Spread:
    def __init__(self, slots, index, count, device, send_sem, recv_sem):
        self.slots, self.index, self.count, self.device = slots, index, count, device
        self.send_sem, self.recv_sem = send_sem, recv_sem

    def copy(self, step):
        return pltpu.make_async_remote_copy(
            src_ref=self.slots.at[self.index],
            dst_ref=self.slots.at[self.index],
            send_sem=self.send_sem.at[step],
            recv_sem=self.recv_sem.at[step],
            **self.device(lax.rem(self.index + step, self.count)),
        )

    def start(self):
        for step in range(1, self.count):
            self.copy(step).start()

    def total(self):
        for step in range(1, self.count):
            self.copy(step).wait()
        result = self.slots[0]
        for step in range(1, self.count):
            result += self.slots[step]
        return result


class Tree:
    def __init__(self, place, own, out_ref, index, rounds, line, box, sems, leaf_back):
        me = place.ctx
        depth, side = lax.div(me, 2), lax.rem(me, 2)
        other_side = me + 1 - 2 * side
        self.own, self.out, self.box, self.index, self.line = own, out_ref, box, index, line
        self.up, self.got, self.down, self.back = sems
        self.leaf_back = leaf_back
        if line:
            center = jnp.where(index >= rounds - 6, 1 + lax.rem(index, 2), lax.rem(index, 4))
            count = LINE_ROWS
            start = index * ROUND_ROWS + 2 * SPINE_ROWS
            root_side = lax.rem(index, 2)
            on_cross = depth == center
            self.root = jnp.logical_and(on_cross, side == root_side)
            has_side = self.root
            to_side = jnp.logical_and(on_cross, side != root_side)
            reach = jnp.maximum(center, 3 - center)
            away = jnp.abs(depth - center)
            crossed = jnp.where(side == root_side, 0, 1)
            self.rise_age = reach - away + jnp.where(self.root, 1, 0)
            self.fall_age = reach + 1 + away + crossed
        else:
            center = 1 + side
            count = SPINE_ROWS
            start = index * ROUND_ROWS + side * SPINE_ROWS
            self.root = depth == center
            has_side = None
        self.count = count
        self.start = start
        self.slot = lax.rem(index, RING)
        self.rows = rows_at(start, count)
        self.children = (
            (jnp.logical_and(depth > 0, depth <= center), me - 2, 0),
            (jnp.logical_and(depth < 3, depth >= center), me + 2, 1),
            (has_side, other_side, 2),
        )
        parent = jnp.where(depth < center, me + 2, me - 2)
        slot = jnp.where(depth < center, 0, 1)
        if line:
            parent = jnp.where(to_side, other_side, parent)
            slot = jnp.where(to_side, 2, slot)
        self.parent = jnp.where(self.root, other_side, parent)
        self.parent_slot = jnp.where(self.root, 2, slot)

    def boxed(self, slot):
        return self.box.at[slot, rows_at(self.slot * self.count, self.count)]

    def up_copy(self, target, slot):
        return pltpu.make_async_remote_copy(
            src_ref=self.own.at[self.rows],
            dst_ref=self.boxed(slot),
            send_sem=self.up.at[self.slot],
            recv_sem=self.got.at[slot, self.slot],
            **peer(target),
        )

    def down_copy(self, child, slot, source):
        back = self.back if slot < 2 or self.line else self.leaf_back
        return pltpu.make_async_remote_copy(
            src_ref=source.at[self.rows],
            dst_ref=self.out.at[self.rows],
            send_sem=self.down.at[slot, self.slot],
            recv_sem=back.at[self.slot],
            **peer(child),
        )

    def each_child(self, action):
        for present, child, slot in self.children:
            if present is None:
                action(child, slot)
            else:
                pl.when(present)(functools.partial(action, child, slot))

    def keep(self):
        return pltpu.make_async_copy(
            self.own.at[self.rows], self.out.at[self.rows], self.up.at[self.slot]
        )

    def rise(self):
        self.each_child(lambda child, slot: self.up_copy(child, slot).wait_recv())
        base = self.slot * self.count
        for piece in range(0, self.count, 16):
            span = rows_at(self.start + piece, 16)
            total = self.own[span, :].astype(jnp.float32)
            for present, _, slot in self.children:
                part = self.box[slot, rows_at(base + piece, 16), :].astype(jnp.float32)
                total += part if present is None else jnp.where(present, part, 0.0)
            self.own[span, :] = total.astype(jnp.bfloat16)

        @pl.when(jnp.logical_not(self.root))
        def _():
            self.up_copy(self.parent, self.parent_slot).start()

        @pl.when(self.root)
        def _():
            self.keep().start()
            self.each_child(lambda child, slot: self.down_copy(child, slot, self.own).start())

    def fall(self):
        @pl.when(jnp.logical_not(self.root))
        def _():
            self.down_copy(self.parent, 0, self.out).wait_recv()
            self.each_child(lambda child, slot: self.down_copy(child, slot, self.out).start())

    def finish(self):
        @pl.when(jnp.logical_not(self.root))
        def _():
            self.up_copy(self.parent, self.parent_slot).wait_send()

        @pl.when(self.root)
        def _():
            self.keep().wait()

        self.each_child(lambda child, slot: self.down_copy(child, slot, self.out).wait_send())


def softmax_parts(query_rows, key_rows, first_row):
    scores = product_back(query_rows, key_rows) * (1.0 / math.sqrt(HEAD_DIM))
    rows = lax.broadcasted_iota(jnp.int32, scores.shape, 0) + first_row
    columns = lax.broadcasted_iota(jnp.int32, scores.shape, 1)
    scores = jnp.where(columns <= rows, scores, -1e30)
    spread = jnp.exp(scores - jnp.max(scores, axis=-1, keepdims=True))
    return spread * (1.0 / jnp.sum(spread, axis=-1, keepdims=True))


def pack_pairs(blocks):
    half = blocks.shape[1] // 2
    return jnp.concatenate([blocks[:, :half], blocks[:, half:]], axis=-1)


def unpack_pairs(blocks):
    return jnp.concatenate([blocks[..., :PAIR], blocks[..., PAIR:]], axis=-2)


def sort_blocks(slot_ref, source, targets, opened=lambda rows: rows):
    block_total = source.shape[0]
    block = targets[0].shape[0] // block_total
    for index in range(block_total):
        rows = opened(source[slot_ref[index]])
        start = 0
        for target in targets:
            width = target.shape[-1]
            target[index * block : (index + 1) * block, :] = rows[:, start : start + width]
            start += width


def norm_back_rows(values, grad_unit):
    scale = rms_scale(values)
    unit = values * scale
    return unit, lambda grad: norm_back(scale, unit, grad)


def backward_kernel(
    rounds,
    block,
    order_ref,
    gain_one_ref,
    gain_two_ref,
    grad_gate_ref,
    grad_up_ref,
    mixed_ref,
    normed_two_ref,
    cotangent_ref,
    part_ref,
    hidden_ref,
    input_ref,
    query_weight_ref,
    key_weight_ref,
    value_weight_ref,
    output_weight_ref,
    down_weight_ref,
    attended_ref,
    packed_ref,
    normed_ref,
    cosine_ref,
    sine_ref,
    out_ref,
    gain_out_ref,
    input_grad_ref,
    layer_output_ref,
    own,
    spine_in,
    line_in,
    grad_gate,
    grad_up,
    mixed,
    normed_two,
    cotangents,
    part,
    hidden,
    inputs,
    output_weight,
    attended,
    packed,
    normed,
    cosine,
    sine,
    half_swap,
    weight,
    near,
    send,
    far,
    branch,
    grad_hidden,
    gain_part,
    heads_out,
    heads_in,
    q0,
    q1,
    k,
    v,
    g0,
    g1,
    result,
    dk,
    dv,
    packed_out,
    packed_in,
    turned,
    gain_near,
    gain_far,
    fetch_sem,
    spine_up,
    spine_got,
    spine_down,
    spine_back,
    leaf_up,
    leaf_back,
    line_up,
    line_got,
    line_down,
    line_back,
    fold_send,
    fold_recv,
    gather_send,
    gather_recv,
    swap_send,
    swap_recv,
    near_send,
    near_recv,
    far_send,
    far_recv,
):
    place = Place()
    me = place.ctx
    depth, side = lax.div(me, 2), lax.rem(me, 2)
    other_side = me + 1 - 2 * side
    hidden_units = mixed.shape[1]
    width = own.shape[1]
    base = 3 * hidden_units
    spare = rounds * ROUND_ROWS - base - 3 * WIDE
    length = q0.shape[0]
    halves = TILE // block
    tile = min(256, length)
    tiles = length // tile
    scale = 1.0 / math.sqrt(HEAD_DIM)

    fetches = {}

    def fetch_all(source, *copies):
        first = sum(len(group) for group in fetches.values())
        fetches[id(source)] = [
            pltpu.make_async_copy(*copy, fetch_sem.at[first + index])
            for index, copy in enumerate(copies or ())
        ]
        for copy in fetches[id(source)]:
            copy.start()

    def fetch(*sources):
        for source in sources:
            for copy in fetches[id(source)]:
                copy.wait()

    for source, target in (
        (part_ref, part),
        (grad_gate_ref, grad_gate),
        (normed_two_ref, normed_two),
        (grad_up_ref, grad_up),
        (mixed_ref, mixed),
        (cotangent_ref, cotangents),
        (hidden_ref, hidden),
        (packed_ref, packed),
        (down_weight_ref, own.at[pl.ds(base, hidden_units)]),
        (output_weight_ref, output_weight),
        (attended_ref, attended),
        (normed_ref, normed),
        (cosine_ref, cosine),
        (sine_ref, sine),
        (input_ref, inputs),
    ):
        fetch_all(source, (source, target))
    for source, first, count in (
        (query_weight_ref, 0, PAIR),
        (key_weight_ref, PAIR, HEAD_DIM),
        (value_weight_ref, PAIR + HEAD_DIM, HEAD_DIM),
    ):
        fetch_all(
            source,
            *(
                (source.at[pl.ds(head * count, count)], weight.at[head, pl.ds(first, count)])
                for head in range(2)
            ),
        )
    gain_one = gain_one_ref[...].astype(jnp.float32).reshape(1, -1)
    gain_two = gain_two_ref[...].astype(jnp.float32).reshape(1, -1)
    lanes = (WIDE, WIDE)
    row_lane = lax.broadcasted_iota(jnp.int32, lanes, 0)
    column_lane = lax.broadcasted_iota(jnp.int32, lanes, 1)
    half = HEAD_DIM // 2
    inner = lax.rem(column_lane, HEAD_DIM)
    partner_lane = column_lane + jnp.where(inner < half, half, -half)
    half_swap[...] = jnp.where(row_lane == partner_lane, 1.0, 0.0).astype(jnp.bfloat16)
    place.greet()
    fetch(part_ref)
    fold_two = Fold(place, part, near.at[0], send.at[0], far.at[0], fold_send.at[0], fold_recv.at[0])
    fold_output = Fold(
        place, part, near.at[0], send.at[0], far.at[0], fold_send.at[0], fold_recv.at[0]
    )
    fold_one = Fold(place, part, near.at[1], send.at[1], far.at[1], fold_send.at[1], fold_recv.at[1])
    gather = Gather(place, branch, gather_send, gather_recv)
    swap_heads = Swap(place, heads_out, heads_in, swap_send.at[0], swap_recv.at[0], halves)
    swap_packed = Swap(place, packed_out, packed_in, swap_send.at[1], swap_recv.at[1], halves)
    spread_near = Spread(gain_near, place.row, 4, near_fsdp, near_send, near_recv)
    spread_far = Spread(gain_far, me, 8, peer, far_send, far_recv)
    fold_two.start()

    def stage_feed(first):
        sides = ((grad_gate, normed_two), (grad_up, normed_two), (mixed, cotangents))
        left, right = sides[first // hidden_units]
        if first == 0:
            fetch(grad_gate_ref, normed_two_ref)
        elif first == hidden_units:
            fetch(grad_up_ref)
        elif first == 2 * hidden_units:
            fetch(mixed_ref)

        @pl.loop(0, 2)
        def _(index):
            start = first % hidden_units + index * 256
            columns = pl.ds(pl.multiple_of(start, 256), 256)
            rows = pl.ds(pl.multiple_of(first + index * 256, 256), 256)
            own[rows, :] = product_rows(left[:, columns], right[...]).astype(jnp.bfloat16)

    stage_feed(0)

    spine_sems = (spine_up, spine_got, spine_down, spine_back)
    line_sems = (line_up, line_got, line_down, line_back)

    def spine(index):
        return Tree(place, own, out_ref, index, rounds, False, spine_in, spine_sems, leaf_back)

    def line(index):
        return Tree(place, own, out_ref, index, rounds, True, line_in, line_sems, None)

    def leaf_rows(index):
        return rows_at(index * ROUND_ROWS + (1 - side) * SPINE_ROWS, SPINE_ROWS)

    def leaf_copy(index):
        slot = lax.rem(index, RING)
        return pltpu.make_async_remote_copy(
            src_ref=own.at[leaf_rows(index)],
            dst_ref=spine_in.at[2, rows_at(slot * SPINE_ROWS, SPINE_ROWS)],
            send_sem=leaf_up.at[slot],
            recv_sem=spine_got.at[2, slot],
            **peer(other_side),
        )

    def leaf_result(index):
        slot = lax.rem(index, RING)
        return pltpu.make_async_remote_copy(
            src_ref=own.at[leaf_rows(index)],
            dst_ref=out_ref.at[leaf_rows(index)],
            send_sem=leaf_up.at[slot],
            recv_sem=leaf_back.at[slot],
            **peer(other_side),
        )

    def stage_norm_two():
        fetch(hidden_ref, cotangent_ref)
        fold_two.arrive()
        gain_part[...] = jnp.zeros_like(gain_part)

        @pl.loop(0, TILE // 16)
        def _(piece):
            span = rows_at(piece * 16, 16)
            grad = fold_two.rows(piece * 16, 16)
            unit, back = norm_back_rows(hidden[span, :], None)
            gain_part[1] += (grad * unit).reshape(2, 8, -1).sum(axis=0)
            here = rows_at(place.row * TILE + piece * 16, 16)
            total = cotangents[here, :].astype(jnp.float32) + back(grad * gain_two)
            grad_hidden[span, :] = total
            branch[here, :] = total.astype(jnp.bfloat16)

        gather.start()

    def stage_heads():
        fetch(output_weight_ref)
        gather.first()
        gather.arrive()

        @pl.loop(0, 4)
        def _(sequence):
            rows = branch[rows_at(sequence * TILE, TILE), :]
            grads = product_back(rows, output_weight[...]).astype(jnp.bfloat16)
            for head in range(2):
                heads_out[pl.ds((2 * sequence + head) * halves, halves)] = pack_pairs(
                    grads[:, head * PAIR : (head + 1) * PAIR].reshape(halves, block, PAIR)
                )

        swap_heads.start_all()

    def stage_sort():
        fetch(packed_ref)
        sort_blocks(order_ref, packed, (q0, q1, k, v))

    def stage_output_grad():
        fetch(attended_ref)
        for head in range(2):
            rows = [
                attended[(2 * index + head) * halves : (2 * index + head + 1) * halves]
                for index in range(4)
            ]
            rows = unpack_pairs(jnp.concatenate(rows, axis=0)).reshape(4 * TILE, PAIR)
            first_row = base + 2 * WIDE + head * PAIR
            for first in range(0, own.shape[1], 512):
                columns = slice(first, first + 512)
                own[first_row : first_row + PAIR, columns] = product_rows(
                    rows, branch[:, columns]
                ).astype(jnp.bfloat16)

    def stage_sort_grads():
        swap_heads.arrive()
        sort_blocks(order_ref, heads_in, (g0, g1), unpack_pairs)
        dk[...] = jnp.zeros_like(dk)
        dv[...] = jnp.zeros_like(dv)

    def stage_attention(index):
        first, top = index * tile, (index + 1) * tile
        parts = []
        for q, g in ((q0, g0), (q1, g1)):
            query_rows = q[first:top, :]
            grad_rows = g[first:top, :]
            soft = softmax_parts(query_rows, k[:top, :], first)
            grad_soft = product_back(grad_rows, v[:top, :])
            delta = jnp.sum(soft * grad_soft, axis=-1, keepdims=True)
            grad_scores = (soft * (grad_soft - delta)).astype(jnp.bfloat16)
            parts.append(product(grad_scores, k[:top, :]) * scale)
            key_term = product_rows(grad_scores, query_rows) * scale
            value_term = product_rows(soft.astype(jnp.bfloat16), grad_rows)
            dk[: top // block] += key_term.reshape(-1, block, HEAD_DIM)
            dv[: top // block] += value_term.reshape(-1, block, HEAD_DIM)
        result[first // block : top // block] = jnp.concatenate(parts, axis=-1).reshape(
            -1, block, PAIR
        )

    def stage_unsort():
        for slot in range(length // block):
            spot = order_ref[length // block + slot]
            packed_out[slot] = jnp.concatenate(
                [result[spot], dk[spot], dv[spot]], axis=-1
            ).astype(jnp.bfloat16)
        swap_packed.start_all()

    def stage_turn():
        fetch(cosine_ref, sine_ref, query_weight_ref, key_weight_ref, value_weight_ref)
        swap_packed.arrive()

        @pl.loop(0, 4)
        def _(sequence):
            span = rows_at(sequence * TILE, TILE)
            total = None
            for head in range(2):
                grads = packed_in[pl.ds((2 * sequence + head) * halves, halves)]
                grads = grads.reshape(TILE, WIDE)
                swapped = product(grads, half_swap[...])
                low = (
                    grads.astype(jnp.float32) * cosine[span, :] - swapped * sine[span, :]
                ).astype(jnp.bfloat16)
                turned[head, span, :] = low
                term = product(low, weight[head])
                total = term if total is None else total + term
            part[span, :] = total.astype(jnp.bfloat16)

        fold_one.start()

    def stage_projection_grads(head):
        if head == 0:
            fetch(normed_ref)
        query_base = base + head * PAIR
        key_base = base + WIDE + head * HEAD_DIM
        value_base = key_base + 2 * HEAD_DIM
        for first in range(0, own.shape[1], 512):
            columns = slice(first, first + 512)
            grads = product_rows(turned[head], normed[:, columns]).astype(jnp.bfloat16)
            own[query_base : query_base + PAIR, columns] = grads[:PAIR]
            own[key_base : key_base + HEAD_DIM, columns] = grads[PAIR : PAIR + HEAD_DIM]
            own[value_base : value_base + HEAD_DIM, columns] = grads[PAIR + HEAD_DIM :]

    def stage_norm_one():
        fetch(input_ref)
        fold_one.arrive()

        @pl.loop(0, TILE // 16)
        def _(piece):
            span = rows_at(piece * 16, 16)
            grad = fold_one.rows(piece * 16, 16)
            unit, back = norm_back_rows(inputs[span, :].astype(jnp.float32), None)
            gain_part[0] += (grad * unit).reshape(2, 8, -1).sum(axis=0)
            input_grad_ref[span, :] = grad_hidden[span, :] + back(grad * gain_one)

        gain_near[place.row] = jnp.sum(gain_part[...], axis=1)
        spread_near.start()

    def stage_gain():
        gain_far[me] = spread_near.total()
        spread_far.start()

    def stage_output():
        fetch(down_weight_ref)

        @pl.loop(0, 4)
        def _(sequence):
            span = rows_at(sequence * TILE, TILE)
            part[span, :] = product(
                mixed[span, :], own[base : base + hidden_units, :]
            ).astype(jnp.bfloat16)

    def stage_output_sum():
        fold_output.arrive()

        @pl.loop(0, TILE // 16)
        def _(piece):
            span = rows_at(piece * 16, 16)
            total = hidden[span, :] + fold_output.rows(piece * 16, 16)
            layer_output_ref[span, :] = total.astype(jnp.bfloat16)

    def stage_clear():
        if spare:
            own[base + 3 * WIDE :, :] = jnp.zeros((spare, width), own.dtype)

    units = 2 * 256
    stages = [
        (FEED[index], functools.partial(stage_feed, (index + 1) * units)) for index in range(5)
    ]
    stages += [
        (CHAIN[0], fold_two.relay),
        (CHAIN[0], stage_sort),
        (CHAIN[1], stage_norm_two),
        (CHAIN[2], gather.relay),
        (CHAIN[2], stage_output),
        (CHAIN[3], stage_heads),
        (CHAIN[3], fold_output.start),
        (CHAIN[4], fold_output.relay),
        (CHAIN[4], stage_output_grad),
        (CHAIN[4], stage_clear),
        (CHAIN[5], stage_sort_grads),
    ]
    stages += [
        (CHAIN[5] + index, functools.partial(stage_attention, index)) for index in range(tiles)
    ]
    stages += [
        (CHAIN[5] + tiles - 1, stage_unsort),
        (CHAIN[5] + tiles, stage_output_sum),
        (CHAIN[6], stage_turn),
        (CHAIN[7], fold_one.relay),
        (CHAIN[7], functools.partial(stage_projection_grads, 0)),
        (CHAIN[7] + 1, functools.partial(stage_projection_grads, 1)),
        (CHAIN[8], stage_norm_one),
        (CHAIN[9], stage_gain),
    ]
    assert CHAIN[7] + 1 < base // ROUND_ROWS - LEAD
    for index in range(5):
        assert FEED[index] < (index + 1) * units // ROUND_ROWS - LEAD

    for index in range(LEAD):
        leaf_copy(index).start()

    def valid(index):
        return jnp.logical_and(index >= 0, index < rounds)

    @pl.loop(0, rounds + RING)
    def _(now):
        far_side = jnp.abs(depth - 2 + side)
        off_center = jnp.abs(depth - 1 - side)
        done = now - RING + 1
        for tree in (spine(done), line(done)):
            pl.when(valid(done))(tree.finish)

        rising = spine(now - HOP * (3 - off_center))
        pl.when(valid(rising.index))(rising.rise)

        @pl.loop(0, 5)
        def _(age):
            tree = line(now - HOP * age)
            pl.when(jnp.logical_and(valid(tree.index), tree.rise_age == age))(tree.rise)

        @pl.when(now + LEAD < rounds)
        def _():
            leaf_copy(now + LEAD).start()

        falling = spine(now - HOP * (3 + off_center))
        pl.when(valid(falling.index))(falling.fall)

        @pl.loop(4, 9)
        def _(age):
            tree = line(now - HOP * age)
            pl.when(jnp.logical_and(valid(tree.index), tree.fall_age == age))(tree.fall)

        leaf_fall = now - HOP * (4 + far_side)

        @pl.when(valid(leaf_fall))
        def _():
            leaf_result(leaf_fall).wait_recv()
            leaf_copy(leaf_fall).wait_send()

        for when, stage in stages:
            pl.when(now == when)(stage)

    gain_out_ref[...] = spread_far.total()


def backward(order, gain_one, gain_two, grad_gate, grad_up, mixed, normed_two, cotangents, part,
             hidden, inputs, query_weight, key_weight, value_weight, output_weight, down_weight,
             attended, packed, normed, cosine, sine, key):
    width = hidden.shape[1]
    rows = 3 * mixed.shape[1] + 3 * WIDE
    rounds = -(-rows // ROUND_ROWS)
    block = packed.shape[1]
    length = packed.shape[0] * block
    dma = pltpu.SemaphoreType.DMA
    low, full = jnp.bfloat16, jnp.float32
    any_spec = pl.BlockSpec(memory_space=pl.ANY)
    operands = (
        order, gain_one, gain_two, grad_gate, grad_up, mixed, normed_two, cotangents, part,
        hidden, inputs, query_weight, key_weight, value_weight, output_weight, down_weight,
        attended, packed, normed, cosine, sine,
    )

    def like(array):
        return pltpu.VMEM(array.shape, array.dtype)

    return pl.pallas_call(
        functools.partial(backward_kernel, rounds, block),
        out_shape=(
            jax.ShapeDtypeStruct((rounds * ROUND_ROWS, width), low),
            jax.ShapeDtypeStruct((2, width), full),
            jax.ShapeDtypeStruct((TILE, width), full),
            jax.ShapeDtypeStruct((TILE, width), low),
        ),
        in_specs=[pl.BlockSpec(memory_space=pltpu.SMEM)] + [vmem()] * 2 + [any_spec] * 18,
        out_specs=(any_spec, vmem(), vmem(), vmem()),
        scratch_shapes=[
            pltpu.VMEM((rounds * ROUND_ROWS, width), low),
            pltpu.VMEM((3, RING * SPINE_ROWS, width), low),
            pltpu.VMEM((3, RING * LINE_ROWS, width), low),
            like(grad_gate), like(grad_up), like(mixed), like(normed_two), like(cotangents),
            like(part), like(hidden), like(inputs), like(output_weight),
            like(attended), like(packed), like(normed), like(cosine), like(sine),
            pltpu.VMEM((WIDE, WIDE), low),
            pltpu.VMEM((2, WIDE, width), low),
            pltpu.VMEM((2, 2, TILE, width), low),
            pltpu.VMEM((2, TILE, width), low),
            pltpu.VMEM((2, TILE, width), low),
            pltpu.VMEM((4 * TILE, width), low),
            pltpu.VMEM((TILE, width), full),
            pltpu.VMEM((2, 8, width), full),
            pltpu.VMEM((length // block, block // 2, 2 * PAIR), low),
            pltpu.VMEM((length // block, block // 2, 2 * PAIR), low),
        ]
        + [pltpu.VMEM((length, HEAD_DIM), low)] * 6
        + [pltpu.VMEM((length // block, block, PAIR), full)]
        + [pltpu.VMEM((length // block, block, HEAD_DIM), full)] * 2
        + [
            pltpu.VMEM((length // block, block, WIDE), low),
            pltpu.VMEM((length // block, block, WIDE), low),
            pltpu.VMEM((2, 4 * TILE, WIDE), low),
            pltpu.VMEM((4, 2, width), full),
            pltpu.VMEM((8, 2, width), full),
            dma((21,)),
            dma((RING,)), dma((3, RING)), dma((3, RING)), dma((RING,)),
            dma((RING,)), dma((RING,)),
            dma((RING,)), dma((3, RING)), dma((3, RING)), dma((RING,)),
            dma((2, 4)), dma((2, 4)),
            dma((3,)), dma((3,)),
            dma((2, 8)), dma((2, 8)),
            dma((4,)), dma((4,)), dma((8,)), dma((8,)),
        ],
        compiler_params=pltpu.CompilerParams(
            collective_id=key, has_side_effects=True, vmem_limit_bytes=63 * 2**20
        ),
        name="backward",
    )(*operands)


def forward_kernel(
    block,
    place_ref,
    table_ref,
    gain_one_ref,
    gain_two_ref,
    input_ref,
    cotangent_ref,
    query_weight_ref,
    key_weight_ref,
    value_weight_ref,
    output_weight_ref,
    gate_weight_ref,
    up_weight_ref,
    down_weight_ref,
    place_out,
    part_out,
    hidden_out,
    attended_out,
    packed_out,
    normed_one_out,
    cosine_out,
    sine_out,
    cotangent_out,
    normed_two_out,
    mixed_out,
    grad_gate_out,
    grad_up_out,
    places,
    tables,
    inputs,
    cotangents,
    normed_one,
    normed_two,
    cosine,
    sine,
    weight,
    output_weight,
    gate_weight,
    up_weight,
    down_weight,
    packed_from,
    packed,
    q0,
    q1,
    k,
    v,
    result,
    heads_from,
    heads,
    part,
    near,
    send,
    far,
    hidden,
    mixed,
    grad_gate,
    grad_up,
    fetch_sem,
    store_sem,
    gather_send,
    gather_recv,
    swap_send,
    swap_recv,
    fold_send,
    fold_recv,
):
    place = Place()
    length, width = q0.shape[0], inputs.shape[1]
    halves = TILE // block
    half = HEAD_DIM // 2
    pair_rows = 2 * TILE
    fetches, stores = {}, []

    def fetch_all(key, *copies):
        base = sum(len(group) for group in fetches.values())
        fetches[key] = [
            pltpu.make_async_copy(part_of, target, fetch_sem.at[base + index])
            for index, (part_of, target) in enumerate(copies)
        ]
        for copy in fetches[key]:
            copy.start()

    def fetch(*keys):
        for key in keys:
            for copy in fetches[key]:
                copy.wait()

    def store(source, target):
        copy = pltpu.make_async_copy(source, target, store_sem.at[len(stores)])
        copy.start()
        stores.append(copy)

    own_rows = rows_at(place.row * TILE, TILE)
    fetch_all("inputs", (input_ref, inputs.at[own_rows]))
    fetch_all("cotangent", (cotangent_ref, cotangents.at[own_rows]))
    copies = []
    for head in range(2):
        query_base, key_base = head * PAIR, head * HEAD_DIM
        target = weight.at[head]
        heads_of = [(query_weight_ref, query_base), (query_weight_ref, query_base + HEAD_DIM)]
        heads_of += [(key_weight_ref, key_base), (value_weight_ref, key_base)]
        for index, (source, first) in enumerate(heads_of):
            copies.append(
                (source.at[pl.ds(first, HEAD_DIM)], target.at[pl.ds(index * HEAD_DIM, HEAD_DIM)])
            )
            for side in range(2):
                copies.append(
                    (
                        source.at[pl.ds(first + (1 - side) * half, half)],
                        target.at[pl.ds(WIDE + index * HEAD_DIM + side * half, half)],
                    )
                )
    fetch_all("weight", *copies)
    fetch_all("output", (output_weight_ref, output_weight))
    fetch_all("gate", (gate_weight_ref, gate_weight))
    fetch_all("up", (up_weight_ref, up_weight))
    fetch_all("down", (down_weight_ref, down_weight))
    places[pl.ds(pl.multiple_of(place.row * 8, 8), 8), :] = jnp.broadcast_to(
        place_ref[...], (8, place_ref.shape[1])
    )
    gain_one = gain_one_ref[...].astype(jnp.float32).reshape(1, -1)
    gain_two = gain_two_ref[...].astype(jnp.float32).reshape(1, -1)
    tables[own_rows, :] = table_ref[...]
    gather_places = Gather(place, places, gather_send.at[0], gather_recv.at[0], 8)
    gather_tables = Gather(place, tables, gather_send.at[1], gather_recv.at[1])
    gather_inputs = Gather(place, inputs, gather_send.at[2], gather_recv.at[2], TILE, 2)
    gather_cotangents = Gather(place, cotangents, gather_send.at[3], gather_recv.at[3])
    gather_two = Gather(place, normed_two, gather_send.at[4], gather_recv.at[4], TILE, 2)
    swap_places = Swap(place, places, place_out, swap_send.at[0], swap_recv.at[0], 8, 2)
    swap_packed = Swap(place, packed_from, packed, swap_send.at[1], swap_recv.at[1], halves)
    swap_heads = Swap(place, heads_from, heads, swap_send.at[2], swap_recv.at[2], halves)
    fold = Fold(place, part, near, send, far, fold_send, fold_recv)
    place.greet()
    fetch("inputs")
    gather_tables.start()
    gather_inputs.start()
    gather_inputs.start(1)
    gather_places.start()
    fetch("cotangent")
    gather_cotangents.start()

    def project(chip):
        base = chip * pair_rows

        @pl.loop(0, pair_rows // 16)
        def _(piece):
            span = rows_at(base + piece * 16, 16)
            rows = inputs[span, :].astype(jnp.float32)
            normed_one[span, :] = (rows * rms_scale(rows) * gain_one).astype(jnp.bfloat16)

        span = rows_at(base, pair_rows)
        low_cosine, low_sine = tables[span, :half], tables[span, half:HEAD_DIM]
        ones = jnp.ones((pair_rows, HEAD_DIM), jnp.float32)
        cosine[span, :] = jnp.concatenate([low_cosine] * 6 + [ones], axis=-1)
        sine[span, :] = jnp.concatenate([-low_sine, low_sine] * 3 + [ones * 0.0], axis=-1)

        for head in range(2):
            products = product_back(normed_one[span, :], weight[head])
            low = (
                products[:, :WIDE] * cosine[span, :] + products[:, WIDE:] * sine[span, :]
            ).astype(jnp.bfloat16)
            for index in range(2):
                packed_from[pl.ds(((2 * chip + index) * 2 + head) * halves, halves)] = low[
                    index * TILE : (index + 1) * TILE
                ].reshape(halves, block, WIDE)
        for index in range(4):
            swap_packed.start(4 * chip + index)

    gather_tables.first()
    gather_inputs.first()
    gather_places.first()
    fetch("weight")
    project(place.chip)
    gather_tables.relay()
    gather_inputs.relay()
    gather_places.relay()
    gather_tables.arrive()
    gather_inputs.arrive()
    gather_places.arrive()
    project(1 - place.chip)
    swap_places.start_all()
    store(normed_one, normed_one_out)
    store(cosine, cosine_out)
    store(sine, sine_out)
    swap_places.arrive()
    swap_packed.arrive()
    store(packed, packed_out)

    def place_row(first, count):
        blocks = [place_out[8 * index : 8 * index + 1, :] for index in range(first, first + count)]
        return jnp.concatenate(blocks, axis=-1)

    tile = min(256, length)
    order = place_row(0, length // TILE)
    flat = packed[...].reshape(length, WIDE)
    for first in range(0, length, tile):
        rows = lax.broadcasted_iota(jnp.int32, (tile, length), 0) + first
        chosen = jnp.where(rows == order, 1.0, 0.0).astype(jnp.bfloat16)
        moved = product(chosen, flat).astype(jnp.bfloat16)
        for index, target in enumerate((q0, q1, k, v)):
            target[first : first + tile, :] = moved[:, index * HEAD_DIM : (index + 1) * HEAD_DIM]
    for first in range(0, length, tile):
        parts = []
        for q in (q0, q1):
            soft = softmax_parts(q[first : first + tile, :], k[: first + tile, :], first)
            parts.append(product(soft.astype(jnp.bfloat16), v[: first + tile, :]))
        result[first : first + tile, :] = jnp.concatenate(parts, axis=-1).astype(jnp.bfloat16)
    for first in range(0, length, tile):
        rows = lax.broadcasted_iota(jnp.int32, (length, tile), 0)
        chosen = jnp.where(rows == place_row(first // TILE, tile // TILE), 1.0, 0.0)
        moved = product_rows(chosen.astype(jnp.bfloat16), result[...]).astype(jnp.bfloat16)
        heads_from[first // block : (first + tile) // block] = pack_pairs(
            moved.reshape(-1, block, PAIR)
        )
    swap_heads.start_all()
    gather_cotangents.first()
    gather_cotangents.relay()
    fetch("output")
    swap_heads.arrive()
    store(heads, attended_out)

    def project_out(sequence):
        total = None
        for head in range(2):
            rows = heads[pl.ds((2 * sequence + head) * halves, halves)]
            rows = unpack_pairs(rows).reshape(TILE, PAIR)
            term = product(rows, output_weight[head * PAIR : (head + 1) * PAIR, :])
            total = term if total is None else total + term
        part[rows_at(sequence * TILE, TILE), :] = total.astype(jnp.bfloat16)

    for chip in (1 - place.chip, place.chip):
        project_out(2 * chip + 1 - place.core)
        fold.partner_copy(chip).start()
        project_out(2 * chip + place.core)
    gather_cotangents.arrive()
    store(cotangents, cotangent_out)
    fold.relay()
    fold.arrive_near()
    for half_rows in range(2):
        fold.arrive_across(half_rows)

        @pl.loop(4 * half_rows, 4 * half_rows + 4)
        def _(piece):
            span = rows_at(piece * 16, 16)
            own = rows_at(place.row * TILE + piece * 16, 16)
            rows = inputs[own, :].astype(jnp.float32) + fold.rows(piece * 16, 16)
            hidden[span, :] = rows
            normed_two[own, :] = (rows * rms_scale(rows) * gain_two).astype(jnp.bfloat16)

        gather_two.start(half_rows)
    store(hidden, hidden_out)
    fetch("gate", "up", "down")

    def feed(chip):
        span = rows_at(chip * pair_rows, pair_rows)

        @pl.loop(0, mixed.shape[1] // 256)
        def _(index):
            units = rows_at(index * 256, 256)
            columns = pl.ds(pl.multiple_of(index * 256, 256), 256)
            gate = product_back(normed_two[span, :], gate_weight[units, :])
            upward = product_back(normed_two[span, :], up_weight[units, :])
            grad_mixed = product_back(cotangents[span, :], down_weight[units, :])
            sigmoid = jax.nn.sigmoid(gate)
            activated = gate * sigmoid
            mixed[span, columns] = (activated * upward).astype(jnp.bfloat16)
            grad_gate[span, columns] = (
                grad_mixed * upward * sigmoid * (1.0 + gate * (1.0 - sigmoid))
            ).astype(jnp.bfloat16)
            grad_up[span, columns] = (grad_mixed * activated).astype(jnp.bfloat16)

        @pl.loop(0, width // 512)
        def _(index):
            columns = pl.ds(pl.multiple_of(index * 512, 512), 512)
            part[span, columns] = (
                product(grad_gate[span, :], gate_weight[:, columns])
                + product(grad_up[span, :], up_weight[:, columns])
            ).astype(jnp.bfloat16)

    def store_feed(chip):
        span = rows_at(chip * pair_rows, pair_rows)
        for source, target in (
            (part, part_out), (mixed, mixed_out), (grad_gate, grad_gate_out),
            (grad_up, grad_up_out),
        ):
            store(source.at[span], target.at[span])

    gather_two.first()
    feed(place.chip)
    store_feed(place.chip)
    gather_two.relay()
    gather_two.arrive()
    store(normed_two, normed_two_out)
    feed(1 - place.chip)
    store_feed(1 - place.chip)
    for copy in stores:
        copy.wait()


def forward(places, table, gain_one, gain_two, inputs, cotangent, query_weight, key_weight, value_weight,
            output_weight, gate_weight, up_weight, down_weight, length, block, key):
    width = inputs.shape[1]
    hidden_units = gate_weight.shape[0]
    rows = 4 * TILE
    blocks = length // block
    low, full = jnp.bfloat16, jnp.float32
    dma = pltpu.SemaphoreType.DMA
    any_spec = pl.BlockSpec(memory_space=pl.ANY)

    def out(shape, dtype):
        return jax.ShapeDtypeStruct(shape, dtype)

    wide = (rows, width)
    return pl.pallas_call(
        functools.partial(forward_kernel, block),
        out_shape=(
            out((64, 128), jnp.int32),
            out(wide, low), out((TILE, width), full),
            out((blocks, block // 2, 2 * PAIR), low), out((blocks, block, WIDE), low),
            out(wide, low), out((rows, WIDE), full), out((rows, WIDE), full),
            out(wide, low), out(wide, low),
            out((rows, hidden_units), low), out((rows, hidden_units), low),
            out((rows, hidden_units), low),
        ),
        in_specs=[vmem()] * 4 + [any_spec] * 9,
        out_specs=(vmem(),) + (any_spec,) * 12,
        scratch_shapes=[
            pltpu.VMEM((32, 128), jnp.int32),
            pltpu.VMEM((rows, 128), full),
            pltpu.VMEM(wide, low), pltpu.VMEM(wide, low),
            pltpu.VMEM(wide, low), pltpu.VMEM(wide, low),
            pltpu.VMEM((rows, WIDE), full), pltpu.VMEM((rows, WIDE), full),
            pltpu.VMEM((2, 2 * WIDE, width), low),
            pltpu.VMEM(output_weight.shape, low),
            pltpu.VMEM((hidden_units, width), low), pltpu.VMEM((hidden_units, width), low),
            pltpu.VMEM((hidden_units, width), low),
            pltpu.VMEM((blocks, block, WIDE), low), pltpu.VMEM((blocks, block, WIDE), low),
        ]
        + [pltpu.VMEM((length, HEAD_DIM), low)] * 4
        + [
            pltpu.VMEM((length, PAIR), low),
            pltpu.VMEM((blocks, block // 2, 2 * PAIR), low),
            pltpu.VMEM((blocks, block // 2, 2 * PAIR), low),
            pltpu.VMEM(wide, low),
            pltpu.VMEM((2, TILE, width), low),
            pltpu.VMEM((TILE, width), low), pltpu.VMEM((TILE, width), low),
            pltpu.VMEM((TILE, width), full),
            pltpu.VMEM((rows, hidden_units), low), pltpu.VMEM((rows, hidden_units), low),
            pltpu.VMEM((rows, hidden_units), low),
            dma((30,)), dma((16,)),
            dma((5, 6)), dma((5, 6)),
            dma((3, 8)), dma((3, 8)),
            dma((4,)), dma((4,)),
        ],
        compiler_params=pltpu.CompilerParams(
            collective_id=key, has_side_effects=True, vmem_limit_bytes=63 * 2**20
        ),
        name="forward",
    )(places, table, gain_one, gain_two, inputs, cotangent, query_weight, key_weight, value_weight,
      output_weight, gate_weight, up_weight, down_weight)


def widen_kernel(plan, kept, source, *refs):
    sources, refs = refs[:kept], refs[kept:]
    holds, refs, hold_sem = refs[-1 - kept : -1], refs[: -1 - kept], refs[-1]
    targets, (low, full, load_sem, store_sem) = refs[:-4], refs[-4:]
    targets, copies = targets[: len(targets) - kept], targets[len(targets) - kept :]
    takes = [
        pltpu.make_async_copy(sources[index], holds[index], hold_sem.at[index])
        for index in range(kept)
    ]
    gives = [
        pltpu.make_async_copy(holds[index], copies[index], hold_sem.at[kept + index])
        for index in range(kept)
    ]
    slots = low.shape[0]
    loads, stores = [], []
    for index, (first, which, target_row, chunk) in enumerate(plan):
        slot = index % slots
        span = pl.ds(0, chunk)
        loads.append(
            pltpu.make_async_copy(
                source.at[pl.ds(first, chunk)], low.at[slot, span], load_sem.at[slot]
            )
        )
        stores.append(
            pltpu.make_async_copy(
                full.at[slot, span],
                targets[which].at[pl.ds(target_row, chunk)],
                store_sem.at[slot],
            )
        )
    for load in loads[:slots] + takes:
        load.start()
    for index, (load, store) in enumerate(zip(loads, stores)):
        slot = index % slots
        load.wait()
        if index >= slots:
            stores[index - slots].wait()

        @pl.loop(0, plan[index][3] // 16)
        def _(piece):
            span = rows_at(piece * 16, 16)
            full[slot, span, :] = low[slot, span, :].astype(jnp.float32)

        store.start()
        if index + slots < len(plan):
            loads[index + slots].start()
        if index == slots:
            for take, give in zip(takes, gives):
                take.wait()
                give.start()
    for store in stores[-slots:] + gives:
        store.wait()


def widen(values, counts, keep):
    slots, width, first, plan = 6, values.shape[1], 0, []
    for which, count in enumerate(counts):
        chunk = math.gcd(count, 256) if count % 192 else 192
        plan += [(first + row, which, row, chunk) for row in range(0, count, chunk)]
        first += count
    any_spec = pl.BlockSpec(memory_space=pl.ANY)
    return pl.pallas_call(
        functools.partial(widen_kernel, plan, len(keep)),
        out_shape=tuple(jax.ShapeDtypeStruct((count, width), jnp.float32) for count in counts)
        + tuple(jax.ShapeDtypeStruct(array.shape, array.dtype) for array in keep),
        in_specs=[any_spec] * (1 + len(keep)),
        out_specs=(any_spec,) * (len(counts) + len(keep)),
        scratch_shapes=[
            pltpu.VMEM((slots, 256, width), values.dtype),
            pltpu.VMEM((slots, 256, width), jnp.float32),
            pltpu.SemaphoreType.DMA((slots,)),
            pltpu.SemaphoreType.DMA((slots,)),
        ]
        + [pltpu.VMEM(array.shape, array.dtype) for array in keep]
        + [pltpu.SemaphoreType.DMA((2 * len(keep),))],
        compiler_params=pltpu.CompilerParams(vmem_limit_bytes=63 * 2**20),
        name="widen",
    )(values, *keep)


def gather_rows(values):
    return lax.all_gather(values, "fsdp", axis=0, tiled=True)


def scatter_rows(values):
    return lax.psum_scatter(
        values.astype(jnp.bfloat16), "fsdp", scatter_dimension=0, tiled=True
    ).astype(jnp.float32)


def per_device_gathered(
    inputs,
    positions,
    cotangent,
    attention_gain,
    query_weight,
    key_weight,
    value_weight,
    output_weight,
    feedforward_gain,
    gate_weight,
    up_weight,
    down_weight,
):
    row_count = inputs.shape[0]
    groups = HEADS // KV_HEADS
    gain_one = attention_gain.astype(jnp.float32)
    gain_two = feedforward_gain.astype(jnp.float32)
    seq_count = lax.axis_size("fsdp")
    first_row = lax.axis_index("fsdp") * row_count

    def own(values):
        return lax.dynamic_slice_in_dim(values, first_row, row_count, 0)

    query_places = gather_rows(positions).reshape(seq_count, row_count)
    key_places = lax.all_gather(query_places, "ctx", axis=1, tiled=True)
    all_cotangent = gather_rows(cotangent)
    flat_in = gather_rows(inputs).astype(jnp.float32)
    scale_one = rms_scale(flat_in)
    unit_one = flat_in * scale_one
    normed_one = (unit_one * gain_one).astype(jnp.bfloat16)
    total_rows = normed_one.shape[0]
    cosine, sine = rotary_tables(query_places.reshape(-1))
    query_heads = query_weight.shape[0] // HEAD_DIM
    kv_heads = key_weight.shape[0] // HEAD_DIM
    kv_width = kv_heads * HEAD_DIM
    query_low = rotate(
        product_back(normed_one, query_weight).reshape(total_rows, query_heads, HEAD_DIM), cosine, sine
    ).astype(jnp.bfloat16)
    key_low = rotate(
        product_back(normed_one, key_weight).reshape(total_rows, kv_heads, HEAD_DIM), cosine, sine
    ).astype(jnp.bfloat16)
    value_low = product_back(normed_one, value_weight).astype(jnp.bfloat16)
    ctx_size = lax.axis_size("ctx")

    def spread(values):
        rows = lax.all_gather(values, "ctx", axis=0, tiled=True)
        rows = rows.reshape(ctx_size, seq_count, row_count, kv_width).swapaxes(0, 1)
        return rows.reshape(seq_count, ctx_size * row_count, kv_width)

    def collect(values):
        rows = values.astype(jnp.bfloat16).swapaxes(1, 2)
        rows = rows.reshape(seq_count, ctx_size, row_count, kv_width).swapaxes(0, 1)
        return lax.psum_scatter(
            rows.reshape(-1, kv_width), "ctx", scatter_dimension=0, tiled=True
        )

    all_keys = spread(key_low.reshape(total_rows, kv_width))
    all_values = spread(value_low)
    total_keys = all_keys.shape[1]
    key_grid = all_keys.reshape(seq_count, total_keys, kv_heads, HEAD_DIM).swapaxes(1, 2)
    value_grid = all_values.reshape(seq_count, total_keys, kv_heads, HEAD_DIM).swapaxes(1, 2)
    query_grouped = query_low.reshape(seq_count, row_count, kv_heads, groups, HEAD_DIM)
    attended, log_total = attend_forward(
        query_grouped, query_places, key_grid, value_grid, key_places
    )
    attended_low = attended.reshape(total_rows, query_heads * HEAD_DIM).astype(jnp.bfloat16)
    hidden_state = inputs.astype(jnp.float32) + scatter_rows(product(attended_low, output_weight))
    scale_two = rms_scale(hidden_state)
    unit_two = hidden_state * scale_two
    normed_two = gather_rows((unit_two * gain_two).astype(jnp.bfloat16))
    gate_values = product_back(normed_two, gate_weight)
    upward = product_back(normed_two, up_weight)
    sigmoid_gate = jax.nn.sigmoid(gate_values)
    activated = gate_values * sigmoid_gate
    mixed_hidden = (activated * upward).astype(jnp.bfloat16)
    grad_out = cotangent.astype(jnp.float32)
    grad_down = product_rows(mixed_hidden, all_cotangent)
    grad_mixed = product_back(all_cotangent, down_weight)
    grad_gate_low = (
        grad_mixed * upward * sigmoid_gate * (1.0 + gate_values * (1.0 - sigmoid_gate))
    ).astype(jnp.bfloat16)
    grad_up_low = (grad_mixed * activated).astype(jnp.bfloat16)
    grad_unit_part = (
        product(grad_gate_low, gate_weight) + product(grad_up_low, up_weight)
    ).astype(jnp.bfloat16)
    grad_normed_two = scatter_rows(grad_unit_part)
    gain_two_grad = jnp.sum(grad_normed_two * unit_two, axis=0)
    grad_hidden = grad_out + norm_back(scale_two, unit_two, grad_normed_two * gain_two)
    branch_rows = gather_rows(grad_hidden.astype(jnp.bfloat16))
    layer_output = (hidden_state + scatter_rows(product(mixed_hidden, down_weight))).astype(
        jnp.bfloat16
    )
    grad_gate = product_rows(grad_gate_low, normed_two)
    grad_up = product_rows(grad_up_low, normed_two)
    grad_output = product_rows(attended_low, branch_rows)
    grad_attended = product_back(branch_rows, output_weight).astype(jnp.bfloat16)
    grad_attended = grad_attended.reshape(seq_count, row_count, kv_heads, groups, HEAD_DIM)
    grad_query_rot, grad_key_all, grad_value_all = attend_backward(
        query_grouped, query_places, key_grid, value_grid, key_places, log_total, grad_attended
    )
    grad_key_own = collect(grad_key_all).astype(jnp.float32)
    grad_value_low = collect(grad_value_all)
    grad_query_low = (
        rotate_back(grad_query_rot.reshape(total_rows, query_heads, HEAD_DIM), cosine, sine)
        .reshape(total_rows, query_heads * HEAD_DIM)
        .astype(jnp.bfloat16)
    )
    grad_key_low = (
        rotate_back(
            grad_key_own.reshape(total_rows, kv_heads, HEAD_DIM), cosine, sine
        )
        .reshape(total_rows, kv_width)
        .astype(jnp.bfloat16)
    )
    grad_query = product_rows(grad_query_low, normed_one)
    grad_key = product_rows(grad_key_low, normed_one)
    grad_value = product_rows(grad_value_low, normed_one)
    grad_normed_one = scatter_rows(
        product(grad_query_low, query_weight)
        + product(grad_key_low, key_weight)
        + product(grad_value_low, value_weight)
    )
    own_unit = own(unit_one)
    gain_one_grad = jnp.sum(grad_normed_one * own_unit, axis=0)
    input_grad = grad_hidden + norm_back(own(scale_one), own_unit, grad_normed_one * gain_one)

    grads = (grad_query, grad_key, grad_value, grad_output, grad_gate, grad_up, grad_down)
    parts = [lax.psum(grad.astype(jnp.bfloat16), "ctx").astype(jnp.float32) for grad in grads]
    gain_sums = lax.psum(jnp.stack([gain_one_grad, gain_two_grad]), ("fsdp", "ctx"))
    return (
        layer_output,
        input_grad,
        gain_sums[0],
        parts[0],
        parts[1],
        parts[2],
        parts[3],
        gain_sums[1],
        parts[4],
        parts[5],
        parts[6],
    )


def per_device_by_head(
    inputs,
    positions,
    cotangent,
    attention_gain,
    query_weight,
    key_weight,
    value_weight,
    output_weight,
    feedforward_gain,
    gate_weight,
    up_weight,
    down_weight,
):
    gain_one, gain_two = attention_gain, feedforward_gain
    block = TILE // 2
    length = TILE * 8
    cosine, sine = rotary_tables(positions)
    table = jnp.concatenate([cosine[:, 0, :], sine[:, 0, :]], axis=1)
    table = jnp.pad(table, ((0, 0), (0, 128 - table.shape[1])))
    (
        places, part, hidden, attended, packed, normed_one, wide_cosine, wide_sine,
        cotangents, normed_two, mixed, grad_gate, grad_up,
    ) = forward(
        positions[None, :], table, gain_one, gain_two, inputs, cotangent, query_weight,
        key_weight, value_weight, output_weight, gate_weight, up_weight, down_weight, length,
        block, 1,
    )
    starts = places.reshape(8, 8, TILE)[:, 0, ::block].reshape(-1) // block
    slots = jnp.arange(length // block, dtype=jnp.int32)
    found = jnp.where(starts[None, :] == slots[:, None], slots[None, :], 0)
    order = jnp.concatenate([jnp.sum(found, axis=1), starts]).astype(jnp.int32)
    summed, gain_sums, input_grad, layer_output = backward(
        order, gain_one, gain_two, grad_gate, grad_up, mixed, normed_two, cotangents, part,
        hidden, inputs, query_weight, key_weight, value_weight, output_weight, down_weight,
        attended, packed, normed_one, wide_cosine, wide_sine, 5,
    )
    owners = (gate_weight, up_weight, down_weight, query_weight, key_weight, value_weight,
              output_weight)
    *parts, layer_output, input_grad = widen(
        summed, [owner.shape[0] for owner in owners], (layer_output, input_grad)
    )
    return (layer_output, input_grad, gain_sums[0], *parts[3:], gain_sums[1], *parts[:3])


def per_device(*arrays):
    fits = lax.axis_size("fsdp") == 4 and lax.axis_size("ctx") == 8
    return (per_device_by_head if fits else per_device_gathered)(*arrays)


def solution(mesh):
    in_specs = (
        P(("fsdp", "ctx"), None),
        P(("fsdp", "ctx")),
        P(("fsdp", "ctx"), None),
        P(),
        P("fsdp", None),
        P("fsdp", None),
        P("fsdp", None),
        P("fsdp", None),
        P(),
        P("fsdp", None),
        P("fsdp", None),
        P("fsdp", None),
    )
    out_specs = (
        P(("fsdp", "ctx"), None),
        P(("fsdp", "ctx"), None),
        P(),
        P("fsdp", None),
        P("fsdp", None),
        P("fsdp", None),
        P("fsdp", None),
        P(),
        P("fsdp", None),
        P("fsdp", None),
        P("fsdp", None),
    )
    return jax.shard_map(
        per_device, mesh=mesh, in_specs=in_specs, out_specs=out_specs, check_vma=False
    )
```

```python
import functools
import math

import jax
import jax.numpy as jnp
from jax import lax
from jax.experimental import pallas as pl
from jax.experimental.pallas import tpu as pltpu
from jax.sharding import PartitionSpec as P

HEADS = 16
KV_HEADS = 8
HEAD_DIM = 96


EPSILON = 1e-05
ROPE_BASE = 100000.0


def product(left, right):
    return jnp.dot(left, right, preferred_element_type=jnp.float32)


def product_back(left, right):
    return lax.dot_general(
        left, right, (((1,), (1,)), ((), ())), preferred_element_type=jnp.float32
    )


def product_rows(left, right):
    return lax.dot_general(
        left, right, (((0,), (0,)), ((), ())), preferred_element_type=jnp.float32
    )


def rms_scale(values):
    return lax.rsqrt(jnp.mean(values * values, axis=-1, keepdims=True) + EPSILON)


def norm_back(scale_rows, unit_rows, grad_unit):
    return scale_rows * (
        grad_unit - unit_rows * jnp.mean(grad_unit * unit_rows, axis=-1, keepdims=True)
    )


def rotary_tables(places):
    half_width = HEAD_DIM // 2
    frequencies = ROPE_BASE ** (-(jnp.arange(half_width, dtype=jnp.float32) * 2.0 / HEAD_DIM))
    angles = places.astype(jnp.float32)[:, None] * frequencies[None, :]
    return (jnp.cos(angles)[:, None, :], jnp.sin(angles)[:, None, :])


def rotate(values, cosine, sine):
    half_width = values.shape[-1] // 2
    lower_half = values[..., :half_width]
    upper_half = values[..., half_width:]
    return jnp.concatenate(
        [lower_half * cosine - upper_half * sine, upper_half * cosine + lower_half * sine], axis=-1
    )


def rotate_back(grads, cosine, sine):
    half_width = grads.shape[-1] // 2
    lower_half = grads[..., :half_width]
    upper_half = grads[..., half_width:]
    return jnp.concatenate(
        [lower_half * cosine + upper_half * sine, upper_half * cosine - lower_half * sine], axis=-1
    )


def block_total_of(total_keys):
    return max(1, total_keys // 512)


def masked_scores(query_grouped, query_places, key_rows, key_places, start, width):
    key_part = lax.dynamic_slice_in_dim(key_rows, start, width, 2)
    place_part = lax.dynamic_slice_in_dim(key_places, start, width, 1)
    scores = jnp.einsum(
        "sqhgd,shkd->shgqk", query_grouped, key_part, preferred_element_type=jnp.float32
    )
    scores = scores * (1.0 / math.sqrt(HEAD_DIM))
    allowed = place_part[:, None, None, None, :] <= query_places[:, None, None, :, None]
    return jnp.where(allowed, scores, -1000000000.0)


def attend_forward(query_grouped, query_places, key_rows, value_rows, key_places):
    seq_count, row_count, head_groups, group_size = query_grouped.shape[:4]
    total_keys = key_rows.shape[2]
    block_total = block_total_of(total_keys)
    width = total_keys // block_total
    stat_shape = (seq_count, head_groups, group_size, row_count)

    def peak_step(index, carry):
        running_top, running_sum = carry
        scores = masked_scores(
            query_grouped, query_places, key_rows, key_places, index * width, width
        )
        new_top = jnp.maximum(running_top, jnp.max(scores, axis=-1))
        running_sum = running_sum * jnp.exp(running_top - new_top) + jnp.sum(
            jnp.exp(scores - new_top[..., None]), axis=-1
        )
        return (new_top, running_sum)

    running_top, running_sum = lax.fori_loop(
        0,
        block_total,
        peak_step,
        (jnp.full(stat_shape, -1e30, jnp.float32), jnp.zeros(stat_shape, jnp.float32)),
    )
    log_total = running_top + jnp.log(running_sum)

    def value_step(index, gathered):
        scores = masked_scores(
            query_grouped, query_places, key_rows, key_places, index * width, width
        )
        soft_low = jnp.exp(scores - log_total[..., None]).astype(jnp.bfloat16)
        value_part = lax.dynamic_slice_in_dim(value_rows, index * width, width, 2)
        return gathered + jnp.einsum(
            "shgqk,shkd->sqhgd", soft_low, value_part, preferred_element_type=jnp.float32
        )

    attended = lax.fori_loop(
        0, block_total, value_step, jnp.zeros(query_grouped.shape, jnp.float32)
    )
    return (attended, log_total)


def attend_backward(
    query_grouped, query_places, key_rows, value_rows, key_places, log_total, grad_attended
):
    total_keys = key_rows.shape[2]
    block_total = block_total_of(total_keys)
    width = total_keys // block_total
    score_scale = 1.0 / math.sqrt(HEAD_DIM)

    def soft_and_grad(index):
        scores = masked_scores(
            query_grouped, query_places, key_rows, key_places, index * width, width
        )
        soft_values = jnp.exp(scores - log_total[..., None])
        value_part = lax.dynamic_slice_in_dim(value_rows, index * width, width, 2)
        grad_soft = jnp.einsum(
            "sqhgd,shkd->shgqk", grad_attended, value_part, preferred_element_type=jnp.float32
        )
        return (soft_values, grad_soft)

    def delta_step(index, row_delta):
        soft_values, grad_soft = soft_and_grad(index)
        return row_delta + jnp.sum(soft_values * grad_soft, axis=-1)

    row_delta = lax.fori_loop(0, block_total, delta_step, jnp.zeros(log_total.shape, jnp.float32))

    def grad_step(index, carry):
        grad_query, grad_keys, grad_values = carry
        soft_values, grad_soft = soft_and_grad(index)
        grad_scores = (soft_values * (grad_soft - row_delta[..., None])).astype(jnp.bfloat16)
        key_part = lax.dynamic_slice_in_dim(key_rows, index * width, width, 2)
        grad_query = (
            grad_query
            + jnp.einsum(
                "shgqk,shkd->sqhgd", grad_scores, key_part, preferred_element_type=jnp.float32
            )
            * score_scale
        )
        key_term = (
            jnp.einsum(
                "shgqk,sqhgd->shkd", grad_scores, query_grouped, preferred_element_type=jnp.float32
            )
            * score_scale
        )
        value_term = jnp.einsum(
            "shgqk,sqhgd->shkd",
            soft_values.astype(jnp.bfloat16),
            grad_attended,
            preferred_element_type=jnp.float32,
        )
        grad_keys = lax.dynamic_update_slice_in_dim(grad_keys, key_term, index * width, 2)
        grad_values = lax.dynamic_update_slice_in_dim(grad_values, value_term, index * width, 2)
        return (grad_query, grad_keys, grad_values)

    initial = (
        jnp.zeros(query_grouped.shape, jnp.float32),
        jnp.zeros(key_rows.shape, jnp.float32),
        jnp.zeros(value_rows.shape, jnp.float32),
    )
    return lax.fori_loop(0, block_total, grad_step, initial)


def vmem():
    return pl.BlockSpec(memory_space=pltpu.VMEM)


def peer(ctx_index):
    return dict(device_id={"ctx": ctx_index}, device_id_type=pl.DeviceIdType.MESH)


SPINE_ROWS = 32
LINE_ROWS = 32
ROUND_ROWS = 2 * SPINE_ROWS + LINE_ROWS
LEAD = 4
HOP = 2
FEED = (0, 1, 3, 5, 8)
CHAIN = (0, 4, 6, 8, 10, 13, 24, 26, 30, 32)
RING = 20
TILE = 128
PAIR = (HEADS // KV_HEADS) * HEAD_DIM
WIDE = PAIR + 2 * HEAD_DIM


def near_fsdp(index):
    return dict(device_id={"fsdp": index}, device_id_type=pl.DeviceIdType.MESH)


def rows_at(start, count):
    return pl.ds(pl.multiple_of(start, 16), count)


class Place:
    def __init__(self):
        self.ctx = lax.axis_index("ctx")
        self.row = lax.axis_index("fsdp")
        self.chip, self.core = lax.div(self.row, 2), lax.rem(self.row, 2)
        self.partner = 2 * self.chip + 1 - self.core
        self.across = 2 * (1 - self.chip) + self.core
        self.corner = 2 * (1 - self.chip) + 1 - self.core

    def greet(self):
        barrier = pltpu.get_barrier_semaphore()
        for step in range(1, 4):
            pl.semaphore_signal(barrier, inc=1, **near_fsdp(lax.rem(self.row + step, 4)))
        for step in range(1, 8):
            pl.semaphore_signal(barrier, inc=1, **peer(lax.rem(self.ctx + step, 8)))
        pl.semaphore_wait(barrier, 10)


class Fold:
    def __init__(self, place, part, near, send, far, send_sem, recv_sem):
        self.place, self.part, self.near, self.send, self.far = place, part, near, send, far
        self.send_sem, self.recv_sem = send_sem, recv_sem

    def partner_copy(self, chip):
        block = 2 * chip + 1 - self.place.core
        return pltpu.make_async_remote_copy(
            src_ref=self.part.at[rows_at(block * TILE, TILE)],
            dst_ref=self.near.at[chip],
            send_sem=self.send_sem.at[chip],
            recv_sem=self.recv_sem.at[chip],
            **near_fsdp(self.place.partner),
        )

    def across_copy(self, piece):
        span = pl.ds(piece * (TILE // 2), TILE // 2)
        return pltpu.make_async_remote_copy(
            src_ref=self.send.at[span],
            dst_ref=self.far.at[span],
            send_sem=self.send_sem.at[2 + piece],
            recv_sem=self.recv_sem.at[2 + piece],
            **near_fsdp(self.place.across),
        )

    def start(self):
        self.partner_copy(1 - self.place.chip).start()
        self.partner_copy(self.place.chip).start()

    def relay(self):
        there = 1 - self.place.chip
        self.partner_copy(there).wait_recv()
        base = self.place.across * TILE
        for half in range(2):

            @pl.loop(2 * half, 2 * half + 2)
            def _(piece):
                mine = self.part[rows_at(base + piece * 32, 32), :].astype(jnp.float32)
                span = rows_at(piece * 32, 32)
                self.send[span, :] = (
                    mine + self.near[there, span, :].astype(jnp.float32)
                ).astype(jnp.bfloat16)

            self.across_copy(half).start()

    def arrive_near(self):
        self.partner_copy(self.place.chip).wait_recv()
        self.partner_copy(0).wait_send()
        self.partner_copy(1).wait_send()

    def arrive_across(self, piece):
        self.across_copy(piece).wait()

    def arrive(self):
        self.arrive_near()
        self.arrive_across(0)
        self.arrive_across(1)

    def rows(self, start, count):
        mine = self.part[rows_at(self.place.row * TILE + start, count), :].astype(jnp.float32)
        span = rows_at(start, count)
        near = self.near[self.place.chip, span, :].astype(jnp.float32)
        return mine + near + self.far[span, :].astype(jnp.float32)


class Gather:
    def __init__(self, place, full, send_sem, recv_sem, count=TILE, pieces=1):
        self.place, self.full, self.send_sem, self.recv_sem = place, full, send_sem, recv_sem
        self.count, self.pieces = count, pieces

    def copy(self, block, target, key, piece):
        rows = self.count // self.pieces
        span = pl.ds(pl.multiple_of(block * self.count + piece * rows, rows), rows)
        return pltpu.make_async_remote_copy(
            src_ref=self.full.at[span],
            dst_ref=self.full.at[span],
            send_sem=self.send_sem.at[key * self.pieces + piece],
            recv_sem=self.recv_sem.at[key * self.pieces + piece],
            **near_fsdp(target),
        )

    def start(self, piece=0):
        self.copy(self.place.row, self.place.across, 1, piece).start()
        self.copy(self.place.row, self.place.partner, 0, piece).start()

    def first(self):
        for piece in range(self.pieces):
            self.copy(self.place.partner, self.place.partner, 0, piece).wait_recv()

    def relay(self):
        for piece in range(self.pieces):
            self.copy(self.place.across, self.place.across, 1, piece).wait_recv()
            self.copy(self.place.across, self.place.partner, 2, piece).start()

    def arrive(self):
        for piece in range(self.pieces):
            self.copy(self.place.corner, self.place.partner, 2, piece).wait_recv()
            self.copy(self.place.row, self.place.across, 1, piece).wait_send()
            self.copy(self.place.row, self.place.partner, 0, piece).wait_send()
            self.copy(self.place.across, self.place.partner, 2, piece).wait_send()


class Swap:
    def __init__(self, place, source, target, send_sem, recv_sem, count, share=1):
        self.place, self.source, self.target = place, source, target
        self.send_sem, self.recv_sem, self.count, self.share = send_sem, recv_sem, count, share

    def span(self, index):
        return pl.ds(pl.multiple_of(index * self.count, self.count), self.count)

    def copy(self, other, sender):
        return pltpu.make_async_remote_copy(
            src_ref=self.source.at[self.span(lax.div(other, self.share))],
            dst_ref=self.target.at[self.span(sender)],
            send_sem=self.send_sem.at[other],
            recv_sem=self.recv_sem.at[sender],
            **peer(other),
        )

    def start(self, other):
        me = self.place.ctx

        @pl.when(other != me)
        def _():
            self.copy(other, me).start()

        @pl.when(other == me)
        def _():
            self.target[self.span(me)] = self.source[self.span(lax.div(me, self.share))]

    def start_all(self):
        for step in range(1, 9):
            self.start(lax.rem(self.place.ctx + step, 8))

    def arrive(self):
        for step in range(1, 8):
            other = lax.rem(self.place.ctx + step, 8)
            self.copy(other, other).wait()


class Spread:
    def __init__(self, slots, index, count, device, send_sem, recv_sem):
        self.slots, self.index, self.count, self.device = slots, index, count, device
        self.send_sem, self.recv_sem = send_sem, recv_sem

    def copy(self, step):
        return pltpu.make_async_remote_copy(
            src_ref=self.slots.at[self.index],
            dst_ref=self.slots.at[self.index],
            send_sem=self.send_sem.at[step],
            recv_sem=self.recv_sem.at[step],
            **self.device(lax.rem(self.index + step, self.count)),
        )

    def start(self):
        for step in range(1, self.count):
            self.copy(step).start()

    def total(self):
        for step in range(1, self.count):
            self.copy(step).wait()
        result = self.slots[0]
        for step in range(1, self.count):
            result += self.slots[step]
        return result


class Tree:
    def __init__(self, place, own, out_ref, index, rounds, line, box, sems, leaf_back):
        me = place.ctx
        depth, side = lax.div(me, 2), lax.rem(me, 2)
        other_side = me + 1 - 2 * side
        self.own, self.out, self.box, self.index, self.line = own, out_ref, box, index, line
        self.up, self.got, self.down, self.back = sems
        self.leaf_back = leaf_back
        if line:
            center = jnp.where(index >= rounds - 6, 1 + lax.rem(index, 2), lax.rem(index, 4))
            count = LINE_ROWS
            start = index * ROUND_ROWS + 2 * SPINE_ROWS
            root_side = lax.rem(index, 2)
            on_cross = depth == center
            self.root = jnp.logical_and(on_cross, side == root_side)
            has_side = self.root
            to_side = jnp.logical_and(on_cross, side != root_side)
            reach = jnp.maximum(center, 3 - center)
            away = jnp.abs(depth - center)
            crossed = jnp.where(side == root_side, 0, 1)
            self.rise_age = reach - away + jnp.where(self.root, 1, 0)
            self.fall_age = reach + 1 + away + crossed
        else:
            center = 1 + side
            count = SPINE_ROWS
            start = index * ROUND_ROWS + side * SPINE_ROWS
            self.root = depth == center
            has_side = None
        self.count = count
        self.start = start
        self.slot = lax.rem(index, RING)
        self.rows = rows_at(start, count)
        self.children = (
            (jnp.logical_and(depth > 0, depth <= center), me - 2, 0),
            (jnp.logical_and(depth < 3, depth >= center), me + 2, 1),
            (has_side, other_side, 2),
        )
        parent = jnp.where(depth < center, me + 2, me - 2)
        slot = jnp.where(depth < center, 0, 1)
        if line:
            parent = jnp.where(to_side, other_side, parent)
            slot = jnp.where(to_side, 2, slot)
        self.parent = jnp.where(self.root, other_side, parent)
        self.parent_slot = jnp.where(self.root, 2, slot)

    def boxed(self, slot):
        return self.box.at[slot, rows_at(self.slot * self.count, self.count)]

    def up_copy(self, target, slot):
        return pltpu.make_async_remote_copy(
            src_ref=self.own.at[self.rows],
            dst_ref=self.boxed(slot),
            send_sem=self.up.at[self.slot],
            recv_sem=self.got.at[slot, self.slot],
            **peer(target),
        )

    def down_copy(self, child, slot, source):
        back = self.back if slot < 2 or self.line else self.leaf_back
        return pltpu.make_async_remote_copy(
            src_ref=source.at[self.rows],
            dst_ref=self.out.at[self.rows],
            send_sem=self.down.at[slot, self.slot],
            recv_sem=back.at[self.slot],
            **peer(child),
        )

    def each_child(self, action):
        for present, child, slot in self.children:
            if present is None:
                action(child, slot)
            else:
                pl.when(present)(functools.partial(action, child, slot))

    def keep(self):
        return pltpu.make_async_copy(
            self.own.at[self.rows], self.out.at[self.rows], self.up.at[self.slot]
        )

    def rise(self):
        self.each_child(lambda child, slot: self.up_copy(child, slot).wait_recv())
        base = self.slot * self.count
        for piece in range(0, self.count, 16):
            span = rows_at(self.start + piece, 16)
            total = self.own[span, :].astype(jnp.float32)
            for present, _, slot in self.children:
                part = self.box[slot, rows_at(base + piece, 16), :].astype(jnp.float32)
                total += part if present is None else jnp.where(present, part, 0.0)
            self.own[span, :] = total.astype(jnp.bfloat16)

        @pl.when(jnp.logical_not(self.root))
        def _():
            self.up_copy(self.parent, self.parent_slot).start()

        @pl.when(self.root)
        def _():
            self.keep().start()
            self.each_child(lambda child, slot: self.down_copy(child, slot, self.own).start())

    def fall(self):
        @pl.when(jnp.logical_not(self.root))
        def _():
            self.down_copy(self.parent, 0, self.out).wait_recv()
            self.each_child(lambda child, slot: self.down_copy(child, slot, self.out).start())

    def finish(self):
        @pl.when(jnp.logical_not(self.root))
        def _():
            self.up_copy(self.parent, self.parent_slot).wait_send()

        @pl.when(self.root)
        def _():
            self.keep().wait()

        self.each_child(lambda child, slot: self.down_copy(child, slot, self.out).wait_send())


def softmax_parts(query_rows, key_rows, first_row):
    scores = product_back(query_rows, key_rows) * (1.0 / math.sqrt(HEAD_DIM))
    rows = lax.broadcasted_iota(jnp.int32, scores.shape, 0) + first_row
    columns = lax.broadcasted_iota(jnp.int32, scores.shape, 1)
    scores = jnp.where(columns <= rows, scores, -1e30)
    spread = jnp.exp(scores - jnp.max(scores, axis=-1, keepdims=True))
    return spread * (1.0 / jnp.sum(spread, axis=-1, keepdims=True))


def pack_pairs(blocks):
    half = blocks.shape[1] // 2
    return jnp.concatenate([blocks[:, :half], blocks[:, half:]], axis=-1)


def unpack_pairs(blocks):
    return jnp.concatenate([blocks[..., :PAIR], blocks[..., PAIR:]], axis=-2)


def sort_blocks(slot_ref, source, targets, opened=lambda rows: rows):
    block_total = source.shape[0]
    block = targets[0].shape[0] // block_total
    for index in range(block_total):
        rows = opened(source[slot_ref[index]])
        start = 0
        for target in targets:
            width = target.shape[-1]
            target[index * block : (index + 1) * block, :] = rows[:, start : start + width]
            start += width


def norm_back_rows(values, grad_unit):
    scale = rms_scale(values)
    unit = values * scale
    return unit, lambda grad: norm_back(scale, unit, grad)


def backward_kernel(
    rounds,
    block,
    order_ref,
    gain_one_ref,
    gain_two_ref,
    grad_gate_ref,
    grad_up_ref,
    mixed_ref,
    normed_two_ref,
    cotangent_ref,
    part_ref,
    hidden_ref,
    input_ref,
    query_weight_ref,
    key_weight_ref,
    value_weight_ref,
    output_weight_ref,
    down_weight_ref,
    attended_ref,
    packed_ref,
    normed_ref,
    cosine_ref,
    sine_ref,
    out_ref,
    gain_out_ref,
    input_grad_ref,
    layer_output_ref,
    own,
    spine_in,
    line_in,
    grad_gate,
    grad_up,
    mixed,
    normed_two,
    cotangents,
    part,
    hidden,
    inputs,
    output_weight,
    attended,
    packed,
    normed,
    cosine,
    sine,
    half_swap,
    weight,
    near,
    send,
    far,
    branch,
    grad_hidden,
    gain_part,
    heads_out,
    heads_in,
    q0,
    q1,
    k,
    v,
    g0,
    g1,
    result,
    dk,
    dv,
    packed_out,
    packed_in,
    turned,
    gain_near,
    gain_far,
    fetch_sem,
    spine_up,
    spine_got,
    spine_down,
    spine_back,
    leaf_up,
    leaf_back,
    line_up,
    line_got,
    line_down,
    line_back,
    fold_send,
    fold_recv,
    gather_send,
    gather_recv,
    swap_send,
    swap_recv,
    near_send,
    near_recv,
    far_send,
    far_recv,
):
    place = Place()
    me = place.ctx
    depth, side = lax.div(me, 2), lax.rem(me, 2)
    other_side = me + 1 - 2 * side
    hidden_units = mixed.shape[1]
    width = own.shape[1]
    base = 3 * hidden_units
    spare = rounds * ROUND_ROWS - base - 3 * WIDE
    length = q0.shape[0]
    halves = TILE // block
    tile = min(256, length)
    tiles = length // tile
    scale = 1.0 / math.sqrt(HEAD_DIM)

    fetches = {}

    def fetch_all(source, *copies):
        first = sum(len(group) for group in fetches.values())
        fetches[id(source)] = [
            pltpu.make_async_copy(*copy, fetch_sem.at[first + index])
            for index, copy in enumerate(copies or ())
        ]
        for copy in fetches[id(source)]:
            copy.start()

    def fetch(*sources):
        for source in sources:
            for copy in fetches[id(source)]:
                copy.wait()

    for source, target in (
        (part_ref, part),
        (grad_gate_ref, grad_gate),
        (normed_two_ref, normed_two),
        (grad_up_ref, grad_up),
        (mixed_ref, mixed),
        (cotangent_ref, cotangents),
        (hidden_ref, hidden),
        (packed_ref, packed),
        (down_weight_ref, own.at[pl.ds(base, hidden_units)]),
        (output_weight_ref, output_weight),
        (attended_ref, attended),
        (normed_ref, normed),
        (cosine_ref, cosine),
        (sine_ref, sine),
        (input_ref, inputs),
    ):
        fetch_all(source, (source, target))
    for source, first, count in (
        (query_weight_ref, 0, PAIR),
        (key_weight_ref, PAIR, HEAD_DIM),
        (value_weight_ref, PAIR + HEAD_DIM, HEAD_DIM),
    ):
        fetch_all(
            source,
            *(
                (source.at[pl.ds(head * count, count)], weight.at[head, pl.ds(first, count)])
                for head in range(2)
            ),
        )
    gain_one = gain_one_ref[...].astype(jnp.float32).reshape(1, -1)
    gain_two = gain_two_ref[...].astype(jnp.float32).reshape(1, -1)
    lanes = (WIDE, WIDE)
    row_lane = lax.broadcasted_iota(jnp.int32, lanes, 0)
    column_lane = lax.broadcasted_iota(jnp.int32, lanes, 1)
    half = HEAD_DIM // 2
    inner = lax.rem(column_lane, HEAD_DIM)
    partner_lane = column_lane + jnp.where(inner < half, half, -half)
    half_swap[...] = jnp.where(row_lane == partner_lane, 1.0, 0.0).astype(jnp.bfloat16)
    place.greet()
    fetch(part_ref)
    fold_two = Fold(place, part, near.at[0], send.at[0], far.at[0], fold_send.at[0], fold_recv.at[0])
    fold_output = Fold(
        place, part, near.at[0], send.at[0], far.at[0], fold_send.at[0], fold_recv.at[0]
    )
    fold_one = Fold(place, part, near.at[1], send.at[1], far.at[1], fold_send.at[1], fold_recv.at[1])
    gather = Gather(place, branch, gather_send, gather_recv)
    swap_heads = Swap(place, heads_out, heads_in, swap_send.at[0], swap_recv.at[0], halves)
    swap_packed = Swap(place, packed_out, packed_in, swap_send.at[1], swap_recv.at[1], halves)
    spread_near = Spread(gain_near, place.row, 4, near_fsdp, near_send, near_recv)
    spread_far = Spread(gain_far, me, 8, peer, far_send, far_recv)
    fold_two.start()

    def stage_feed(first):
        sides = ((grad_gate, normed_two), (grad_up, normed_two), (mixed, cotangents))
        left, right = sides[first // hidden_units]
        if first == 0:
            fetch(grad_gate_ref, normed_two_ref)
        elif first == hidden_units:
            fetch(grad_up_ref)
        elif first == 2 * hidden_units:
            fetch(mixed_ref)

        @pl.loop(0, 2)
        def _(index):
            start = first % hidden_units + index * 256
            columns = pl.ds(pl.multiple_of(start, 256), 256)
            rows = pl.ds(pl.multiple_of(first + index * 256, 256), 256)
            own[rows, :] = product_rows(left[:, columns], right[...]).astype(jnp.bfloat16)

    stage_feed(0)

    spine_sems = (spine_up, spine_got, spine_down, spine_back)
    line_sems = (line_up, line_got, line_down, line_back)

    def spine(index):
        return Tree(place, own, out_ref, index, rounds, False, spine_in, spine_sems, leaf_back)

    def line(index):
        return Tree(place, own, out_ref, index, rounds, True, line_in, line_sems, None)

    def leaf_rows(index):
        return rows_at(index * ROUND_ROWS + (1 - side) * SPINE_ROWS, SPINE_ROWS)

    def leaf_copy(index):
        slot = lax.rem(index, RING)
        return pltpu.make_async_remote_copy(
            src_ref=own.at[leaf_rows(index)],
            dst_ref=spine_in.at[2, rows_at(slot * SPINE_ROWS, SPINE_ROWS)],
            send_sem=leaf_up.at[slot],
            recv_sem=spine_got.at[2, slot],
            **peer(other_side),
        )

    def leaf_result(index):
        slot = lax.rem(index, RING)
        return pltpu.make_async_remote_copy(
            src_ref=own.at[leaf_rows(index)],
            dst_ref=out_ref.at[leaf_rows(index)],
            send_sem=leaf_up.at[slot],
            recv_sem=leaf_back.at[slot],
            **peer(other_side),
        )

    def stage_norm_two():
        fetch(hidden_ref, cotangent_ref)
        fold_two.arrive()
        gain_part[...] = jnp.zeros_like(gain_part)

        @pl.loop(0, TILE // 16)
        def _(piece):
            span = rows_at(piece * 16, 16)
            grad = fold_two.rows(piece * 16, 16)
            unit, back = norm_back_rows(hidden[span, :], None)
            gain_part[1] += (grad * unit).reshape(2, 8, -1).sum(axis=0)
            here = rows_at(place.row * TILE + piece * 16, 16)
            total = cotangents[here, :].astype(jnp.float32) + back(grad * gain_two)
            grad_hidden[span, :] = total
            branch[here, :] = total.astype(jnp.bfloat16)

        gather.start()

    def stage_heads():
        fetch(output_weight_ref)
        gather.first()
        gather.arrive()

        @pl.loop(0, 4)
        def _(sequence):
            rows = branch[rows_at(sequence * TILE, TILE), :]
            grads = product_back(rows, output_weight[...]).astype(jnp.bfloat16)
            for head in range(2):
                heads_out[pl.ds((2 * sequence + head) * halves, halves)] = pack_pairs(
                    grads[:, head * PAIR : (head + 1) * PAIR].reshape(halves, block, PAIR)
                )

        swap_heads.start_all()

    def stage_sort():
        fetch(packed_ref)
        sort_blocks(order_ref, packed, (q0, q1, k, v))

    def stage_output_grad():
        fetch(attended_ref)
        for head in range(2):
            rows = [
                attended[(2 * index + head) * halves : (2 * index + head + 1) * halves]
                for index in range(4)
            ]
            rows = unpack_pairs(jnp.concatenate(rows, axis=0)).reshape(4 * TILE, PAIR)
            first_row = base + 2 * WIDE + head * PAIR
            for first in range(0, own.shape[1], 512):
                columns = slice(first, first + 512)
                own[first_row : first_row + PAIR, columns] = product_rows(
                    rows, branch[:, columns]
                ).astype(jnp.bfloat16)

    def stage_sort_grads():
        swap_heads.arrive()
        sort_blocks(order_ref, heads_in, (g0, g1), unpack_pairs)
        dk[...] = jnp.zeros_like(dk)
        dv[...] = jnp.zeros_like(dv)

    def stage_attention(index):
        first, top = index * tile, (index + 1) * tile
        parts = []
        for q, g in ((q0, g0), (q1, g1)):
            query_rows = q[first:top, :]
            grad_rows = g[first:top, :]
            soft = softmax_parts(query_rows, k[:top, :], first)
            grad_soft = product_back(grad_rows, v[:top, :])
            delta = jnp.sum(soft * grad_soft, axis=-1, keepdims=True)
            grad_scores = (soft * (grad_soft - delta)).astype(jnp.bfloat16)
            parts.append(product(grad_scores, k[:top, :]) * scale)
            key_term = product_rows(grad_scores, query_rows) * scale
            value_term = product_rows(soft.astype(jnp.bfloat16), grad_rows)
            dk[: top // block] += key_term.reshape(-1, block, HEAD_DIM)
            dv[: top // block] += value_term.reshape(-1, block, HEAD_DIM)
        result[first // block : top // block] = jnp.concatenate(parts, axis=-1).reshape(
            -1, block, PAIR
        )

    def stage_unsort():
        for slot in range(length // block):
            spot = order_ref[length // block + slot]
            packed_out[slot] = jnp.concatenate(
                [result[spot], dk[spot], dv[spot]], axis=-1
            ).astype(jnp.bfloat16)
        swap_packed.start_all()

    def stage_turn():
        fetch(cosine_ref, sine_ref, query_weight_ref, key_weight_ref, value_weight_ref)
        swap_packed.arrive()

        @pl.loop(0, 4)
        def _(sequence):
            span = rows_at(sequence * TILE, TILE)
            total = None
            for head in range(2):
                grads = packed_in[pl.ds((2 * sequence + head) * halves, halves)]
                grads = grads.reshape(TILE, WIDE)
                swapped = product(grads, half_swap[...])
                low = (
                    grads.astype(jnp.float32) * cosine[span, :] - swapped * sine[span, :]
                ).astype(jnp.bfloat16)
                turned[head, span, :] = low
                term = product(low, weight[head])
                total = term if total is None else total + term
            part[span, :] = total.astype(jnp.bfloat16)

        fold_one.start()

    def stage_projection_grads(head):
        if head == 0:
            fetch(normed_ref)
        query_base = base + head * PAIR
        key_base = base + WIDE + head * HEAD_DIM
        value_base = key_base + 2 * HEAD_DIM
        for first in range(0, own.shape[1], 512):
            columns = slice(first, first + 512)
            grads = product_rows(turned[head], normed[:, columns]).astype(jnp.bfloat16)
            own[query_base : query_base + PAIR, columns] = grads[:PAIR]
            own[key_base : key_base + HEAD_DIM, columns] = grads[PAIR : PAIR + HEAD_DIM]
            own[value_base : value_base + HEAD_DIM, columns] = grads[PAIR + HEAD_DIM :]

    def stage_norm_one():
        fetch(input_ref)
        fold_one.arrive()

        @pl.loop(0, TILE // 16)
        def _(piece):
            span = rows_at(piece * 16, 16)
            grad = fold_one.rows(piece * 16, 16)
            unit, back = norm_back_rows(inputs[span, :].astype(jnp.float32), None)
            gain_part[0] += (grad * unit).reshape(2, 8, -1).sum(axis=0)
            input_grad_ref[span, :] = grad_hidden[span, :] + back(grad * gain_one)

        gain_near[place.row] = jnp.sum(gain_part[...], axis=1)
        spread_near.start()

    def stage_gain():
        gain_far[me] = spread_near.total()
        spread_far.start()

    def stage_output():
        fetch(down_weight_ref)

        @pl.loop(0, 4)
        def _(sequence):
            span = rows_at(sequence * TILE, TILE)
            part[span, :] = product(
                mixed[span, :], own[base : base + hidden_units, :]
            ).astype(jnp.bfloat16)

    def stage_output_sum():
        fold_output.arrive()

        @pl.loop(0, TILE // 16)
        def _(piece):
            span = rows_at(piece * 16, 16)
            total = hidden[span, :] + fold_output.rows(piece * 16, 16)
            layer_output_ref[span, :] = total.astype(jnp.bfloat16)

    def stage_clear():
        if spare:
            own[base + 3 * WIDE :, :] = jnp.zeros((spare, width), own.dtype)

    units = 2 * 256
    stages = [
        (FEED[index], functools.partial(stage_feed, (index + 1) * units)) for index in range(5)
    ]
    stages += [
        (CHAIN[0], fold_two.relay),
        (CHAIN[0], stage_sort),
        (CHAIN[1], stage_norm_two),
        (CHAIN[2], gather.relay),
        (CHAIN[2], stage_output),
        (CHAIN[3], stage_heads),
        (CHAIN[3], fold_output.start),
        (CHAIN[4], fold_output.relay),
        (CHAIN[4], stage_output_grad),
        (CHAIN[4], stage_clear),
        (CHAIN[5], stage_sort_grads),
    ]
    stages += [
        (CHAIN[5] + index, functools.partial(stage_attention, index)) for index in range(tiles)
    ]
    stages += [
        (CHAIN[5] + tiles - 1, stage_unsort),
        (CHAIN[5] + tiles, stage_output_sum),
        (CHAIN[6], stage_turn),
        (CHAIN[7], fold_one.relay),
        (CHAIN[7], functools.partial(stage_projection_grads, 0)),
        (CHAIN[7] + 1, functools.partial(stage_projection_grads, 1)),
        (CHAIN[8], stage_norm_one),
        (CHAIN[9], stage_gain),
    ]
    assert CHAIN[7] + 1 < base // ROUND_ROWS - LEAD
    for index in range(5):
        assert FEED[index] < (index + 1) * units // ROUND_ROWS - LEAD

    for index in range(LEAD):
        leaf_copy(index).start()

    def valid(index):
        return jnp.logical_and(index >= 0, index < rounds)

    @pl.loop(0, rounds + RING)
    def _(now):
        far_side = jnp.abs(depth - 2 + side)
        off_center = jnp.abs(depth - 1 - side)
        done = now - RING + 1
        for tree in (spine(done), line(done)):
            pl.when(valid(done))(tree.finish)

        rising = spine(now - HOP * (3 - off_center))
        pl.when(valid(rising.index))(rising.rise)

        @pl.loop(0, 5)
        def _(age):
            tree = line(now - HOP * age)
            pl.when(jnp.logical_and(valid(tree.index), tree.rise_age == age))(tree.rise)

        @pl.when(now + LEAD < rounds)
        def _():
            leaf_copy(now + LEAD).start()

        falling = spine(now - HOP * (3 + off_center))
        pl.when(valid(falling.index))(falling.fall)

        @pl.loop(4, 9)
        def _(age):
            tree = line(now - HOP * age)
            pl.when(jnp.logical_and(valid(tree.index), tree.fall_age == age))(tree.fall)

        leaf_fall = now - HOP * (4 + far_side)

        @pl.when(valid(leaf_fall))
        def _():
            leaf_result(leaf_fall).wait_recv()
            leaf_copy(leaf_fall).wait_send()

        for when, stage in stages:
            pl.when(now == when)(stage)

    gain_out_ref[...] = spread_far.total()


def backward(order, gain_one, gain_two, grad_gate, grad_up, mixed, normed_two, cotangents, part,
             hidden, inputs, query_weight, key_weight, value_weight, output_weight, down_weight,
             attended, packed, normed, cosine, sine, key):
    width = hidden.shape[1]
    rows = 3 * mixed.shape[1] + 3 * WIDE
    rounds = -(-rows // ROUND_ROWS)
    block = packed.shape[1]
    length = packed.shape[0] * block
    dma = pltpu.SemaphoreType.DMA
    low, full = jnp.bfloat16, jnp.float32
    any_spec = pl.BlockSpec(memory_space=pl.ANY)
    operands = (
        order, gain_one, gain_two, grad_gate, grad_up, mixed, normed_two, cotangents, part,
        hidden, inputs, query_weight, key_weight, value_weight, output_weight, down_weight,
        attended, packed, normed, cosine, sine,
    )

    def like(array):
        return pltpu.VMEM(array.shape, array.dtype)

    return pl.pallas_call(
        functools.partial(backward_kernel, rounds, block),
        out_shape=(
            jax.ShapeDtypeStruct((rounds * ROUND_ROWS, width), low),
            jax.ShapeDtypeStruct((2, width), full),
            jax.ShapeDtypeStruct((TILE, width), full),
            jax.ShapeDtypeStruct((TILE, width), low),
        ),
        in_specs=[pl.BlockSpec(memory_space=pltpu.SMEM)] + [vmem()] * 2 + [any_spec] * 18,
        out_specs=(any_spec, vmem(), vmem(), vmem()),
        scratch_shapes=[
            pltpu.VMEM((rounds * ROUND_ROWS, width), low),
            pltpu.VMEM((3, RING * SPINE_ROWS, width), low),
            pltpu.VMEM((3, RING * LINE_ROWS, width), low),
            like(grad_gate), like(grad_up), like(mixed), like(normed_two), like(cotangents),
            like(part), like(hidden), like(inputs), like(output_weight),
            like(attended), like(packed), like(normed), like(cosine), like(sine),
            pltpu.VMEM((WIDE, WIDE), low),
            pltpu.VMEM((2, WIDE, width), low),
            pltpu.VMEM((2, 2, TILE, width), low),
            pltpu.VMEM((2, TILE, width), low),
            pltpu.VMEM((2, TILE, width), low),
            pltpu.VMEM((4 * TILE, width), low),
            pltpu.VMEM((TILE, width), full),
            pltpu.VMEM((2, 8, width), full),
            pltpu.VMEM((length // block, block // 2, 2 * PAIR), low),
            pltpu.VMEM((length // block, block // 2, 2 * PAIR), low),
        ]
        + [pltpu.VMEM((length, HEAD_DIM), low)] * 6
        + [pltpu.VMEM((length // block, block, PAIR), full)]
        + [pltpu.VMEM((length // block, block, HEAD_DIM), full)] * 2
        + [
            pltpu.VMEM((length // block, block, WIDE), low),
            pltpu.VMEM((length // block, block, WIDE), low),
            pltpu.VMEM((2, 4 * TILE, WIDE), low),
            pltpu.VMEM((4, 2, width), full),
            pltpu.VMEM((8, 2, width), full),
            dma((21,)),
            dma((RING,)), dma((3, RING)), dma((3, RING)), dma((RING,)),
            dma((RING,)), dma((RING,)),
            dma((RING,)), dma((3, RING)), dma((3, RING)), dma((RING,)),
            dma((2, 4)), dma((2, 4)),
            dma((3,)), dma((3,)),
            dma((2, 8)), dma((2, 8)),
            dma((4,)), dma((4,)), dma((8,)), dma((8,)),
        ],
        compiler_params=pltpu.CompilerParams(
            collective_id=key, has_side_effects=True, vmem_limit_bytes=63 * 2**20
        ),
        name="backward",
    )(*operands)


def forward_kernel(
    block,
    place_ref,
    table_ref,
    gain_one_ref,
    gain_two_ref,
    input_ref,
    cotangent_ref,
    query_weight_ref,
    key_weight_ref,
    value_weight_ref,
    output_weight_ref,
    gate_weight_ref,
    up_weight_ref,
    down_weight_ref,
    place_out,
    part_out,
    hidden_out,
    attended_out,
    packed_out,
    normed_one_out,
    cosine_out,
    sine_out,
    cotangent_out,
    normed_two_out,
    mixed_out,
    grad_gate_out,
    grad_up_out,
    places,
    tables,
    inputs,
    cotangents,
    normed_one,
    normed_two,
    cosine,
    sine,
    weight,
    output_weight,
    gate_weight,
    up_weight,
    down_weight,
    packed_from,
    packed,
    q0,
    q1,
    k,
    v,
    result,
    heads_from,
    heads,
    part,
    near,
    send,
    far,
    hidden,
    mixed,
    grad_gate,
    grad_up,
    fetch_sem,
    store_sem,
    gather_send,
    gather_recv,
    swap_send,
    swap_recv,
    fold_send,
    fold_recv,
):
    place = Place()
    length, width = q0.shape[0], inputs.shape[1]
    halves = TILE // block
    half = HEAD_DIM // 2
    pair_rows = 2 * TILE
    fetches, stores = {}, []

    def fetch_all(key, *copies):
        base = sum(len(group) for group in fetches.values())
        fetches[key] = [
            pltpu.make_async_copy(part_of, target, fetch_sem.at[base + index])
            for index, (part_of, target) in enumerate(copies)
        ]
        for copy in fetches[key]:
            copy.start()

    def fetch(*keys):
        for key in keys:
            for copy in fetches[key]:
                copy.wait()

    def store(source, target):
        copy = pltpu.make_async_copy(source, target, store_sem.at[len(stores)])
        copy.start()
        stores.append(copy)

    own_rows = rows_at(place.row * TILE, TILE)
    fetch_all("inputs", (input_ref, inputs.at[own_rows]))
    fetch_all("cotangent", (cotangent_ref, cotangents.at[own_rows]))
    copies = []
    for head in range(2):
        query_base, key_base = head * PAIR, head * HEAD_DIM
        target = weight.at[head]
        heads_of = [(query_weight_ref, query_base), (query_weight_ref, query_base + HEAD_DIM)]
        heads_of += [(key_weight_ref, key_base), (value_weight_ref, key_base)]
        for index, (source, first) in enumerate(heads_of):
            copies.append(
                (source.at[pl.ds(first, HEAD_DIM)], target.at[pl.ds(index * HEAD_DIM, HEAD_DIM)])
            )
            for side in range(2):
                copies.append(
                    (
                        source.at[pl.ds(first + (1 - side) * half, half)],
                        target.at[pl.ds(WIDE + index * HEAD_DIM + side * half, half)],
                    )
                )
    fetch_all("weight", *copies)
    fetch_all("output", (output_weight_ref, output_weight))
    fetch_all("gate", (gate_weight_ref, gate_weight))
    fetch_all("up", (up_weight_ref, up_weight))
    fetch_all("down", (down_weight_ref, down_weight))
    places[pl.ds(pl.multiple_of(place.row * 8, 8), 8), :] = jnp.broadcast_to(
        place_ref[...], (8, place_ref.shape[1])
    )
    gain_one = gain_one_ref[...].astype(jnp.float32).reshape(1, -1)
    gain_two = gain_two_ref[...].astype(jnp.float32).reshape(1, -1)
    tables[own_rows, :] = table_ref[...]
    gather_places = Gather(place, places, gather_send.at[0], gather_recv.at[0], 8)
    gather_tables = Gather(place, tables, gather_send.at[1], gather_recv.at[1])
    gather_inputs = Gather(place, inputs, gather_send.at[2], gather_recv.at[2], TILE, 2)
    gather_cotangents = Gather(place, cotangents, gather_send.at[3], gather_recv.at[3])
    gather_two = Gather(place, normed_two, gather_send.at[4], gather_recv.at[4], TILE, 2)
    swap_places = Swap(place, places, place_out, swap_send.at[0], swap_recv.at[0], 8, 2)
    swap_packed = Swap(place, packed_from, packed, swap_send.at[1], swap_recv.at[1], halves)
    swap_heads = Swap(place, heads_from, heads, swap_send.at[2], swap_recv.at[2], halves)
    fold = Fold(place, part, near, send, far, fold_send, fold_recv)
    place.greet()
    fetch("inputs")
    gather_tables.start()
    gather_inputs.start()
    gather_inputs.start(1)
    gather_places.start()
    fetch("cotangent")
    gather_cotangents.start()

    def project(chip):
        base = chip * pair_rows

        @pl.loop(0, pair_rows // 16)
        def _(piece):
            span = rows_at(base + piece * 16, 16)
            rows = inputs[span, :].astype(jnp.float32)
            normed_one[span, :] = (rows * rms_scale(rows) * gain_one).astype(jnp.bfloat16)

        span = rows_at(base, pair_rows)
        low_cosine, low_sine = tables[span, :half], tables[span, half:HEAD_DIM]
        ones = jnp.ones((pair_rows, HEAD_DIM), jnp.float32)
        cosine[span, :] = jnp.concatenate([low_cosine] * 6 + [ones], axis=-1)
        sine[span, :] = jnp.concatenate([-low_sine, low_sine] * 3 + [ones * 0.0], axis=-1)

        for head in range(2):
            products = product_back(normed_one[span, :], weight[head])
            low = (
                products[:, :WIDE] * cosine[span, :] + products[:, WIDE:] * sine[span, :]
            ).astype(jnp.bfloat16)
            for index in range(2):
                packed_from[pl.ds(((2 * chip + index) * 2 + head) * halves, halves)] = low[
                    index * TILE : (index + 1) * TILE
                ].reshape(halves, block, WIDE)
        for index in range(4):
            swap_packed.start(4 * chip + index)

    gather_tables.first()
    gather_inputs.first()
    gather_places.first()
    fetch("weight")
    project(place.chip)
    gather_tables.relay()
    gather_inputs.relay()
    gather_places.relay()
    gather_tables.arrive()
    gather_inputs.arrive()
    gather_places.arrive()
    project(1 - place.chip)
    swap_places.start_all()
    store(normed_one, normed_one_out)
    store(cosine, cosine_out)
    store(sine, sine_out)
    swap_places.arrive()
    swap_packed.arrive()
    store(packed, packed_out)

    def place_row(first, count):
        blocks = [place_out[8 * index : 8 * index + 1, :] for index in range(first, first + count)]
        return jnp.concatenate(blocks, axis=-1)

    tile = min(256, length)
    order = place_row(0, length // TILE)
    flat = packed[...].reshape(length, WIDE)
    for first in range(0, length, tile):
        rows = lax.broadcasted_iota(jnp.int32, (tile, length), 0) + first
        chosen = jnp.where(rows == order, 1.0, 0.0).astype(jnp.bfloat16)
        moved = product(chosen, flat).astype(jnp.bfloat16)
        for index, target in enumerate((q0, q1, k, v)):
            target[first : first + tile, :] = moved[:, index * HEAD_DIM : (index + 1) * HEAD_DIM]
    for first in range(0, length, tile):
        parts = []
        for q in (q0, q1):
            soft = softmax_parts(q[first : first + tile, :], k[: first + tile, :], first)
            parts.append(product(soft.astype(jnp.bfloat16), v[: first + tile, :]))
        result[first : first + tile, :] = jnp.concatenate(parts, axis=-1).astype(jnp.bfloat16)
    for first in range(0, length, tile):
        rows = lax.broadcasted_iota(jnp.int32, (length, tile), 0)
        chosen = jnp.where(rows == place_row(first // TILE, tile // TILE), 1.0, 0.0)
        moved = product_rows(chosen.astype(jnp.bfloat16), result[...]).astype(jnp.bfloat16)
        heads_from[first // block : (first + tile) // block] = pack_pairs(
            moved.reshape(-1, block, PAIR)
        )
        for index in range(first // TILE, (first + tile) // TILE):
            swap_heads.start(index)
    gather_cotangents.first()
    gather_cotangents.relay()
    fetch("output")
    swap_heads.arrive()
    store(heads, attended_out)

    def project_out(sequence):
        total = None
        for head in range(2):
            rows = heads[pl.ds((2 * sequence + head) * halves, halves)]
            rows = unpack_pairs(rows).reshape(TILE, PAIR)
            term = product(rows, output_weight[head * PAIR : (head + 1) * PAIR, :])
            total = term if total is None else total + term
        part[rows_at(sequence * TILE, TILE), :] = total.astype(jnp.bfloat16)

    for chip in (1 - place.chip, place.chip):
        project_out(2 * chip + 1 - place.core)
        fold.partner_copy(chip).start()
        project_out(2 * chip + place.core)
    gather_cotangents.arrive()
    store(cotangents, cotangent_out)
    fold.relay()
    fold.arrive_near()
    for half_rows in range(2):
        fold.arrive_across(half_rows)

        @pl.loop(4 * half_rows, 4 * half_rows + 4)
        def _(piece):
            span = rows_at(piece * 16, 16)
            own = rows_at(place.row * TILE + piece * 16, 16)
            rows = inputs[own, :].astype(jnp.float32) + fold.rows(piece * 16, 16)
            hidden[span, :] = rows
            normed_two[own, :] = (rows * rms_scale(rows) * gain_two).astype(jnp.bfloat16)

        gather_two.start(half_rows)
    store(hidden, hidden_out)
    fetch("gate", "up", "down")

    def feed(chip):
        span = rows_at(chip * pair_rows, pair_rows)

        @pl.loop(0, mixed.shape[1] // 256)
        def _(index):
            units = rows_at(index * 256, 256)
            columns = pl.ds(pl.multiple_of(index * 256, 256), 256)
            gate = product_back(normed_two[span, :], gate_weight[units, :])
            upward = product_back(normed_two[span, :], up_weight[units, :])
            grad_mixed = product_back(cotangents[span, :], down_weight[units, :])
            sigmoid = jax.nn.sigmoid(gate)
            activated = gate * sigmoid
            mixed[span, columns] = (activated * upward).astype(jnp.bfloat16)
            grad_gate[span, columns] = (
                grad_mixed * upward * sigmoid * (1.0 + gate * (1.0 - sigmoid))
            ).astype(jnp.bfloat16)
            grad_up[span, columns] = (grad_mixed * activated).astype(jnp.bfloat16)

        @pl.loop(0, width // 512)
        def _(index):
            columns = pl.ds(pl.multiple_of(index * 512, 512), 512)
            part[span, columns] = (
                product(grad_gate[span, :], gate_weight[:, columns])
                + product(grad_up[span, :], up_weight[:, columns])
            ).astype(jnp.bfloat16)

    def store_feed(chip):
        span = rows_at(chip * pair_rows, pair_rows)
        for source, target in (
            (part, part_out), (mixed, mixed_out), (grad_gate, grad_gate_out),
            (grad_up, grad_up_out),
        ):
            store(source.at[span], target.at[span])

    gather_two.first()
    feed(place.chip)
    store_feed(place.chip)
    gather_two.relay()
    gather_two.arrive()
    store(normed_two, normed_two_out)
    feed(1 - place.chip)
    store_feed(1 - place.chip)
    for copy in stores:
        copy.wait()


def forward(places, table, gain_one, gain_two, inputs, cotangent, query_weight, key_weight, value_weight,
            output_weight, gate_weight, up_weight, down_weight, length, block, key):
    width = inputs.shape[1]
    hidden_units = gate_weight.shape[0]
    rows = 4 * TILE
    blocks = length // block
    low, full = jnp.bfloat16, jnp.float32
    dma = pltpu.SemaphoreType.DMA
    any_spec = pl.BlockSpec(memory_space=pl.ANY)

    def out(shape, dtype):
        return jax.ShapeDtypeStruct(shape, dtype)

    wide = (rows, width)
    return pl.pallas_call(
        functools.partial(forward_kernel, block),
        out_shape=(
            out((64, 128), jnp.int32),
            out(wide, low), out((TILE, width), full),
            out((blocks, block // 2, 2 * PAIR), low), out((blocks, block, WIDE), low),
            out(wide, low), out((rows, WIDE), full), out((rows, WIDE), full),
            out(wide, low), out(wide, low),
            out((rows, hidden_units), low), out((rows, hidden_units), low),
            out((rows, hidden_units), low),
        ),
        in_specs=[vmem()] * 4 + [any_spec] * 9,
        out_specs=(vmem(),) + (any_spec,) * 12,
        scratch_shapes=[
            pltpu.VMEM((32, 128), jnp.int32),
            pltpu.VMEM((rows, 128), full),
            pltpu.VMEM(wide, low), pltpu.VMEM(wide, low),
            pltpu.VMEM(wide, low), pltpu.VMEM(wide, low),
            pltpu.VMEM((rows, WIDE), full), pltpu.VMEM((rows, WIDE), full),
            pltpu.VMEM((2, 2 * WIDE, width), low),
            pltpu.VMEM(output_weight.shape, low),
            pltpu.VMEM((hidden_units, width), low), pltpu.VMEM((hidden_units, width), low),
            pltpu.VMEM((hidden_units, width), low),
            pltpu.VMEM((blocks, block, WIDE), low), pltpu.VMEM((blocks, block, WIDE), low),
        ]
        + [pltpu.VMEM((length, HEAD_DIM), low)] * 4
        + [
            pltpu.VMEM((length, PAIR), low),
            pltpu.VMEM((blocks, block // 2, 2 * PAIR), low),
            pltpu.VMEM((blocks, block // 2, 2 * PAIR), low),
            pltpu.VMEM(wide, low),
            pltpu.VMEM((2, TILE, width), low),
            pltpu.VMEM((TILE, width), low), pltpu.VMEM((TILE, width), low),
            pltpu.VMEM((TILE, width), full),
            pltpu.VMEM((rows, hidden_units), low), pltpu.VMEM((rows, hidden_units), low),
            pltpu.VMEM((rows, hidden_units), low),
            dma((30,)), dma((16,)),
            dma((5, 6)), dma((5, 6)),
            dma((3, 8)), dma((3, 8)),
            dma((4,)), dma((4,)),
        ],
        compiler_params=pltpu.CompilerParams(
            collective_id=key, has_side_effects=True, vmem_limit_bytes=63 * 2**20
        ),
        name="forward",
    )(places, table, gain_one, gain_two, inputs, cotangent, query_weight, key_weight, value_weight,
      output_weight, gate_weight, up_weight, down_weight)


def widen_kernel(plan, kept, source, *refs):
    sources, refs = refs[:kept], refs[kept:]
    holds, refs, hold_sem = refs[-1 - kept : -1], refs[: -1 - kept], refs[-1]
    targets, (low, full, load_sem, store_sem) = refs[:-4], refs[-4:]
    targets, copies = targets[: len(targets) - kept], targets[len(targets) - kept :]
    takes = [
        pltpu.make_async_copy(sources[index], holds[index], hold_sem.at[index])
        for index in range(kept)
    ]
    gives = [
        pltpu.make_async_copy(holds[index], copies[index], hold_sem.at[kept + index])
        for index in range(kept)
    ]
    slots = low.shape[0]
    loads, stores = [], []
    for index, (first, which, target_row, chunk) in enumerate(plan):
        slot = index % slots
        span = pl.ds(0, chunk)
        loads.append(
            pltpu.make_async_copy(
                source.at[pl.ds(first, chunk)], low.at[slot, span], load_sem.at[slot]
            )
        )
        stores.append(
            pltpu.make_async_copy(
                full.at[slot, span],
                targets[which].at[pl.ds(target_row, chunk)],
                store_sem.at[slot],
            )
        )
    for load in loads[:slots] + takes:
        load.start()
    for index, (load, store) in enumerate(zip(loads, stores)):
        slot = index % slots
        load.wait()
        if index >= slots:
            stores[index - slots].wait()

        @pl.loop(0, plan[index][3] // 16)
        def _(piece):
            span = rows_at(piece * 16, 16)
            full[slot, span, :] = low[slot, span, :].astype(jnp.float32)

        store.start()
        if index + slots < len(plan):
            loads[index + slots].start()
        if index == slots:
            for take, give in zip(takes, gives):
                take.wait()
                give.start()
    for store in stores[-slots:] + gives:
        store.wait()


def widen(values, counts, keep):
    slots, width, first, plan = 6, values.shape[1], 0, []
    for which, count in enumerate(counts):
        chunk = math.gcd(count, 256) if count % 192 else 192
        plan += [(first + row, which, row, chunk) for row in range(0, count, chunk)]
        first += count
    any_spec = pl.BlockSpec(memory_space=pl.ANY)
    return pl.pallas_call(
        functools.partial(widen_kernel, plan, len(keep)),
        out_shape=tuple(jax.ShapeDtypeStruct((count, width), jnp.float32) for count in counts)
        + tuple(jax.ShapeDtypeStruct(array.shape, array.dtype) for array in keep),
        in_specs=[any_spec] * (1 + len(keep)),
        out_specs=(any_spec,) * (len(counts) + len(keep)),
        scratch_shapes=[
            pltpu.VMEM((slots, 256, width), values.dtype),
            pltpu.VMEM((slots, 256, width), jnp.float32),
            pltpu.SemaphoreType.DMA((slots,)),
            pltpu.SemaphoreType.DMA((slots,)),
        ]
        + [pltpu.VMEM(array.shape, array.dtype) for array in keep]
        + [pltpu.SemaphoreType.DMA((2 * len(keep),))],
        compiler_params=pltpu.CompilerParams(vmem_limit_bytes=63 * 2**20),
        name="widen",
    )(values, *keep)


def gather_rows(values):
    return lax.all_gather(values, "fsdp", axis=0, tiled=True)


def scatter_rows(values):
    return lax.psum_scatter(
        values.astype(jnp.bfloat16), "fsdp", scatter_dimension=0, tiled=True
    ).astype(jnp.float32)


def per_device_gathered(
    inputs,
    positions,
    cotangent,
    attention_gain,
    query_weight,
    key_weight,
    value_weight,
    output_weight,
    feedforward_gain,
    gate_weight,
    up_weight,
    down_weight,
):
    row_count = inputs.shape[0]
    groups = HEADS // KV_HEADS
    gain_one = attention_gain.astype(jnp.float32)
    gain_two = feedforward_gain.astype(jnp.float32)
    seq_count = lax.axis_size("fsdp")
    first_row = lax.axis_index("fsdp") * row_count

    def own(values):
        return lax.dynamic_slice_in_dim(values, first_row, row_count, 0)

    query_places = gather_rows(positions).reshape(seq_count, row_count)
    key_places = lax.all_gather(query_places, "ctx", axis=1, tiled=True)
    all_cotangent = gather_rows(cotangent)
    flat_in = gather_rows(inputs).astype(jnp.float32)
    scale_one = rms_scale(flat_in)
    unit_one = flat_in * scale_one
    normed_one = (unit_one * gain_one).astype(jnp.bfloat16)
    total_rows = normed_one.shape[0]
    cosine, sine = rotary_tables(query_places.reshape(-1))
    query_heads = query_weight.shape[0] // HEAD_DIM
    kv_heads = key_weight.shape[0] // HEAD_DIM
    kv_width = kv_heads * HEAD_DIM
    query_low = rotate(
        product_back(normed_one, query_weight).reshape(total_rows, query_heads, HEAD_DIM), cosine, sine
    ).astype(jnp.bfloat16)
    key_low = rotate(
        product_back(normed_one, key_weight).reshape(total_rows, kv_heads, HEAD_DIM), cosine, sine
    ).astype(jnp.bfloat16)
    value_low = product_back(normed_one, value_weight).astype(jnp.bfloat16)
    ctx_size = lax.axis_size("ctx")

    def spread(values):
        rows = lax.all_gather(values, "ctx", axis=0, tiled=True)
        rows = rows.reshape(ctx_size, seq_count, row_count, kv_width).swapaxes(0, 1)
        return rows.reshape(seq_count, ctx_size * row_count, kv_width)

    def collect(values):
        rows = values.astype(jnp.bfloat16).swapaxes(1, 2)
        rows = rows.reshape(seq_count, ctx_size, row_count, kv_width).swapaxes(0, 1)
        return lax.psum_scatter(
            rows.reshape(-1, kv_width), "ctx", scatter_dimension=0, tiled=True
        )

    all_keys = spread(key_low.reshape(total_rows, kv_width))
    all_values = spread(value_low)
    total_keys = all_keys.shape[1]
    key_grid = all_keys.reshape(seq_count, total_keys, kv_heads, HEAD_DIM).swapaxes(1, 2)
    value_grid = all_values.reshape(seq_count, total_keys, kv_heads, HEAD_DIM).swapaxes(1, 2)
    query_grouped = query_low.reshape(seq_count, row_count, kv_heads, groups, HEAD_DIM)
    attended, log_total = attend_forward(
        query_grouped, query_places, key_grid, value_grid, key_places
    )
    attended_low = attended.reshape(total_rows, query_heads * HEAD_DIM).astype(jnp.bfloat16)
    hidden_state = inputs.astype(jnp.float32) + scatter_rows(product(attended_low, output_weight))
    scale_two = rms_scale(hidden_state)
    unit_two = hidden_state * scale_two
    normed_two = gather_rows((unit_two * gain_two).astype(jnp.bfloat16))
    gate_values = product_back(normed_two, gate_weight)
    upward = product_back(normed_two, up_weight)
    sigmoid_gate = jax.nn.sigmoid(gate_values)
    activated = gate_values * sigmoid_gate
    mixed_hidden = (activated * upward).astype(jnp.bfloat16)
    grad_out = cotangent.astype(jnp.float32)
    grad_down = product_rows(mixed_hidden, all_cotangent)
    grad_mixed = product_back(all_cotangent, down_weight)
    grad_gate_low = (
        grad_mixed * upward * sigmoid_gate * (1.0 + gate_values * (1.0 - sigmoid_gate))
    ).astype(jnp.bfloat16)
    grad_up_low = (grad_mixed * activated).astype(jnp.bfloat16)
    grad_unit_part = (
        product(grad_gate_low, gate_weight) + product(grad_up_low, up_weight)
    ).astype(jnp.bfloat16)
    grad_normed_two = scatter_rows(grad_unit_part)
    gain_two_grad = jnp.sum(grad_normed_two * unit_two, axis=0)
    grad_hidden = grad_out + norm_back(scale_two, unit_two, grad_normed_two * gain_two)
    branch_rows = gather_rows(grad_hidden.astype(jnp.bfloat16))
    layer_output = (hidden_state + scatter_rows(product(mixed_hidden, down_weight))).astype(
        jnp.bfloat16
    )
    grad_gate = product_rows(grad_gate_low, normed_two)
    grad_up = product_rows(grad_up_low, normed_two)
    grad_output = product_rows(attended_low, branch_rows)
    grad_attended = product_back(branch_rows, output_weight).astype(jnp.bfloat16)
    grad_attended = grad_attended.reshape(seq_count, row_count, kv_heads, groups, HEAD_DIM)
    grad_query_rot, grad_key_all, grad_value_all = attend_backward(
        query_grouped, query_places, key_grid, value_grid, key_places, log_total, grad_attended
    )
    grad_key_own = collect(grad_key_all).astype(jnp.float32)
    grad_value_low = collect(grad_value_all)
    grad_query_low = (
        rotate_back(grad_query_rot.reshape(total_rows, query_heads, HEAD_DIM), cosine, sine)
        .reshape(total_rows, query_heads * HEAD_DIM)
        .astype(jnp.bfloat16)
    )
    grad_key_low = (
        rotate_back(
            grad_key_own.reshape(total_rows, kv_heads, HEAD_DIM), cosine, sine
        )
        .reshape(total_rows, kv_width)
        .astype(jnp.bfloat16)
    )
    grad_query = product_rows(grad_query_low, normed_one)
    grad_key = product_rows(grad_key_low, normed_one)
    grad_value = product_rows(grad_value_low, normed_one)
    grad_normed_one = scatter_rows(
        product(grad_query_low, query_weight)
        + product(grad_key_low, key_weight)
        + product(grad_value_low, value_weight)
    )
    own_unit = own(unit_one)
    gain_one_grad = jnp.sum(grad_normed_one * own_unit, axis=0)
    input_grad = grad_hidden + norm_back(own(scale_one), own_unit, grad_normed_one * gain_one)

    grads = (grad_query, grad_key, grad_value, grad_output, grad_gate, grad_up, grad_down)
    parts = [lax.psum(grad.astype(jnp.bfloat16), "ctx").astype(jnp.float32) for grad in grads]
    gain_sums = lax.psum(jnp.stack([gain_one_grad, gain_two_grad]), ("fsdp", "ctx"))
    return (
        layer_output,
        input_grad,
        gain_sums[0],
        parts[0],
        parts[1],
        parts[2],
        parts[3],
        gain_sums[1],
        parts[4],
        parts[5],
        parts[6],
    )


def per_device_by_head(
    inputs,
    positions,
    cotangent,
    attention_gain,
    query_weight,
    key_weight,
    value_weight,
    output_weight,
    feedforward_gain,
    gate_weight,
    up_weight,
    down_weight,
):
    gain_one, gain_two = attention_gain, feedforward_gain
    block = TILE // 2
    length = TILE * 8
    cosine, sine = rotary_tables(positions)
    table = jnp.concatenate([cosine[:, 0, :], sine[:, 0, :]], axis=1)
    table = jnp.pad(table, ((0, 0), (0, 128 - table.shape[1])))
    (
        places, part, hidden, attended, packed, normed_one, wide_cosine, wide_sine,
        cotangents, normed_two, mixed, grad_gate, grad_up,
    ) = forward(
        positions[None, :], table, gain_one, gain_two, inputs, cotangent, query_weight,
        key_weight, value_weight, output_weight, gate_weight, up_weight, down_weight, length,
        block, 1,
    )
    starts = places.reshape(8, 8, TILE)[:, 0, ::block].reshape(-1) // block
    slots = jnp.arange(length // block, dtype=jnp.int32)
    found = jnp.where(starts[None, :] == slots[:, None], slots[None, :], 0)
    order = jnp.concatenate([jnp.sum(found, axis=1), starts]).astype(jnp.int32)
    summed, gain_sums, input_grad, layer_output = backward(
        order, gain_one, gain_two, grad_gate, grad_up, mixed, normed_two, cotangents, part,
        hidden, inputs, query_weight, key_weight, value_weight, output_weight, down_weight,
        attended, packed, normed_one, wide_cosine, wide_sine, 5,
    )
    owners = (gate_weight, up_weight, down_weight, query_weight, key_weight, value_weight,
              output_weight)
    *parts, layer_output, input_grad = widen(
        summed, [owner.shape[0] for owner in owners], (layer_output, input_grad)
    )
    return (layer_output, input_grad, gain_sums[0], *parts[3:], gain_sums[1], *parts[:3])


def per_device(*arrays):
    fits = lax.axis_size("fsdp") == 4 and lax.axis_size("ctx") == 8
    return (per_device_by_head if fits else per_device_gathered)(*arrays)


def solution(mesh):
    in_specs = (
        P(("fsdp", "ctx"), None),
        P(("fsdp", "ctx")),
        P(("fsdp", "ctx"), None),
        P(),
        P("fsdp", None),
        P("fsdp", None),
        P("fsdp", None),
        P("fsdp", None),
        P(),
        P("fsdp", None),
        P("fsdp", None),
        P("fsdp", None),
    )
    out_specs = (
        P(("fsdp", "ctx"), None),
        P(("fsdp", "ctx"), None),
        P(),
        P("fsdp", None),
        P("fsdp", None),
        P("fsdp", None),
        P("fsdp", None),
        P(),
        P("fsdp", None),
        P("fsdp", None),
        P("fsdp", None),
    )
    return jax.shard_map(
        per_device, mesh=mesh, in_specs=in_specs, out_specs=out_specs, check_vma=False
    )
```
